32 devices in a mesh: data: 32 (over z, y, x, core).
Axes of the slice: x: 2, y: 2, z: 4, core: 2. Of those that a mesh axis runs over, the one named last changes fastest.
Arguments:
- h_a: bfloat16 [16384, 2048], P('data')
- h_b: bfloat16 [16384, 2048], P('data')
- w_one: bfloat16 [2048, 2048], replicated
- w_two: bfloat16 [2048, 2048], replicated
- w_three: bfloat16 [2048, 2048], replicated
- gain_one: float32 [2048], replicated
- shift_one: float32 [2048], replicated
- gain_two: float32 [2048], replicated
- shift_two: float32 [2048], replicated
- lam_off: float32 [], replicated
Outputs:
- output 1: float32 [], replicated
- output 2: float32 [2048, 2048], P('data')
- output 3: float32 [2048, 2048], P('data')
- output 4: float32 [2048, 2048], P('data')
- output 5: float32 [2048], replicated
- output 6: float32 [2048], replicated
- output 7: float32 [2048], replicated
- output 8: float32 [2048], replicated
All inputs are finite; a program needn't handle non-finite values.
Results may differ from the reference program's by a relative error of at most 0.00508914.
Values are sent between devices in bfloat16 or wider.
A program may use at most 1 GiB of HBM per device.

```python
import jax
import jax.numpy as jnp
from jax import lax

FEAT_DIM = 2048
PROJ_DIM = 2048
ROWS_DEV = 512
SHARDS = 32
TOTAL_ROWS = ROWS_DEV * SHARDS
NORM_EPS = 1e-5


def setup_inputs(seed: int = 0) -> dict:
    key_list = jax.random.split(jax.random.key(seed), 14)
    common = jax.random.normal(key_list[0], (TOTAL_ROWS, FEAT_DIM), jnp.float32)
    shard_shift = 0.6 * jax.random.normal(key_list[1], (SHARDS, 1, FEAT_DIM), jnp.float32)
    shard_scale = jnp.exp(0.3 * jax.random.normal(key_list[2], (SHARDS, 1, FEAT_DIM), jnp.float32))

    def make_view(view_key):
        noise_vals = jax.random.normal(view_key, (TOTAL_ROWS, FEAT_DIM), jnp.float32)
        mixed_rows = (0.77 * common + 0.64 * noise_vals).reshape(SHARDS, ROWS_DEV, FEAT_DIM)
        return (mixed_rows * shard_scale + shard_shift).reshape(TOTAL_ROWS, FEAT_DIM).astype(jnp.bfloat16)

    def make_weight(weight_key, fan_in, fan_out):
        weight_scale = fan_in ** -0.5
        return (jax.random.normal(weight_key, (fan_in, fan_out), jnp.float32) * weight_scale).astype(jnp.bfloat16)

    def make_vector(vec_key, center):
        return center + 0.25 * jax.random.normal(vec_key, (PROJ_DIM,), jnp.float32)

    lam_off = (0.1 + 0.2 * jax.random.uniform(key_list[12], (), jnp.float32)) * TOTAL_ROWS / PROJ_DIM
    return {
        "h_a": make_view(key_list[3]),
        "h_b": make_view(key_list[4]),
        "w_one": make_weight(key_list[5], FEAT_DIM, PROJ_DIM),
        "w_two": make_weight(key_list[6], PROJ_DIM, PROJ_DIM),
        "w_three": make_weight(key_list[7], PROJ_DIM, PROJ_DIM),
        "gain_one": make_vector(key_list[8], 1.0),
        "shift_one": make_vector(key_list[9], 0.0),
        "gain_two": make_vector(key_list[10], 1.0),
        "shift_two": make_vector(key_list[11], 0.0),
        "lam_off": lam_off,
    }


def batch_norm(values):
    col_mean = jnp.sum(values, axis=0) / TOTAL_ROWS
    col_var = jnp.sum(values * values, axis=0) / TOTAL_ROWS - col_mean * col_mean
    return (values - col_mean) * lax.rsqrt(col_var + NORM_EPS)


def project(feat_rows, params):
    w_one, w_two, w_three, gain_one, shift_one, gain_two, shift_two = params
    hidden_one = jnp.dot(feat_rows.astype(jnp.float32), w_one, preferred_element_type=jnp.float32)
    act_one = jax.nn.relu(gain_one * batch_norm(hidden_one) + shift_one).astype(jnp.bfloat16)
    hidden_two = jnp.dot(act_one.astype(jnp.float32), w_two, preferred_element_type=jnp.float32)
    act_two = jax.nn.relu(gain_two * batch_norm(hidden_two) + shift_two).astype(jnp.bfloat16)
    proj_out = jnp.dot(act_two.astype(jnp.float32), w_three, preferred_element_type=jnp.float32)
    return batch_norm(proj_out).astype(jnp.bfloat16)


def barlow_loss(params, h_a, h_b, lam_off):
    embed_a = project(h_a, params).astype(jnp.float32)
    embed_b = project(h_b, params).astype(jnp.float32)
    corr_mat = jnp.dot(embed_a.T, embed_b, preferred_element_type=jnp.float32) / TOTAL_ROWS
    feat_index = jnp.arange(PROJ_DIM)
    diag_mask = feat_index[:, None] == feat_index[None, :]
    diag_gap = 1.0 - jnp.diagonal(corr_mat)
    off_square = jnp.sum(jnp.where(diag_mask, 0.0, corr_mat * corr_mat))
    return jnp.sum(diag_gap * diag_gap) + lam_off * off_square


def reference(h_a, h_b, w_one, w_two, w_three, gain_one, shift_one, gain_two, shift_two, lam_off):
    params = (w_one.astype(jnp.float32), w_two.astype(jnp.float32), w_three.astype(jnp.float32),
              gain_one, shift_one, gain_two, shift_two)
    loss_total, grad_list = jax.value_and_grad(barlow_loss)(params, h_a, h_b, lam_off)
    return (loss_total, grad_list[0], grad_list[1], grad_list[2],
            grad_list[3], grad_list[4], grad_list[5], grad_list[6])
```

```python
import functools

import jax
import jax.numpy as jnp
from jax import lax
from jax.experimental import pallas as pl
from jax.experimental.pallas import tpu as pltpu
from jax.sharding import PartitionSpec as P

NORM_EPS = 1e-5
ROW_DIMS = (((0, 1), (0, 1)), ((), ()))
FIRST_DIMS = (((0,), (0,)), ((), ()))
LAST_DIMS = (((2,), (1,)), ((), ()))
MESH = pl.DeviceIdType.MESH
F32 = jnp.float32
BF16 = jnp.bfloat16


class Place:
    def __init__(self):
        me = lax.axis_index("data")
        self.core = lax.rem(me, 2)
        self.x = lax.rem(lax.div(me, 2), 2)
        self.y = lax.rem(lax.div(me, 4), 2)
        self.z = lax.div(me, 8)
        self.plane = lax.rem(lax.div(me, 2), 4)
        self.partner = me + 1 - 2 * self.core
        self.x_peer = me + 2 - 4 * self.x
        self.y_peer = me + 4 - 8 * self.y
        low = lax.rem(me, 8)
        self.z_peers = [lax.rem(self.z + d, 4) * 8 + low for d in (1, 2, 3)]
        self.plane_peers = [
            self.z * 8 + lax.rem(self.plane + d, 4) * 2 + self.core for d in (1, 2, 3)
        ]


def enter(peers):
    barrier = pltpu.get_barrier_semaphore()
    for peer in peers:
        pl.semaphore_signal(barrier, inc=1, device_id=(peer,), device_id_type=MESH)
    pl.semaphore_wait(barrier, len(peers))


def remote(src, dst, send_sem, recv_sem, peer):
    return pltpu.make_async_remote_copy(
        src_ref=src, dst_ref=dst, send_sem=send_sem, recv_sem=recv_sem,
        device_id=(peer,), device_id_type=MESH)


def sums_kernel(in_ref, out_ref, recv0, slots1, slots2, send_sem, recv_sem):
    at = Place()
    half = in_ref.shape[1] // 2
    enter([at.partner] + at.plane_peers + at.z_peers)
    mine = pl.ds(pl.multiple_of(at.core * half, 128), half)
    theirs = pl.ds(pl.multiple_of((1 - at.core) * half, 128), half)
    first = remote(in_ref.at[:, theirs], recv0, send_sem.at[0], recv_sem.at[0], at.partner)
    first.start()
    first.wait()
    slots1[at.plane] = in_ref[:, mine] + recv0[...]
    copies = []
    for d in range(3):
        copies.append(remote(slots1.at[at.plane], slots1.at[at.plane], send_sem.at[1 + d], recv_sem.at[1 + d],
                             at.plane_peers[d]))
        copies[-1].start()
    for copy in copies:
        copy.wait()
    slots2[at.z] = (slots1[0] + slots1[1]) + (slots1[2] + slots1[3])
    copies = []
    for d in range(3):
        copies.append(remote(slots2.at[at.z], slots2.at[at.z], send_sem.at[4 + d], recv_sem.at[4 + d],
                             at.z_peers[d]))
        copies[-1].start()
    for copy in copies:
        copy.wait()
    out_ref[:, mine] = (slots2[0] + slots2[1]) + (slots2[2] + slots2[3])
    last = remote(out_ref.at[:, mine], out_ref.at[:, mine], send_sem.at[7], recv_sem.at[7], at.partner)
    last.start()
    last.wait()


def all_sums(values, collective_id):
    rows, cols = values.shape
    return pl.pallas_call(
        sums_kernel,
        out_shape=jax.ShapeDtypeStruct(values.shape, F32),
        in_specs=[pl.BlockSpec(memory_space=pltpu.VMEM)],
        out_specs=pl.BlockSpec(memory_space=pltpu.VMEM),
        scratch_shapes=[
            pltpu.VMEM((rows, cols // 2), F32),
            pltpu.VMEM((4, rows, cols // 2), F32),
            pltpu.VMEM((4, rows, cols // 2), F32),
            pltpu.SemaphoreType.DMA((8,)),
            pltpu.SemaphoreType.DMA((8,)),
        ],
        compiler_params=pltpu.CompilerParams(collective_id=collective_id, has_side_effects=True),
    )(values)


class Scatter:
    def __init__(self, at, part, bufs, send_sem, recv_sem, chunk):
        self.at, self.part, self.chunk = at, part, chunk
        self.recv0, self.snd1, self.recv1, self.snd2, self.recv2, self.snd3, self.recv3 = bufs
        self.send_sem, self.recv_sem = send_sem, recv_sem
        self.copies = {}

    def cols(self, j):
        return pl.ds(j * self.chunk, self.chunk)

    def start(self, j, stage, src, dst, peer):
        copy = remote(src, dst, self.send_sem.at[j, stage], self.recv_sem.at[j, stage], peer)
        copy.start()
        self.copies[j, stage] = copy

    def total(self, j, z, y, x, depth):
        cs, c = self.cols(j), self.at.core
        total = self.part[z, y, x, c, :, cs].astype(F32) + self.recv0[z, y, x, :, cs].astype(F32)
        if depth > 1:
            total += self.recv1[z, y if j % 2 == 0 else x, :, cs].astype(F32)
        if depth > 2:
            total += self.recv2[z, :, cs].astype(F32)
        return total

    def stage0(self, j):
        cs, at = self.cols(j), self.at
        self.start(j, 0, self.part.at[:, :, :, 1 - at.core, :, cs], self.recv0.at[:, :, :, :, cs], at.partner)

    def stage1(self, j):
        cs, at = self.cols(j), self.at
        self.copies[j, 0].wait()
        for z in range(4):
            for k in range(2):
                y, x = (k, 1 - at.x) if j % 2 == 0 else (1 - at.y, k)
                self.snd1[z, k, :, cs] = self.total(j, z, y, x, 1).astype(BF16)
        self.start(j, 1, self.snd1.at[:, :, :, cs], self.recv1.at[:, :, :, cs], at.x_peer if j % 2 == 0 else at.y_peer)

    def stage2(self, j):
        cs, at = self.cols(j), self.at
        self.copies[j, 1].wait()
        for z in range(4):
            y, x = (1 - at.y, at.x) if j % 2 == 0 else (at.y, 1 - at.x)
            self.snd2[z, :, cs] = self.total(j, z, y, x, 2).astype(BF16)
        self.start(j, 2, self.snd2.at[:, :, cs], self.recv2.at[:, :, cs], at.y_peer if j % 2 == 0 else at.x_peer)

    def stage3(self, j):
        cs, at = self.cols(j), self.at
        self.copies[j, 2].wait()
        for d in range(3):
            z = lax.rem(at.z + d + 1, 4)
            self.snd3[d, :, cs] = self.total(j, z, at.y, at.x, 3).astype(BF16)
            self.start(j, 3 + d, self.snd3.at[d, :, cs], self.recv3.at[d, :, cs], at.z_peers[d])

    def final(self, j):
        cs, at = self.cols(j), self.at
        total = self.total(j, at.z, at.y, at.x, 3)
        for d in range(3):
            self.copies[j, 3 + d].wait()
            total += self.recv3[d, :, cs].astype(F32)
        return total


def scatter_scratch(rows, cols, chunks, stages):
    return [
        pltpu.VMEM((4, 2, 2, rows, cols), BF16),
        pltpu.VMEM((4, 2, rows, cols), BF16),
        pltpu.VMEM((4, 2, rows, cols), BF16),
        pltpu.VMEM((4, rows, cols), BF16),
        pltpu.VMEM((4, rows, cols), BF16),
        pltpu.VMEM((3, rows, cols), BF16),
        pltpu.VMEM((3, rows, cols), BF16),
        pltpu.SemaphoreType.DMA((chunks, stages)),
        pltpu.SemaphoreType.DMA((chunks, stages)),
    ]


def scatter_kernel(chunks, part_ref, out_ref, *scratch):
    at = Place()
    enter([at.partner, at.x_peer, at.y_peer] + at.z_peers)
    send_sem, recv_sem = scratch[7:]
    chunk = part_ref.shape[-1] // chunks
    scatter = Scatter(at, part_ref, scratch[:7], send_sem, recv_sem, chunk)
    for j in range(chunks):
        scatter.stage0(j)
    for t in range(chunks + 3):
        for stage, step in enumerate((scatter.stage1, scatter.stage2, scatter.stage3)):
            if 0 <= t - stage < chunks:
                step(t - stage)
        j = t - 3
        if j >= 0:
            out_ref[:, scatter.cols(j)] = scatter.final(j)


def scatter_sum(part, collective_id, chunks=8):
    full, cols = part.shape
    rows = full // 32
    return pl.pallas_call(
        functools.partial(scatter_kernel, chunks),
        out_shape=jax.ShapeDtypeStruct((rows, cols), F32),
        in_specs=[pl.BlockSpec(memory_space=pltpu.VMEM)],
        out_specs=pl.BlockSpec(memory_space=pltpu.VMEM),
        scratch_shapes=scatter_scratch(rows, cols, chunks, 6),
        compiler_params=pltpu.CompilerParams(
            collective_id=collective_id, has_side_effects=True, vmem_limit_bytes=40 * 2**20),
    )(part.reshape(4, 2, 2, 2, rows, cols))


def corr_kernel(chunks, total_rows, part_ref, lam_ref, grad_ref, loss_ref, *scratch):
    at = Place()
    enter([at.partner, at.x_peer, at.y_peer] + at.z_peers)
    send_sem, recv_sem = scratch[7:]
    rows, cols = part_ref.shape[-2:]
    chunk = cols // chunks
    scatter = Scatter(at, part_ref, scratch[:7], send_sem, recv_sem, chunk)
    lam = lam_ref[0]
    block = grad_ref.at[at.z, at.y, at.x, at.core]
    first_row = (((at.z * 2 + at.y) * 2 + at.x) * 2 + at.core) * rows

    def spread_z(j):
        cs = scatter.cols(j)
        corr = scatter.final(j) / total_rows
        row = first_row + lax.broadcasted_iota(jnp.int32, corr.shape, 0)
        col = j * chunk + lax.broadcasted_iota(jnp.int32, corr.shape, 1)
        diag = row == col
        gap = 1.0 - corr
        loss_ref[:, cs] = jnp.sum(jnp.where(diag, gap * gap, lam * corr * corr), axis=0, keepdims=True)
        grad = jnp.where(diag, -2.0 * gap, 2.0 * lam * corr)
        block[:, cs] = (grad / total_rows).astype(BF16)
        for d in range(3):
            scatter.start(j, 6 + d, block.at[:, cs], block.at[:, cs], at.z_peers[d])

    def spread_one(j):
        cs = scatter.cols(j)
        for d in range(3):
            scatter.copies[j, 6 + d].wait()
        here = grad_ref.at[:, at.y, at.x, at.core, :, cs]
        scatter.start(j, 9, here, here, at.y_peer if j % 2 == 0 else at.x_peer)

    def spread_two(j):
        cs = scatter.cols(j)
        scatter.copies[j, 9].wait()
        if j % 2 == 0:
            here, peer = grad_ref.at[:, :, at.x, at.core, :, cs], at.x_peer
        else:
            here, peer = grad_ref.at[:, at.y, :, at.core, :, cs], at.y_peer
        scatter.start(j, 10, here, here, peer)

    def spread_core(j):
        cs = scatter.cols(j)
        scatter.copies[j, 10].wait()
        here = grad_ref.at[:, :, :, at.core, :, cs]
        scatter.start(j, 11, here, here, at.partner)

    def finish(j):
        scatter.copies[j, 11].wait()

    steps = (scatter.stage1, scatter.stage2, scatter.stage3, spread_z, spread_one, spread_two, spread_core, finish)
    for j in range(chunks):
        scatter.stage0(j)
    for t in range(chunks + len(steps) - 1):
        for stage, step in enumerate(steps):
            if 0 <= t - stage < chunks:
                step(t - stage)


def corr_grad(part, lam, total_rows, collective_id, chunks=8):
    full, cols = part.shape
    rows = full // 32
    grad, loss = pl.pallas_call(
        functools.partial(corr_kernel, chunks, total_rows),
        out_shape=(jax.ShapeDtypeStruct((4, 2, 2, 2, rows, cols), BF16), jax.ShapeDtypeStruct((1, cols), F32)),
        in_specs=[pl.BlockSpec(memory_space=pltpu.VMEM), pl.BlockSpec(memory_space=pltpu.SMEM)],
        out_specs=(pl.BlockSpec(memory_space=pltpu.VMEM), pl.BlockSpec(memory_space=pltpu.VMEM)),
        scratch_shapes=scatter_scratch(rows, cols, chunks, 12),
        compiler_params=pltpu.CompilerParams(
            collective_id=collective_id, has_side_effects=True, vmem_limit_bytes=48 * 2**20),
    )(part.reshape(4, 2, 2, 2, rows, cols), lam.reshape(1))
    return grad.reshape(full, cols), loss


def norm_forward(values, total_rows, collective_id):
    cols = values.shape[-1]
    col_sums = jnp.concatenate([jnp.sum(values, axis=1), jnp.sum(values * values, axis=1)])
    col_sums = all_sums(col_sums, collective_id).reshape(2, 2, cols)
    col_mean = col_sums[0] / total_rows
    inv_std = lax.rsqrt(col_sums[1] / total_rows - col_mean * col_mean + NORM_EPS)
    return (values - col_mean[:, None, :]) * inv_std[:, None, :], inv_std


def norm_backward(grad_out, normed, inv_std, total_rows, collective_id, extra=None):
    cols = grad_out.shape[-1]
    rows = [jnp.sum(grad_out, axis=1), jnp.sum(grad_out * normed, axis=1)]
    if extra is not None:
        rows.append(extra)
    summed = all_sums(jnp.concatenate(rows), collective_id)
    col_sums = summed[:4].reshape(2, 2, cols)
    grad_in = inv_std[:, None, :] * (grad_out - (col_sums[0][:, None, :] + normed * col_sums[1][:, None, :]) / total_rows)
    return grad_in, col_sums, summed[4:]


def solution(mesh):
    shards = mesh.shape["data"]

    def local_step(h_a, h_b, w_one, w_two, w_three, gain_one, shift_one, gain_two, shift_two, lam_off):
        rows_dev = h_a.shape[0]
        total_rows = rows_dev * shards
        feat_rows = jnp.concatenate([h_a, h_b], axis=0)
        hidden_one = jnp.dot(feat_rows, w_one, preferred_element_type=F32).reshape(2, rows_dev, -1)
        normed_one, inv_one = norm_forward(hidden_one, total_rows, 0)
        pre_one = gain_one * normed_one + shift_one
        act_one = jax.nn.relu(pre_one).astype(BF16)
        hidden_two = jnp.dot(act_one, w_two, preferred_element_type=F32)
        normed_two, inv_two = norm_forward(hidden_two, total_rows, 1)
        pre_two = gain_two * normed_two + shift_two
        act_two = jax.nn.relu(pre_two).astype(BF16)
        proj_out = jnp.dot(act_two, w_three, preferred_element_type=F32)
        normed_out, inv_out = norm_forward(proj_out, total_rows, 2)
        embed_pair = normed_out.astype(BF16)
        corr_part = lax.dot_general(embed_pair[0], embed_pair[1], FIRST_DIMS, preferred_element_type=F32)
        grad_scaled, loss_cols = corr_grad(corr_part.astype(BF16), lam_off, total_rows, 3)
        grad_embed_a = lax.dot_general(embed_pair[1], grad_scaled, (((1,), (1,)), ((), ())),
                                       preferred_element_type=F32)
        grad_embed_b = jnp.dot(embed_pair[0], grad_scaled, preferred_element_type=F32)
        grad_embed = jnp.stack([grad_embed_a, grad_embed_b])
        grad_proj, _, loss_cols = norm_backward(grad_embed, normed_out, inv_out, total_rows, 4, loss_cols)
        loss_total = jnp.sum(loss_cols)
        grad_proj = grad_proj.astype(BF16)
        grad_w_three = scatter_sum(
            lax.dot_general(act_two, grad_proj, ROW_DIMS, preferred_element_type=F32).astype(BF16), 5)
        grad_act_two = lax.dot_general(grad_proj, w_three, LAST_DIMS, preferred_element_type=F32)
        grad_pre_two = jnp.where(pre_two > 0, grad_act_two, 0.0)
        grad_hidden_two, sums_two, _ = norm_backward(grad_pre_two, normed_two, inv_two, total_rows, 6)
        grad_hidden_two = (gain_two * grad_hidden_two).astype(BF16)
        grad_w_two = scatter_sum(
            lax.dot_general(act_one, grad_hidden_two, ROW_DIMS, preferred_element_type=F32).astype(BF16), 7)
        grad_act_one = lax.dot_general(grad_hidden_two, w_two, LAST_DIMS, preferred_element_type=F32)
        grad_pre_one = jnp.where(pre_one > 0, grad_act_one, 0.0)
        grad_hidden_one, sums_one, _ = norm_backward(grad_pre_one, normed_one, inv_one, total_rows, 8)
        grad_hidden_one = (gain_one * grad_hidden_one).astype(BF16).reshape(2 * rows_dev, -1)
        grad_w_one = scatter_sum(
            lax.dot_general(feat_rows, grad_hidden_one, FIRST_DIMS, preferred_element_type=F32).astype(BF16), 9)
        return (loss_total, grad_w_one, grad_w_two, grad_w_three,
                jnp.sum(sums_one[1], axis=0), jnp.sum(sums_one[0], axis=0),
                jnp.sum(sums_two[1], axis=0), jnp.sum(sums_two[0], axis=0))

    row_spec = P("data", None)
    whole_mat = P(None, None)
    whole_vec = P(None)
    return jax.shard_map(
        local_step, mesh=mesh,
        in_specs=(row_spec, row_spec, whole_mat, whole_mat, whole_mat,
                  whole_vec, whole_vec, whole_vec, whole_vec, P()),
        out_specs=(P(), row_spec, row_spec, row_spec, whole_vec, whole_vec, whole_vec, whole_vec),
        check_vma=False)
```

```python
import functools

import jax
import jax.numpy as jnp
from jax import lax
from jax.experimental import pallas as pl
from jax.experimental.pallas import tpu as pltpu
from jax.sharding import PartitionSpec as P

NORM_EPS = 1e-5
FIRST_DIMS = (((0,), (0,)), ((), ()))
MESH = pl.DeviceIdType.MESH
F32 = jnp.float32
BF16 = jnp.bfloat16


class Place:
    def __init__(self):
        me = lax.axis_index("data")
        self.core = lax.rem(me, 2)
        self.x = lax.rem(lax.div(me, 2), 2)
        self.y = lax.rem(lax.div(me, 4), 2)
        self.z = lax.div(me, 8)
        self.plane = lax.rem(lax.div(me, 2), 4)
        self.partner = me + 1 - 2 * self.core
        self.x_peer = me + 2 - 4 * self.x
        self.y_peer = me + 4 - 8 * self.y
        low = lax.rem(me, 8)
        self.z_peers = [lax.rem(self.z + d, 4) * 8 + low for d in (1, 2, 3)]
        self.plane_peers = [
            self.z * 8 + lax.rem(self.plane + d, 4) * 2 + self.core for d in (1, 2, 3)
        ]


def enter(peers):
    barrier = pltpu.get_barrier_semaphore()
    for peer in peers:
        pl.semaphore_signal(barrier, inc=1, device_id=(peer,), device_id_type=MESH)
    pl.semaphore_wait(barrier, len(peers))


def remote(src, dst, send_sem, recv_sem, peer):
    return pltpu.make_async_remote_copy(
        src_ref=src, dst_ref=dst, send_sem=send_sem, recv_sem=recv_sem,
        device_id=(peer,), device_id_type=MESH)


def sums_kernel(in_ref, out_ref, recv0, slots1, slots2, send_sem, recv_sem):
    at = Place()
    half = in_ref.shape[1] // 2
    enter([at.partner] + at.plane_peers + at.z_peers)
    mine = pl.ds(pl.multiple_of(at.core * half, 128), half)
    theirs = pl.ds(pl.multiple_of((1 - at.core) * half, 128), half)
    first = remote(in_ref.at[:, theirs], recv0, send_sem.at[0], recv_sem.at[0], at.partner)
    first.start()
    first.wait()
    slots1[at.plane] = in_ref[:, mine] + recv0[...]
    copies = []
    for d in range(3):
        copies.append(remote(slots1.at[at.plane], slots1.at[at.plane], send_sem.at[1 + d], recv_sem.at[1 + d],
                             at.plane_peers[d]))
        copies[-1].start()
    for copy in copies:
        copy.wait()
    slots2[at.z] = (slots1[0] + slots1[1]) + (slots1[2] + slots1[3])
    copies = []
    for d in range(3):
        copies.append(remote(slots2.at[at.z], slots2.at[at.z], send_sem.at[4 + d], recv_sem.at[4 + d],
                             at.z_peers[d]))
        copies[-1].start()
    for copy in copies:
        copy.wait()
    out_ref[:, mine] = (slots2[0] + slots2[1]) + (slots2[2] + slots2[3])
    last = remote(out_ref.at[:, mine], out_ref.at[:, mine], send_sem.at[7], recv_sem.at[7], at.partner)
    last.start()
    last.wait()


def all_sums(values, collective_id):
    rows, cols = values.shape
    return pl.pallas_call(
        sums_kernel,
        out_shape=jax.ShapeDtypeStruct(values.shape, F32),
        in_specs=[pl.BlockSpec(memory_space=pltpu.VMEM)],
        out_specs=pl.BlockSpec(memory_space=pltpu.VMEM),
        scratch_shapes=[
            pltpu.VMEM((rows, cols // 2), F32),
            pltpu.VMEM((4, rows, cols // 2), F32),
            pltpu.VMEM((4, rows, cols // 2), F32),
            pltpu.SemaphoreType.DMA((8,)),
            pltpu.SemaphoreType.DMA((8,)),
        ],
        compiler_params=pltpu.CompilerParams(collective_id=collective_id, has_side_effects=True),
    )(values)


class Scatter:
    def __init__(self, at, part, bufs, send_sem, recv_sem, chunk):
        self.at, self.part, self.chunk = at, part, chunk
        self.recv0, self.snd1, self.recv1, self.snd2, self.recv2, self.snd3, self.recv3 = bufs
        self.send_sem, self.recv_sem = send_sem, recv_sem
        self.copies = {}

    def cols(self, j):
        return pl.ds(j * self.chunk, self.chunk)

    def start(self, j, stage, src, dst, peer):
        copy = remote(src, dst, self.send_sem.at[j, stage], self.recv_sem.at[j, stage], peer)
        copy.start()
        self.copies[j, stage] = copy

    def total(self, j, z, y, x, depth):
        cs, c = self.cols(j), self.at.core
        total = self.part[z, y, x, c, :, cs].astype(F32) + self.recv0[z, y, x, :, cs].astype(F32)
        if depth > 1:
            total += self.recv1[z, y if j % 2 == 0 else x, :, cs].astype(F32)
        if depth > 2:
            total += self.recv2[z, :, cs].astype(F32)
        return total

    def stage0(self, j):
        cs, at = self.cols(j), self.at
        self.start(j, 0, self.part.at[:, :, :, 1 - at.core, :, cs], self.recv0.at[:, :, :, :, cs], at.partner)

    def stage1(self, j):
        cs, at = self.cols(j), self.at
        self.copies[j, 0].wait()
        for z in range(4):
            for k in range(2):
                y, x = (k, 1 - at.x) if j % 2 == 0 else (1 - at.y, k)
                self.snd1[z, k, :, cs] = self.total(j, z, y, x, 1).astype(BF16)
        self.start(j, 1, self.snd1.at[:, :, :, cs], self.recv1.at[:, :, :, cs], at.x_peer if j % 2 == 0 else at.y_peer)

    def stage2(self, j):
        cs, at = self.cols(j), self.at
        self.copies[j, 1].wait()
        for z in range(4):
            y, x = (1 - at.y, at.x) if j % 2 == 0 else (at.y, 1 - at.x)
            self.snd2[z, :, cs] = self.total(j, z, y, x, 2).astype(BF16)
        self.start(j, 2, self.snd2.at[:, :, cs], self.recv2.at[:, :, cs], at.y_peer if j % 2 == 0 else at.x_peer)

    def stage3(self, j):
        cs, at = self.cols(j), self.at
        self.copies[j, 2].wait()
        for d in range(3):
            z = lax.rem(at.z + d + 1, 4)
            self.snd3[d, :, cs] = self.total(j, z, at.y, at.x, 3).astype(BF16)
            self.start(j, 3 + d, self.snd3.at[d, :, cs], self.recv3.at[d, :, cs], at.z_peers[d])

    def final(self, j):
        cs, at = self.cols(j), self.at
        total = self.total(j, at.z, at.y, at.x, 3)
        for d in range(3):
            self.copies[j, 3 + d].wait()
            total += self.recv3[d, :, cs].astype(F32)
        return total


def scatter_scratch(rows, cols, chunks, stages):
    return [
        pltpu.VMEM((4, 2, 2, rows, cols), BF16),
        pltpu.VMEM((4, 2, rows, cols), BF16),
        pltpu.VMEM((4, 2, rows, cols), BF16),
        pltpu.VMEM((4, rows, cols), BF16),
        pltpu.VMEM((4, rows, cols), BF16),
        pltpu.VMEM((3, rows, cols), BF16),
        pltpu.VMEM((3, rows, cols), BF16),
        pltpu.SemaphoreType.DMA((chunks, stages)),
        pltpu.SemaphoreType.DMA((chunks, stages)),
    ]


def corr_kernel(chunks, total_rows, part_ref, lam_ref, grad_ref, loss_ref, *scratch):
    at = Place()
    enter([at.partner, at.x_peer, at.y_peer] + at.z_peers)
    send_sem, recv_sem = scratch[7:]
    rows, cols = part_ref.shape[-2:]
    chunk = cols // chunks
    scatter = Scatter(at, part_ref, scratch[:7], send_sem, recv_sem, chunk)
    lam = lam_ref[0]
    block = grad_ref.at[at.z, at.y, at.x, at.core]
    first_row = (((at.z * 2 + at.y) * 2 + at.x) * 2 + at.core) * rows

    def spread_z(j):
        cs = scatter.cols(j)
        corr = scatter.final(j) / total_rows
        row = first_row + lax.broadcasted_iota(jnp.int32, corr.shape, 0)
        col = j * chunk + lax.broadcasted_iota(jnp.int32, corr.shape, 1)
        diag = row == col
        gap = 1.0 - corr
        loss_ref[:, cs] = jnp.sum(jnp.where(diag, gap * gap, lam * corr * corr), axis=0, keepdims=True)
        grad = jnp.where(diag, -2.0 * gap, 2.0 * lam * corr)
        block[:, cs] = (grad / total_rows).astype(BF16)
        for d in range(3):
            scatter.start(j, 6 + d, block.at[:, cs], block.at[:, cs], at.z_peers[d])

    def spread_one(j):
        cs = scatter.cols(j)
        for d in range(3):
            scatter.copies[j, 6 + d].wait()
        here = grad_ref.at[:, at.y, at.x, at.core, :, cs]
        scatter.start(j, 9, here, here, at.y_peer if j % 2 == 0 else at.x_peer)

    def spread_two(j):
        cs = scatter.cols(j)
        scatter.copies[j, 9].wait()
        if j % 2 == 0:
            here, peer = grad_ref.at[:, :, at.x, at.core, :, cs], at.x_peer
        else:
            here, peer = grad_ref.at[:, at.y, :, at.core, :, cs], at.y_peer
        scatter.start(j, 10, here, here, peer)

    def spread_core(j):
        cs = scatter.cols(j)
        scatter.copies[j, 10].wait()
        here = grad_ref.at[:, :, :, at.core, :, cs]
        scatter.start(j, 11, here, here, at.partner)

    def finish(j):
        scatter.copies[j, 11].wait()

    steps = (scatter.stage1, scatter.stage2, scatter.stage3, spread_z, spread_one, spread_two, spread_core, finish)
    for j in range(chunks):
        scatter.stage0(j)
    for t in range(chunks + len(steps) - 1):
        for stage, step in enumerate(steps):
            if 0 <= t - stage < chunks:
                step(t - stage)


def corr_grad(part, lam, total_rows, collective_id, chunks=8):
    full, cols = part.shape
    rows = full // 32
    grad, loss = pl.pallas_call(
        functools.partial(corr_kernel, chunks, total_rows),
        out_shape=(jax.ShapeDtypeStruct((4, 2, 2, 2, rows, cols), BF16), jax.ShapeDtypeStruct((1, cols), F32)),
        in_specs=[pl.BlockSpec(memory_space=pltpu.VMEM), pl.BlockSpec(memory_space=pltpu.SMEM)],
        out_specs=(pl.BlockSpec(memory_space=pltpu.VMEM), pl.BlockSpec(memory_space=pltpu.VMEM)),
        scratch_shapes=scatter_scratch(rows, cols, chunks, 12),
        compiler_params=pltpu.CompilerParams(
            collective_id=collective_id, has_side_effects=True, vmem_limit_bytes=48 * 2**20),
    )(part.reshape(4, 2, 2, 2, rows, cols), lam.reshape(1))
    return grad.reshape(full, cols), loss


class Sums:
    def __init__(self, at, local, total, recv0, slots1, slots2, send_sem, recv_sem):
        self.at, self.local, self.total = at, local, total
        self.recv0, self.slots1, self.slots2 = recv0, slots1, slots2
        self.send_sem, self.recv_sem = send_sem, recv_sem
        half = local.shape[-1] // 2
        self.mine = pl.ds(pl.multiple_of(at.core * half, 128), half)
        self.theirs = pl.ds(pl.multiple_of((1 - at.core) * half, 128), half)
        self.copies = []

    def start(self, k, src, dst, peer):
        copy = remote(src, dst, self.send_sem.at[k], self.recv_sem.at[k], peer)
        copy.start()
        self.copies.append(copy)

    def arrive(self):
        for copy in self.copies:
            copy.wait()
        self.copies = []

    def begin(self):
        self.start(0, self.local.at[:, self.theirs], self.recv0, self.at.partner)

    def over_plane(self):
        self.arrive()
        here = self.slots1.at[self.at.plane]
        here[...] = self.local[:, self.mine] + self.recv0[...]
        for d in range(3):
            self.start(1 + d, here, here, self.at.plane_peers[d])

    def over_line(self):
        self.arrive()
        here = self.slots2.at[self.at.z]
        here[...] = (self.slots1[0] + self.slots1[1]) + (self.slots1[2] + self.slots1[3])
        for d in range(3):
            self.start(4 + d, here, here, self.at.z_peers[d])

    def over_pair(self):
        self.arrive()
        here = self.total.at[:, self.mine]
        here[...] = (self.slots2[0] + self.slots2[1]) + (self.slots2[2] + self.slots2[3])
        self.start(7, here, here, self.at.partner)


def sums_scratch(rows, cols):
    return [
        pltpu.VMEM((rows, cols // 2), F32),
        pltpu.VMEM((4, rows, cols // 2), F32),
        pltpu.VMEM((4, rows, cols // 2), F32),
        pltpu.SemaphoreType.DMA((8,)),
        pltpu.SemaphoreType.DMA((8,)),
    ]


class Ring:
    def __init__(self, at, chunks, total, part, recv0, kept, snd1, recv1, snd2, recv2, snd3, recv3, send_sem, recv_sem, credit):
        self.at, self.chunks, self.total_chunks = at, chunks, total
        self.part, self.recv0, self.kept = part, recv0, kept
        self.snd1, self.recv1, self.snd2, self.recv2, self.snd3, self.recv3 = snd1, recv1, snd2, recv2, snd3, recv3
        self.send_sem, self.recv_sem, self.credit = send_sem, recv_sem, credit
        self.copies = {}

    def start(self, q, stage, src, dst, peer, again):
        j = q % self.chunks
        if q >= again:
            pl.semaphore_wait(self.credit.at[j if again > 2 else q % 2, stage], 1)
        copy = remote(src, dst, self.send_sem.at[j, stage], self.recv_sem.at[j, stage], peer)
        copy.start()
        self.copies[q, stage] = copy

    def give(self, q, stage, peer, again):
        if q + again < self.total_chunks:
            slot = q % self.chunks if again > 2 else q % 2
            pl.semaphore_signal(self.credit.at[slot, stage], inc=1, device_id=(peer,), device_id_type=MESH)

    def pair(self, q):
        at, s = self.at, q % 2
        self.start(q, 0, self.part.at[s, :, :, :, 1 - at.core], self.recv0.at[s], at.partner, 2)

    def first(self, q):
        at, s, j = self.at, q % 2, q % self.chunks
        self.copies[q, 0].wait()

        @pl.loop(0, 4)
        def _(z):
            for k in range(2):
                (y, x), (oy, ox) = ((k, at.x), (k, 1 - at.x)) if q % 2 == 0 else ((at.y, k), (1 - at.y, k))
                self.snd1[j, z, k] = (self.part[s, z, oy, ox, at.core] + self.recv0[s, z, oy, ox]).astype(BF16)
                self.kept[j, z, k] = self.part[s, z, y, x, at.core] + self.recv0[s, z, y, x]

        self.give(q, 0, at.partner, 2)
        self.start(q, 1, self.snd1.at[j], self.recv1.at[j], at.x_peer if q % 2 == 0 else at.y_peer, self.chunks)

    def second(self, q):
        at, j = self.at, q % self.chunks
        own = at.y if q % 2 == 0 else at.x
        self.copies[q, 1].wait()

        @pl.loop(0, 4)
        def _(z):
            self.snd2[j, z] = (self.kept[j, z, 1 - own] + self.recv1[j, z, 1 - own].astype(F32)).astype(BF16)
            self.kept[j, z, own] = self.kept[j, z, own] + self.recv1[j, z, own].astype(F32)

        self.give(q, 1, at.x_peer if q % 2 == 0 else at.y_peer, self.chunks)
        self.start(q, 2, self.snd2.at[j], self.recv2.at[j], at.y_peer if q % 2 == 0 else at.x_peer, self.chunks)

    def third(self, q):
        at, j = self.at, q % self.chunks
        own = at.y if q % 2 == 0 else at.x
        self.copies[q, 2].wait()
        for d in range(3):
            z = lax.rem(at.z + d + 1, 4)
            self.snd3[j, d] = (self.kept[j, z, own] + self.recv2[j, z].astype(F32)).astype(BF16)
            self.start(q, 3 + d, self.snd3.at[j, d], self.recv3.at[j, d], at.z_peers[d], self.chunks)

    def last(self, q):
        at, j = self.at, q % self.chunks
        own = at.y if q % 2 == 0 else at.x
        total = self.kept[j, at.z, own] + self.recv2[j, at.z].astype(F32)
        self.give(q, 2, at.y_peer if q % 2 == 0 else at.x_peer, self.chunks)
        for d in range(3):
            self.copies[q, 3 + d].wait()
            total += self.recv3[j, d].astype(F32)
            self.give(q, 3 + d, at.z_peers[2 - d], self.chunks)
        return total


def ring_scratch(chunks, rows, width):
    return [
        pltpu.VMEM((2, 4, 2, 2, 2, rows, width), F32),
        pltpu.VMEM((2, 4, 2, 2, rows, width), F32),
        pltpu.VMEM((chunks, 4, 2, rows, width), F32),
        pltpu.VMEM((chunks, 4, 2, rows, width), BF16),
        pltpu.VMEM((chunks, 4, 2, rows, width), BF16),
        pltpu.VMEM((chunks, 4, rows, width), BF16),
        pltpu.VMEM((chunks, 4, rows, width), BF16),
        pltpu.VMEM((chunks, 3, rows, width), BF16),
        pltpu.VMEM((chunks, 3, rows, width), BF16),
        pltpu.SemaphoreType.DMA((chunks, 6)),
        pltpu.SemaphoreType.DMA((chunks, 6)),
        pltpu.SemaphoreType.REGULAR((chunks, 6)),
    ]


CHUNKS = 8
RING = 12
SUMS = 5


def backward_kernel(
        total_rows, embed_sums, grad_embed, embed, norm_two, norm_one, act_two, act_one,
        act_two_t, act_one_t, feat_t, w_three, w_two, scale_three, scale_two, scale_one,
        grad_w_three, grad_w_two, grad_w_one, total_three, total_two, total_one,
        grad, pre, turned, weight, normed, act, local, w_sem, load_sem, *scratch):
    at = Place()
    enter([at.partner] + at.plane_peers + at.z_peers)
    ring = Ring(at, CHUNKS, 3 * CHUNKS, *scratch[:RING])
    dim = grad.shape[1]
    width = dim // CHUNKS
    view_rows = grad.shape[0] // 2
    block_rows = min(64, view_rows)
    count = 1.0 / total_rows
    feeds = [act_two_t, act_one_t, feat_t]
    norms = [embed, norm_two, norm_one]
    masks = [act_two, act_one]
    weights = [w_three, w_two]
    scales = [scale_three, scale_two, scale_one]
    outs = [grad_w_three, grad_w_two, grad_w_one]
    totals = [total_three, total_two, total_one]
    sums = {}
    sums[0, 0] = Sums(at, embed_sums, total_three, *scratch[RING:RING + SUMS])
    for layer in (1, 2):
        for h in range(2):
            first = RING + SUMS * (2 * layer - 1 + h)
            sums[layer, h] = Sums(at, local.at[layer - 1, h], totals[layer].at[h], *scratch[first:first + SUMS])

    def load(src, dst, k):
        copy = pltpu.make_async_copy(src, dst, load_sem.at[k])
        copy.start()
        return copy

    sums[0, 0].begin()
    loads = {
        "pre": load(grad_embed, pre, 0),
        ("norm", 0): load(embed, normed.at[0], 1),
        ("feed", 0): load(act_two_t, turned.at[0], 3),
        ("norm", 1): load(norm_two, normed.at[1], 2),
        ("act", 0): load(act_two, act, 5),
    }
    slots = weight.shape[0]
    w_loads = {}

    def load_weight(layer, n):
        copy = pltpu.make_async_copy(weights[layer].at[pl.ds(n * width, width), :], weight.at[n % slots],
                                     w_sem.at[n % slots])
        copy.start()
        w_loads[layer, n] = copy

    for n in range(slots):
        load_weight(0, n)
    sums[0, 0].over_plane()
    sums[0, 0].over_line()
    sums[0, 0].over_pair()

    def finish_grad(layer, j):
        cols = pl.ds(j * width, width)
        total, first = (total_three, j * width) if layer == 0 else (
            totals[layer].at[j // (CHUNKS // 2)], (j % (CHUNKS // 2)) * width)
        sel = pl.ds(first, width)
        for v in range(2):
            mean0 = total[v:v + 1, sel] * count
            mean1 = total[2 + v:3 + v, sel] * count
            scale = scales[layer][v:v + 1, cols]

            @pl.loop(0, view_rows // block_rows)
            def _(r):
                rows = pl.ds(pl.multiple_of(v * view_rows + r * block_rows, block_rows), block_rows)
                xhat = normed[layer % 2, rows, cols].astype(F32)
                grad[rows, cols] = (scale * (pre[rows, cols] - (mean0 + xhat * mean1))).astype(BF16)

    def weight_grad(layer, j):
        cols = pl.ds(j * width, width)
        s = j % 2

        @pl.loop(0, 4)
        def _(z):
            rows = pl.ds(pl.multiple_of(z * (dim // 4), dim // 4), dim // 4)
            out = jnp.dot(turned[layer % 2, rows, :], grad[:, cols], preferred_element_type=F32)
            ring.part[s, z] = out.reshape(ring.part.shape[2:])

        ring.pair(layer * CHUNKS + j)

    def input_grad(layer, n):
        cols = pl.ds(n * width, width)
        w_loads[layer, n].wait()
        half = local.at[layer, n // (CHUNKS // 2)]
        sel = pl.ds((n % (CHUNKS // 2)) * width, width)

        @pl.loop(0, 2)
        def _(v):
            rows = pl.ds(pl.multiple_of(v * view_rows, view_rows), view_rows)
            out = lax.dot_general(grad[rows, :], weight[n % slots], (((1,), (1,)), ((), ())),
                                  preferred_element_type=F32)
            out = jnp.where(act[rows, cols] > 0, out, 0.0)
            pre[rows, cols] = out
            half[pl.ds(v, 1), sel] = jnp.sum(out, axis=0, keepdims=True)
            half[pl.ds(2 + v, 1), sel] = jnp.sum(out * normed[(layer + 1) % 2, rows, cols].astype(F32), axis=0, keepdims=True)

        if n + slots < CHUNKS:
            load_weight(layer, n + slots)

    last = 3 * CHUNKS - 1

    def serve(q):
        if q <= last:
            ring.first(q)
        if 0 <= q - 2 <= last:
            ring.second(q - 2)
        if 0 <= q - 3 <= last:
            ring.third(q - 3)
        if 0 <= q - 5 <= last:
            done = q - 5
            outs[done // CHUNKS][:, pl.ds((done % CHUNKS) * width, width)] = ring.last(done)

    for layer in range(3):
        q = layer * CHUNKS
        if layer == 0:
            sums[0, 0].arrive()
            loads["pre"].wait()
        else:
            sums[layer, 0].arrive()
        if layer == 0:
            loads["norm", 0].wait()
        finish_grad(layer, 0)
        loads["feed", layer].wait()
        weight_grad(layer, 0)
        if layer < 2:
            loads["feed", layer + 1] = load(feeds[layer + 1], turned.at[(layer + 1) % 2], 3 + (layer + 1) % 2)
        if layer > 0:
            sums[layer, 1].over_pair()
        serve(q)
        finish_grad(layer, 1)
        weight_grad(layer, 1)
        serve(q + 1)
        finish_grad(layer, 2)
        weight_grad(layer, 2)
        finish_grad(layer, 3)
        if layer > 0:
            sums[layer, 1].arrive()
        for j in range(4, CHUNKS):
            finish_grad(layer, j)
        if layer == 0:
            loads["norm", 2] = load(norm_one, normed.at[0], 1)
        serve(q + 2)
        if layer == 2:
            for j in range(3, CHUNKS):
                weight_grad(layer, j)
                serve(q + j)
            break
        loads["norm", layer + 1].wait()
        loads["act", layer].wait()
        input_grad(layer, 0)
        input_grad(layer, 1)
        weight_grad(layer, 3)
        input_grad(layer, 2)
        serve(q + 3)
        input_grad(layer, 3)
        sums[layer + 1, 0].begin()
        weight_grad(layer, 4)
        sums[layer + 1, 0].over_plane()
        input_grad(layer, 4)
        serve(q + 4)
        input_grad(layer, 5)
        sums[layer + 1, 0].over_line()
        weight_grad(layer, 5)
        input_grad(layer, 6)
        serve(q + 5)
        input_grad(layer, 7)
        sums[layer + 1, 1].begin()
        if layer == 0:
            loads["act", 1] = load(masks[1], act, 5)
            for n in range(slots):
                load_weight(1, n)
        sums[layer + 1, 0].over_pair()
        weight_grad(layer, 6)
        sums[layer + 1, 1].over_plane()
        serve(q + 6)
        weight_grad(layer, 7)
        sums[layer + 1, 1].over_line()
        serve(q + 7)
    for q in range(3 * CHUNKS, 3 * CHUNKS + 5):
        serve(q)


def backward(total_rows, vmem, *args):
    grad_embed = args[1]
    rows, dim = grad_embed.shape
    width, blocks = dim // CHUNKS, dim // 32
    hbm = pl.BlockSpec(memory_space=pl.ANY)
    vm = pl.BlockSpec(memory_space=pltpu.VMEM)
    scratch = [
        pltpu.VMEM((rows, dim), BF16),
        pltpu.VMEM((rows, dim), F32),
        pltpu.VMEM((2, dim, rows), BF16),
        pltpu.VMEM((3, width, dim), BF16),
        pltpu.VMEM((2, rows, dim), BF16),
        pltpu.VMEM((rows, dim), BF16),
        pltpu.VMEM((2, 2, 4, dim // 2), F32),
        pltpu.SemaphoreType.DMA((3,)),
        pltpu.SemaphoreType.DMA((6,)),
    ] + ring_scratch(CHUNKS, blocks, width) + sums_scratch(5, dim)
    for _ in range(4):
        scratch += sums_scratch(4, dim // 2)
    return pl.pallas_call(
        functools.partial(backward_kernel, total_rows),
        out_shape=[jax.ShapeDtypeStruct((blocks, dim), F32)] * 3 + [
            jax.ShapeDtypeStruct((5, dim), F32),
            jax.ShapeDtypeStruct((2, 4, dim // 2), F32),
            jax.ShapeDtypeStruct((2, 4, dim // 2), F32)],
        in_specs=[vm] + [hbm] * 11 + [vm] * 3,
        out_specs=[vm] * 6,
        scratch_shapes=scratch,
        compiler_params=pltpu.CompilerParams(collective_id=5, has_side_effects=True, vmem_limit_bytes=vmem),
    )(*args)


def norm_forward(values, total_rows, collective_id):
    cols = values.shape[-1]
    col_sums = jnp.concatenate([jnp.sum(values, axis=1), jnp.sum(values * values, axis=1)])
    col_sums = all_sums(col_sums, collective_id).reshape(2, 2, cols)
    col_mean = col_sums[0] / total_rows
    inv_std = lax.rsqrt(col_sums[1] / total_rows - col_mean * col_mean + NORM_EPS)
    return (values - col_mean[:, None, :]) * inv_std[:, None, :], inv_std


def solution(mesh):
    shards = mesh.shape["data"]

    def local_step(h_a, h_b, w_one, w_two, w_three, gain_one, shift_one, gain_two, shift_two, lam_off):
        rows_dev = h_a.shape[0]
        total_rows = rows_dev * shards
        feat_rows = jnp.concatenate([h_a, h_b], axis=0)
        hidden_one = jnp.dot(feat_rows, w_one, preferred_element_type=F32).reshape(2, rows_dev, -1)
        normed_one, inv_one = norm_forward(hidden_one, total_rows, 0)
        pre_one = gain_one * normed_one + shift_one
        act_one = jax.nn.relu(pre_one).astype(BF16)
        hidden_two = jnp.dot(act_one, w_two, preferred_element_type=F32)
        normed_two, inv_two = norm_forward(hidden_two, total_rows, 1)
        pre_two = gain_two * normed_two + shift_two
        act_two = jax.nn.relu(pre_two).astype(BF16)
        proj_out = jnp.dot(act_two, w_three, preferred_element_type=F32)
        normed_out, inv_out = norm_forward(proj_out, total_rows, 2)
        embed_pair = normed_out.astype(BF16)
        corr_part = lax.dot_general(embed_pair[0], embed_pair[1], FIRST_DIMS, preferred_element_type=F32)
        grad_scaled, loss_cols = corr_grad(corr_part.astype(BF16), lam_off, total_rows, 3)
        grad_embed_a = lax.dot_general(embed_pair[1], grad_scaled, (((1,), (1,)), ((), ())),
                                       preferred_element_type=F32)
        grad_embed_b = jnp.dot(embed_pair[0], grad_scaled, preferred_element_type=F32)
        grad_embed = jnp.concatenate([grad_embed_a, grad_embed_b])
        products = grad_embed.reshape(2, rows_dev, -1)
        embed_sums = jnp.concatenate(
            [jnp.sum(products, axis=1), jnp.sum(products * embed_pair.astype(F32), axis=1), loss_cols])
        flat = lambda values: values.reshape(2 * rows_dev, -1)
        act_one, act_two = flat(act_one), flat(act_two)
        grad_w_three, grad_w_two, grad_w_one, total_three, total_two, total_one = backward(
            total_rows, 62 * 2**20, embed_sums, grad_embed, flat(embed_pair), flat(normed_two.astype(BF16)),
            flat(normed_one.astype(BF16)), act_two, act_one, act_two.T, act_one.T, feat_rows.T, w_three, w_two,
            inv_out, gain_two * inv_two, gain_one * inv_one)
        loss_total = jnp.sum(total_three[4])
        both = lambda total, row: (total[:, row] + total[:, row + 1]).reshape(-1)
        return (loss_total, grad_w_one, grad_w_two, grad_w_three,
                both(total_one, 2), both(total_one, 0), both(total_two, 2), both(total_two, 0))

    row_spec = P("data", None)
    whole_mat = P(None, None)
    whole_vec = P(None)
    return jax.shard_map(
        local_step, mesh=mesh,
        in_specs=(row_spec, row_spec, whole_mat, whole_mat, whole_mat,
                  whole_vec, whole_vec, whole_vec, whole_vec, P()),
        out_specs=(P(), row_spec, row_spec, row_spec, whole_vec, whole_vec, whole_vec, whole_vec),
        check_vma=False)
```

```python
import functools

import jax
import jax.numpy as jnp
from jax import lax
from jax.experimental import pallas as pl
from jax.experimental.pallas import tpu as pltpu
from jax.sharding import PartitionSpec as P

NORM_EPS = 1e-5
MESH = pl.DeviceIdType.MESH
F32 = jnp.float32
BF16 = jnp.bfloat16


class Place:
    def __init__(self):
        me = lax.axis_index("data")
        self.core = lax.rem(me, 2)
        self.x = lax.rem(lax.div(me, 2), 2)
        self.y = lax.rem(lax.div(me, 4), 2)
        self.z = lax.div(me, 8)
        self.plane = lax.rem(lax.div(me, 2), 4)
        self.partner = me + 1 - 2 * self.core
        self.x_peer = me + 2 - 4 * self.x
        self.y_peer = me + 4 - 8 * self.y
        low = lax.rem(me, 8)
        self.z_peers = [lax.rem(self.z + d, 4) * 8 + low for d in (1, 2, 3)]
        self.plane_peers = [
            self.z * 8 + lax.rem(self.plane + d, 4) * 2 + self.core for d in (1, 2, 3)
        ]


def enter(peers):
    barrier = pltpu.get_barrier_semaphore()
    for peer in peers:
        pl.semaphore_signal(barrier, inc=1, device_id=(peer,), device_id_type=MESH)
    pl.semaphore_wait(barrier, len(peers))


def remote(src, dst, send_sem, recv_sem, peer):
    return pltpu.make_async_remote_copy(
        src_ref=src, dst_ref=dst, send_sem=send_sem, recv_sem=recv_sem,
        device_id=(peer,), device_id_type=MESH)


class Scatter:
    def __init__(self, at, part, bufs, send_sem, recv_sem, chunk):
        self.at, self.part, self.chunk = at, part, chunk
        self.recv0, self.snd1, self.recv1, self.snd2, self.recv2, self.snd3, self.recv3 = bufs
        self.send_sem, self.recv_sem = send_sem, recv_sem
        self.copies = {}

    def cols(self, j):
        return pl.ds(j * self.chunk, self.chunk)

    def start(self, j, stage, src, dst, peer):
        copy = remote(src, dst, self.send_sem.at[j, stage], self.recv_sem.at[j, stage], peer)
        copy.start()
        self.copies[j, stage] = copy

    def total(self, j, z, y, x, depth):
        cs, c = self.cols(j), self.at.core
        total = self.part[z, y, x, c, :, cs].astype(F32) + self.recv0[z, y, x, :, cs].astype(F32)
        if depth > 1:
            total += self.recv1[z, y if j % 2 == 0 else x, :, cs].astype(F32)
        if depth > 2:
            total += self.recv2[z, :, cs].astype(F32)
        return total

    def stage0(self, j):
        cs, at = self.cols(j), self.at
        self.start(j, 0, self.part.at[:, :, :, 1 - at.core, :, cs], self.recv0.at[:, :, :, :, cs], at.partner)

    def stage1(self, j):
        cs, at = self.cols(j), self.at
        self.copies[j, 0].wait()
        for z in range(4):
            for k in range(2):
                y, x = (k, 1 - at.x) if j % 2 == 0 else (1 - at.y, k)
                self.snd1[z, k, :, cs] = self.total(j, z, y, x, 1).astype(BF16)
        self.start(j, 1, self.snd1.at[:, :, :, cs], self.recv1.at[:, :, :, cs], at.x_peer if j % 2 == 0 else at.y_peer)

    def stage2(self, j):
        cs, at = self.cols(j), self.at
        self.copies[j, 1].wait()
        for z in range(4):
            y, x = (1 - at.y, at.x) if j % 2 == 0 else (at.y, 1 - at.x)
            self.snd2[z, :, cs] = self.total(j, z, y, x, 2).astype(BF16)
        self.start(j, 2, self.snd2.at[:, :, cs], self.recv2.at[:, :, cs], at.y_peer if j % 2 == 0 else at.x_peer)

    def stage3(self, j):
        cs, at = self.cols(j), self.at
        self.copies[j, 2].wait()
        for d in range(3):
            z = lax.rem(at.z + d + 1, 4)
            self.snd3[d, :, cs] = self.total(j, z, at.y, at.x, 3).astype(BF16)
            self.start(j, 3 + d, self.snd3.at[d, :, cs], self.recv3.at[d, :, cs], at.z_peers[d])

    def final(self, j):
        cs, at = self.cols(j), self.at
        total = self.total(j, at.z, at.y, at.x, 3)
        for d in range(3):
            self.copies[j, 3 + d].wait()
            total += self.recv3[d, :, cs].astype(F32)
        return total


def scatter_scratch(rows, cols, chunks, stages):
    return [
        pltpu.VMEM((4, 2, 2, rows, cols), BF16),
        pltpu.VMEM((4, 2, rows, cols), BF16),
        pltpu.VMEM((4, 2, rows, cols), BF16),
        pltpu.VMEM((4, rows, cols), BF16),
        pltpu.VMEM((4, rows, cols), BF16),
        pltpu.VMEM((3, rows, cols), BF16),
        pltpu.VMEM((3, rows, cols), BF16),
        pltpu.SemaphoreType.DMA((chunks, stages)),
        pltpu.SemaphoreType.DMA((chunks, stages)),
    ]


def corr_kernel(chunks, total_rows, part_ref, lam_ref, grad_ref, loss_ref, *scratch):
    at = Place()
    enter([at.partner, at.x_peer, at.y_peer] + at.z_peers)
    send_sem, recv_sem = scratch[7:]
    rows, cols = part_ref.shape[-2:]
    chunk = cols // chunks
    scatter = Scatter(at, part_ref, scratch[:7], send_sem, recv_sem, chunk)
    lam = lam_ref[0]
    block = grad_ref.at[at.z, at.y, at.x, at.core]
    first_row = (((at.z * 2 + at.y) * 2 + at.x) * 2 + at.core) * rows

    def spread_z(j):
        cs = scatter.cols(j)
        corr = scatter.final(j) / total_rows
        row = first_row + lax.broadcasted_iota(jnp.int32, corr.shape, 0)
        col = j * chunk + lax.broadcasted_iota(jnp.int32, corr.shape, 1)
        diag = row == col
        gap = 1.0 - corr
        loss_ref[:, cs] = jnp.sum(jnp.where(diag, gap * gap, lam * corr * corr), axis=0, keepdims=True)
        grad = jnp.where(diag, -2.0 * gap, 2.0 * lam * corr)
        block[:, cs] = (grad / total_rows).astype(BF16)
        for d in range(3):
            scatter.start(j, 6 + d, block.at[:, cs], block.at[:, cs], at.z_peers[d])

    def spread_one(j):
        cs = scatter.cols(j)
        for d in range(3):
            scatter.copies[j, 6 + d].wait()
        here = grad_ref.at[:, at.y, at.x, at.core, :, cs]
        scatter.start(j, 9, here, here, at.y_peer if j % 2 == 0 else at.x_peer)

    def spread_two(j):
        cs = scatter.cols(j)
        scatter.copies[j, 9].wait()
        if j % 2 == 0:
            here, peer = grad_ref.at[:, :, at.x, at.core, :, cs], at.x_peer
        else:
            here, peer = grad_ref.at[:, at.y, :, at.core, :, cs], at.y_peer
        scatter.start(j, 10, here, here, peer)

    def spread_core(j):
        cs = scatter.cols(j)
        scatter.copies[j, 10].wait()
        here = grad_ref.at[:, :, :, at.core, :, cs]
        scatter.start(j, 11, here, here, at.partner)

    def finish(j):
        scatter.copies[j, 11].wait()

    steps = (scatter.stage1, scatter.stage2, scatter.stage3, spread_z, spread_one, spread_two, spread_core, finish)
    for j in range(chunks):
        scatter.stage0(j)
    for t in range(chunks + len(steps) - 1):
        for stage, step in enumerate(steps):
            if 0 <= t - stage < chunks:
                step(t - stage)


def corr_grad(part, lam, total_rows, collective_id, chunks=8):
    full, cols = part.shape
    rows = full // 32
    grad, loss = pl.pallas_call(
        functools.partial(corr_kernel, chunks, total_rows),
        out_shape=(jax.ShapeDtypeStruct((4, 2, 2, 2, rows, cols), BF16), jax.ShapeDtypeStruct((1, cols), F32)),
        in_specs=[pl.BlockSpec(memory_space=pltpu.VMEM), pl.BlockSpec(memory_space=pltpu.SMEM)],
        out_specs=(pl.BlockSpec(memory_space=pltpu.VMEM), pl.BlockSpec(memory_space=pltpu.VMEM)),
        scratch_shapes=scatter_scratch(rows, cols, chunks, 12),
        compiler_params=pltpu.CompilerParams(
            collective_id=collective_id, has_side_effects=True, vmem_limit_bytes=48 * 2**20),
    )(part.reshape(4, 2, 2, 2, rows, cols), lam.reshape(1))
    return grad.reshape(full, cols), loss


class Sums:
    def __init__(self, at, local, total, recv0, slots1, slots2, send_sem, recv_sem):
        self.at, self.refs = at, (local, total)
        self.recv0, self.slots1, self.slots2 = recv0, slots1, slots2
        self.send_sem, self.recv_sem = send_sem, recv_sem
        self.half = recv0.shape[-1]
        self.mine = pl.multiple_of(at.core * self.half, 128)
        self.theirs = pl.multiple_of((1 - at.core) * self.half, 128)

    def pick(self, k, first):
        ref, index = self.refs[k]
        return ref.at[(*index, slice(None), pl.ds(first, self.half))]

    def copies(self, stage):
        at = self.at
        if stage == 0:
            pairs = [(0, self.pick(0, self.theirs), self.recv0, at.partner)]
        elif stage == 1:
            here = self.slots1.at[at.plane]
            pairs = [(1 + d, here, here, at.plane_peers[d]) for d in range(3)]
        elif stage == 2:
            here = self.slots2.at[at.z]
            pairs = [(4 + d, here, here, at.z_peers[d]) for d in range(3)]
        else:
            here = self.pick(1, self.mine)
            pairs = [(7, here, here, at.partner)]
        return [remote(src, dst, self.send_sem.at[k], self.recv_sem.at[k], peer) for k, src, dst, peer in pairs]

    def send(self, stage):
        for copy in self.copies(stage):
            copy.start()

    def arrive(self, stage=3):
        for copy in self.copies(stage):
            copy.wait()

    def begin(self):
        self.send(0)

    def over_plane(self):
        self.arrive(0)
        self.slots1[self.at.plane] = self.pick(0, self.mine)[...] + self.recv0[...]
        self.send(1)

    def over_line(self):
        self.arrive(1)
        self.slots2[self.at.z] = (self.slots1[0] + self.slots1[1]) + (self.slots1[2] + self.slots1[3])
        self.send(2)

    def over_pair(self):
        self.arrive(2)
        self.pick(1, self.mine)[...] = (self.slots2[0] + self.slots2[1]) + (self.slots2[2] + self.slots2[3])
        self.send(3)


def sums_scratch(rows, cols):
    return [
        pltpu.VMEM((rows, cols // 2), F32),
        pltpu.VMEM((4, rows, cols // 2), F32),
        pltpu.VMEM((4, rows, cols // 2), F32),
        pltpu.SemaphoreType.DMA((8,)),
        pltpu.SemaphoreType.DMA((8,)),
    ]


class Ring:
    def __init__(self, at, chunks, total, part, recv0, kept, snd1, recv1, snd2, recv2, snd3, recv3, send_sem, recv_sem, credit):
        self.at, self.chunks, self.total_chunks = at, chunks, total
        self.part, self.recv0, self.kept = part, recv0, kept
        self.snd1, self.recv1, self.snd2, self.recv2, self.snd3, self.recv3 = snd1, recv1, snd2, recv2, snd3, recv3
        self.send_sem, self.recv_sem, self.credit = send_sem, recv_sem, credit
        self.copies = {}

    def start(self, q, stage, src, dst, peer, again):
        j = q % self.chunks
        if q >= again:
            pl.semaphore_wait(self.credit.at[j if again > 2 else q % 2, stage], 1)
        copy = remote(src, dst, self.send_sem.at[j, stage], self.recv_sem.at[j, stage], peer)
        copy.start()
        self.copies[q, stage] = copy

    def give(self, q, stage, peer, again):
        if q + again < self.total_chunks:
            slot = q % self.chunks if again > 2 else q % 2
            pl.semaphore_signal(self.credit.at[slot, stage], inc=1, device_id=(peer,), device_id_type=MESH)

    def pair(self, q):
        at, s = self.at, q % 2
        self.start(q, 0, self.part.at[s, :, :, :, 1 - at.core], self.recv0.at[s], at.partner, 2)

    def first(self, q):
        at, s, j = self.at, q % 2, q % self.chunks
        self.copies[q, 0].wait()

        @pl.loop(0, 4)
        def _(z):
            for k in range(2):
                (y, x), (oy, ox) = ((k, at.x), (k, 1 - at.x)) if q % 2 == 0 else ((at.y, k), (1 - at.y, k))
                self.snd1[j, z, k] = (self.part[s, z, oy, ox, at.core] + self.recv0[s, z, oy, ox]).astype(BF16)
                self.kept[j, z, k] = self.part[s, z, y, x, at.core] + self.recv0[s, z, y, x]

        self.give(q, 0, at.partner, 2)
        self.start(q, 1, self.snd1.at[j], self.recv1.at[j], at.x_peer if q % 2 == 0 else at.y_peer, self.chunks)

    def second(self, q):
        at, j = self.at, q % self.chunks
        own = at.y if q % 2 == 0 else at.x
        self.copies[q, 1].wait()

        @pl.loop(0, 4)
        def _(z):
            self.snd2[j, z] = (self.kept[j, z, 1 - own] + self.recv1[j, z, 1 - own].astype(F32)).astype(BF16)
            self.kept[j, z, own] = self.kept[j, z, own] + self.recv1[j, z, own].astype(F32)

        self.give(q, 1, at.x_peer if q % 2 == 0 else at.y_peer, self.chunks)
        self.start(q, 2, self.snd2.at[j], self.recv2.at[j], at.y_peer if q % 2 == 0 else at.x_peer, self.chunks)

    def third(self, q):
        at, j = self.at, q % self.chunks
        own = at.y if q % 2 == 0 else at.x
        self.copies[q, 2].wait()
        for d in range(3):
            z = lax.rem(at.z + d + 1, 4)
            self.snd3[j, d] = (self.kept[j, z, own] + self.recv2[j, z].astype(F32)).astype(BF16)
            self.start(q, 3 + d, self.snd3.at[j, d], self.recv3.at[j, d], at.z_peers[d], self.chunks)

    def last(self, q):
        at, j = self.at, q % self.chunks
        own = at.y if q % 2 == 0 else at.x
        total = self.kept[j, at.z, own] + self.recv2[j, at.z].astype(F32)
        self.give(q, 2, at.y_peer if q % 2 == 0 else at.x_peer, self.chunks)
        for d in range(3):
            self.copies[q, 3 + d].wait()
            total += self.recv3[j, d].astype(F32)
            self.give(q, 3 + d, at.z_peers[2 - d], self.chunks)
        return total


def ring_scratch(chunks, rows, width):
    return [
        pltpu.VMEM((2, 4, 2, 2, 2, rows, width), F32),
        pltpu.VMEM((2, 4, 2, 2, rows, width), F32),
        pltpu.VMEM((chunks, 4, 2, rows, width), F32),
        pltpu.VMEM((chunks, 4, 2, rows, width), BF16),
        pltpu.VMEM((chunks, 4, 2, rows, width), BF16),
        pltpu.VMEM((chunks, 4, rows, width), BF16),
        pltpu.VMEM((chunks, 4, rows, width), BF16),
        pltpu.VMEM((chunks, 3, rows, width), BF16),
        pltpu.VMEM((chunks, 3, rows, width), BF16),
        pltpu.SemaphoreType.DMA((chunks, 6)),
        pltpu.SemaphoreType.DMA((chunks, 6)),
        pltpu.SemaphoreType.REGULAR((chunks, 6)),
    ]


CHUNKS = 8
RING = 12
SUMS = 5


def backward_kernel(
        total_rows, embed_sums, grad_embed, embed, norm_two, norm_one, act_two, act_one,
        act_two_t, act_one_t, feat_t, w_three, w_two, scale_three, scale_two, scale_one,
        grad_w_three, grad_w_two, grad_w_one, total_three, total_two, total_one,
        grad, pre, turned, weight, normed, act, local, w_sem, load_sem, *scratch):
    at = Place()
    enter([at.partner] + at.plane_peers + at.z_peers)
    ring = Ring(at, CHUNKS, 3 * CHUNKS, *scratch[:RING])
    dim = grad.shape[1]
    width = dim // CHUNKS
    view_rows = grad.shape[0] // 2
    block_rows = min(64, view_rows)
    count = 1.0 / total_rows
    feeds = [act_two_t, act_one_t, feat_t]
    norms = [embed, norm_two, norm_one]
    masks = [act_two, act_one]
    weights = [w_three, w_two]
    scales = [scale_three, scale_two, scale_one]
    outs = [grad_w_three, grad_w_two, grad_w_one]
    totals = [total_three, total_two, total_one]
    sums = {}
    sums[0, 0] = Sums(at, (embed_sums, ()), (total_three, ()), *scratch[RING:RING + SUMS])
    for layer in (1, 2):
        for h in range(2):
            first = RING + SUMS * (2 * layer - 1 + h)
            sums[layer, h] = Sums(at, (local, (layer - 1, h)), (totals[layer], (h,)), *scratch[first:first + SUMS])

    def load(src, dst, k):
        copy = pltpu.make_async_copy(src, dst, load_sem.at[k])
        copy.start()
        return copy

    sums[0, 0].begin()
    loads = {
        "pre": load(grad_embed, pre, 0),
        ("norm", 0): load(embed, normed.at[0], 1),
        ("feed", 0): load(act_two_t, turned.at[0], 3),
        ("norm", 1): load(norm_two, normed.at[1], 2),
        ("act", 0): load(act_two, act, 5),
    }
    slots = weight.shape[0]
    w_loads = {}

    def load_weight(layer, n):
        copy = pltpu.make_async_copy(weights[layer].at[pl.ds(n * width, width), :], weight.at[n % slots],
                                     w_sem.at[n % slots])
        copy.start()
        w_loads[layer, n] = copy

    for n in range(slots):
        load_weight(0, n)
    sums[0, 0].over_plane()
    sums[0, 0].over_line()
    sums[0, 0].over_pair()

    def finish_grad(layer, j):
        cols = pl.ds(j * width, width)
        total, first = (total_three, j * width) if layer == 0 else (
            totals[layer].at[j // (CHUNKS // 2)], (j % (CHUNKS // 2)) * width)
        sel = pl.ds(first, width)
        for v in range(2):
            mean0 = total[v:v + 1, sel] * count
            mean1 = total[2 + v:3 + v, sel] * count
            scale = scales[layer][v:v + 1, cols]

            @pl.loop(0, view_rows // block_rows)
            def _(r):
                rows = pl.ds(pl.multiple_of(v * view_rows + r * block_rows, block_rows), block_rows)
                xhat = normed[layer % 2, rows, cols].astype(F32)
                grad[rows, cols] = (scale * (pre[rows, cols] - (mean0 + xhat * mean1))).astype(BF16)

    def weight_grad(layer, j):
        cols = pl.ds(j * width, width)
        s = j % 2

        @pl.loop(0, 4)
        def _(z):
            rows = pl.ds(pl.multiple_of(z * (dim // 4), dim // 4), dim // 4)
            out = jnp.dot(turned[layer % 2, rows, :], grad[:, cols], preferred_element_type=F32)
            ring.part[s, z] = out.reshape(ring.part.shape[2:])

        ring.pair(layer * CHUNKS + j)

    def input_grad(layer, n):
        cols = pl.ds(n * width, width)
        w_loads[layer, n].wait()
        half = local.at[layer, n // (CHUNKS // 2)]
        sel = pl.ds((n % (CHUNKS // 2)) * width, width)

        @pl.loop(0, 2)
        def _(v):
            rows = pl.ds(pl.multiple_of(v * view_rows, view_rows), view_rows)
            out = lax.dot_general(grad[rows, :], weight[n % slots], (((1,), (1,)), ((), ())),
                                  preferred_element_type=F32)
            out = jnp.where(act[rows, cols] > 0, out, 0.0)
            pre[rows, cols] = out
            half[pl.ds(v, 1), sel] = jnp.sum(out, axis=0, keepdims=True)
            half[pl.ds(2 + v, 1), sel] = jnp.sum(out * normed[(layer + 1) % 2, rows, cols].astype(F32), axis=0, keepdims=True)

        if n + slots < CHUNKS:
            load_weight(layer, n + slots)

    last = 3 * CHUNKS - 1

    def serve(q):
        if q <= last:
            ring.first(q)
        if 0 <= q - 2 <= last:
            ring.second(q - 2)
        if 0 <= q - 4 <= last:
            ring.third(q - 4)
        if 0 <= q - 6 <= last:
            done = q - 6
            outs[done // CHUNKS][:, pl.ds((done % CHUNKS) * width, width)] = ring.last(done)

    for layer in range(3):
        q = layer * CHUNKS
        if layer == 0:
            sums[0, 0].arrive()
            loads["pre"].wait()
        else:
            sums[layer, 0].arrive()
        if layer == 0:
            loads["norm", 0].wait()
        finish_grad(layer, 0)
        loads["feed", layer].wait()
        weight_grad(layer, 0)
        if layer < 2:
            loads["feed", layer + 1] = load(feeds[layer + 1], turned.at[(layer + 1) % 2], 3 + (layer + 1) % 2)
        if layer > 0:
            sums[layer, 1].over_pair()
        serve(q)
        finish_grad(layer, 1)
        weight_grad(layer, 1)
        serve(q + 1)
        finish_grad(layer, 2)
        weight_grad(layer, 2)
        finish_grad(layer, 3)
        if layer > 0:
            sums[layer, 1].arrive()
        for j in range(4, CHUNKS):
            finish_grad(layer, j)
        if layer == 0:
            loads["norm", 2] = load(norm_one, normed.at[0], 1)
        serve(q + 2)
        if layer == 2:
            for j in range(3, CHUNKS):
                weight_grad(layer, j)
                serve(q + j)
            break
        loads["norm", layer + 1].wait()
        loads["act", layer].wait()
        input_grad(layer, 0)
        input_grad(layer, 1)
        weight_grad(layer, 3)
        input_grad(layer, 2)
        serve(q + 3)
        input_grad(layer, 3)
        sums[layer + 1, 0].begin()
        weight_grad(layer, 4)
        sums[layer + 1, 0].over_plane()
        input_grad(layer, 4)
        serve(q + 4)
        input_grad(layer, 5)
        sums[layer + 1, 0].over_line()
        weight_grad(layer, 5)
        input_grad(layer, 6)
        serve(q + 5)
        input_grad(layer, 7)
        sums[layer + 1, 1].begin()
        if layer == 0:
            loads["act", 1] = load(masks[1], act, 5)
            for n in range(slots):
                load_weight(1, n)
        sums[layer + 1, 0].over_pair()
        weight_grad(layer, 6)
        sums[layer + 1, 1].over_plane()
        serve(q + 6)
        weight_grad(layer, 7)
        sums[layer + 1, 1].over_line()
        serve(q + 7)
    for q in range(3 * CHUNKS, 3 * CHUNKS + 6):
        serve(q)


def backward(total_rows, vmem, *args):
    grad_embed = args[1]
    rows, dim = grad_embed.shape
    width, blocks = dim // CHUNKS, dim // 32
    hbm = pl.BlockSpec(memory_space=pl.ANY)
    vm = pl.BlockSpec(memory_space=pltpu.VMEM)
    scratch = [
        pltpu.VMEM((rows, dim), BF16),
        pltpu.VMEM((rows, dim), F32),
        pltpu.VMEM((2, dim, rows), BF16),
        pltpu.VMEM((3, width, dim), BF16),
        pltpu.VMEM((2, rows, dim), BF16),
        pltpu.VMEM((rows, dim), BF16),
        pltpu.VMEM((2, 2, 4, dim // 2), F32),
        pltpu.SemaphoreType.DMA((3,)),
        pltpu.SemaphoreType.DMA((6,)),
    ] + ring_scratch(CHUNKS, blocks, width) + sums_scratch(5, dim)
    for _ in range(4):
        scratch += sums_scratch(4, dim // 2)
    return pl.pallas_call(
        functools.partial(backward_kernel, total_rows),
        out_shape=[jax.ShapeDtypeStruct((blocks, dim), F32)] * 3 + [
            jax.ShapeDtypeStruct((5, dim), F32),
            jax.ShapeDtypeStruct((2, 4, dim // 2), F32),
            jax.ShapeDtypeStruct((2, 4, dim // 2), F32)],
        in_specs=[vm] + [hbm] * 11 + [vm] * 3,
        out_specs=[vm] * 6,
        scratch_shapes=scratch,
        compiler_params=pltpu.CompilerParams(collective_id=5, has_side_effects=True, vmem_limit_bytes=vmem),
    )(*args)


def forward_kernel(
        total_rows, feat_a, feat_b, w_one, w_two, w_three, gain_one, shift_one, gain_two, shift_two,
        act_one, act_two, norm_one, norm_two, embed, feat_t, act_one_t, act_two_t, embed_t, scale_one, scale_two, scale_three,
        acts, hidden, normed, turned, weight, local, total, w_sem, in_sem, out_sem, *scratch):
    at = Place()
    view_rows, dim = acts.shape[2:]
    width = dim // CHUNKS
    quarter = dim // 4
    block_rows = min(64, view_rows)
    weights = [w_one, w_two, w_three]
    gains, shifts = [gain_one, gain_two], [shift_one, shift_two]
    scales = [scale_one, scale_two, scale_three]
    natural, normals, turns = [act_one, act_two, embed], [norm_one, norm_two], [feat_t, act_one_t, act_two_t, embed_t]
    sums = {(layer, v): Sums(at, (local, (layer, v)), (total, (layer, v)), *scratch[SUMS * k:SUMS * k + SUMS])
            for k, (layer, v) in enumerate((layer, v) for layer in range(3) for v in range(2))}

    ins = [pltpu.make_async_copy((feat_a, feat_b)[v], acts.at[0, v], in_sem.at[v]) for v in range(2)]

    def weight_copy(layer, k):
        cols = pl.ds(k * quarter, quarter)
        return pltpu.make_async_copy(weights[layer].at[:, cols], weight.at[layer % 2, :, cols], w_sem.at[layer % 2, k])

    def load_weight(layer, k):
        weight_copy(layer, k).start()

    ins[0].start()
    load_weight(0, 0)
    ins[1].start()
    for k in range(1, 4):
        load_weight(0, k)
    for k in range(4):
        load_weight(1, k)
    outs = {}

    def put(name, v, src, dst, k):
        copy = pltpu.make_async_copy(src, dst, out_sem.at[k, v])
        copy.start()
        outs[name, v] = copy

    def drain(name, v):
        outs.pop((name, v)).wait()

    def matmul(layer, v, hooks=()):
        hooks = list(hooks)
        if v == 0:
            hooks += [(2 * k, lambda k=k: weight_copy(layer, k).wait()) for k in range(4)]

        @pl.loop(0, CHUNKS)
        def _(n):
            for k, step in hooks:
                pl.when(n == k)(step)
            cols = pl.ds(pl.multiple_of(n * width, width), width)
            out = jnp.dot(acts[layer % 2, v], weight[layer % 2, :, cols], preferred_element_type=F32)
            hidden[v, :, cols] = out
            local[layer, v, 0:1, cols] = jnp.sum(out, axis=0, keepdims=True)
            local[layer, v, 1:2, cols] = jnp.sum(out * out, axis=0, keepdims=True)

    def normalise(layer, v):
        mean = total[layer, v, 0:1, :] / total_rows
        inv = lax.rsqrt(total[layer, v, 1:2, :] / total_rows - mean * mean + NORM_EPS)
        if layer < 2:
            scales[layer][v:v + 1, :] = gains[layer][...] * inv
        else:
            scales[layer][v:v + 1, :] = inv
        local[layer, v, 0:1, :] = mean
        local[layer, v, 1:2, :] = inv

        @pl.loop(0, CHUNKS)
        def _(n):
            cols = pl.ds(pl.multiple_of(n * width, width), width)
            mean, inv = local[layer, v, 0:1, cols], local[layer, v, 1:2, cols]
            if layer < 2:
                gain, shift = gains[layer][:, cols], shifts[layer][:, cols]

            @pl.loop(0, view_rows // block_rows)
            def _(r):
                rows = pl.ds(pl.multiple_of(r * block_rows, block_rows), block_rows)
                value = (hidden[v, rows, cols] - mean) * inv
                if layer < 2:
                    normed[v, rows, cols] = value.astype(BF16)
                    value = jnp.maximum(gain * value + shift, 0.0)
                acts[(layer + 1) % 2, v, rows, cols] = value.astype(BF16)

        put(("act", layer), v, acts.at[(layer + 1) % 2, v], natural[layer].at[v], layer % 2)
        if layer < 2:
            put(("norm", layer), v, normed.at[v], normals[layer].at[v], 2)

    def turn(k, v):
        @pl.loop(0, CHUNKS)
        def _(n):
            cols = pl.ds(pl.multiple_of(n * width, width), width)
            turned[cols, v * view_rows:(v + 1) * view_rows] = acts[k % 2, v, :, cols].T

        span = pl.ds(v * view_rows, view_rows)
        dst = turns[k].at[:, span] if k < 3 else turns[k]
        put(("turn", k), v, turned.at[:, span], dst, 3)

    enter([at.partner] + at.plane_peers + at.z_peers)
    ins[0].wait()
    matmul(0, 0)
    sums[0, 0].begin()
    ins[1].wait()
    matmul(0, 1, [(2, sums[0, 0].over_plane), (7, sums[0, 0].over_line)])
    sums[0, 1].begin()
    turn(0, 0)
    sums[0, 1].over_plane()
    turn(0, 1)
    for layer in range(3):
        sums[layer, 0].over_pair()
        if layer == 0:
            for k in range(4):
                load_weight(2, k)
        sums[layer, 0].arrive()
        for v in range(2):
            if layer > 0:
                if layer < 2:
                    drain(("norm", layer - 1), v)
                if layer == 2:
                    drain(("act", 0), v)
        normalise(layer, 0)
        if layer < 2:
            matmul(layer + 1, 0, [(0, sums[layer, 1].over_line), (7, sums[layer, 1].over_pair)])
            sums[layer + 1, 0].begin()
            sums[layer, 1].arrive()
            normalise(layer, 1)
            matmul(layer + 1, 1, [(0, sums[layer + 1, 0].over_plane), (6, sums[layer + 1, 0].over_line)])
            sums[layer + 1, 1].begin()
            drain(("turn", layer), 0)
            turn(layer + 1, 0)
            sums[layer + 1, 1].over_plane()
            drain(("turn", layer), 1)
            turn(layer + 1, 1)
        else:
            drain(("turn", 2), 0)
            turn(3, 0)
            sums[2, 1].over_line()
            sums[2, 1].over_pair()
            sums[2, 1].arrive()
            normalise(2, 1)
    for copy in outs.values():
        copy.wait()


def forward(total_rows, vmem, feat_a, feat_b, weights, vectors):
    view_rows, dim = feat_a.shape
    hbm = pl.BlockSpec(memory_space=pl.ANY)
    vm = pl.BlockSpec(memory_space=pltpu.VMEM)
    scratch = [
        pltpu.VMEM((2, 2, view_rows, dim), BF16),
        pltpu.VMEM((2, view_rows, dim), F32),
        pltpu.VMEM((2, view_rows, dim), BF16),
        pltpu.VMEM((dim, 2 * view_rows), BF16),
        pltpu.VMEM((2, dim, dim), BF16),
        pltpu.VMEM((3, 2, 2, dim), F32),
        pltpu.VMEM((3, 2, 2, dim), F32),
        pltpu.SemaphoreType.DMA((2, 4)),
        pltpu.SemaphoreType.DMA((2,)),
        pltpu.SemaphoreType.DMA((4, 2)),
    ]
    for _ in range(6):
        scratch += sums_scratch(2, dim)
    pair = jax.ShapeDtypeStruct((2, view_rows, dim), BF16)
    turned = jax.ShapeDtypeStruct((dim, 2 * view_rows), BF16)
    vector = jax.ShapeDtypeStruct((2, dim), F32)
    return pl.pallas_call(
        functools.partial(forward_kernel, total_rows),
        out_shape=[pair] * 5 + [turned] * 3 + [jax.ShapeDtypeStruct((dim, view_rows), BF16)] + [vector] * 3,
        in_specs=[hbm] * 5 + [vm] * 4,
        out_specs=[hbm] * 9 + [vm] * 3,
        scratch_shapes=scratch,
        compiler_params=pltpu.CompilerParams(collective_id=0, has_side_effects=True, vmem_limit_bytes=vmem),
    )(feat_a, feat_b, *weights, *[value.reshape(1, dim) for value in vectors])


def solution(mesh):
    shards = mesh.shape["data"]

    def local_step(h_a, h_b, w_one, w_two, w_three, gain_one, shift_one, gain_two, shift_two, lam_off):
        rows_dev = h_a.shape[0]
        total_rows = rows_dev * shards
        (act_one, act_two, norm_one, norm_two, embed_pair, feat_t, act_one_t, act_two_t, embed_t,
         scale_one, scale_two, scale_three) = forward(
            total_rows, 56 * 2**20, h_a, h_b, (w_one, w_two, w_three), (gain_one, shift_one, gain_two, shift_two))
        corr_part = jnp.dot(embed_t, embed_pair[1], preferred_element_type=F32)
        grad_scaled, loss_cols = corr_grad(corr_part.astype(BF16), lam_off, total_rows, 3)
        grad_embed_a = lax.dot_general(embed_pair[1], grad_scaled, (((1,), (1,)), ((), ())),
                                       preferred_element_type=F32)
        grad_embed_b = jnp.dot(embed_pair[0], grad_scaled, preferred_element_type=F32)
        grad_embed = jnp.concatenate([grad_embed_a, grad_embed_b])
        products = grad_embed.reshape(2, rows_dev, -1)
        embed_sums = jnp.concatenate(
            [jnp.sum(products, axis=1), jnp.sum(products * embed_pair.astype(F32), axis=1), loss_cols])
        flat = lambda values: values.reshape(2 * rows_dev, -1)
        grad_w_three, grad_w_two, grad_w_one, total_three, total_two, total_one = backward(
            total_rows, 62 * 2**20, embed_sums, grad_embed, flat(embed_pair), flat(norm_two), flat(norm_one),
            flat(act_two), flat(act_one), act_two_t, act_one_t, feat_t, w_three, w_two,
            scale_three, scale_two, scale_one)
        loss_total = jnp.sum(total_three[4])
        both = lambda total, row: (total[:, row] + total[:, row + 1]).reshape(-1)
        return (loss_total, grad_w_one, grad_w_two, grad_w_three,
                both(total_one, 2), both(total_one, 0), both(total_two, 2), both(total_two, 0))

    row_spec = P("data", None)
    whole_mat = P(None, None)
    whole_vec = P(None)
    return jax.shard_map(
        local_step, mesh=mesh,
        in_specs=(row_spec, row_spec, whole_mat, whole_mat, whole_mat,
                  whole_vec, whole_vec, whole_vec, whole_vec, P()),
        out_specs=(P(), row_spec, row_spec, row_spec, whole_vec, whole_vec, whole_vec, whole_vec),
        check_vma=False)
```

```python
import functools

import jax
import jax.numpy as jnp
from jax import lax
from jax.experimental import pallas as pl
from jax.experimental.pallas import tpu as pltpu
from jax.sharding import PartitionSpec as P

NORM_EPS = 1e-5
MESH = pl.DeviceIdType.MESH
F32 = jnp.float32
BF16 = jnp.bfloat16


ALL = slice(None)
PAIR = range(2)
OTHERS = range(3)
LINE = 4
DEPTH_DIMS = (((0,), (0,)), ((), ()))
LANE_DIMS = (((1,), (1,)), ((), ()))
DMA_SEM = pltpu.SemaphoreType.DMA


def loop(count):
    return pl.loop(0, count)


def col_sum(values):
    return jnp.sum(values, axis=0, keepdims=True)


class Place:
    def __init__(self):
        me = lax.axis_index("data")
        self.core = lax.rem(me, 2)
        self.x = lax.rem(lax.div(me, 2), 2)
        self.y = lax.rem(lax.div(me, 4), 2)
        self.z = lax.div(me, 8)
        self.plane = lax.rem(lax.div(me, 2), 4)
        self.partner = me + 1 - 2 * self.core
        self.x_peer = me + 2 - 4 * self.x
        self.y_peer = me + 4 - 8 * self.y
        step, low = 8, lax.rem(me, 8)
        self.z_peers = [lax.rem(self.z + d + 1, LINE) * step + low for d in OTHERS]
        self.plane_peers = [self.z * step + lax.rem(self.plane + d + 1, LINE) * 2 + self.core for d in OTHERS]
        self.near = [self.partner] + self.plane_peers + self.z_peers


def enter(peers):
    barrier = pltpu.get_barrier_semaphore()
    for peer in peers:
        pl.semaphore_signal(barrier, inc=1, device_id=(peer,), device_id_type=MESH)
    pl.semaphore_wait(barrier, len(peers))


def remote(src, dst, send_sem, recv_sem, peer):
    return pltpu.make_async_remote_copy(
        src_ref=src, dst_ref=dst, send_sem=send_sem, recv_sem=recv_sem,
        device_id=(peer,), device_id_type=MESH)


class Sums:
    def __init__(self, at, local, total, recv0, slots1, slots2, send_sem, recv_sem):
        self.at, self.refs = at, (local, total)
        self.recv0, self.slots1, self.slots2 = recv0, slots1, slots2
        self.send_sem, self.recv_sem = send_sem, recv_sem
        self.half = recv0.shape[-1]
        self.mine = pl.multiple_of(at.core * self.half, 128)
        self.theirs = pl.multiple_of((1 - at.core) * self.half, 128)

    def pick(self, k, first):
        ref, index = self.refs[k]
        return ref.at[(*index, ALL, pl.ds(first, self.half))]

    def copies(self, stage):
        at = self.at
        if stage == 0:
            pairs = [(0, self.pick(0, self.theirs), self.recv0, at.partner)]
        elif stage == 1:
            here = self.slots1.at[at.plane]
            pairs = [(1 + d, here, here, at.plane_peers[d]) for d in OTHERS]
        elif stage == 2:
            here = self.slots2.at[at.z]
            pairs = [(4 + d, here, here, at.z_peers[d]) for d in OTHERS]
        else:
            here = self.pick(1, self.mine)
            pairs = [(7, here, here, at.partner)]
        return [remote(src, dst, self.send_sem.at[k], self.recv_sem.at[k], peer) for k, src, dst, peer in pairs]

    def send(self, stage):
        for copy in self.copies(stage):
            copy.start()

    def arrive(self, stage=3):
        for copy in self.copies(stage):
            copy.wait()

    def begin(self):
        self.send(0)

    def over_plane(self):
        self.arrive(0)
        self.slots1[self.at.plane] = self.pick(0, self.mine)[...] + self.recv0[...]
        self.send(1)

    def over_line(self):
        self.arrive(1)
        self.slots2[self.at.z] = (self.slots1[0] + self.slots1[1]) + (self.slots1[2] + self.slots1[3])
        self.send(2)

    def over_pair(self):
        self.arrive(2)
        self.pick(1, self.mine)[...] = (self.slots2[0] + self.slots2[1]) + (self.slots2[2] + self.slots2[3])
        self.send(3)


def sums_scratch(rows, cols):
    return [
        pltpu.VMEM((rows, cols // 2), F32),
        pltpu.VMEM((4, rows, cols // 2), F32),
        pltpu.VMEM((4, rows, cols // 2), F32),
        DMA_SEM((8,)),
        DMA_SEM((8,)),
    ]


class Ring:
    def __init__(self, at, total, part, recv0, kept, snd1, recv1, snd2, recv2, snd3, recv3, send_sem, recv_sem, credit):
        self.at, self.total, self.slots = at, total, kept.shape[0]
        self.part, self.recv0, self.kept = part, recv0, kept
        self.snd1, self.recv1, self.snd2, self.recv2, self.snd3, self.recv3 = snd1, recv1, snd2, recv2, snd3, recv3
        self.send_sem, self.recv_sem, self.credit = send_sem, recv_sem, credit
        self.half = snd1.shape[-1]
        self.copies = {}
        self.peers = [at.partner, at.x_peer, at.y_peer, at.y_peer, at.x_peer] + at.z_peers
        self.givers = self.peers[:5] + at.z_peers[::-1]
        self.own = [at.y, at.x]

    def cols(self, half):
        return pl.ds(half * self.half, self.half)

    def depth(self, stage):
        return self.slots if stage else self.part.shape[0]

    def start(self, q, stage, src, dst, peer):
        copy = remote(src, dst, self.send_sem.at[q % self.slots, stage], self.recv_sem.at[q % self.slots, stage], peer)
        copy.start()
        self.copies[q, stage] = copy

    def send(self, q, stage, src, dst):
        depth = self.depth(stage)
        if q >= depth:
            pl.semaphore_wait(self.credit.at[q % depth, stage], 1)
        self.start(q, stage, src, dst, self.peers[stage])

    def give(self, q, stage):
        depth = self.depth(stage)
        if q + depth < self.total:
            pl.semaphore_signal(self.credit.at[q % depth, stage], inc=1, device_id=(self.givers[stage],),
                                device_id_type=MESH)

    def wait(self, q, stage):
        self.copies.pop((q, stage)).wait()

    def pair(self, q):
        s = q % self.depth(0)
        self.send(q, 0, self.part.at[s, :, :, :, 1 - self.at.core], self.recv0.at[s])

    def first(self, q):
        at, s, j = self.at, q % self.depth(0), q % self.slots
        self.wait(q, 0)

        @loop(LINE)
        def _(z):
            for half in PAIR:
                cols = self.cols(half)
                for k in PAIR:
                    (y, x), (oy, ox) = ((at.y, k), (1 - at.y, k)) if half else ((k, at.x), (k, 1 - at.x))
                    self.snd1[j, half, z, k] = (
                        self.part[s, z, oy, ox, at.core, :, cols] + self.recv0[s, z, oy, ox, :, cols]).astype(BF16)
                    self.kept[j, half, z, k] = self.part[s, z, y, x, at.core, :, cols] + self.recv0[s, z, y, x, :, cols]

        self.give(q, 0)
        for half in PAIR:
            self.send(q, 1 + half, self.snd1.at[j, half], self.recv1.at[j, half])

    def second(self, q):
        j = q % self.slots
        for half in PAIR:
            own = self.own[half]
            self.wait(q, 1 + half)

            @loop(LINE)
            def _(z):
                self.snd2[j, half, z] = (
                    self.kept[j, half, z, 1 - own] + self.recv1[j, half, z, 1 - own].astype(F32)).astype(BF16)
                self.kept[j, half, z, own] = self.kept[j, half, z, own] + self.recv1[j, half, z, own].astype(F32)

            self.give(q, 1 + half)
            self.send(q, 3 + half, self.snd2.at[j, half], self.recv2.at[j, half])

    def summed(self, j, half, z):
        return self.kept[j, half, z, self.own[half]] + self.recv2[j, half, z].astype(F32)

    def third(self, q):
        j = q % self.slots
        for half in PAIR:
            self.wait(q, 3 + half)
        for d in OTHERS:
            z = lax.rem(self.at.z + d + 1, 4)
            for half in PAIR:
                self.snd3[j, d, :, self.cols(half)] = self.summed(j, half, z).astype(BF16)
            self.send(q, 5 + d, self.snd3.at[j, d], self.recv3.at[j, d])

    def last(self, q):
        j = q % self.slots
        totals = [self.summed(j, half, self.at.z) for half in PAIR]
        for d in OTHERS:
            self.wait(q, 5 + d)
            totals = [total + self.recv3[j, d, :, self.cols(half)].astype(F32) for half, total in enumerate(totals)]
            self.give(q, 5 + d)
        for half in PAIR:
            self.give(q, 3 + half)
        return totals


def ring_scratch(slots, rows, width):
    half = width // 2
    return [
        pltpu.VMEM((2, 4, 2, 2, 2, rows, width), F32),
        pltpu.VMEM((2, 4, 2, 2, rows, width), F32),
        pltpu.VMEM((slots, 2, 4, 2, rows, half), F32),
    ] + [pltpu.VMEM((slots, 2, 4, 2, rows, half), BF16)] * 2 + [pltpu.VMEM((slots, 2, 4, rows, half), BF16)] * 2 + [
        pltpu.VMEM((slots, 3, rows, width), BF16)] * 2 + [DMA_SEM((slots, 16))] * 2 + [
        pltpu.SemaphoreType.REGULAR((slots, 8))]


CHUNKS = 8
RING = 12
SUMS = 5
SPREAD_LAGS = (1, 2, 3, 4, 6, 7, 8, 9)
RING_LAGS = (1, 3, 5, 8)
INPUT_STEPS = (((0, 1), (2,)), ((3,), (4,)), ((5,), (6,)), ((7,), ()), ((), ()))


def backward_kernel(
        total_rows, lam_ref, embed, norm_two, norm_one, act_two, act_one, act_two_t, act_one_t, feat_t, w_three, w_two,
        scale_three, scale_two, scale_one,
        grad_w_three, grad_w_two, grad_w_one, total_three, total_two, total_one,
        grad, pre, wide, weight, normed, act, local, embed_local, w_sem, load_sem, *scratch):
    at = Place()
    ring = Ring(at, 4 * CHUNKS, *scratch[:RING])
    rows_dev, dim = grad.shape
    width = dim // CHUNKS
    view_rows = rows_dev // 2
    block_rows = min(64, view_rows)
    quarter = dim // 4
    count = 1.0 / total_rows
    feeds = [act_two_t, act_one_t, feat_t]
    masks = [act_two, act_one]
    weights = [w_three, w_two]
    scales = [scale_three, scale_two, scale_one]
    outs = [grad_w_three, grad_w_two, grad_w_one]
    totals = [total_three, total_two, total_one]
    sets = [scratch[k:k + SUMS] for k in range(RING, len(scratch), SUMS)]
    sums = [[Sums(at, (embed_local, ()), (total_three, ()), *sets[0])]]
    for layer in PAIR:
        sums.append([Sums(at, (local, (layer, h)), (totals[layer + 1], (h,)), *sets.pop()) for h in PAIR])

    def load(src, dst, k):
        copy = pltpu.make_async_copy(src, dst, load_sem.at[k])
        copy.start()
        return copy

    views = [pl.ds(v * view_rows, view_rows) for v in PAIR]
    embeds = [load(embed.at[views[v]], normed.at[0, views[v]], v) for v in PAIR]
    loads = {("norm", 0): load(norm_two, normed.at[1], 2), ("act", 0): load(act_two, act, 3)}
    slots = weight.shape[0]
    w_loads = {}

    def load_weight(layer, n):
        copy = pltpu.make_async_copy(weights[layer].at[pl.ds(n * width, width), :], weight.at[n % slots],
                                     w_sem.at[n % slots])
        copy.start()
        w_loads[layer, n] = copy

    for n in range(slots):
        load_weight(0, n)
    enter(at.near)
    for copy in embeds:
        copy.wait()

    lam = lam_ref[0]
    place = (at.z, at.y, at.x, at.core)
    first_row = (((at.z * 2 + at.y) * 2 + at.x) * 2 + at.core) * ring.snd1.shape[-2]

    def correlate(q):
        @loop(LINE)
        def _(z):
            rows = pl.ds(pl.multiple_of(z * quarter, quarter), quarter)
            out = lax.dot_general(normed[0, views[0], rows], normed[0, views[1], pl.ds(q * width, width)],
                                  DEPTH_DIMS, preferred_element_type=F32)
            ring.part[q % 2, z] = out.reshape(ring.part.shape[2:])

        ring.pair(q)

    def spread_line(q):
        for half, total in enumerate(ring.last(q)):
            corr = total * count
            start = q * width + half * ring.half
            row = first_row + lax.broadcasted_iota(jnp.int32, corr.shape, 0)
            col = start + lax.broadcasted_iota(jnp.int32, corr.shape, 1)
            gap = 1.0 - corr
            loss = jnp.where(row == col, gap * gap, lam * corr * corr)
            embed_local[4:5, pl.ds(start, ring.half)] = col_sum(loss)
            slope = jnp.where(row == col, -2.0 * gap, 2.0 * lam * corr)
            wide[(q, *place, ALL, ring.cols(half))] = (slope * count).astype(BF16)
        here = wide.at[(q, *place)]
        for d in OTHERS:
            ring.start(q, 8 + d, here, here, at.z_peers[d])

    def spread_one(q):
        for d in OTHERS:
            ring.wait(q, 8 + d)
        for half, peer in enumerate((at.y_peer, at.x_peer)):
            here = wide.at[q, :, at.y, at.x, at.core, :, ring.cols(half)]
            ring.start(q, 11 + half, here, here, peer)

    def spread_two(q):
        for half, peer in enumerate((at.x_peer, at.y_peer)):
            ring.wait(q, 11 + half)
            here = wide.at[(q, ALL, *((at.y, ALL) if half else (ALL, at.x)), at.core, ALL,
                            ring.cols(half))]
            ring.start(q, 13 + half, here, here, peer)

    def spread_pair(q):
        for half in PAIR:
            ring.wait(q, 13 + half)
        here = wide.at[q, :, :, :, at.core]
        ring.start(q, 15, here, here, at.partner)

    def embed_grad(q):
        ring.wait(q, 15)
        cols = pl.ds(q * width, width)
        out = jnp.dot(normed[0, views[0]], wide[q].reshape(dim, width), preferred_element_type=F32)
        pre[views[1], cols] = out
        embed_local[1:2, cols] = col_sum(out)
        embed_local[3:4, cols] = col_sum(out * normed[0, views[1], cols].astype(F32))

        @loop(LINE)
        def _(z):
            into = pl.ds(pl.multiple_of(z * quarter, quarter), quarter)
            out = lax.dot_general(normed[0, views[1], cols], wide[q, z].reshape(quarter, width), LANE_DIMS,
                                  preferred_element_type=F32)
            pre[views[0], into] = out if q == 0 else pre[views[0], into] + out

    steps = (ring.first, ring.second, ring.third, spread_line, spread_one, spread_two, spread_pair, embed_grad)
    for t in range(CHUNKS + SPREAD_LAGS[-1]):
        if t < CHUNKS:
            correlate(t)
        for step, lag in zip(steps, SPREAD_LAGS):
            if 0 <= t - lag < CHUNKS:
                step(t - lag)

    @loop(CHUNKS)
    def _(n):
        cols = pl.ds(pl.multiple_of(n * width, width), width)
        out = pre[views[0], cols]
        embed_local[0:1, cols] = col_sum(out)
        embed_local[2:3, cols] = col_sum(out * normed[0, views[0], cols].astype(F32))

    first_sums = sums[0][0]
    first_sums.begin()

    def load_feed(layer):
        p = layer % 2
        loads["feed", layer] = load(feeds[layer], wide.at[pl.ds(LINE * p, LINE)], LINE + p)

    load_feed(0)
    first_sums.over_plane()
    first_sums.over_line()
    first_sums.over_pair()

    def finish_grad(layer, j):
        cols = pl.ds(j * width, width)
        total, first = (total_three, j * width) if layer == 0 else (
            totals[layer].at[j // (CHUNKS // 2)], (j % (CHUNKS // 2)) * width)
        sel = pl.ds(first, width)
        for v in PAIR:
            mean0 = total[v:v + 1, sel] * count
            mean1 = total[2 + v:3 + v, sel] * count
            scale = scales[layer][v:v + 1, cols]

            @loop(view_rows // block_rows)
            def _(r):
                rows = pl.ds(pl.multiple_of(v * view_rows + r * block_rows, block_rows), block_rows)
                xhat = normed[layer % 2, rows, cols].astype(F32)
                grad[rows, cols] = (scale * (pre[rows, cols] - (mean0 + xhat * mean1))).astype(BF16)

    def weight_grad(layer, j):
        cols = pl.ds(j * width, width)
        q = (layer + 1) * CHUNKS + j

        @loop(LINE)
        def _(z):
            feed = jnp.concatenate([wide[4 * (layer % 2) + k, z].reshape(quarter, width) for k in range(LINE)], axis=1)
            out = jnp.dot(feed, grad[:, cols], preferred_element_type=F32)
            ring.part[q % 2, z] = out.reshape(ring.part.shape[2:])

        ring.pair(q)

    def input_grad(layer, n):
        cols = pl.ds(n * width, width)
        w_loads[layer, n].wait()
        half = local.at[layer, n // (CHUNKS // 2)]
        sel = pl.ds((n % (CHUNKS // 2)) * width, width)

        @loop(2)
        def _(v):
            rows = pl.ds(pl.multiple_of(v * view_rows, view_rows), view_rows)
            out = lax.dot_general(grad[rows, :], weight[n % slots], LANE_DIMS,
                                  preferred_element_type=F32)
            out = jnp.where(act[rows, cols] > 0, out, 0.0)
            pre[rows, cols] = out
            half[pl.ds(v, 1), sel] = col_sum(out)
            half[pl.ds(2 + v, 1), sel] = col_sum(out * normed[(layer + 1) % 2, rows, cols].astype(F32))

        if n + slots < CHUNKS:
            load_weight(layer, n + slots)

    def serve(t):
        for step, lag in zip((ring.first, ring.second, ring.third, ring.last), RING_LAGS):
            k = t - lag
            if 0 <= k < 3 * CHUNKS:
                blocks = step(CHUNKS + k)
        if 0 <= k < 3 * CHUNKS:
            for half, block in enumerate(blocks):
                outs[k // CHUNKS][:, pl.ds((k % CHUNKS) * width + half * ring.half, ring.half)] = block

    for layer in OTHERS:
        old, new = sums[layer], sums[layer + 1] if layer < 2 else None
        old[0].arrive()
        for j in range(CHUNKS):
            if j == 3 and new:
                loads["norm", layer].wait()
                loads["act", layer].wait()
            if j < 3:
                finish_grad(layer, j)
            elif new:
                for n in INPUT_STEPS[j - 3][0]:
                    input_grad(layer, n)
            if new and j == 4:
                new[0].begin()
            if new and j == 5:
                new[0].over_line()
            if new and j == 6:
                new[1].begin()
                new[0].over_pair()
                if layer == 0:
                    loads["act", 1] = load(masks[1], act, 3)
                    for n in range(slots):
                        load_weight(1, n)
            if j == 0:
                loads["feed", layer].wait()
            weight_grad(layer, j)
            if j == 0 and new:
                load_feed(layer + 1)
            if j == 0 and layer:
                old[1].over_pair()
            if j == 2:
                finish_grad(layer, 3)
                if layer:
                    old[1].arrive()
                for k in range(CHUNKS // 2, CHUNKS):
                    finish_grad(layer, k)
                if layer == 0:
                    loads["norm", 1] = load(norm_one, normed.at[0], 0)
            if new and j > 2:
                if j == 4:
                    new[0].over_plane()
                for n in INPUT_STEPS[j - 3][1]:
                    input_grad(layer, n)
                if j == 6:
                    new[1].over_plane()
                if j == 7:
                    new[1].over_line()
            serve(layer * CHUNKS + j)
    for k in range(RING_LAGS[-1]):
        serve(3 * CHUNKS + k)


def backward(total_rows, vmem, lam, *args):
    rows, dim = args[0].shape
    width, blocks = dim // CHUNKS, dim // 32
    hbm = pl.BlockSpec(memory_space=pl.ANY)
    vm = pl.BlockSpec(memory_space=pltpu.VMEM)
    scratch = [
        pltpu.VMEM((rows, dim), BF16),
        pltpu.VMEM((rows, dim), F32),
        pltpu.VMEM((CHUNKS, 4, 2, 2, 2, blocks, width), BF16),
        pltpu.VMEM((3, width, dim), BF16),
        pltpu.VMEM((2, rows, dim), BF16),
        pltpu.VMEM((rows, dim), BF16),
        pltpu.VMEM((2, 2, 4, dim // 2), F32),
        pltpu.VMEM((5, dim), F32),
        DMA_SEM((3,)),
        DMA_SEM((6,)),
    ] + ring_scratch(CHUNKS, blocks, width) + sums_scratch(5, dim)
    for _ in range(LINE):
        scratch += sums_scratch(4, dim // 2)
    halves = jax.ShapeDtypeStruct((2, 4, dim // 2), F32)
    return pl.pallas_call(
        functools.partial(backward_kernel, total_rows),
        out_shape=[jax.ShapeDtypeStruct((blocks, dim), F32)] * 3 + [jax.ShapeDtypeStruct((5, dim), F32), halves, halves],
        in_specs=[pl.BlockSpec(memory_space=pltpu.SMEM)] + [hbm] * 10 + [vm] * 3,
        out_specs=[vm] * 6,
        scratch_shapes=scratch,
        compiler_params=pltpu.CompilerParams(collective_id=1, has_side_effects=True, vmem_limit_bytes=vmem),
    )(lam.reshape(1), *args)


def forward_kernel(
        total_rows, feat_a, feat_b, w_one, w_two, w_three, gain_one, shift_one, gain_two, shift_two,
        act_one, act_two, norm_one, norm_two, embed, feat_t, act_one_t, act_two_t, scale_one, scale_two, scale_three,
        acts, hidden, normed, turned, weight, local, total, w_sem, in_sem, out_sem, *scratch):
    at = Place()
    view_rows, dim = acts.shape[2:]
    width = dim // CHUNKS
    quarter = dim // 4
    block_rows = min(64, view_rows)
    weights = [w_one, w_two, w_three]
    gains, shifts = [gain_one, gain_two], [shift_one, shift_two]
    scales = [scale_one, scale_two, scale_three]
    natural, normals, turns = [act_one, act_two, embed], [norm_one, norm_two], [feat_t, act_one_t, act_two_t]
    sets = [scratch[k:k + SUMS] for k in range(0, len(scratch), SUMS)]
    sums = [[Sums(at, (local, (layer, v)), (total, (layer, v)), *sets.pop()) for v in PAIR] for layer in OTHERS]

    ins = [pltpu.make_async_copy((feat_a, feat_b)[v], acts.at[0, v], in_sem.at[v]) for v in PAIR]

    def weight_copy(layer, k):
        cols = pl.ds(k * quarter, quarter)
        return pltpu.make_async_copy(weights[layer].at[:, cols], weight.at[layer % 2, :, cols], w_sem.at[layer % 2, k])

    def load_weight(layer, k):
        weight_copy(layer, k).start()

    ins[0].start()
    load_weight(0, 0)
    ins[1].start()
    for k in range(1, 4):
        load_weight(0, k)
    for k in range(LINE):
        load_weight(1, k)
    outs = {}

    def put(name, v, src, dst, k):
        copy = pltpu.make_async_copy(src, dst, out_sem.at[k, v])
        copy.start()
        outs[name, v] = copy

    def drain(name, v):
        outs.pop((name, v)).wait()

    def matmul(layer, v, hooks=()):
        hooks = list(hooks)
        if v == 0:
            hooks += [(2 * k, lambda k=k: weight_copy(layer, k).wait()) for k in range(LINE)]

        @loop(CHUNKS)
        def _(n):
            for k, step in hooks:
                pl.when(n == k)(step)
            cols = pl.ds(pl.multiple_of(n * width, width), width)
            out = jnp.dot(acts[layer % 2, v], weight[layer % 2, :, cols], preferred_element_type=F32)
            hidden[v, :, cols] = out
            local[layer, v, 0:1, cols] = col_sum(out)
            local[layer, v, 1:2, cols] = col_sum(out * out)

    def normalise(layer, v):
        mean = total[layer, v, 0:1, :] / total_rows
        inv = lax.rsqrt(total[layer, v, 1:2, :] / total_rows - mean * mean + NORM_EPS)
        if layer < 2:
            scales[layer][v:v + 1, :] = gains[layer][...] * inv
        else:
            scales[layer][v:v + 1, :] = inv
        local[layer, v, 0:1, :] = mean
        local[layer, v, 1:2, :] = inv

        @loop(CHUNKS)
        def _(n):
            cols = pl.ds(pl.multiple_of(n * width, width), width)
            mean, inv = local[layer, v, 0:1, cols], local[layer, v, 1:2, cols]
            if layer < 2:
                gain, shift = gains[layer][:, cols], shifts[layer][:, cols]

            @loop(view_rows // block_rows)
            def _(r):
                rows = pl.ds(pl.multiple_of(r * block_rows, block_rows), block_rows)
                value = (hidden[v, rows, cols] - mean) * inv
                if layer < 2:
                    normed[v, rows, cols] = value.astype(BF16)
                    value = jnp.maximum(gain * value + shift, 0.0)
                acts[(layer + 1) % 2, v, rows, cols] = value.astype(BF16)

        put(("act", layer), v, acts.at[(layer + 1) % 2, v], natural[layer].at[v], layer % 2)
        if layer < 2:
            put(("norm", layer), v, normed.at[v], normals[layer].at[v], 2)

    def turn(layer, v):
        part = view_rows // 2

        @loop(CHUNKS)
        def _(n):
            cols = pl.ds(pl.multiple_of(n * width, width), width)
            for k in PAIR:
                block = acts[layer % 2, v, k * part:(k + 1) * part, cols].T
                turned[2 * v + k, lax.div(n, 2), lax.rem(n, 2)] = block.reshape(turned.shape[3:])

        span = pl.ds(2 * v, 2)
        put(("turn", layer), v, turned.at[span], turns[layer].at[span], 3)

    enter(at.near)
    ins[0].wait()
    matmul(0, 0)
    now, later = sums[0]
    now.begin()
    ins[1].wait()
    matmul(0, 1, [(2, now.over_plane), (7, now.over_line)])
    later.begin()
    turn(0, 0)
    later.over_plane()
    turn(0, 1)
    for layer in OTHERS:
        now, later = sums[layer]
        now.over_pair()
        if layer == 0:
            for k in range(LINE):
                load_weight(2, k)
        now.arrive()
        for v in PAIR:
            if layer == 1:
                drain(("norm", 0), v)
            if layer == 2:
                drain(("act", 0), v)
        normalise(layer, 0)
        if layer == 2:
            later.over_line()
            later.over_pair()
            later.arrive()
            normalise(layer, 1)
            break
        matmul(layer + 1, 0, [(0, later.over_line), (7, later.over_pair)])
        now = sums[layer + 1][0]
        now.begin()
        later.arrive()
        normalise(layer, 1)
        matmul(layer + 1, 1, [(0, now.over_plane), (6, now.over_line)])
        later = sums[layer + 1][1]
        later.begin()
        drain(("turn", layer), 0)
        turn(layer + 1, 0)
        later.over_plane()
        drain(("turn", layer), 1)
        turn(layer + 1, 1)
    for copy in outs.values():
        copy.wait()


def forward(total_rows, vmem, feat_a, feat_b, weights, vectors):
    view_rows, dim = feat_a.shape
    hbm = pl.BlockSpec(memory_space=pl.ANY)
    vm = pl.BlockSpec(memory_space=pltpu.VMEM)
    turned = jax.ShapeDtypeStruct((4, 4, 2, 2, 2, dim // 32, view_rows // 2), BF16)
    scratch = [
        pltpu.VMEM((2, 2, view_rows, dim), BF16),
        pltpu.VMEM((2, view_rows, dim), F32),
        pltpu.VMEM((2, view_rows, dim), BF16),
        pltpu.VMEM(turned.shape, BF16),
        pltpu.VMEM((2, dim, dim), BF16),
        pltpu.VMEM((3, 2, 2, dim), F32),
        pltpu.VMEM((3, 2, 2, dim), F32),
        DMA_SEM((2, 4)),
        DMA_SEM((2,)),
        DMA_SEM((4, 2)),
    ]
    for _ in range(6):
        scratch += sums_scratch(2, dim)
    pair = jax.ShapeDtypeStruct((2, view_rows, dim), BF16)
    vector = jax.ShapeDtypeStruct((2, dim), F32)
    return pl.pallas_call(
        functools.partial(forward_kernel, total_rows),
        out_shape=[pair] * 5 + [turned] * 3 + [vector] * 3,
        in_specs=[hbm] * 5 + [vm] * 4,
        out_specs=[hbm] * 8 + [vm] * 3,
        scratch_shapes=scratch,
        compiler_params=pltpu.CompilerParams(collective_id=0, has_side_effects=True, vmem_limit_bytes=vmem),
    )(feat_a, feat_b, *weights, *[value.reshape(1, dim) for value in vectors])


def solution(mesh):
    shards = mesh.shape["data"]

    def local_step(h_a, h_b, w_one, w_two, w_three, gain_one, shift_one, gain_two, shift_two, lam_off):
        rows_dev = h_a.shape[0]
        total_rows = rows_dev * shards
        (act_one, act_two, norm_one, norm_two, embed, feat_t, act_one_t, act_two_t, scale_one, scale_two, scale_three) = forward(
            total_rows, 56 * 2**20, h_a, h_b, (w_one, w_two, w_three), (gain_one, shift_one, gain_two, shift_two))
        flat = lambda values: values.reshape(2 * rows_dev, -1)
        grad_w_three, grad_w_two, grad_w_one, total_three, total_two, total_one = backward(
            total_rows, 62 * 2**20, lam_off, flat(embed), flat(norm_two), flat(norm_one), flat(act_two), flat(act_one),
            act_two_t, act_one_t, feat_t, w_three, w_two, scale_three, scale_two, scale_one)
        loss_total = jnp.sum(total_three[4])
        both = lambda total, row: (total[:, row] + total[:, row + 1]).reshape(-1)
        return (loss_total, grad_w_one, grad_w_two, grad_w_three,
                both(total_one, 2), both(total_one, 0), both(total_two, 2), both(total_two, 0))

    row_spec = P("data", None)
    whole_mat = P(None, None)
    whole_vec = P(None)
    return jax.shard_map(
        local_step, mesh=mesh,
        in_specs=(row_spec, row_spec, whole_mat, whole_mat, whole_mat,
                  whole_vec, whole_vec, whole_vec, whole_vec, P()),
        out_specs=(P(), row_spec, row_spec, row_spec, whole_vec, whole_vec, whole_vec, whole_vec),
        check_vma=False)
```

```python
import functools

import jax
import jax.numpy as jnp
from jax import lax
from jax.experimental import pallas as pl
from jax.experimental.pallas import tpu as pltpu
from jax.sharding import PartitionSpec as P

NORM_EPS = 1e-5
MESH = pl.DeviceIdType.MESH
F32 = jnp.float32
BF16 = jnp.bfloat16


ALL = slice(None)
PAIR = range(2)
OTHERS = range(3)
LINE = 4
CUBE = 8
DEPTH_DIMS = (((0,), (0,)), ((), ()))
LANE_DIMS = (((1,), (1,)), ((), ()))
DMA_SEM = pltpu.SemaphoreType.DMA


def loop(count):
    return pl.loop(0, count)


def col_sum(values):
    return jnp.sum(values, axis=0, keepdims=True)


class Place:
    def __init__(self):
        me = lax.axis_index("data")
        self.core = lax.rem(me, 2)
        self.x = lax.rem(lax.div(me, 2), 2)
        self.y = lax.rem(lax.div(me, 4), 2)
        self.z = lax.div(me, 8)
        self.plane = lax.rem(lax.div(me, 2), 4)
        self.partner = me + 1 - 2 * self.core
        self.x_peer = me + 2 - 4 * self.x
        self.y_peer = me + 4 - 8 * self.y
        self.low = lax.rem(me, CUBE)
        self.z_peers = [lax.rem(self.z + d + 1, LINE) * CUBE + self.low for d in OTHERS]
        self.plane_peers = [self.z * CUBE + lax.rem(self.plane + d + 1, LINE) * 2 + self.core for d in OTHERS]
        self.cube_peers = [self.z * CUBE + lax.rem(self.low + d + 1, CUBE) for d in range(CUBE - 1)]
        self.near = [self.partner] + self.plane_peers + self.z_peers


def enter(peers):
    barrier = pltpu.get_barrier_semaphore()
    for peer in peers:
        pl.semaphore_signal(barrier, inc=1, device_id=(peer,), device_id_type=MESH)
    pl.semaphore_wait(barrier, len(peers))


def remote(src, dst, send_sem, recv_sem, peer):
    return pltpu.make_async_remote_copy(
        src_ref=src, dst_ref=dst, send_sem=send_sem, recv_sem=recv_sem,
        device_id=(peer,), device_id_type=MESH)


class Sums:
    def __init__(self, at, local, total, recv0, slots1, slots2, send_sem, recv_sem):
        self.at, self.refs = at, (local, total)
        self.recv0, self.slots1, self.slots2 = recv0, slots1, slots2
        self.send_sem, self.recv_sem = send_sem, recv_sem
        self.half = recv0.shape[-1]
        self.mine = pl.multiple_of(at.core * self.half, 128)
        self.theirs = pl.multiple_of((1 - at.core) * self.half, 128)

    def pick(self, k, first):
        ref, index = self.refs[k]
        return ref.at[(*index, ALL, pl.ds(first, self.half))]

    def copies(self, stage):
        at = self.at
        if stage == 0:
            pairs = [(0, self.pick(0, self.theirs), self.recv0, at.partner)]
        elif stage == 1:
            here = self.slots1.at[at.plane]
            pairs = [(1 + d, here, here, at.plane_peers[d]) for d in OTHERS]
        elif stage == 2:
            here = self.slots2.at[at.z]
            pairs = [(4 + d, here, here, at.z_peers[d]) for d in OTHERS]
        else:
            here = self.pick(1, self.mine)
            pairs = [(7, here, here, at.partner)]
        return [remote(src, dst, self.send_sem.at[k], self.recv_sem.at[k], peer) for k, src, dst, peer in pairs]

    def send(self, stage):
        for copy in self.copies(stage):
            copy.start()

    def arrive(self, stage=3):
        for copy in self.copies(stage):
            copy.wait()

    def begin(self):
        self.send(0)

    def over_plane(self):
        self.arrive(0)
        self.slots1[self.at.plane] = self.pick(0, self.mine)[...] + self.recv0[...]
        self.send(1)

    def over_line(self):
        self.arrive(1)
        self.slots2[self.at.z] = (self.slots1[0] + self.slots1[1]) + (self.slots1[2] + self.slots1[3])
        self.send(2)

    def over_pair(self):
        self.arrive(2)
        self.pick(1, self.mine)[...] = (self.slots2[0] + self.slots2[1]) + (self.slots2[2] + self.slots2[3])
        self.send(3)


class QuickSums:
    def __init__(self, at, local, total, slots1, slots2, send_sem, recv_sem):
        self.at, self.local, self.total = at, local, total
        self.slots1, self.slots2 = slots1, slots2
        self.send_sem, self.recv_sem = send_sem, recv_sem

    def copies(self, across):
        at = self.at
        if across:
            here, peers, first = self.slots2.at[at.low], at.cube_peers, len(at.z_peers)
        else:
            here, peers, first = self.slots1.at[at.z], at.z_peers, 0
        return [remote(here, here, self.send_sem.at[first + d], self.recv_sem.at[first + d], peer)
                for d, peer in enumerate(peers)]

    def begin(self):
        ref, index = self.local
        self.slots1[self.at.z] = ref[index]
        for copy in self.copies(False):
            copy.start()

    def over_plane(self):
        for copy in self.copies(False):
            copy.wait()
        parts = [self.slots1[k] for k in range(LINE)]
        self.slots2[self.at.low] = (parts[0] + parts[1]) + (parts[2] + parts[3])
        for copy in self.copies(True):
            copy.start()

    def arrive(self):
        for copy in self.copies(True):
            copy.wait()
        parts = [self.slots2[k] for k in range(CUBE)]
        while len(parts) > 1:
            parts = [a + b for a, b in zip(parts[::2], parts[1::2])]
        ref, index = self.total
        ref[index] = parts[0]


def quick_scratch(rows, cols):
    return [
        pltpu.VMEM((LINE, rows, cols), F32),
        pltpu.VMEM((CUBE, rows, cols), F32),
        DMA_SEM((LINE + CUBE,)),
        DMA_SEM((LINE + CUBE,)),
    ]


def sums_scratch(rows, cols):
    return [
        pltpu.VMEM((rows, cols // 2), F32),
        pltpu.VMEM((4, rows, cols // 2), F32),
        pltpu.VMEM((4, rows, cols // 2), F32),
        DMA_SEM((8,)),
        DMA_SEM((8,)),
    ]


class Ring:
    def __init__(self, at, total, part, recv0, kept, snd1, recv1, snd2, recv2, snd3, recv3, send_sem, recv_sem, credit):
        self.at, self.total, self.slots = at, total, kept.shape[0]
        self.part, self.recv0, self.kept = part, recv0, kept
        self.snd1, self.recv1, self.snd2, self.recv2, self.snd3, self.recv3 = snd1, recv1, snd2, recv2, snd3, recv3
        self.send_sem, self.recv_sem, self.credit = send_sem, recv_sem, credit
        self.half = snd1.shape[-1]
        self.copies = {}
        self.peers = [at.partner, at.x_peer, at.y_peer, at.y_peer, at.x_peer] + at.z_peers
        self.givers = self.peers[:5] + at.z_peers[::-1]
        self.own = [at.y, at.x]

    def cols(self, half):
        return pl.ds(half * self.half, self.half)

    def depth(self, stage):
        return self.slots if stage else self.part.shape[0]

    def start(self, q, stage, src, dst, peer):
        copy = remote(src, dst, self.send_sem.at[q % self.slots, stage], self.recv_sem.at[q % self.slots, stage], peer)
        copy.start()
        self.copies[q, stage] = copy

    def send(self, q, stage, src, dst):
        depth = self.depth(stage)
        if q >= depth:
            pl.semaphore_wait(self.credit.at[q % depth, stage], 1)
        self.start(q, stage, src, dst, self.peers[stage])

    def give(self, q, stage):
        depth = self.depth(stage)
        if q + depth < self.total:
            pl.semaphore_signal(self.credit.at[q % depth, stage], inc=1, device_id=(self.givers[stage],),
                                device_id_type=MESH)

    def wait(self, q, stage):
        self.copies.pop((q, stage)).wait()

    def pair(self, q):
        s = q % self.depth(0)
        self.send(q, 0, self.part.at[s, :, :, :, 1 - self.at.core], self.recv0.at[s])

    def first(self, q):
        at, s, j = self.at, q % self.depth(0), q % self.slots
        self.wait(q, 0)

        @loop(LINE)
        def _(z):
            for half in PAIR:
                cols = self.cols(half)
                for k in PAIR:
                    (y, x), (oy, ox) = ((at.y, k), (1 - at.y, k)) if half else ((k, at.x), (k, 1 - at.x))
                    self.snd1[j, half, z, k] = (
                        self.part[s, z, oy, ox, at.core, :, cols] + self.recv0[s, z, oy, ox, :, cols]).astype(BF16)
                    self.kept[j, half, z, k] = self.part[s, z, y, x, at.core, :, cols] + self.recv0[s, z, y, x, :, cols]

        self.give(q, 0)
        for half in PAIR:
            self.send(q, 1 + half, self.snd1.at[j, half], self.recv1.at[j, half])

    def second(self, q):
        j = q % self.slots
        for half in PAIR:
            own = self.own[half]
            self.wait(q, 1 + half)

            @loop(LINE)
            def _(z):
                self.snd2[j, half, z] = (
                    self.kept[j, half, z, 1 - own] + self.recv1[j, half, z, 1 - own].astype(F32)).astype(BF16)
                self.kept[j, half, z, own] = self.kept[j, half, z, own] + self.recv1[j, half, z, own].astype(F32)

            self.give(q, 1 + half)
            self.send(q, 3 + half, self.snd2.at[j, half], self.recv2.at[j, half])

    def summed(self, j, half, z):
        return self.kept[j, half, z, self.own[half]] + self.recv2[j, half, z].astype(F32)

    def third(self, q):
        j = q % self.slots
        for half in PAIR:
            self.wait(q, 3 + half)
        for d in OTHERS:
            z = lax.rem(self.at.z + d + 1, 4)
            for half in PAIR:
                self.snd3[j, d, :, self.cols(half)] = self.summed(j, half, z).astype(BF16)
            self.send(q, 5 + d, self.snd3.at[j, d], self.recv3.at[j, d])

    def last(self, q):
        j = q % self.slots
        totals = [self.summed(j, half, self.at.z) for half in PAIR]
        for d in OTHERS:
            self.wait(q, 5 + d)
            totals = [total + self.recv3[j, d, :, self.cols(half)].astype(F32) for half, total in enumerate(totals)]
            self.give(q, 5 + d)
        for half in PAIR:
            self.give(q, 3 + half)
        return totals


def ring_scratch(slots, rows, width):
    half = width // 2
    return [
        pltpu.VMEM((2, 4, 2, 2, 2, rows, width), F32),
        pltpu.VMEM((2, 4, 2, 2, rows, width), F32),
        pltpu.VMEM((slots, 2, 4, 2, rows, half), F32),
    ] + [pltpu.VMEM((slots, 2, 4, 2, rows, half), BF16)] * 2 + [pltpu.VMEM((slots, 2, 4, rows, half), BF16)] * 2 + [
        pltpu.VMEM((slots, 3, rows, width), BF16)] * 2 + [DMA_SEM((slots, 16))] * 2 + [
        pltpu.SemaphoreType.REGULAR((slots, 8))]


CHUNKS = 8
RING = 12
SUMS = 5
QUICK = 4
SPREAD_LAGS = (1, 2, 3, 4, 6, 7, 8, 9)
RING_LAGS = (1, 3, 5, 8)
INPUT_STEPS = (((0, 1), (2,)), ((3,), (4,)), ((5,), (6,)), ((7,), ()), ((), ()))


def backward_kernel(
        total_rows, lam_ref, embed, norm_two, norm_one, act_two, act_one, act_two_t, act_one_t, feat_t, w_three, w_two,
        scale_three, scale_two, scale_one,
        grad_w_three, grad_w_two, grad_w_one, total_three, total_two, total_one,
        grad, pre, wide, weight, normed, act, local, embed_local, w_sem, load_sem, *scratch):
    at = Place()
    ring = Ring(at, 4 * CHUNKS, *scratch[:RING])
    rows_dev, dim = grad.shape
    width = dim // CHUNKS
    view_rows = rows_dev // 2
    block_rows = min(64, view_rows)
    quarter = dim // 4
    count = 1.0 / total_rows
    feeds = [act_two_t, act_one_t, feat_t]
    masks = [act_two, act_one]
    weights = [w_three, w_two]
    scales = [scale_three, scale_two, scale_one]
    outs = [grad_w_three, grad_w_two, grad_w_one]
    totals = [total_three, total_two, total_one]
    sets = [scratch[k:k + SUMS] for k in range(RING, len(scratch), SUMS)]
    sums = [[Sums(at, (embed_local, ()), (total_three, ()), *sets[0])]]
    for layer in PAIR:
        sums.append([Sums(at, (local, (layer, h)), (totals[layer + 1], (h,)), *sets.pop()) for h in PAIR])

    def load(src, dst, k):
        copy = pltpu.make_async_copy(src, dst, load_sem.at[k])
        copy.start()
        return copy

    views = [pl.ds(v * view_rows, view_rows) for v in PAIR]
    embeds = [load(embed.at[views[v]], normed.at[0, views[v]], v) for v in PAIR]
    loads = {("norm", 0): load(norm_two, normed.at[1], 2), ("act", 0): load(act_two, act, 3)}
    slots = weight.shape[0]
    w_loads = {}

    def load_weight(layer, n):
        copy = pltpu.make_async_copy(weights[layer].at[pl.ds(n * width, width), :], weight.at[n % slots],
                                     w_sem.at[n % slots])
        copy.start()
        w_loads[layer, n] = copy

    for n in range(slots):
        load_weight(0, n)
    enter(at.near)
    for copy in embeds:
        copy.wait()

    lam = lam_ref[0]
    place = (at.z, at.y, at.x, at.core)
    first_row = (((at.z * 2 + at.y) * 2 + at.x) * 2 + at.core) * ring.snd1.shape[-2]

    def correlate(q):
        @loop(LINE)
        def _(z):
            rows = pl.ds(pl.multiple_of(z * quarter, quarter), quarter)
            out = lax.dot_general(normed[0, views[0], rows], normed[0, views[1], pl.ds(q * width, width)],
                                  DEPTH_DIMS, preferred_element_type=F32)
            ring.part[q % 2, z] = out.reshape(ring.part.shape[2:])

        ring.pair(q)

    def spread_line(q):
        for half, total in enumerate(ring.last(q)):
            corr = total * count
            start = q * width + half * ring.half
            row = first_row + lax.broadcasted_iota(jnp.int32, corr.shape, 0)
            col = start + lax.broadcasted_iota(jnp.int32, corr.shape, 1)
            gap = 1.0 - corr
            loss = jnp.where(row == col, gap * gap, lam * corr * corr)
            embed_local[4:5, pl.ds(start, ring.half)] = col_sum(loss)
            slope = jnp.where(row == col, -2.0 * gap, 2.0 * lam * corr)
            wide[(q, *place, ALL, ring.cols(half))] = (slope * count).astype(BF16)
        here = wide.at[(q, *place)]
        for d in OTHERS:
            ring.start(q, 8 + d, here, here, at.z_peers[d])

    def spread_one(q):
        for d in OTHERS:
            ring.wait(q, 8 + d)
        for half, peer in enumerate((at.y_peer, at.x_peer)):
            here = wide.at[q, :, at.y, at.x, at.core, :, ring.cols(half)]
            ring.start(q, 11 + half, here, here, peer)

    def spread_two(q):
        for half, peer in enumerate((at.x_peer, at.y_peer)):
            ring.wait(q, 11 + half)
            here = wide.at[(q, ALL, *((at.y, ALL) if half else (ALL, at.x)), at.core, ALL,
                            ring.cols(half))]
            ring.start(q, 13 + half, here, here, peer)

    def spread_pair(q):
        for half in PAIR:
            ring.wait(q, 13 + half)
        here = wide.at[q, :, :, :, at.core]
        ring.start(q, 15, here, here, at.partner)

    def embed_grad(q):
        ring.wait(q, 15)
        cols = pl.ds(q * width, width)
        out = jnp.dot(normed[0, views[0]], wide[q].reshape(dim, width), preferred_element_type=F32)
        pre[views[1], cols] = out
        embed_local[1:2, cols] = col_sum(out)
        embed_local[3:4, cols] = col_sum(out * normed[0, views[1], cols].astype(F32))

        @loop(LINE)
        def _(z):
            into = pl.ds(pl.multiple_of(z * quarter, quarter), quarter)
            out = lax.dot_general(normed[0, views[1], cols], wide[q, z].reshape(quarter, width), LANE_DIMS,
                                  preferred_element_type=F32)
            pre[views[0], into] = out if q == 0 else pre[views[0], into] + out

    steps = (ring.first, ring.second, ring.third, spread_line, spread_one, spread_two, spread_pair, embed_grad)
    for t in range(CHUNKS + SPREAD_LAGS[-1]):
        if t < CHUNKS:
            correlate(t)
        for step, lag in zip(steps, SPREAD_LAGS):
            if 0 <= t - lag < CHUNKS:
                step(t - lag)

    @loop(CHUNKS)
    def _(n):
        cols = pl.ds(pl.multiple_of(n * width, width), width)
        out = pre[views[0], cols]
        embed_local[0:1, cols] = col_sum(out)
        embed_local[2:3, cols] = col_sum(out * normed[0, views[0], cols].astype(F32))

    first_sums = sums[0][0]
    first_sums.begin()

    def load_feed(layer):
        p = layer % 2
        loads["feed", layer] = load(feeds[layer], wide.at[pl.ds(LINE * p, LINE)], LINE + p)

    load_feed(0)
    first_sums.over_plane()
    first_sums.over_line()
    first_sums.over_pair()

    def finish_grad(layer, j):
        cols = pl.ds(j * width, width)
        total, first = (total_three, j * width) if layer == 0 else (
            totals[layer].at[j // (CHUNKS // 2)], (j % (CHUNKS // 2)) * width)
        sel = pl.ds(first, width)
        for v in PAIR:
            mean0 = total[v:v + 1, sel] * count
            mean1 = total[2 + v:3 + v, sel] * count
            scale = scales[layer][v:v + 1, cols]

            @loop(view_rows // block_rows)
            def _(r):
                rows = pl.ds(pl.multiple_of(v * view_rows + r * block_rows, block_rows), block_rows)
                xhat = normed[layer % 2, rows, cols].astype(F32)
                grad[rows, cols] = (scale * (pre[rows, cols] - (mean0 + xhat * mean1))).astype(BF16)

    def weight_grad(layer, j):
        cols = pl.ds(j * width, width)
        q = (layer + 1) * CHUNKS + j

        @loop(LINE)
        def _(z):
            feed = jnp.concatenate([wide[4 * (layer % 2) + k, z].reshape(quarter, width) for k in range(LINE)], axis=1)
            out = jnp.dot(feed, grad[:, cols], preferred_element_type=F32)
            ring.part[q % 2, z] = out.reshape(ring.part.shape[2:])

        ring.pair(q)

    def input_grad(layer, n):
        cols = pl.ds(n * width, width)
        w_loads[layer, n].wait()
        half = local.at[layer, n // (CHUNKS // 2)]
        sel = pl.ds((n % (CHUNKS // 2)) * width, width)

        @loop(2)
        def _(v):
            rows = pl.ds(pl.multiple_of(v * view_rows, view_rows), view_rows)
            out = lax.dot_general(grad[rows, :], weight[n % slots], LANE_DIMS,
                                  preferred_element_type=F32)
            out = jnp.where(act[rows, cols] > 0, out, 0.0)
            pre[rows, cols] = out
            half[pl.ds(v, 1), sel] = col_sum(out)
            half[pl.ds(2 + v, 1), sel] = col_sum(out * normed[(layer + 1) % 2, rows, cols].astype(F32))

        if n + slots < CHUNKS:
            load_weight(layer, n + slots)

    def serve(t):
        for step, lag in zip((ring.first, ring.second, ring.third, ring.last), RING_LAGS):
            k = t - lag
            if 0 <= k < 3 * CHUNKS:
                blocks = step(CHUNKS + k)
        if 0 <= k < 3 * CHUNKS:
            for half, block in enumerate(blocks):
                outs[k // CHUNKS][:, pl.ds((k % CHUNKS) * width + half * ring.half, ring.half)] = block

    for layer in OTHERS:
        old, new = sums[layer], sums[layer + 1] if layer < 2 else None
        old[0].arrive()
        for j in range(CHUNKS):
            if j == 3 and new:
                loads["norm", layer].wait()
                loads["act", layer].wait()
            if j < 3:
                finish_grad(layer, j)
            elif new:
                for n in INPUT_STEPS[j - 3][0]:
                    input_grad(layer, n)
            if new and j == 4:
                new[0].begin()
            if new and j == 5:
                new[0].over_line()
            if new and j == 6:
                new[1].begin()
                new[0].over_pair()
                if layer == 0:
                    loads["act", 1] = load(masks[1], act, 3)
                    for n in range(slots):
                        load_weight(1, n)
            if j == 0:
                loads["feed", layer].wait()
            weight_grad(layer, j)
            if j == 0 and new:
                load_feed(layer + 1)
            if j == 0 and layer:
                old[1].over_pair()
            if j == 2:
                finish_grad(layer, 3)
                if layer:
                    old[1].arrive()
                for k in range(CHUNKS // 2, CHUNKS):
                    finish_grad(layer, k)
                if layer == 0:
                    loads["norm", 1] = load(norm_one, normed.at[0], 0)
            if new and j > 2:
                if j == 4:
                    new[0].over_plane()
                for n in INPUT_STEPS[j - 3][1]:
                    input_grad(layer, n)
                if j == 6:
                    new[1].over_plane()
                if j == 7:
                    new[1].over_line()
            serve(layer * CHUNKS + j)
    for k in range(RING_LAGS[-1]):
        serve(3 * CHUNKS + k)


def backward(total_rows, vmem, lam, *args):
    rows, dim = args[0].shape
    width, blocks = dim // CHUNKS, dim // 32
    hbm = pl.BlockSpec(memory_space=pl.ANY)
    vm = pl.BlockSpec(memory_space=pltpu.VMEM)
    scratch = [
        pltpu.VMEM((rows, dim), BF16),
        pltpu.VMEM((rows, dim), F32),
        pltpu.VMEM((CHUNKS, 4, 2, 2, 2, blocks, width), BF16),
        pltpu.VMEM((3, width, dim), BF16),
        pltpu.VMEM((2, rows, dim), BF16),
        pltpu.VMEM((rows, dim), BF16),
        pltpu.VMEM((2, 2, 4, dim // 2), F32),
        pltpu.VMEM((5, dim), F32),
        DMA_SEM((3,)),
        DMA_SEM((6,)),
    ] + ring_scratch(CHUNKS, blocks, width) + sums_scratch(5, dim)
    for _ in range(LINE):
        scratch += sums_scratch(4, dim // 2)
    halves = jax.ShapeDtypeStruct((2, 4, dim // 2), F32)
    return pl.pallas_call(
        functools.partial(backward_kernel, total_rows),
        out_shape=[jax.ShapeDtypeStruct((blocks, dim), F32)] * 3 + [jax.ShapeDtypeStruct((5, dim), F32), halves, halves],
        in_specs=[pl.BlockSpec(memory_space=pltpu.SMEM)] + [hbm] * 10 + [vm] * 3,
        out_specs=[vm] * 6,
        scratch_shapes=scratch,
        compiler_params=pltpu.CompilerParams(collective_id=1, has_side_effects=True, vmem_limit_bytes=vmem),
    )(lam.reshape(1), *args)


def forward_kernel(
        total_rows, feat_a, feat_b, w_one, w_two, w_three, gain_one, shift_one, gain_two, shift_two,
        act_one, act_two, norm_one, norm_two, embed, feat_t, act_one_t, act_two_t, scale_one, scale_two, scale_three,
        acts, hidden, normed, turned, weight, local, total, w_sem, in_sem, out_sem, *scratch):
    at = Place()
    view_rows, dim = acts.shape[2:]
    width = dim // CHUNKS
    quarter = dim // 4
    block_rows = min(64, view_rows)
    weights = [w_one, w_two, w_three]
    gains, shifts = [gain_one, gain_two], [shift_one, shift_two]
    scales = [scale_one, scale_two, scale_three]
    natural, normals, turns = [act_one, act_two, embed], [norm_one, norm_two], [feat_t, act_one_t, act_two_t]
    sets = [scratch[k:k + QUICK] for k in range(0, len(scratch), QUICK)]
    sums = [[QuickSums(at, (local, (layer, v)), (total, (layer, v)), *sets.pop()) for v in PAIR] for layer in OTHERS]

    ins = [pltpu.make_async_copy((feat_a, feat_b)[v], acts.at[0, v], in_sem.at[v]) for v in PAIR]

    def weight_copy(layer, k):
        cols = pl.ds(k * quarter, quarter)
        return pltpu.make_async_copy(weights[layer].at[:, cols], weight.at[layer % 2, :, cols], w_sem.at[layer % 2, k])

    def load_weight(layer, k):
        weight_copy(layer, k).start()

    ins[0].start()
    for k in range(LINE):
        load_weight(0, k)
    ins[1].start()
    outs = {}

    def put(name, v, src, dst, k):
        copy = pltpu.make_async_copy(src, dst, out_sem.at[k, v])
        copy.start()
        outs[name, v] = copy

    def drain(name, v):
        outs.pop((name, v)).wait()

    def matmul(layer, v, hooks=()):
        hooks = list(hooks)
        if v == 0:
            hooks += [(2 * k, lambda k=k: weight_copy(layer, k).wait()) for k in range(LINE)]

        @loop(CHUNKS)
        def _(n):
            for k, step in hooks:
                pl.when(n == k)(step)
            cols = pl.ds(pl.multiple_of(n * width, width), width)
            out = jnp.dot(acts[layer % 2, v], weight[layer % 2, :, cols], preferred_element_type=F32)
            hidden[v, :, cols] = out
            local[layer, v, 0:1, cols] = col_sum(out)
            local[layer, v, 1:2, cols] = col_sum(out * out)

    def normalise(layer, v):
        mean = total[layer, v, 0:1, :] / total_rows
        inv = lax.rsqrt(total[layer, v, 1:2, :] / total_rows - mean * mean + NORM_EPS)
        if layer < 2:
            scales[layer][v:v + 1, :] = gains[layer][...] * inv
        else:
            scales[layer][v:v + 1, :] = inv
        local[layer, v, 0:1, :] = mean
        local[layer, v, 1:2, :] = inv

        @loop(CHUNKS)
        def _(n):
            cols = pl.ds(pl.multiple_of(n * width, width), width)
            mean, inv = local[layer, v, 0:1, cols], local[layer, v, 1:2, cols]
            if layer < 2:
                gain, shift = gains[layer][:, cols], shifts[layer][:, cols]

            @loop(view_rows // block_rows)
            def _(r):
                rows = pl.ds(pl.multiple_of(r * block_rows, block_rows), block_rows)
                value = (hidden[v, rows, cols] - mean) * inv
                if layer < 2:
                    normed[v, rows, cols] = value.astype(BF16)
                    value = jnp.maximum(gain * value + shift, 0.0)
                acts[(layer + 1) % 2, v, rows, cols] = value.astype(BF16)

        put(("act", layer), v, acts.at[(layer + 1) % 2, v], natural[layer].at[v], layer % 2)
        if layer < 2:
            put(("norm", layer), v, normed.at[v], normals[layer].at[v], 2)

    def turn(layer, v):
        part = view_rows // 2

        @loop(CHUNKS)
        def _(n):
            cols = pl.ds(pl.multiple_of(n * width, width), width)
            for k in PAIR:
                block = acts[layer % 2, v, k * part:(k + 1) * part, cols].T
                turned[2 * v + k, lax.div(n, 2), lax.rem(n, 2)] = block.reshape(turned.shape[3:])

        span = pl.ds(2 * v, 2)
        put(("turn", layer), v, turned.at[span], turns[layer].at[span], 3)

    enter(at.z_peers + at.cube_peers)
    ins[0].wait()
    matmul(0, 0)
    now, later = sums[0]
    now.begin()
    for k in range(LINE):
        load_weight(1, k)
    ins[1].wait()
    matmul(0, 1, [(7, now.over_plane)])
    later.begin()
    for v in PAIR:
        turn(0, v)
    for layer in OTHERS:
        now, later = sums[layer]
        if layer == 0:
            for k in range(LINE):
                load_weight(2, k)
        now.arrive()
        for v in PAIR:
            if layer == 1:
                drain(("norm", 0), v)
            if layer == 2:
                drain(("act", 0), v)
        normalise(layer, 0)
        if layer == 2:
            later.over_plane()
            later.arrive()
            normalise(layer, 1)
            break
        matmul(layer + 1, 0, [(0, later.over_plane)])
        now = sums[layer + 1][0]
        now.begin()
        later.arrive()
        normalise(layer, 1)
        matmul(layer + 1, 1, [(5, now.over_plane)])
        sums[layer + 1][1].begin()
        for v in PAIR:
            drain(("turn", layer), v)
            turn(layer + 1, v)
    for copy in outs.values():
        copy.wait()


def forward(total_rows, vmem, feat_a, feat_b, weights, vectors):
    view_rows, dim = feat_a.shape
    hbm = pl.BlockSpec(memory_space=pl.ANY)
    vm = pl.BlockSpec(memory_space=pltpu.VMEM)
    turned = jax.ShapeDtypeStruct((4, 4, 2, 2, 2, dim // 32, view_rows // 2), BF16)
    scratch = [
        pltpu.VMEM((2, 2, view_rows, dim), BF16),
        pltpu.VMEM((2, view_rows, dim), F32),
        pltpu.VMEM((2, view_rows, dim), BF16),
        pltpu.VMEM(turned.shape, BF16),
        pltpu.VMEM((2, dim, dim), BF16),
        pltpu.VMEM((3, 2, 2, dim), F32),
        pltpu.VMEM((3, 2, 2, dim), F32),
        DMA_SEM((2, 4)),
        DMA_SEM((2,)),
        DMA_SEM((4, 2)),
    ]
    for _ in range(6):
        scratch += quick_scratch(2, dim)
    pair = jax.ShapeDtypeStruct((2, view_rows, dim), BF16)
    vector = jax.ShapeDtypeStruct((2, dim), F32)
    return pl.pallas_call(
        functools.partial(forward_kernel, total_rows),
        out_shape=[pair] * 5 + [turned] * 3 + [vector] * 3,
        in_specs=[hbm] * 5 + [vm] * 4,
        out_specs=[hbm] * 8 + [vm] * 3,
        scratch_shapes=scratch,
        compiler_params=pltpu.CompilerParams(collective_id=0, has_side_effects=True, vmem_limit_bytes=vmem),
    )(feat_a, feat_b, *weights, *[value.reshape(1, dim) for value in vectors])


def finish_kernel(total_two, total_one, loss_cols, *refs):
    gain_one, shift_one, gain_two, shift_two, loss = refs[6:]
    for grad, out in zip(refs[:3], refs[3:6]):
        out[...] = grad[...]
    half = total_two.shape[-1]
    for total, gain, shift in ((total_two, gain_two, shift_two), (total_one, gain_one, shift_one)):
        for h in PAIR:
            cols = pl.ds(h * half, half)
            shift[:, cols] = total[h, 0:1] + total[h, 1:2]
            gain[:, cols] = total[h, 2:3] + total[h, 3:4]
    loss[...] = jnp.sum(loss_cols[4:5, :], axis=1, keepdims=True)


def finish(total_two, total_one, loss_cols, grads):
    vm = pl.BlockSpec(memory_space=pltpu.VMEM)
    row = jax.ShapeDtypeStruct((1, loss_cols.shape[1]), F32)
    outs = pl.pallas_call(
        finish_kernel,
        out_shape=[jax.ShapeDtypeStruct(grad.shape, F32) for grad in grads] + [row] * 4 + [jax.ShapeDtypeStruct((1, 1), F32)],
        in_specs=[vm] * 6,
        out_specs=[vm] * 8,
    )(total_two, total_one, loss_cols, *grads)
    return outs[:3], [row.reshape(-1) for row in outs[3:7]], outs[7].reshape(())


def solution(mesh):
    shards = mesh.shape["data"]

    def local_step(h_a, h_b, w_one, w_two, w_three, gain_one, shift_one, gain_two, shift_two, lam_off):
        rows_dev = h_a.shape[0]
        total_rows = rows_dev * shards
        (act_one, act_two, norm_one, norm_two, embed, feat_t, act_one_t, act_two_t, scale_one, scale_two, scale_three) = forward(
            total_rows, 56 * 2**20, h_a, h_b, (w_one, w_two, w_three), (gain_one, shift_one, gain_two, shift_two))
        flat = lambda values: values.reshape(2 * rows_dev, -1)
        grad_w_three, grad_w_two, grad_w_one, total_three, total_two, total_one = backward(
            total_rows, 62 * 2**20, lam_off, flat(embed), flat(norm_two), flat(norm_one), flat(act_two), flat(act_one),
            act_two_t, act_one_t, feat_t, w_three, w_two, scale_three, scale_two, scale_one)
        grads, vectors, loss_total = finish(total_two, total_one, total_three, [grad_w_one, grad_w_two, grad_w_three])
        return (loss_total, *grads, *vectors)

    row_spec = P("data", None)
    whole_mat = P(None, None)
    whole_vec = P(None)
    return jax.shard_map(
        local_step, mesh=mesh,
        in_specs=(row_spec, row_spec, whole_mat, whole_mat, whole_mat,
                  whole_vec, whole_vec, whole_vec, whole_vec, P()),
        out_specs=(P(), row_spec, row_spec, row_spec, whole_vec, whole_vec, whole_vec, whole_vec),
        check_vma=False)
```

```python
import functools

import jax
import jax.numpy as jnp
from jax import lax
from jax.experimental import pallas as pl
from jax.experimental.pallas import tpu as pltpu
from jax.sharding import PartitionSpec as P

NORM_EPS = 1e-5
MESH = pl.DeviceIdType.MESH
F32 = jnp.float32
BF16 = jnp.bfloat16


ALL = slice(None)
PAIR = range(2)
OTHERS = range(3)
LINE = 4
CUBE = 8
DEPTH_DIMS = (((0,), (0,)), ((), ()))
LANE_DIMS = (((1,), (1,)), ((), ()))
DMA_SEM = pltpu.SemaphoreType.DMA


def loop(count):
    return pl.loop(0, count)


def col_sum(values):
    return jnp.sum(values, axis=0, keepdims=True)


class Place:
    def __init__(self):
        me = lax.axis_index("data")
        self.core = lax.rem(me, 2)
        self.x = lax.rem(lax.div(me, 2), 2)
        self.y = lax.rem(lax.div(me, 4), 2)
        self.z = lax.div(me, 8)
        self.plane = lax.rem(lax.div(me, 2), 4)
        self.partner = me + 1 - 2 * self.core
        self.x_peer = me + 2 - 4 * self.x
        self.y_peer = me + 4 - 8 * self.y
        self.low = lax.rem(me, CUBE)
        self.z_peers = [lax.rem(self.z + d + 1, LINE) * CUBE + self.low for d in OTHERS]
        self.plane_peers = [self.z * CUBE + lax.rem(self.plane + d + 1, LINE) * 2 + self.core for d in OTHERS]
        self.cube_peers = [self.z * CUBE + lax.rem(self.low + d + 1, CUBE) for d in range(CUBE - 1)]
        self.near = [self.partner] + self.plane_peers + self.z_peers


def enter(peers):
    barrier = pltpu.get_barrier_semaphore()
    for peer in peers:
        pl.semaphore_signal(barrier, inc=1, device_id=(peer,), device_id_type=MESH)
    pl.semaphore_wait(barrier, len(peers))


def remote(src, dst, send_sem, recv_sem, peer):
    return pltpu.make_async_remote_copy(
        src_ref=src, dst_ref=dst, send_sem=send_sem, recv_sem=recv_sem,
        device_id=(peer,), device_id_type=MESH)


class Sums:
    def __init__(self, at, local, total, recv0, slots1, slots2, send_sem, recv_sem):
        self.at, self.refs = at, (local, total)
        self.recv0, self.slots1, self.slots2 = recv0, slots1, slots2
        self.send_sem, self.recv_sem = send_sem, recv_sem
        self.half = recv0.shape[-1]
        self.mine = pl.multiple_of(at.core * self.half, 128)
        self.theirs = pl.multiple_of((1 - at.core) * self.half, 128)

    def pick(self, k, first):
        ref, index = self.refs[k]
        return ref.at[(*index, ALL, pl.ds(first, self.half))]

    def copies(self, stage):
        at = self.at
        if stage == 0:
            pairs = [(0, self.pick(0, self.theirs), self.recv0, at.partner)]
        elif stage == 1:
            here = self.slots1.at[at.plane]
            pairs = [(1 + d, here, here, at.plane_peers[d]) for d in OTHERS]
        elif stage == 2:
            here = self.slots2.at[at.z]
            pairs = [(4 + d, here, here, at.z_peers[d]) for d in OTHERS]
        else:
            here = self.pick(1, self.mine)
            pairs = [(7, here, here, at.partner)]
        return [remote(src, dst, self.send_sem.at[k], self.recv_sem.at[k], peer) for k, src, dst, peer in pairs]

    def send(self, stage):
        for copy in self.copies(stage):
            copy.start()

    def arrive(self, stage=3):
        for copy in self.copies(stage):
            copy.wait()

    def begin(self):
        self.send(0)

    def over_plane(self):
        self.arrive(0)
        self.slots1[self.at.plane] = self.pick(0, self.mine)[...] + self.recv0[...]
        self.send(1)

    def over_line(self):
        self.arrive(1)
        self.slots2[self.at.z] = (self.slots1[0] + self.slots1[1]) + (self.slots1[2] + self.slots1[3])
        self.send(2)

    def over_pair(self):
        self.arrive(2)
        self.pick(1, self.mine)[...] = (self.slots2[0] + self.slots2[1]) + (self.slots2[2] + self.slots2[3])
        self.send(3)


class QuickSums:
    def __init__(self, at, local, total, slots1, slots2, send_sem, recv_sem):
        self.at, self.local, self.total = at, local, total
        self.slots1, self.slots2 = slots1, slots2
        self.send_sem, self.recv_sem = send_sem, recv_sem

    def copies(self, across):
        at = self.at
        if across:
            here, peers, first = self.slots2.at[at.low], at.cube_peers, len(at.z_peers)
        else:
            here, peers, first = self.slots1.at[at.z], at.z_peers, 0
        return [remote(here, here, self.send_sem.at[first + d], self.recv_sem.at[first + d], peer)
                for d, peer in enumerate(peers)]

    def begin(self):
        ref, index = self.local
        self.slots1[self.at.z] = ref[index]
        for copy in self.copies(False):
            copy.start()

    def over_plane(self):
        for copy in self.copies(False):
            copy.wait()
        parts = [self.slots1[k] for k in range(LINE)]
        self.slots2[self.at.low] = (parts[0] + parts[1]) + (parts[2] + parts[3])
        for copy in self.copies(True):
            copy.start()

    def arrive(self):
        for copy in self.copies(True):
            copy.wait()
        parts = [self.slots2[k] for k in range(CUBE)]
        while len(parts) > 1:
            parts = [a + b for a, b in zip(parts[::2], parts[1::2])]
        ref, index = self.total
        ref[index] = parts[0]


def quick_scratch(rows, cols):
    return [
        pltpu.VMEM((LINE, rows, cols), F32),
        pltpu.VMEM((CUBE, rows, cols), F32),
        DMA_SEM((LINE + CUBE,)),
        DMA_SEM((LINE + CUBE,)),
    ]


def sums_scratch(rows, cols):
    return [
        pltpu.VMEM((rows, cols // 2), F32),
        pltpu.VMEM((4, rows, cols // 2), F32),
        pltpu.VMEM((4, rows, cols // 2), F32),
        DMA_SEM((8,)),
        DMA_SEM((8,)),
    ]


class Ring:
    def __init__(self, at, total, part, recv0, kept, snd1, recv1, snd2, recv2, snd3, recv3, send_sem, recv_sem, credit):
        self.at, self.total, self.slots = at, total, kept.shape[0]
        self.part, self.recv0, self.kept = part, recv0, kept
        self.snd1, self.recv1, self.snd2, self.recv2, self.snd3, self.recv3 = snd1, recv1, snd2, recv2, snd3, recv3
        self.send_sem, self.recv_sem, self.credit = send_sem, recv_sem, credit
        self.half = snd1.shape[-1]
        self.copies = {}
        self.peers = [at.partner, at.x_peer, at.y_peer, at.y_peer, at.x_peer] + at.z_peers
        self.givers = self.peers[:5] + at.z_peers[::-1]
        self.own = [at.y, at.x]

    def cols(self, half):
        return pl.ds(half * self.half, self.half)

    def depth(self, stage):
        return self.slots if stage else self.part.shape[0]

    def start(self, q, stage, src, dst, peer):
        copy = remote(src, dst, self.send_sem.at[q % self.slots, stage], self.recv_sem.at[q % self.slots, stage], peer)
        copy.start()
        self.copies[q, stage] = copy

    def send(self, q, stage, src, dst):
        depth = self.depth(stage)
        if q >= depth:
            pl.semaphore_wait(self.credit.at[q % depth, stage], 1)
        self.start(q, stage, src, dst, self.peers[stage])

    def give(self, q, stage):
        depth = self.depth(stage)
        if q + depth < self.total:
            pl.semaphore_signal(self.credit.at[q % depth, stage], inc=1, device_id=(self.givers[stage],),
                                device_id_type=MESH)

    def wait(self, q, stage):
        self.copies.pop((q, stage)).wait()

    def pair(self, q):
        s = q % self.depth(0)
        self.send(q, 0, self.part.at[s, :, :, :, 1 - self.at.core], self.recv0.at[s])

    def first(self, q):
        at, s, j = self.at, q % self.depth(0), q % self.slots
        self.wait(q, 0)

        @loop(LINE)
        def _(z):
            for half in PAIR:
                cols = self.cols(half)
                for k in PAIR:
                    (y, x), (oy, ox) = ((at.y, k), (1 - at.y, k)) if half else ((k, at.x), (k, 1 - at.x))
                    self.snd1[j, half, z, k] = (
                        self.part[s, z, oy, ox, at.core, :, cols] + self.recv0[s, z, oy, ox, :, cols]).astype(BF16)
                    self.kept[j, half, z, k] = self.part[s, z, y, x, at.core, :, cols] + self.recv0[s, z, y, x, :, cols]

        self.give(q, 0)
        for half in PAIR:
            self.send(q, 1 + half, self.snd1.at[j, half], self.recv1.at[j, half])

    def second(self, q):
        j = q % self.slots
        for half in PAIR:
            own = self.own[half]
            self.wait(q, 1 + half)

            @loop(LINE)
            def _(z):
                self.snd2[j, half, z] = (
                    self.kept[j, half, z, 1 - own] + self.recv1[j, half, z, 1 - own].astype(F32)).astype(BF16)
                self.kept[j, half, z, own] = self.kept[j, half, z, own] + self.recv1[j, half, z, own].astype(F32)

            self.give(q, 1 + half)
            self.send(q, 3 + half, self.snd2.at[j, half], self.recv2.at[j, half])

    def summed(self, j, half, z):
        return self.kept[j, half, z, self.own[half]] + self.recv2[j, half, z].astype(F32)

    def third(self, q):
        j = q % self.slots
        for half in PAIR:
            self.wait(q, 3 + half)
        for d in OTHERS:
            z = lax.rem(self.at.z + d + 1, 4)
            for half in PAIR:
                self.snd3[j, d, :, self.cols(half)] = self.summed(j, half, z).astype(BF16)
            self.send(q, 5 + d, self.snd3.at[j, d], self.recv3.at[j, d])

    def last(self, q):
        j = q % self.slots
        totals = [self.summed(j, half, self.at.z) for half in PAIR]
        for d in OTHERS:
            self.wait(q, 5 + d)
            totals = [total + self.recv3[j, d, :, self.cols(half)].astype(F32) for half, total in enumerate(totals)]
            self.give(q, 5 + d)
        for half in PAIR:
            self.give(q, 3 + half)
        return totals


def ring_scratch(slots, rows, width):
    half = width // 2
    return [
        pltpu.VMEM((2, 4, 2, 2, 2, rows, width), F32),
        pltpu.VMEM((2, 4, 2, 2, rows, width), F32),
        pltpu.VMEM((slots, 2, 4, 2, rows, half), F32),
    ] + [pltpu.VMEM((slots, 2, 4, 2, rows, half), BF16)] * 2 + [pltpu.VMEM((slots, 2, 4, rows, half), BF16)] * 2 + [
        pltpu.VMEM((slots, 3, rows, width), BF16)] * 2 + [DMA_SEM((slots, 16))] * 2 + [
        pltpu.SemaphoreType.REGULAR((slots, 8))]


CHUNKS = 8
RING = 12
SUMS = 5
QUICK = 4
SPREAD_LAGS = (1, 2, 3, 4, 6, 7, 8, 9)
RING_LAGS = (1, 3, 5, 8)
INPUT_STEPS = (((0, 1), (2,)), ((3,), (4,)), ((5,), (6,)), ((7,), ()), ((), ()))


def step_kernel(
        total_rows, lam_ref, feat_a, feat_b, w_one, w_two, w_three, gain_one, shift_one, gain_two, shift_two,
        grad_w_three, grad_w_two, grad_w_one, total_three, total_two, total_one, saved_act, saved_norm,
        grad, pre, wide, turned, weight, normed, act, sides, side_sums, local, embed_local, scales,
        wide_sem, w_sem, load_sem, out_sem, *scratch):
    at = Place()
    ring = Ring(at, 4 * CHUNKS, *scratch[:RING])
    rows_dev, dim = grad.shape
    width = dim // CHUNKS
    view_rows = rows_dev // 2
    block_rows = min(64, view_rows)
    quarter = dim // 4
    count = 1.0 / total_rows
    weights = [w_one, w_two, w_three]
    gains, shifts = [gain_one, gain_two], [shift_one, shift_two]
    outs = [grad_w_three, grad_w_two, grad_w_one]
    totals = [total_three, total_two, total_one]
    views = [pl.ds(v * view_rows, view_rows) for v in PAIR]
    rest = list(scratch[RING:])

    def take(number):
        taken, rest[:] = rest[:number], rest[number:]
        return taken

    side = [[QuickSums(at, (sides, (layer, v)), (side_sums, (layer, v)), *take(QUICK)) for v in PAIR] for layer in OTHERS]
    sums = [[QuickSums(at, (embed_local, ...), (total_three, ...), *take(QUICK))]]
    for layer in PAIR:
        sums.append([Sums(at, (local, (layer, h)), (totals[layer + 1], (h,)), *take(SUMS)) for h in PAIR])

    def load(src, dst, k):
        copy = pltpu.make_async_copy(src, dst, load_sem.at[k])
        copy.start()
        return copy

    def wide_copy(layer, n):
        cols = pl.ds(pl.multiple_of(n * width, width), width)
        return pltpu.make_async_copy(weights[layer].at[:, :, :, :, :, cols], wide.at[n], wide_sem.at[n])

    feats = [load(feat_a, normed.at[0, views[0]], 0)]
    lead = 3
    for n in range(lead):
        wide_copy(0, n).start()
    feats.append(load(feat_b, normed.at[0, views[1]], 1))
    puts = {}

    def put(name, v, src, dst, k):
        copy = pltpu.make_async_copy(src, dst, out_sem.at[k, v])
        copy.start()
        puts[name, v] = copy

    def drain(*names):
        for name in names:
            for v in PAIR:
                puts.pop((name, v)).wait()

    def matmul(layer, v, hook, step):
        @loop(CHUNKS)
        def _(n):
            if step:
                pl.when(n == hook)(step)
            if v == 0:
                if layer == 0:
                    pl.when(n + lead < CHUNKS)(lambda: wide_copy(0, n + lead).start())
                wide_copy(layer, n).wait()
            elif layer < 2:
                pl.when(n > 0)(lambda: wide_copy(layer + 1, n - 1).start())
            cols = pl.ds(pl.multiple_of(n * width, width), width)
            out = jnp.dot(normed[layer % 2, views[v]], wide[n].reshape(dim, width), preferred_element_type=F32)
            pre[views[v], cols] = out
            sides[layer, v, 0:1, cols] = col_sum(out)
            sides[layer, v, 1:2, cols] = col_sum(out * out)

        if v and layer < 2:
            wide_copy(layer + 1, CHUNKS - 1).start()
        side[layer][v].begin()

    def normalise(layer, v):
        side[layer][v].arrive()
        mean = side_sums[layer, v, 0:1, :] / total_rows
        inv = lax.rsqrt(side_sums[layer, v, 1:2, :] / total_rows - mean * mean + NORM_EPS)
        scales[2 - layer, v:v + 1, :] = gains[layer][...] * inv if layer < 2 else inv
        sides[layer, v, 0:1, :] = mean
        sides[layer, v, 1:2, :] = inv

        @loop(CHUNKS)
        def _(n):
            cols = pl.ds(pl.multiple_of(n * width, width), width)
            mean, inv = sides[layer, v, 0:1, cols], sides[layer, v, 1:2, cols]
            if layer < 2:
                gain, shift = gains[layer][:, cols], shifts[layer][:, cols]

            @loop(view_rows // block_rows)
            def _(r):
                rows = pl.ds(pl.multiple_of(v * view_rows + r * block_rows, block_rows), block_rows)
                value = (pre[rows, cols] - mean) * inv
                if layer < 2:
                    grad[rows, cols] = value.astype(BF16)
                    value = jnp.maximum(gain * value + shift, 0.0)
                normed[(layer + 1) % 2, rows, cols] = value.astype(BF16)

        if layer < 2:
            put(("act", layer), v, normed.at[(layer + 1) % 2, views[v]], saved_act.at[layer, views[v]], layer)
            put(("norm", layer), v, grad.at[views[v]], saved_norm.at[layer, views[v]], 2)

    def turn(src, dst, first, v):
        part = view_rows // 2

        @loop(CHUNKS)
        def _(n):
            cols = pl.ds(pl.multiple_of(n * width, width), width)
            for k in PAIR:
                block = src[pl.ds(v * view_rows + k * part, part), cols].T
                dst[first + 2 * v + k, lax.div(n, 2), lax.rem(n, 2)] = block.reshape(dst.shape[3:])

    enter(at.z_peers + at.cube_peers)
    feats[0].wait()
    matmul(0, 0, 0, None)
    feats[1].wait()
    matmul(0, 1, CHUNKS - 1, side[0][0].over_plane)
    for v in PAIR:
        turn(normed.at[0], turned, 0, v)
    normalise(0, 0)
    for layer in PAIR:
        matmul(layer + 1, 0, 0, side[layer][1].over_plane)
        normalise(layer, 1)
        matmul(layer + 1, 1, 5, side[layer + 1][0].over_plane)
        if layer == 0:
            drain(("norm", 0))
        else:
            drain(("act", 0))
        normalise(layer + 1, 0)
    side[2][1].over_plane()
    normalise(2, 1)

    drain(("act", 1), ("norm", 1))
    loads = {("act", 0): load(saved_act.at[1], act, 0), "turn": load(saved_act.at[0], grad, 1)}
    slots = weight.shape[0]
    w_loads = {}

    def load_weight(layer, n):
        copy = pltpu.make_async_copy(weights[2 - layer].at[n // 2, n % 2], weight.at[n % slots], w_sem.at[n % slots])
        copy.start()
        w_loads[layer, n] = copy

    for n in range(slots):
        load_weight(0, n)

    lam = lam_ref[0]
    place = (at.z, at.y, at.x, at.core)
    first_row = (((at.z * 2 + at.y) * 2 + at.x) * 2 + at.core) * ring.snd1.shape[-2]

    def correlate(q):
        @loop(LINE)
        def _(z):
            rows = pl.ds(pl.multiple_of(z * quarter, quarter), quarter)
            out = lax.dot_general(normed[1, views[0], rows], normed[1, views[1], pl.ds(q * width, width)],
                                  DEPTH_DIMS, preferred_element_type=F32)
            ring.part[q % 2, z] = out.reshape(ring.part.shape[2:])

        ring.pair(q)

    def spread_line(q):
        for half, total in enumerate(ring.last(q)):
            corr = total * count
            start = q * width + half * ring.half
            row = first_row + lax.broadcasted_iota(jnp.int32, corr.shape, 0)
            col = start + lax.broadcasted_iota(jnp.int32, corr.shape, 1)
            gap = 1.0 - corr
            loss = jnp.where(row == col, gap * gap, lam * corr * corr)
            embed_local[4:5, pl.ds(start, ring.half)] = col_sum(loss)
            slope = jnp.where(row == col, -2.0 * gap, 2.0 * lam * corr)
            wide[(q, *place, ALL, ring.cols(half))] = (slope * count).astype(BF16)
        here = wide.at[(q, *place)]
        for d in OTHERS:
            ring.start(q, 8 + d, here, here, at.z_peers[d])

    def spread_one(q):
        for d in OTHERS:
            ring.wait(q, 8 + d)
        for half, peer in enumerate((at.y_peer, at.x_peer)):
            here = wide.at[q, :, at.y, at.x, at.core, :, ring.cols(half)]
            ring.start(q, 11 + half, here, here, peer)

    def spread_two(q):
        for half, peer in enumerate((at.x_peer, at.y_peer)):
            ring.wait(q, 11 + half)
            here = wide.at[(q, ALL, *((at.y, ALL) if half else (ALL, at.x)), at.core, ALL,
                            ring.cols(half))]
            ring.start(q, 13 + half, here, here, peer)

    def spread_pair(q):
        for half in PAIR:
            ring.wait(q, 13 + half)
        here = wide.at[q, :, :, :, at.core]
        ring.start(q, 15, here, here, at.partner)

    def embed_grad(q):
        ring.wait(q, 15)
        cols = pl.ds(q * width, width)
        out = jnp.dot(normed[1, views[0]], wide[q].reshape(dim, width), preferred_element_type=F32)
        pre[views[1], cols] = out
        embed_local[1:2, cols] = col_sum(out)
        embed_local[3:4, cols] = col_sum(out * normed[1, views[1], cols].astype(F32))

        @loop(LINE)
        def _(z):
            into = pl.ds(pl.multiple_of(z * quarter, quarter), quarter)
            out = lax.dot_general(normed[1, views[1], cols], wide[q, z].reshape(quarter, width), LANE_DIMS,
                                  preferred_element_type=F32)
            pre[views[0], into] = out if q == 0 else pre[views[0], into] + out

    steps = (ring.first, ring.second, ring.third, spread_line, spread_one, spread_two, spread_pair, embed_grad)
    for t in range(CHUNKS + SPREAD_LAGS[-1]):
        if t < CHUNKS:
            correlate(t)
        for step, lag in zip(steps, SPREAD_LAGS):
            if 0 <= t - lag < CHUNKS:
                step(t - lag)

    @loop(CHUNKS)
    def _(n):
        cols = pl.ds(pl.multiple_of(n * width, width), width)
        out = pre[views[0], cols]
        embed_local[0:1, cols] = col_sum(out)
        embed_local[2:3, cols] = col_sum(out * normed[1, views[0], cols].astype(F32))

    first_sums = sums[0][0]
    first_sums.begin()
    for v in PAIR:
        turn(normed.at[0], wide, 0, v)
    loads["norm", 0] = load(saved_norm.at[1], normed.at[0], 2)
    first_sums.over_plane()
    loads["turn"].wait()
    for v in PAIR:
        turn(grad, wide, LINE, v)

    def finish_grad(layer, j):
        cols = pl.ds(j * width, width)
        total, first = (total_three, j * width) if layer == 0 else (
            totals[layer].at[j // (CHUNKS // 2)], (j % (CHUNKS // 2)) * width)
        sel = pl.ds(first, width)
        for v in PAIR:
            mean0 = total[v:v + 1, sel] * count
            mean1 = total[2 + v:3 + v, sel] * count
            scale = scales[layer, v:v + 1, cols]

            @loop(view_rows // block_rows)
            def _(r):
                rows = pl.ds(pl.multiple_of(v * view_rows + r * block_rows, block_rows), block_rows)
                xhat = normed[(layer + 1) % 2, rows, cols].astype(F32)
                grad[rows, cols] = (scale * (pre[rows, cols] - (mean0 + xhat * mean1))).astype(BF16)

    def weight_grad(layer, j):
        cols = pl.ds(j * width, width)
        q = (layer + 1) * CHUNKS + j

        @loop(LINE)
        def _(z):
            source, first = (turned, 0) if layer == 2 else (wide, LINE * layer)
            feed = jnp.concatenate([source[first + k, z].reshape(quarter, -1) for k in range(LINE)], axis=1)
            out = jnp.dot(feed, grad[:, cols], preferred_element_type=F32)
            ring.part[q % 2, z] = out.reshape(ring.part.shape[2:])

        ring.pair(q)

    def input_grad(layer, n):
        cols = pl.ds(n * width, width)
        w_loads[layer, n].wait()
        half = local.at[layer, n // (CHUNKS // 2)]
        sel = pl.ds((n % (CHUNKS // 2)) * width, width)

        @loop(2)
        def _(v):
            rows = pl.ds(pl.multiple_of(v * view_rows, view_rows), view_rows)
            out = lax.dot_general(grad[rows, :], weight[n % slots].reshape(width, dim), LANE_DIMS,
                                  preferred_element_type=F32)
            out = jnp.where(act[rows, cols] > 0, out, 0.0)
            pre[rows, cols] = out
            half[pl.ds(v, 1), sel] = col_sum(out)
            half[pl.ds(2 + v, 1), sel] = col_sum(out * normed[layer % 2, rows, cols].astype(F32))

        if n + slots < CHUNKS:
            load_weight(layer, n + slots)

    def serve(t):
        for step, lag in zip((ring.first, ring.second, ring.third, ring.last), RING_LAGS):
            k = t - lag
            if 0 <= k < 3 * CHUNKS:
                blocks = step(CHUNKS + k)
        if 0 <= k < 3 * CHUNKS:
            for half, block in enumerate(blocks):
                outs[k // CHUNKS][:, pl.ds((k % CHUNKS) * width + half * ring.half, ring.half)] = block

    for layer in OTHERS:
        old, new = sums[layer], sums[layer + 1] if layer < 2 else None
        old[0].arrive()
        for j in range(CHUNKS):
            if j == 3 and new:
                loads["norm", layer].wait()
                loads["act", layer].wait()
            if j < 3:
                finish_grad(layer, j)
            elif new:
                for n in INPUT_STEPS[j - 3][0]:
                    input_grad(layer, n)
            if new and j == 4:
                new[0].begin()
            if new and j == 5:
                new[0].over_line()
            if new and j == 6:
                new[1].begin()
                new[0].over_pair()
                if layer == 0:
                    loads["act", 1] = load(saved_act.at[0], act, 0)
                    for n in range(slots):
                        load_weight(1, n)
            weight_grad(layer, j)
            if j == 0 and layer:
                old[1].over_pair()
            if j == 2:
                finish_grad(layer, 3)
                if layer:
                    old[1].arrive()
                for k in range(CHUNKS // 2, CHUNKS):
                    finish_grad(layer, k)
                if layer == 0:
                    loads["norm", 1] = load(saved_norm.at[0], normed.at[1], 1)
            if new and j > 2:
                if j == 4:
                    new[0].over_plane()
                for n in INPUT_STEPS[j - 3][1]:
                    input_grad(layer, n)
                if j == 6:
                    new[1].over_plane()
                if j == 7:
                    new[1].over_line()
            serve(layer * CHUNKS + j)
    for k in range(RING_LAGS[-1]):
        serve(3 * CHUNKS + k)


def step(total_rows, vmem, lam, feat_a, feat_b, weights, vectors):
    view_rows, dim = feat_a.shape
    rows, width, blocks = 2 * view_rows, dim // CHUNKS, dim // 32
    hbm = pl.BlockSpec(memory_space=pl.ANY)
    vm = pl.BlockSpec(memory_space=pltpu.VMEM)
    cube = (LINE, 2, 2, 2, blocks)
    scratch = [
        pltpu.VMEM((rows, dim), BF16),
        pltpu.VMEM((rows, dim), F32),
        pltpu.VMEM((CHUNKS, *cube, width), BF16),
        pltpu.VMEM((LINE, *cube, view_rows // 2), BF16),
        pltpu.VMEM((3, 2, 2, blocks, dim), BF16),
        pltpu.VMEM((2, rows, dim), BF16),
        pltpu.VMEM((rows, dim), BF16),
        pltpu.VMEM((3, 2, 2, dim), F32),
        pltpu.VMEM((3, 2, 2, dim), F32),
        pltpu.VMEM((2, 2, 4, dim // 2), F32),
        pltpu.VMEM((5, dim), F32),
        pltpu.VMEM((3, 2, dim), F32),
        DMA_SEM((CHUNKS,)),
        DMA_SEM((3,)),
        DMA_SEM((3,)),
        DMA_SEM((3, 2)),
    ] + ring_scratch(CHUNKS, blocks, width)
    for _ in range(6):
        scratch += quick_scratch(2, dim)
    scratch += quick_scratch(5, dim)
    for _ in range(4):
        scratch += sums_scratch(4, dim // 2)
    halves = jax.ShapeDtypeStruct((2, 4, dim // 2), F32)
    saved = jax.ShapeDtypeStruct((2, rows, dim), BF16)
    return pl.pallas_call(
        functools.partial(step_kernel, total_rows),
        out_shape=[jax.ShapeDtypeStruct((blocks, dim), F32)] * 3 + [
            jax.ShapeDtypeStruct((5, dim), F32), halves, halves, saved, saved],
        in_specs=[pl.BlockSpec(memory_space=pltpu.SMEM)] + [hbm] * 5 + [vm] * 4,
        out_specs=[vm] * 6 + [hbm] * 2,
        scratch_shapes=scratch,
        compiler_params=pltpu.CompilerParams(collective_id=0, has_side_effects=True, vmem_limit_bytes=vmem),
    )(lam.reshape(1), feat_a, feat_b, *[weight.reshape(*cube, dim) for weight in weights],
      *[value.reshape(1, dim) for value in vectors])


def finish_kernel(total_two, total_one, loss_cols, *refs):
    gain_one, shift_one, gain_two, shift_two, loss = refs[6:]
    for grad, out in zip(refs[:3], refs[3:6]):
        out[...] = grad[...]
    half = total_two.shape[-1]
    for total, gain, shift in ((total_two, gain_two, shift_two), (total_one, gain_one, shift_one)):
        for h in PAIR:
            cols = pl.ds(h * half, half)
            shift[:, cols] = total[h, 0:1] + total[h, 1:2]
            gain[:, cols] = total[h, 2:3] + total[h, 3:4]
    loss[...] = jnp.sum(loss_cols[4:5, :], axis=1, keepdims=True)


def finish(total_two, total_one, loss_cols, grads):
    vm = pl.BlockSpec(memory_space=pltpu.VMEM)
    row = jax.ShapeDtypeStruct((1, loss_cols.shape[1]), F32)
    outs = pl.pallas_call(
        finish_kernel,
        out_shape=[jax.ShapeDtypeStruct(grad.shape, F32) for grad in grads] + [row] * 4 + [jax.ShapeDtypeStruct((1, 1), F32)],
        in_specs=[vm] * 6,
        out_specs=[vm] * 8,
    )(total_two, total_one, loss_cols, *grads)
    return outs[:3], [row.reshape(-1) for row in outs[3:7]], outs[7].reshape(())


def solution(mesh):
    shards = mesh.shape["data"]

    def local_step(h_a, h_b, w_one, w_two, w_three, gain_one, shift_one, gain_two, shift_two, lam_off):
        rows_dev = h_a.shape[0]
        total_rows = rows_dev * shards
        grad_w_three, grad_w_two, grad_w_one, total_three, total_two, total_one = step(
            total_rows, 63 * 2**20, lam_off, h_a, h_b, (w_one, w_two, w_three),
            (gain_one, shift_one, gain_two, shift_two))[:6]
        grads, vectors, loss_total = finish(total_two, total_one, total_three, [grad_w_one, grad_w_two, grad_w_three])
        return (loss_total, *grads, *vectors)

    row_spec = P("data", None)
    whole_mat = P(None, None)
    whole_vec = P(None)
    return jax.shard_map(
        local_step, mesh=mesh,
        in_specs=(row_spec, row_spec, whole_mat, whole_mat, whole_mat,
                  whole_vec, whole_vec, whole_vec, whole_vec, P()),
        out_specs=(P(), row_spec, row_spec, row_spec, whole_vec, whole_vec, whole_vec, whole_vec),
        check_vma=False)
```

```python
import functools

import jax
import jax.numpy as jnp
from jax import lax
from jax.experimental import pallas as pl
from jax.experimental.pallas import tpu as pltpu
from jax.sharding import PartitionSpec as P

NORM_EPS = 1e-5
TINY = 1e-37
MESH = pl.DeviceIdType.MESH
F32 = jnp.float32
BF16 = jnp.bfloat16


ALL = slice(None)
FIRST, SECOND, THIRD, FOURTH = [slice(k, k + 1) for k in range(4)]
PAIR = range(2)
OTHERS = range(3)
LINE = 4
CUBE = 8
DEPTH_DIMS = (((0,), (0,)), ((), ()))
LANE_DIMS = (((1,), (1,)), ((), ()))
DMA_SEM = pltpu.SemaphoreType.DMA


def loop(count):
    return pl.loop(0, count)


def col_sum(values):
    return jnp.sum(values, axis=0, keepdims=True)


class Place:
    def __init__(self):
        me = lax.axis_index("data")
        self.core = lax.rem(me, 2)
        self.x = lax.rem(lax.div(me, 2), 2)
        self.y = lax.rem(lax.div(me, 4), 2)
        self.z = lax.div(me, 8)
        self.plane = lax.rem(lax.div(me, 2), 4)
        self.partner = me + 1 - 2 * self.core
        self.x_peer = me + 2 - 4 * self.x
        self.y_peer = me + 4 - 8 * self.y
        self.low = lax.rem(me, CUBE)
        self.others = [lax.rem(self.z + d + 1, LINE) for d in OTHERS]
        self.z_peers = [z * CUBE + self.low for z in self.others]
        self.plane_peers = [self.z * CUBE + lax.rem(self.plane + d + 1, LINE) * 2 + self.core for d in OTHERS]
        self.cube_peers = [self.z * CUBE + lax.rem(self.low + d + 1, CUBE) for d in range(CUBE - 1)]
        self.near = [self.partner] + self.plane_peers + self.z_peers


def enter(peers):
    barrier = pltpu.get_barrier_semaphore()
    for peer in peers:
        pl.semaphore_signal(barrier, inc=1, device_id=(peer,), device_id_type=MESH)
    pl.semaphore_wait(barrier, len(peers))


def remote(src, dst, send_sem, recv_sem, peer):
    return pltpu.make_async_remote_copy(
        src_ref=src, dst_ref=dst, send_sem=send_sem, recv_sem=recv_sem,
        device_id=(peer,), device_id_type=MESH)


class Sums:
    def __init__(self, at, local, total, recv0, slots1, slots2, send_sem, recv_sem):
        self.at, self.refs = at, (local, total)
        self.recv0, self.slots1, self.slots2 = recv0, slots1, slots2
        self.send_sem, self.recv_sem = send_sem, recv_sem
        self.half = recv0.shape[-1]
        self.mine = pl.multiple_of(at.core * self.half, 128)
        self.theirs = pl.multiple_of((1 - at.core) * self.half, 128)

    def pick(self, k, first):
        ref, index = self.refs[k]
        return ref.at[(*index, ALL, pl.ds(first, self.half))]

    def copies(self, stage):
        at = self.at
        if stage == 0:
            pairs = [(0, self.pick(0, self.theirs), self.recv0, at.partner)]
        elif stage == 1:
            here = self.slots1.at[at.plane]
            pairs = [(1 + d, here, here, at.plane_peers[d]) for d in OTHERS]
        elif stage == 2:
            here = self.slots2.at[at.z]
            pairs = [(4 + d, here, here, at.z_peers[d]) for d in OTHERS]
        else:
            here = self.pick(1, self.mine)
            pairs = [(7, here, here, at.partner)]
        return [remote(src, dst, self.send_sem.at[k], self.recv_sem.at[k], peer) for k, src, dst, peer in pairs]

    def send(self, stage):
        for copy in self.copies(stage):
            copy.start()

    def arrive(self, stage=3):
        for copy in self.copies(stage):
            copy.wait()

    def begin(self):
        self.send(0)

    def over_plane(self):
        self.arrive(0)
        self.slots1[self.at.plane] = self.pick(0, self.mine)[...] + self.recv0[...]
        self.send(1)

    def over_line(self):
        self.arrive(1)
        self.slots2[self.at.z] = jnp.sum(self.slots1[...], axis=0)
        self.send(2)

    def over_pair(self):
        self.arrive(2)
        self.pick(1, self.mine)[...] = jnp.sum(self.slots2[...], axis=0)
        self.send(3)


class QuickSums:
    def __init__(self, at, local, total, slots1, slots2, send_sem, recv_sem):
        self.at, self.local, self.total = at, local, total
        self.slots1, self.slots2 = slots1, slots2
        self.send_sem, self.recv_sem = send_sem, recv_sem

    def copies(self, across):
        at = self.at
        if across:
            here, peers, first = self.slots2.at[at.low], at.cube_peers, len(at.z_peers)
        else:
            here, peers, first = self.slots1.at[at.z], at.z_peers, 0
        return [remote(here, here, self.send_sem.at[first + d], self.recv_sem.at[first + d], peer)
                for d, peer in enumerate(peers)]

    def begin(self):
        ref, index = self.local
        self.slots1[self.at.z] = ref[index]
        for copy in self.copies(False):
            copy.start()

    def over_plane(self):
        for copy in self.copies(False):
            copy.wait()
        self.slots2[self.at.low] = jnp.sum(self.slots1[...], axis=0)
        for copy in self.copies(True):
            copy.start()

    def arrive(self):
        for copy in self.copies(True):
            copy.wait()
        ref, index = self.total
        ref[index] = jnp.sum(self.slots2[...], axis=0)


def quick_scratch(rows, cols):
    return [
        pltpu.VMEM((LINE, rows, cols), F32),
        pltpu.VMEM((CUBE, rows, cols), F32),
        DMA_SEM((LINE + CUBE,)),
        DMA_SEM((LINE + CUBE,)),
    ]


def sums_scratch(rows, cols):
    return [
        pltpu.VMEM((rows, cols // 2), F32),
        pltpu.VMEM((4, rows, cols // 2), F32),
        pltpu.VMEM((4, rows, cols // 2), F32),
        DMA_SEM((8,)),
        DMA_SEM((8,)),
    ]


class Ring:
    def __init__(self, at, total, part, recv0, kept, snd1, recv1, snd2, recv2, snd3, recv3, send_sem, recv_sem, credit):
        self.at, self.total, self.slots = at, total, kept.shape[0]
        self.part, self.recv0, self.kept = part, recv0, kept
        self.snd1, self.recv1, self.snd2, self.recv2, self.snd3, self.recv3 = snd1, recv1, snd2, recv2, snd3, recv3
        self.send_sem, self.recv_sem, self.credit = send_sem, recv_sem, credit
        self.half = snd1.shape[-1]
        self.copies = {}
        self.peers = [at.partner, at.x_peer, at.y_peer, at.y_peer, at.x_peer] + at.z_peers
        self.givers = self.peers[:5] + at.z_peers[::-1]
        self.own = [at.y, at.x]

    def cols(self, half):
        return pl.ds(half * self.half, self.half)

    def depth(self, stage):
        return self.slots if stage else self.part.shape[0]

    def start(self, q, stage, src, dst, peer):
        copy = remote(src, dst, self.send_sem.at[q % self.slots, stage], self.recv_sem.at[q % self.slots, stage], peer)
        copy.start()
        self.copies[q, stage] = copy

    def send(self, q, stage, src, dst):
        depth = self.depth(stage)
        if q >= depth:
            pl.semaphore_wait(self.credit.at[q % depth, stage], 1)
        self.start(q, stage, src, dst, self.peers[stage])

    def give(self, q, stage):
        depth = self.depth(stage)
        if q + depth < self.total:
            pl.semaphore_signal(self.credit.at[q % depth, stage], inc=1, device_id=(self.givers[stage],),
                                device_id_type=MESH)

    def wait(self, q, stage):
        self.copies.pop((q, stage)).wait()

    def pair(self, q):
        s = q % self.depth(0)
        self.send(q, 0, self.part.at[s, :, :, :, 1 - self.at.core], self.recv0.at[s])

    def first(self, q):
        at, s, j = self.at, q % self.depth(0), q % self.slots
        self.wait(q, 0)

        @loop(LINE)
        def _(z):
            for half in PAIR:
                cols = self.cols(half)
                for k in PAIR:
                    (y, x), (oy, ox) = ((at.y, k), (1 - at.y, k)) if half else ((k, at.x), (k, 1 - at.x))
                    self.snd1[j, half, z, k] = (
                        self.part[s, z, oy, ox, at.core, :, cols] + self.recv0[s, z, oy, ox, :, cols]).astype(BF16)
                    self.kept[j, half, z, k] = self.part[s, z, y, x, at.core, :, cols] + self.recv0[s, z, y, x, :, cols]

        self.give(q, 0)
        for half in PAIR:
            self.send(q, 1 + half, self.snd1.at[j, half], self.recv1.at[j, half])

    def second(self, q):
        j = q % self.slots
        for half in PAIR:
            own = self.own[half]
            self.wait(q, 1 + half)

            @loop(LINE)
            def _(z):
                self.snd2[j, half, z] = (
                    self.kept[j, half, z, 1 - own] + self.recv1[j, half, z, 1 - own].astype(F32)).astype(BF16)
                self.kept[j, half, z, own] = self.kept[j, half, z, own] + self.recv1[j, half, z, own].astype(F32)

            self.give(q, 1 + half)
            self.send(q, 3 + half, self.snd2.at[j, half], self.recv2.at[j, half])

    def summed(self, j, half, z):
        return self.kept[j, half, z, self.own[half]] + self.recv2[j, half, z].astype(F32)

    def third(self, q):
        j = q % self.slots
        for half in PAIR:
            self.wait(q, 3 + half)

        @loop(len(OTHERS))
        def _(d):
            z = lax.rem(self.at.z + d + 1, LINE)
            for half in PAIR:
                self.snd3[j, d, :, self.cols(half)] = self.summed(j, half, z).astype(BF16)

        for d in OTHERS:
            self.send(q, 5 + d, self.snd3.at[j, d], self.recv3.at[j, d])

    def last(self, q):
        j = q % self.slots
        totals = [self.summed(j, half, self.at.z) for half in PAIR]
        for d in OTHERS:
            self.wait(q, 5 + d)
            totals = [total + self.recv3[j, d, :, self.cols(half)].astype(F32) for half, total in enumerate(totals)]
            self.give(q, 5 + d)
        for half in PAIR:
            self.give(q, 3 + half)
        return totals


def ring_scratch(slots, rows, width):
    half = width // 2
    return [
        pltpu.VMEM((2, 4, 2, 2, 2, rows, width), F32),
        pltpu.VMEM((2, 4, 2, 2, rows, width), F32),
        pltpu.VMEM((slots, 2, 4, 2, rows, half), F32),
    ] + [pltpu.VMEM((slots, 2, 4, 2, rows, half), BF16)] * 2 + [pltpu.VMEM((slots, 2, 4, rows, half), BF16)] * 2 + [
        pltpu.VMEM((slots, 3, rows, width), BF16)] * 2 + [DMA_SEM((slots, 16))] * 2 + [
        pltpu.SemaphoreType.REGULAR((slots, 8))]


CHUNKS = 8
RING = 12
SUMS = 5
QUICK = 4
SPREAD_LAGS = (1, 2, 3, 4, 6, 7, 8, 9)
RING_LAGS = (1, 3, 5, 8)
PAD = 16
INPUT_STEPS = (((0, 1), (2,)), ((3,), (4,)), ((5,), (6,)), ((7,), ()), ((), ()))


def step_kernel(
        total_rows, lam_ref, feat_a, feat_b, w_one, w_two, w_three, gain_one, shift_one, gain_two, shift_two,
        grad_w_three, grad_w_two, grad_w_one, loss_total, total_two, total_one, saved_act, saved_norm,
        grad, pre, wide, turned, weight, normed, act, sides, side_sums, local, embed_total, loss_local, mean_rows, lanes, scales,
        wide_sem, w_sem, load_sem, out_sem, *scratch):
    at = Place()
    ring = Ring(at, 4 * CHUNKS, *scratch[:RING])
    rows_dev, dim = grad.shape
    width = dim // CHUNKS
    view_rows = rows_dev // 2
    block_rows = min(64, view_rows)
    quarter = dim // 4
    count = 1.0 / total_rows
    weights = [w_one, w_two, w_three]
    gains, shifts = [gain_one, gain_two], [shift_one, shift_two]
    outs = [grad_w_three, grad_w_two, grad_w_one]
    totals = [embed_total, total_two, total_one]
    views = [pl.ds(v * view_rows, view_rows) for v in PAIR]
    rest = list(scratch[RING:])

    def take(number):
        taken, rest[:] = rest[:number], rest[number:]
        return taken

    top = pl.ds(0, 2)
    side = [[QuickSums(at, (sides, (layer, v, top)), (side_sums, (layer, v, top)), *take(QUICK)) for v in PAIR] for layer in OTHERS]
    pair_sums = QuickSums(at, (sides, (0, 0)), (side_sums, (0, 0)), *take(QUICK))
    loss_sums = QuickSums(at, (loss_local, ...), (loss_total, ...), *take(QUICK))
    sums = [None]
    for layer in PAIR:
        sums.append([Sums(at, (local, (layer, h)), (totals[layer + 1], (h,)), *take(SUMS)) for h in PAIR])

    def load(src, dst, k):
        copy = pltpu.make_async_copy(src, dst, load_sem.at[k])
        copy.start()
        return copy

    def wide_copy(layer, n):
        cols = pl.ds(pl.multiple_of(n * width, width), width)
        return pltpu.make_async_copy(weights[layer].at[:, :, :, :, :, cols], wide.at[n], wide_sem.at[n])

    feats = [load(feat_a, normed.at[0, views[0]], 0)]
    lead = 3
    for n in range(lead):
        wide_copy(0, n).start()
    feats.append(load(feat_b, normed.at[0, views[1]], 1))
    puts = {}

    def put(name, v, src, dst, k):
        copy = pltpu.make_async_copy(src, dst, out_sem.at[k, v])
        copy.start()
        puts[name, v] = copy

    def drain(*names):
        for name in names:
            for v in PAIR:
                puts.pop((name, v)).wait()

    def matmul(layer, v, hook, step):
        @loop(CHUNKS)
        def _(n):
            if step:
                pl.when(n == hook)(step)
            if v == 0:
                if layer == 0:
                    pl.when(n + lead < CHUNKS)(lambda: wide_copy(0, n + lead).start())
                wide_copy(layer, n).wait()
            elif layer < 2:
                pl.when(n > 0)(lambda: wide_copy(layer + 1, n - 1).start())
            cols = pl.ds(pl.multiple_of(n * width, width), width)
            out = jnp.dot(normed[layer % 2, views[v]], wide[n].reshape(dim, width), preferred_element_type=F32)
            pre[views[v], cols] = out
            sides[layer, v, FIRST, cols] = col_sum(out)
            sides[layer, v, SECOND, cols] = col_sum(out * out)

        if v and layer < 2:
            wide_copy(layer + 1, CHUNKS - 1).start()
        side[layer][v].begin()

    def normalise(layer, v):
        side[layer][v].arrive()
        mean = side_sums[layer, v, FIRST, :] / total_rows
        inv = lax.rsqrt(side_sums[layer, v, SECOND, :] / total_rows - mean * mean + NORM_EPS)
        scales[2 - layer, v:v + 1, :] = gains[layer][...] * inv if layer < 2 else inv
        sides[layer, v, FIRST, :] = mean
        sides[layer, v, SECOND, :] = inv

        @loop(CHUNKS)
        def _(n):
            cols = pl.ds(pl.multiple_of(n * width, width), width)
            mean, inv = sides[layer, v, FIRST, cols], sides[layer, v, SECOND, cols]
            if layer < 2:
                gain, shift = gains[layer][:, cols], shifts[layer][:, cols]

            @loop(view_rows // block_rows)
            def _(r):
                rows = pl.ds(pl.multiple_of(v * view_rows + r * block_rows, block_rows), block_rows)
                value = (pre[rows, cols] - mean) * inv
                if layer < 2:
                    grad[rows, cols] = value.astype(BF16)
                    value = jnp.maximum(gain * value + shift, 0.0)
                normed[(layer + 1) % 2, rows, cols] = value.astype(BF16)

        if layer < 2:
            put(("act", layer), v, normed.at[(layer + 1) % 2, views[v]], saved_act.at[layer, views[v]], layer)
            put(("norm", layer), v, grad.at[views[v]], saved_norm.at[layer, views[v]], 2)

    def turn(src, dst, first, v):
        part = view_rows // 2

        @loop(CHUNKS)
        def _(n):
            cols = pl.ds(pl.multiple_of(n * width, width), width)
            for k in PAIR:
                block = src[pl.ds(v * view_rows + k * part, part), cols].T
                dst[first + 2 * v + k, lax.div(n, 2), lax.rem(n, 2)] = block.reshape(dst.shape[3:])

    enter(at.z_peers + at.cube_peers)
    feats[0].wait()
    matmul(0, 0, 0, None)
    feats[1].wait()
    matmul(0, 1, CHUNKS - 1, side[0][0].over_plane)
    for v in PAIR:
        turn(normed.at[0], turned, 0, v)
    normalise(0, 0)
    for layer in PAIR:
        matmul(layer + 1, 0, 0, side[layer][1].over_plane)
        normalise(layer, 1)
        matmul(layer + 1, 1, 5, side[layer + 1][0].over_plane)
        if layer == 0:
            drain(("norm", 0))
        else:
            drain(("act", 0))
        normalise(layer + 1, 0)
    side[2][1].over_plane()
    normalise(2, 1)

    drain(("act", 1), ("norm", 1))
    loads = {("act", 0): load(saved_act.at[1], act, 0)}
    slots = weight.shape[0]
    w_loads = {}

    def load_weight(layer, n):
        copy = pltpu.make_async_copy(weights[2 - layer].at[n // 2, n % 2], weight.at[n % slots], w_sem.at[n % slots])
        copy.start()
        w_loads[layer, n] = copy

    for n in range(slots):
        load_weight(0, n)

    lam = lam_ref[0]
    half_lam = lam_ref[1]

    def pair_rows():
        @loop(CHUNKS)
        def _(n):
            cols = pl.ds(pl.multiple_of(n * width, width), width)
            one, two = [normed[1, views[v], cols].astype(F32) for v in PAIR]
            sides[0, 0, FIRST, cols] = col_sum(one)
            sides[0, 0, SECOND, cols] = col_sum(two)
            sides[0, 0, THIRD, cols] = col_sum(one * two)
            sides[0, 0, FOURTH, cols] = jnp.zeros((1, width), F32)

        pair_sums.begin()

    def keep_means():
        pair_sums.arrive()
        for v in PAIR:
            first = lax.broadcasted_iota(jnp.int32, (PAD, dim), 0) == 0
            mean_rows[v] = jnp.where(first, side_sums[0, 0, v:v + 1, :], 0.0).astype(BF16)
    place = (at.z, at.y, at.x, at.core)
    first_row = (((at.z * 2 + at.y) * 2 + at.x) * 2 + at.core) * ring.snd1.shape[-2]

    def correlate(q):
        @loop(LINE)
        def _(z):
            rows = pl.ds(pl.multiple_of(z * quarter, quarter), quarter)
            out = lax.dot_general(normed[1, views[0], rows], normed[1, views[1], pl.ds(q * width, width)],
                                  DEPTH_DIMS, preferred_element_type=F32)
            ring.part[q % 2, z] = out.reshape(ring.part.shape[2:])

        ring.pair(q)

    def spread_line(q):
        for half, total in enumerate(ring.last(q)):
            start = q * width + half * ring.half
            row = first_row + lax.broadcasted_iota(jnp.int32, total.shape, 0)
            col = start + lax.broadcasted_iota(jnp.int32, total.shape, 1)
            diag = row == col
            cols = pl.ds(start, ring.half)
            corr = jnp.where(diag, side_sums[0, 0, THIRD, cols], total) * count
            gap = 1.0 - corr
            loss = jnp.where(diag, gap * gap, lam * corr * corr)
            loss_local[:, cols] = col_sum(loss)
            slope = jnp.where(diag, -2.0 * gap, 2.0 * lam * corr)
            wide[(q, *place, ALL, ring.cols(half))] = (slope * count).astype(BF16)
        here = wide.at[(q, *place)]
        for d in OTHERS:
            ring.start(q, 8 + d, here, here, at.z_peers[d])

    def spread_one(q):
        for d in OTHERS:
            ring.wait(q, 8 + d)
        for half, peer in enumerate((at.y_peer, at.x_peer)):
            here = wide.at[q, :, at.y, at.x, at.core, :, ring.cols(half)]
            ring.start(q, 11 + half, here, here, peer)

    def spread_two(q):
        for half, peer in enumerate((at.x_peer, at.y_peer)):
            ring.wait(q, 11 + half)
            here = wide.at[(q, ALL, *((at.y, ALL) if half else (ALL, at.x)), at.core, ALL,
                            ring.cols(half))]
            ring.start(q, 13 + half, here, here, peer)

    def spread_pair(q):
        for half in PAIR:
            ring.wait(q, 13 + half)
        here = wide.at[q, :, :, :, at.core]
        ring.start(q, 15, here, here, at.partner)

    def embed_grad(q):
        ring.wait(q, 15)
        cols = pl.ds(q * width, width)
        chunk = wide[q].reshape(dim, width)
        pre[views[1], cols] = jnp.dot(normed[1, views[0]], chunk, preferred_element_type=F32)
        embed_total[SECOND, cols] = col_sum(jnp.dot(mean_rows[0], chunk, preferred_element_type=F32))

        @loop(LINE)
        def _(z):
            into = pl.ds(pl.multiple_of(z * quarter, quarter), quarter)
            block = wide[q, z].reshape(quarter, width)
            rows = lax.dot_general(normed[1, views[1], cols], block, LANE_DIMS, preferred_element_type=F32)
            mean = col_sum(lax.dot_general(mean_rows[1, :, cols], block, LANE_DIMS, preferred_element_type=F32))
            pre[views[0], into] = rows if q == 0 else pre[views[0], into] + rows
            embed_total[FIRST, into] = mean if q == 0 else embed_total[FIRST, into] + mean

        embed_total[FOURTH, cols] = jnp.zeros((1, width), F32)
        row, col = [lax.broadcasted_iota(jnp.int32, (width, width), axis) for axis in PAIR]
        corr = side_sums[0, 0, THIRD, cols] * count

        @loop(LINE)
        def _(z):
            for y in PAIR:
                slope = wide[q, z, y].reshape(width, width).astype(F32) * total_rows
                diag = row + (z * quarter + (y - q) * width) == col
                value = slope * jnp.where(diag, corr, slope * half_lam)
                embed_total[FOURTH, cols] = embed_total[FOURTH, cols] + col_sum(value)
                lanes[z, y] = value if q == 0 else lanes[z, y] + value

    steps = (ring.first, ring.second, ring.third, spread_line, spread_one, spread_two, spread_pair, embed_grad)
    for t in range(CHUNKS + SPREAD_LAGS[-1]):
        if t < CHUNKS:
            correlate(t)
        if t == 0:
            pair_rows()
        if t == 1:
            pair_sums.over_plane()
        if t == 3:
            keep_means()
        for step, lag in zip(steps, SPREAD_LAGS):
            if 0 <= t - lag < CHUNKS:
                step(t - lag)
                if step == embed_grad and t - lag == LINE:
                    for v in PAIR:
                        turn(normed.at[0], wide, 0, v)
                    loads["norm", 0] = load(saved_norm.at[1], normed.at[0], 2)

    loss_sums.begin()

    @loop(LINE)
    def _(z):
        for y in PAIR:
            cols = pl.ds(pl.multiple_of(z * quarter + y * width, width), width)
            embed_total[THIRD, cols] = col_sum(lanes[z, y].T)

    def finish_grad(layer, j):
        cols = pl.ds(j * width, width)
        total, first = (embed_total, j * width) if layer == 0 else (
            totals[layer].at[j // (CHUNKS // 2)], (j % (CHUNKS // 2)) * width)
        sel = pl.ds(first, width)
        for v in PAIR:
            mean0 = total[v:v + 1, sel] * count
            mean1 = total[2 + v:3 + v, sel] * count
            scale = scales[layer, v:v + 1, cols]

            @loop(view_rows // block_rows)
            def _(r):
                rows = pl.ds(pl.multiple_of(v * view_rows + r * block_rows, block_rows), block_rows)
                xhat = normed[(layer + 1) % 2, rows, cols].astype(F32)
                grad[rows, cols] = (scale * (pre[rows, cols] - (mean0 + xhat * mean1))).astype(BF16)

    def weight_grad(layer, j):
        cols = pl.ds(j * width, width)
        q = (layer + 1) * CHUNKS + j

        @loop(LINE)
        def _(z):
            source, first = (turned, 0) if layer == 2 else (wide, LINE * layer)
            feed = jnp.concatenate([source[first + k, z].reshape(quarter, -1) for k in range(LINE)], axis=1)
            out = jnp.dot(feed, grad[:, cols], preferred_element_type=F32)
            ring.part[q % 2, z] = out.reshape(ring.part.shape[2:])

        ring.pair(q)

    def input_grad(layer, n):
        cols = pl.ds(n * width, width)
        w_loads[layer, n].wait()
        half = local.at[layer, n // (CHUNKS // 2)]
        sel = pl.ds((n % (CHUNKS // 2)) * width, width)

        @loop(2)
        def _(v):
            rows = pl.ds(pl.multiple_of(v * view_rows, view_rows), view_rows)
            out = lax.dot_general(grad[rows, :], weight[n % slots].reshape(width, dim), LANE_DIMS,
                                  preferred_element_type=F32)
            out = jnp.where(act[rows, cols] > 0, out, 0.0)
            pre[rows, cols] = out
            half[pl.ds(v, 1), sel] = col_sum(out)
            half[pl.ds(2 + v, 1), sel] = col_sum(out * normed[layer % 2, rows, cols].astype(F32))

        if n + slots < CHUNKS:
            load_weight(layer, n + slots)

    def serve(t):
        for step, lag in zip((ring.first, ring.second, ring.third, ring.last), RING_LAGS):
            k = t - lag
            if 0 <= k < 3 * CHUNKS:
                blocks = step(CHUNKS + k)
        if 0 <= k < 3 * CHUNKS:
            for half, block in enumerate(blocks):
                outs[k // CHUNKS][:, pl.ds((k % CHUNKS) * width + half * ring.half, ring.half)] = block

    for layer in OTHERS:
        old, new = sums[layer], sums[layer + 1] if layer < 2 else None
        if layer:
            old[0].arrive()
        for j in range(CHUNKS):
            if j == 3 and new:
                loads["norm", layer].wait()
                if layer == 0:
                    loads["act", layer].wait()
            if j < 3:
                finish_grad(layer, j)
            elif new:
                for n in INPUT_STEPS[j - 3][0]:
                    input_grad(layer, n)
            if new and j == 4:
                new[0].begin()
            if new and j == 5:
                new[0].over_line()
            if new and j == 6:
                new[1].begin()
                new[0].over_pair()
                if layer == 0:
                    loads["act", 1] = load(saved_act.at[0], act, 0)
                    for n in range(slots):
                        load_weight(1, n)
            weight_grad(layer, j)
            if j == 0 and layer:
                old[1].over_pair()
            if j == 2:
                finish_grad(layer, 3)
                if layer:
                    old[1].arrive()
                for k in range(CHUNKS // 2, CHUNKS):
                    finish_grad(layer, k)
                if layer == 0:
                    loads["norm", 1] = load(saved_norm.at[0], normed.at[1], 1)
            if new and j > 2:
                if j == 4:
                    new[0].over_plane()
                for n in INPUT_STEPS[j - 3][1]:
                    input_grad(layer, n)
                if j == 6:
                    new[1].over_plane()
                if j == 7:
                    new[1].over_line()
            serve(layer * CHUNKS + j)
        if layer == 0:
            loads["act", 1].wait()
            for v in PAIR:
                turn(act, wide, LINE, v)
            loss_sums.over_plane()
    for k in range(RING_LAGS[-1]):
        serve(3 * CHUNKS + k)
    loss_sums.arrive()


def step(total_rows, vmem, lam, feat_a, feat_b, weights, vectors):
    view_rows, dim = feat_a.shape
    rows, width, blocks = 2 * view_rows, dim // CHUNKS, dim // 32
    hbm = pl.BlockSpec(memory_space=pl.ANY)
    vm = pl.BlockSpec(memory_space=pltpu.VMEM)
    cube = (LINE, 2, 2, 2, blocks)
    scratch = [
        pltpu.VMEM((rows, dim), BF16),
        pltpu.VMEM((rows, dim), F32),
        pltpu.VMEM((CHUNKS, *cube, width), BF16),
        pltpu.VMEM((LINE, *cube, view_rows // 2), BF16),
        pltpu.VMEM((3, 2, 2, blocks, dim), BF16),
        pltpu.VMEM((2, rows, dim), BF16),
        pltpu.VMEM((rows, dim), BF16),
        pltpu.VMEM((3, 2, 4, dim), F32),
        pltpu.VMEM((3, 2, 4, dim), F32),
        pltpu.VMEM((2, 2, 4, dim // 2), F32),
        pltpu.VMEM((4, dim), F32),
        pltpu.VMEM((1, dim), F32),
        pltpu.VMEM((2, PAD, dim), BF16),
        pltpu.VMEM((LINE, 2, width, width), F32),
        pltpu.VMEM((3, 2, dim), F32),
        DMA_SEM((CHUNKS,)),
        DMA_SEM((3,)),
        DMA_SEM((3,)),
        DMA_SEM((3, 2)),
    ] + ring_scratch(CHUNKS, blocks, width)
    for _ in range(6):
        scratch += quick_scratch(2, dim)
    scratch += quick_scratch(4, dim) + quick_scratch(1, dim)
    for _ in range(4):
        scratch += sums_scratch(4, dim // 2)
    halves = jax.ShapeDtypeStruct((2, 4, dim // 2), F32)
    saved = jax.ShapeDtypeStruct((2, rows, dim), BF16)
    return pl.pallas_call(
        functools.partial(step_kernel, total_rows),
        out_shape=[jax.ShapeDtypeStruct((blocks, dim), F32)] * 3 + [
            jax.ShapeDtypeStruct((1, dim), F32), halves, halves, saved, saved],
        in_specs=[pl.BlockSpec(memory_space=pltpu.SMEM)] + [hbm] * 5 + [vm] * 4,
        out_specs=[vm] * 6 + [hbm] * 2,
        scratch_shapes=scratch,
        compiler_params=pltpu.CompilerParams(collective_id=0, has_side_effects=True, vmem_limit_bytes=vmem),
    )(jnp.stack([lam, 0.5 / jnp.maximum(lam, TINY)]), feat_a, feat_b, *[weight.reshape(*cube, dim) for weight in weights],
      *[value.reshape(1, dim) for value in vectors])


def finish_kernel(total_two, total_one, loss_cols, *refs):
    gain_one, shift_one, gain_two, shift_two, loss = refs[6:]
    for grad, out in zip(refs[:3], refs[3:6]):
        out[...] = grad[...]
    half = total_two.shape[-1]
    for total, gain, shift in ((total_two, gain_two, shift_two), (total_one, gain_one, shift_one)):
        for h in PAIR:
            cols = pl.ds(h * half, half)
            shift[:, cols] = total[h, FIRST] + total[h, SECOND]
            gain[:, cols] = total[h, THIRD] + total[h, FOURTH]
    loss[...] = jnp.sum(loss_cols[...], axis=1, keepdims=True)


def finish(total_two, total_one, loss_cols, grads):
    vm = pl.BlockSpec(memory_space=pltpu.VMEM)
    row = jax.ShapeDtypeStruct((1, loss_cols.shape[1]), F32)
    outs = pl.pallas_call(
        finish_kernel,
        out_shape=[jax.ShapeDtypeStruct(grad.shape, F32) for grad in grads] + [row] * 4 + [jax.ShapeDtypeStruct((1, 1), F32)],
        in_specs=[vm] * 6,
        out_specs=[vm] * 8,
    )(total_two, total_one, loss_cols, *grads)
    return outs[:3], [row.reshape(-1) for row in outs[3:7]], outs[7].reshape(())


def solution(mesh):
    shards = mesh.shape["data"]

    def local_step(h_a, h_b, w_one, w_two, w_three, gain_one, shift_one, gain_two, shift_two, lam_off):
        rows_dev = h_a.shape[0]
        total_rows = rows_dev * shards
        grad_w_three, grad_w_two, grad_w_one, loss_cols, total_two, total_one = step(
            total_rows, 67000000, lam_off, h_a, h_b, (w_one, w_two, w_three),
            (gain_one, shift_one, gain_two, shift_two))[:6]
        grads, vectors, loss_total = finish(total_two, total_one, loss_cols, [grad_w_one, grad_w_two, grad_w_three])
        return (loss_total, *grads, *vectors)

    row_spec = P("data", None)
    whole_mat = P(None, None)
    whole_vec = P(None)
    return jax.shard_map(
        local_step, mesh=mesh,
        in_specs=(row_spec, row_spec, whole_mat, whole_mat, whole_mat,
                  whole_vec, whole_vec, whole_vec, whole_vec, P()),
        out_specs=(P(), row_spec, row_spec, row_spec, whole_vec, whole_vec, whole_vec, whole_vec),
        check_vma=False)
```

```python
import functools

import jax
import jax.numpy as jnp
from jax import lax
from jax.experimental import pallas as pl
from jax.experimental.pallas import tpu as pltpu
from jax.sharding import PartitionSpec as P

NORM_EPS = 1e-5
MESH = pl.DeviceIdType.MESH
F32 = jnp.float32
BF16 = jnp.bfloat16


ALL = slice(None)
FIRST, SECOND, THIRD, FOURTH = [slice(k, k + 1) for k in range(4)]
PAIR = range(2)
OTHERS = range(3)
LINE = 4
CUBE = 8
DEPTH_DIMS = (((0,), (0,)), ((), ()))
LANE_DIMS = (((1,), (1,)), ((), ()))
DMA_SEM = pltpu.SemaphoreType.DMA


def loop(count):
    return pl.loop(0, count)


def col_sum(values):
    return jnp.sum(values, axis=0, keepdims=True)


class Place:
    def __init__(self):
        me = lax.axis_index("data")
        self.core = lax.rem(me, 2)
        self.x = lax.rem(lax.div(me, 2), 2)
        self.y = lax.rem(lax.div(me, 4), 2)
        self.z = lax.div(me, 8)
        self.plane = lax.rem(lax.div(me, 2), 4)
        self.partner = me + 1 - 2 * self.core
        self.x_peer = me + 2 - 4 * self.x
        self.y_peer = me + 4 - 8 * self.y
        self.low = lax.rem(me, CUBE)
        self.others = [lax.rem(self.z + d + 1, LINE) for d in OTHERS]
        self.z_peers = [z * CUBE + self.low for z in self.others]
        self.plane_peers = [self.z * CUBE + lax.rem(self.plane + d + 1, LINE) * 2 + self.core for d in OTHERS]
        self.cube_peers = [self.z * CUBE + lax.rem(self.low + d + 1, CUBE) for d in range(CUBE - 1)]
        self.near = [self.partner] + self.plane_peers + self.z_peers


def enter(peers):
    barrier = pltpu.get_barrier_semaphore()
    for peer in peers:
        pl.semaphore_signal(barrier, inc=1, device_id=(peer,), device_id_type=MESH)
    pl.semaphore_wait(barrier, len(peers))


def remote(src, dst, send_sem, recv_sem, peer):
    return pltpu.make_async_remote_copy(
        src_ref=src, dst_ref=dst, send_sem=send_sem, recv_sem=recv_sem,
        device_id=(peer,), device_id_type=MESH)


class Sums:
    def __init__(self, at, local, total, recv0, slots1, slots2, send_sem, recv_sem):
        self.at, self.refs = at, (local, total)
        self.recv0, self.slots1, self.slots2 = recv0, slots1, slots2
        self.send_sem, self.recv_sem = send_sem, recv_sem
        self.half = recv0.shape[-1]
        self.mine = pl.multiple_of(at.core * self.half, 128)
        self.theirs = pl.multiple_of((1 - at.core) * self.half, 128)

    def pick(self, k, first):
        ref, index = self.refs[k]
        return ref.at[(*index, ALL, pl.ds(first, self.half))]

    def copies(self, stage):
        at = self.at
        if stage == 0:
            pairs = [(0, self.pick(0, self.theirs), self.recv0, at.partner)]
        elif stage == 1:
            here = self.slots1.at[at.plane]
            pairs = [(1 + d, here, here, at.plane_peers[d]) for d in OTHERS]
        elif stage == 2:
            here = self.slots2.at[at.z]
            pairs = [(4 + d, here, here, at.z_peers[d]) for d in OTHERS]
        else:
            here = self.pick(1, self.mine)
            pairs = [(7, here, here, at.partner)]
        return [remote(src, dst, self.send_sem.at[k], self.recv_sem.at[k], peer) for k, src, dst, peer in pairs]

    def send(self, stage):
        for copy in self.copies(stage):
            copy.start()

    def arrive(self, stage=3):
        for copy in self.copies(stage):
            copy.wait()

    def begin(self):
        self.send(0)

    def over_plane(self):
        self.arrive(0)
        self.slots1[self.at.plane] = self.pick(0, self.mine)[...] + self.recv0[...]
        self.send(1)

    def over_line(self):
        self.arrive(1)
        self.slots2[self.at.z] = jnp.sum(self.slots1[...], axis=0)
        self.send(2)

    def over_pair(self):
        self.arrive(2)
        self.pick(1, self.mine)[...] = jnp.sum(self.slots2[...], axis=0)
        self.send(3)


class QuickSums:
    def __init__(self, at, local, total, slots1, slots2, send_sem, recv_sem):
        self.at, self.local, self.total = at, local, total
        self.slots1, self.slots2 = slots1, slots2
        self.send_sem, self.recv_sem = send_sem, recv_sem

    def copies(self, across):
        at = self.at
        if across:
            here, peers, first = self.slots2.at[at.low], at.cube_peers, len(at.z_peers)
        else:
            here, peers, first = self.slots1.at[at.z], at.z_peers, 0
        return [remote(here, here, self.send_sem.at[first + d], self.recv_sem.at[first + d], peer)
                for d, peer in enumerate(peers)]

    def begin(self):
        ref, index = self.local
        self.slots1[self.at.z] = ref[index]
        for copy in self.copies(False):
            copy.start()

    def over_plane(self):
        for copy in self.copies(False):
            copy.wait()
        self.slots2[self.at.low] = jnp.sum(self.slots1[...], axis=0)
        for copy in self.copies(True):
            copy.start()

    def arrive(self):
        for copy in self.copies(True):
            copy.wait()
        ref, index = self.total
        ref[index] = jnp.sum(self.slots2[...], axis=0)


def quick_scratch(rows, cols):
    return [
        pltpu.VMEM((LINE, rows, cols), F32),
        pltpu.VMEM((CUBE, rows, cols), F32),
        DMA_SEM((LINE + CUBE,)),
        DMA_SEM((LINE + CUBE,)),
    ]


def sums_scratch(rows, cols):
    return [
        pltpu.VMEM((rows, cols // 2), F32),
        pltpu.VMEM((4, rows, cols // 2), F32),
        pltpu.VMEM((4, rows, cols // 2), F32),
        DMA_SEM((8,)),
        DMA_SEM((8,)),
    ]


class Ring:
    def __init__(self, at, total, part, recv0, kept, snd1, recv1, snd2, recv2, snd3, recv3, send_sem, recv_sem, credit):
        self.at, self.total, self.slots = at, total, kept.shape[0]
        self.part, self.recv0, self.kept = part, recv0, kept
        self.snd1, self.recv1, self.snd2, self.recv2, self.snd3, self.recv3 = snd1, recv1, snd2, recv2, snd3, recv3
        self.send_sem, self.recv_sem, self.credit = send_sem, recv_sem, credit
        self.half = snd1.shape[-1]
        self.copies = {}
        self.peers = [at.partner, at.x_peer, at.y_peer, at.y_peer, at.x_peer] + at.z_peers
        self.givers = self.peers[:5] + at.z_peers[::-1]
        self.own = [at.y, at.x]

    def cols(self, half):
        return pl.ds(half * self.half, self.half)

    def depth(self, stage):
        return self.slots if stage else self.part.shape[0]

    def start(self, q, stage, src, dst, peer):
        copy = remote(src, dst, self.send_sem.at[q % self.slots, stage], self.recv_sem.at[q % self.slots, stage], peer)
        copy.start()
        self.copies[q, stage] = copy

    def send(self, q, stage, src, dst):
        depth = self.depth(stage)
        if q >= depth:
            pl.semaphore_wait(self.credit.at[q % depth, stage], 1)
        self.start(q, stage, src, dst, self.peers[stage])

    def give(self, q, stage):
        depth = self.depth(stage)
        if q + depth < self.total:
            pl.semaphore_signal(self.credit.at[q % depth, stage], inc=1, device_id=(self.givers[stage],),
                                device_id_type=MESH)

    def wait(self, q, stage):
        self.copies.pop((q, stage)).wait()

    def pair(self, q):
        s = q % self.depth(0)
        self.send(q, 0, self.part.at[s, :, :, :, 1 - self.at.core], self.recv0.at[s])

    def first(self, q):
        at, s, j = self.at, q % self.depth(0), q % self.slots
        self.wait(q, 0)

        @loop(LINE)
        def _(z):
            for half in PAIR:
                cols = self.cols(half)
                for k in PAIR:
                    (y, x), (oy, ox) = ((at.y, k), (1 - at.y, k)) if half else ((k, at.x), (k, 1 - at.x))
                    self.snd1[j, half, z, k] = (
                        self.part[s, z, oy, ox, at.core, :, cols] + self.recv0[s, z, oy, ox, :, cols]).astype(BF16)
                    self.kept[j, half, z, k] = self.part[s, z, y, x, at.core, :, cols] + self.recv0[s, z, y, x, :, cols]

        self.give(q, 0)
        for half in PAIR:
            self.send(q, 1 + half, self.snd1.at[j, half], self.recv1.at[j, half])

    def second(self, q):
        j = q % self.slots
        for half in PAIR:
            own = self.own[half]
            self.wait(q, 1 + half)

            @loop(LINE)
            def _(z):
                self.snd2[j, half, z] = (
                    self.kept[j, half, z, 1 - own] + self.recv1[j, half, z, 1 - own].astype(F32)).astype(BF16)
                self.kept[j, half, z, own] = self.kept[j, half, z, own] + self.recv1[j, half, z, own].astype(F32)

            self.give(q, 1 + half)
            self.send(q, 3 + half, self.snd2.at[j, half], self.recv2.at[j, half])

    def summed(self, j, half, z):
        return self.kept[j, half, z, self.own[half]] + self.recv2[j, half, z].astype(F32)

    def third(self, q):
        j = q % self.slots
        for half in PAIR:
            self.wait(q, 3 + half)

        @loop(len(OTHERS))
        def _(d):
            z = lax.rem(self.at.z + d + 1, LINE)
            for half in PAIR:
                self.snd3[j, d, :, self.cols(half)] = self.summed(j, half, z).astype(BF16)

        for d in OTHERS:
            self.send(q, 5 + d, self.snd3.at[j, d], self.recv3.at[j, d])

    def last(self, q):
        j = q % self.slots
        totals = [self.summed(j, half, self.at.z) for half in PAIR]
        for d in OTHERS:
            self.wait(q, 5 + d)
            totals = [total + self.recv3[j, d, :, self.cols(half)].astype(F32) for half, total in enumerate(totals)]
            self.give(q, 5 + d)
        for half in PAIR:
            self.give(q, 3 + half)
        return totals


def ring_scratch(slots, rows, width):
    half = width // 2
    return [
        pltpu.VMEM((2, 4, 2, 2, 2, rows, width), F32),
        pltpu.VMEM((2, 4, 2, 2, rows, width), F32),
        pltpu.VMEM((slots, 2, 4, 2, rows, half), F32),
    ] + [pltpu.VMEM((slots, 2, 4, 2, rows, half), BF16)] * 2 + [pltpu.VMEM((slots, 2, 4, rows, half), BF16)] * 2 + [
        pltpu.VMEM((slots, 3, rows, width), BF16)] * 2 + [DMA_SEM((slots, 16))] * 2 + [
        pltpu.SemaphoreType.REGULAR((slots, 8))]


CHUNKS = 8
RING = 12
SUMS = 5
QUICK = 4
SPREAD_LAGS = (1, 2, 3, 4, 6, 7, 8, 9)
RING_LAGS = (1, 3, 5, 8)
INPUT_STEPS = (((0, 1), (2,)), ((3,), (4,)), ((5,), (6,)), ((7,), ()), ((), ()))


def step_kernel(
        total_rows, lam_ref, feat_a, feat_b, w_one, w_two, w_three, gain_one, shift_one, gain_two, shift_two,
        grad_w_three, grad_w_two, grad_w_one, loss_total, total_two, total_one, saved_act, saved_norm,
        grad, pre, wide, turned, weight, normed, act, sides, side_sums, local, embed_local, embed_total, loss_local, mean_col, turned_sums, by_row, scales,
        wide_sem, w_sem, load_sem, out_sem, *scratch):
    at = Place()
    ring = Ring(at, 4 * CHUNKS, *scratch[:RING])
    rows_dev, dim = grad.shape
    width = dim // CHUNKS
    view_rows = rows_dev // 2
    block_rows = min(64, view_rows)
    quarter = dim // 4
    count = 1.0 / total_rows
    weights = [w_one, w_two, w_three]
    gains, shifts = [gain_one, gain_two], [shift_one, shift_two]
    outs = [grad_w_three, grad_w_two, grad_w_one]
    totals = [embed_total, total_two, total_one]
    views = [pl.ds(v * view_rows, view_rows) for v in PAIR]
    rest = list(scratch[RING:])

    def take(number):
        taken, rest[:] = rest[:number], rest[number:]
        return taken

    top = pl.ds(0, 2)
    side = [[QuickSums(at, (sides, (layer, v, top)), (side_sums, (layer, v, top)), *take(QUICK)) for v in PAIR] for layer in OTHERS]
    pair_sums = QuickSums(at, (sides, (0, 0)), (side_sums, (0, 0)), *take(QUICK))
    loss_sums = QuickSums(at, (loss_local, ...), (loss_total, ...), *take(QUICK))
    sums = [[Sums(at, (embed_local, ()), (embed_total, ()), *take(SUMS))]]
    for layer in PAIR:
        sums.append([Sums(at, (local, (layer, h)), (totals[layer + 1], (h,)), *take(SUMS)) for h in PAIR])

    def load(src, dst, k):
        copy = pltpu.make_async_copy(src, dst, load_sem.at[k])
        copy.start()
        return copy

    def wide_copy(layer, n):
        cols = pl.ds(pl.multiple_of(n * width, width), width)
        return pltpu.make_async_copy(weights[layer].at[:, :, :, :, :, cols], wide.at[n], wide_sem.at[n])

    feats = [load(feat_a, normed.at[0, views[0]], 0)]
    lead = 3
    for n in range(lead):
        wide_copy(0, n).start()
    feats.append(load(feat_b, normed.at[0, views[1]], 1))
    puts = {}

    def put(name, v, src, dst, k):
        copy = pltpu.make_async_copy(src, dst, out_sem.at[k, v])
        copy.start()
        puts[name, v] = copy

    def drain(*names):
        for name in names:
            for v in PAIR:
                puts.pop((name, v)).wait()

    def matmul(layer, v, hook, step):
        @loop(CHUNKS)
        def _(n):
            if step:
                pl.when(n == hook)(step)
            if v == 0:
                if layer == 0:
                    pl.when(n + lead < CHUNKS)(lambda: wide_copy(0, n + lead).start())
                wide_copy(layer, n).wait()
            elif layer < 2:
                pl.when(n > 0)(lambda: wide_copy(layer + 1, n - 1).start())
            cols = pl.ds(pl.multiple_of(n * width, width), width)
            out = jnp.dot(normed[layer % 2, views[v]], wide[n].reshape(dim, width), preferred_element_type=F32)
            pre[views[v], cols] = out
            sides[layer, v, FIRST, cols] = col_sum(out)
            sides[layer, v, SECOND, cols] = col_sum(out * out)

        if v and layer < 2:
            wide_copy(layer + 1, CHUNKS - 1).start()
        side[layer][v].begin()

    def normalise(layer, v):
        side[layer][v].arrive()
        mean = side_sums[layer, v, FIRST, :] / total_rows
        inv = lax.rsqrt(side_sums[layer, v, SECOND, :] / total_rows - mean * mean + NORM_EPS)
        scales[2 - layer, v:v + 1, :] = gains[layer][...] * inv if layer < 2 else inv
        sides[layer, v, FIRST, :] = mean
        sides[layer, v, SECOND, :] = inv

        @loop(CHUNKS)
        def _(n):
            cols = pl.ds(pl.multiple_of(n * width, width), width)
            mean, inv = sides[layer, v, FIRST, cols], sides[layer, v, SECOND, cols]
            if layer < 2:
                gain, shift = gains[layer][:, cols], shifts[layer][:, cols]

            @loop(view_rows // block_rows)
            def _(r):
                rows = pl.ds(pl.multiple_of(v * view_rows + r * block_rows, block_rows), block_rows)
                value = (pre[rows, cols] - mean) * inv
                if layer < 2:
                    grad[rows, cols] = value.astype(BF16)
                    value = jnp.maximum(gain * value + shift, 0.0)
                normed[(layer + 1) % 2, rows, cols] = value.astype(BF16)

        if layer < 2:
            put(("act", layer), v, normed.at[(layer + 1) % 2, views[v]], saved_act.at[layer, views[v]], layer)
            put(("norm", layer), v, grad.at[views[v]], saved_norm.at[layer, views[v]], 2)

    def turn(src, dst, first, v):
        part = view_rows // 2

        @loop(CHUNKS)
        def _(n):
            cols = pl.ds(pl.multiple_of(n * width, width), width)
            for k in PAIR:
                block = src[pl.ds(v * view_rows + k * part, part), cols].T
                dst[first + 2 * v + k, lax.div(n, 2), lax.rem(n, 2)] = block.reshape(dst.shape[3:])

    enter(at.z_peers + at.cube_peers)
    feats[0].wait()
    matmul(0, 0, 0, None)
    feats[1].wait()
    matmul(0, 1, CHUNKS - 1, side[0][0].over_plane)
    for v in PAIR:
        turn(normed.at[0], turned, 0, v)
    normalise(0, 0)
    for layer in PAIR:
        matmul(layer + 1, 0, 0, side[layer][1].over_plane)
        normalise(layer, 1)
        matmul(layer + 1, 1, 5, side[layer + 1][0].over_plane)
        if layer == 0:
            drain(("norm", 0))
        else:
            drain(("act", 0))
        normalise(layer + 1, 0)
    side[2][1].over_plane()
    normalise(2, 1)

    drain(("act", 1), ("norm", 1))
    loads = {("act", 0): load(saved_act.at[1], act, 0)}
    slots = weight.shape[0]
    w_loads = {}

    def load_weight(layer, n):
        copy = pltpu.make_async_copy(weights[2 - layer].at[n // 2, n % 2], weight.at[n % slots], w_sem.at[n % slots])
        copy.start()
        w_loads[layer, n] = copy

    for n in range(slots):
        load_weight(0, n)

    lam = lam_ref[0]
    lane = 128
    place = (at.z, at.y, at.x, at.core)
    block_rows_dev = ring.snd1.shape[-2]
    first_row = (((at.z * 2 + at.y) * 2 + at.x) * 2 + at.core) * block_rows_dev

    def pair_rows():
        @loop(CHUNKS)
        def _(n):
            cols = pl.ds(pl.multiple_of(n * width, width), width)
            one, two = [normed[1, views[v], cols].astype(F32) for v in PAIR]
            sides[0, 0, FIRST, cols] = col_sum(one)
            sides[0, 0, SECOND, cols] = col_sum(two)
            sides[0, 0, THIRD, cols] = col_sum(one * two)
            sides[0, 0, FOURTH, cols] = jnp.zeros((1, width), F32)

        pair_sums.begin()

    block = pl.ds(pl.multiple_of(lax.div(first_row, lane) * lane, lane), lane)
    part = lax.rem(first_row, lane)

    def keep_means():
        pair_sums.arrive()
        turned_sums[...] = jnp.broadcast_to(side_sums[0, 0, FIRST, block], (lane, lane)).T
        mean_col[...] = turned_sums[pl.ds(pl.multiple_of(part, 8), block_rows_dev), :]

    def row_sums():
        for k, row in enumerate((FIRST, THIRD)):
            sums_here = col_sum(by_row[k].T)
            spread = jnp.concatenate([sums_here] * (lane // block_rows_dev), axis=1)
            position = lax.broadcasted_iota(jnp.int32, spread.shape, 1)
            mine = (position >= part) & (position < part + block_rows_dev)
            embed_local[row, :] = jnp.zeros((1, dim), F32)
            embed_local[row, block] = jnp.where(mine, spread, 0.0)


    def correlate(q):
        @loop(LINE)
        def _(z):
            rows = pl.ds(pl.multiple_of(z * quarter, quarter), quarter)
            out = lax.dot_general(normed[1, views[0], rows], normed[1, views[1], pl.ds(q * width, width)],
                                  DEPTH_DIMS, preferred_element_type=F32)
            ring.part[q % 2, z] = out.reshape(ring.part.shape[2:])

        ring.pair(q)

    def spread_line(q):
        for half, total in enumerate(ring.last(q)):
            start = q * width + half * ring.half
            row = first_row + lax.broadcasted_iota(jnp.int32, total.shape, 0)
            col = start + lax.broadcasted_iota(jnp.int32, total.shape, 1)
            diag = row == col
            cols = pl.ds(start, ring.half)
            total = jnp.where(diag, side_sums[0, 0, THIRD, cols], total)
            corr = total * count
            gap = 1.0 - corr
            loss_local[:, cols] = col_sum(jnp.where(diag, gap * gap, lam * corr * corr))
            slope = (jnp.where(diag, -2.0 * gap, 2.0 * lam * corr) * count).astype(BF16)
            wide[(q, *place, ALL, ring.cols(half))] = slope
            slope = slope.astype(F32)
            embed_local[SECOND, cols] = col_sum(slope * mean_col[:, :ring.half])
            embed_local[FOURTH, cols] = col_sum(slope * total)
            terms = [slope * side_sums[0, 0, SECOND, cols], slope * total]
            for k, term in enumerate(terms):
                by_row[k] = by_row[k] + term if q or half else term
        here = wide.at[(q, *place)]
        for d in OTHERS:
            ring.start(q, 8 + d, here, here, at.z_peers[d])

    def spread_one(q):
        for d in OTHERS:
            ring.wait(q, 8 + d)
        for half, peer in enumerate((at.y_peer, at.x_peer)):
            here = wide.at[q, :, at.y, at.x, at.core, :, ring.cols(half)]
            ring.start(q, 11 + half, here, here, peer)

    def spread_two(q):
        for half, peer in enumerate((at.x_peer, at.y_peer)):
            ring.wait(q, 11 + half)
            here = wide.at[(q, ALL, *((at.y, ALL) if half else (ALL, at.x)), at.core, ALL,
                            ring.cols(half))]
            ring.start(q, 13 + half, here, here, peer)

    def spread_pair(q):
        for half in PAIR:
            ring.wait(q, 13 + half)
        here = wide.at[q, :, :, :, at.core]
        ring.start(q, 15, here, here, at.partner)

    def embed_grad(q):
        ring.wait(q, 15)
        cols = pl.ds(q * width, width)
        pre[views[1], cols] = jnp.dot(normed[1, views[0]], wide[q].reshape(dim, width), preferred_element_type=F32)

        @loop(LINE)
        def _(z):
            into = pl.ds(pl.multiple_of(z * quarter, quarter), quarter)
            rows = lax.dot_general(normed[1, views[1], cols], wide[q, z].reshape(quarter, width), LANE_DIMS,
                                   preferred_element_type=F32)
            pre[views[0], into] = rows if q == 0 else pre[views[0], into] + rows

    first_sums = sums[0][0]
    relay = [first_sums.over_plane, first_sums.over_line, first_sums.over_pair]
    steps = (ring.first, ring.second, ring.third, spread_line, spread_one, spread_two, spread_pair, embed_grad)
    for t in range(CHUNKS + SPREAD_LAGS[-1]):
        if t < CHUNKS:
            correlate(t)
        if t == 0:
            pair_rows()
        if t == 1:
            pair_sums.over_plane()
        if t == 3:
            keep_means()
        since = t - CHUNKS - SPREAD_LAGS[3]
        if since == 0:
            row_sums()
            first_sums.begin()
        if 0 < since <= len(relay):
            relay[since - 1]()
        for step, lag in zip(steps, SPREAD_LAGS):
            if 0 <= t - lag < CHUNKS:
                step(t - lag)
                if step == embed_grad and t - lag == LINE:
                    for v in PAIR:
                        turn(normed.at[0], wide, 0, v)
                    loads["norm", 0] = load(saved_norm.at[1], normed.at[0], 2)

    loss_sums.begin()

    def finish_grad(layer, j):
        cols = pl.ds(j * width, width)
        total, first = (embed_total, j * width) if layer == 0 else (
            totals[layer].at[j // (CHUNKS // 2)], (j % (CHUNKS // 2)) * width)
        sel = pl.ds(first, width)
        for v in PAIR:
            mean0 = total[v:v + 1, sel] * count
            mean1 = total[2 + v:3 + v, sel] * count
            scale = scales[layer, v:v + 1, cols]

            @loop(view_rows // block_rows)
            def _(r):
                rows = pl.ds(pl.multiple_of(v * view_rows + r * block_rows, block_rows), block_rows)
                xhat = normed[(layer + 1) % 2, rows, cols].astype(F32)
                grad[rows, cols] = (scale * (pre[rows, cols] - (mean0 + xhat * mean1))).astype(BF16)

    def weight_grad(layer, j):
        cols = pl.ds(j * width, width)
        q = (layer + 1) * CHUNKS + j

        @loop(LINE)
        def _(z):
            source, first = (turned, 0) if layer == 2 else (wide, LINE * layer)
            feed = jnp.concatenate([source[first + k, z].reshape(quarter, -1) for k in range(LINE)], axis=1)
            out = jnp.dot(feed, grad[:, cols], preferred_element_type=F32)
            ring.part[q % 2, z] = out.reshape(ring.part.shape[2:])

        ring.pair(q)

    def input_grad(layer, n):
        cols = pl.ds(n * width, width)
        w_loads[layer, n].wait()
        half = local.at[layer, n // (CHUNKS // 2)]
        sel = pl.ds((n % (CHUNKS // 2)) * width, width)

        @loop(2)
        def _(v):
            rows = pl.ds(pl.multiple_of(v * view_rows, view_rows), view_rows)
            out = lax.dot_general(grad[rows, :], weight[n % slots].reshape(width, dim), LANE_DIMS,
                                  preferred_element_type=F32)
            out = jnp.where(act[rows, cols] > 0, out, 0.0)
            pre[rows, cols] = out
            half[pl.ds(v, 1), sel] = col_sum(out)
            half[pl.ds(2 + v, 1), sel] = col_sum(out * normed[layer % 2, rows, cols].astype(F32))

        if n + slots < CHUNKS:
            load_weight(layer, n + slots)

    def serve(t):
        for step, lag in zip((ring.first, ring.second, ring.third, ring.last), RING_LAGS):
            k = t - lag
            if 0 <= k < 3 * CHUNKS:
                blocks = step(CHUNKS + k)
        if 0 <= k < 3 * CHUNKS:
            for half, block in enumerate(blocks):
                outs[k // CHUNKS][:, pl.ds((k % CHUNKS) * width + half * ring.half, ring.half)] = block

    for layer in OTHERS:
        old, new = sums[layer], sums[layer + 1] if layer < 2 else None
        old[0].arrive()
        for j in range(CHUNKS):
            if j == 3 and new:
                loads["norm", layer].wait()
                if layer == 0:
                    loads["act", layer].wait()
            if j < 3:
                finish_grad(layer, j)
            elif new:
                for n in INPUT_STEPS[j - 3][0]:
                    input_grad(layer, n)
            if new and j == 4:
                new[0].begin()
            if new and j == 5:
                new[0].over_line()
            if new and j == 6:
                new[1].begin()
                new[0].over_pair()
                if layer == 0:
                    loads["act", 1] = load(saved_act.at[0], act, 0)
                    for n in range(slots):
                        load_weight(1, n)
            weight_grad(layer, j)
            if j == 0 and layer:
                old[1].over_pair()
            if j == 2:
                finish_grad(layer, 3)
                if layer:
                    old[1].arrive()
                for k in range(CHUNKS // 2, CHUNKS):
                    finish_grad(layer, k)
                if layer == 0:
                    loads["norm", 1] = load(saved_norm.at[0], normed.at[1], 1)
            if new and j > 2:
                if j == 4:
                    new[0].over_plane()
                for n in INPUT_STEPS[j - 3][1]:
                    input_grad(layer, n)
                if j == 6:
                    new[1].over_plane()
                if j == 7:
                    new[1].over_line()
            serve(layer * CHUNKS + j)
        if layer == 0:
            loads["act", 1].wait()
            for v in PAIR:
                turn(act, wide, LINE, v)
            loss_sums.over_plane()
    for k in range(RING_LAGS[-1]):
        serve(3 * CHUNKS + k)
    loss_sums.arrive()


def step(total_rows, vmem, lam, feat_a, feat_b, weights, vectors):
    view_rows, dim = feat_a.shape
    rows, width, blocks = 2 * view_rows, dim // CHUNKS, dim // 32
    hbm = pl.BlockSpec(memory_space=pl.ANY)
    vm = pl.BlockSpec(memory_space=pltpu.VMEM)
    cube = (LINE, 2, 2, 2, blocks)
    scratch = [
        pltpu.VMEM((rows, dim), BF16),
        pltpu.VMEM((rows, dim), F32),
        pltpu.VMEM((CHUNKS, *cube, width), BF16),
        pltpu.VMEM((LINE, *cube, view_rows // 2), BF16),
        pltpu.VMEM((3, 2, 2, blocks, dim), BF16),
        pltpu.VMEM((2, rows, dim), BF16),
        pltpu.VMEM((rows, dim), BF16),
        pltpu.VMEM((3, 2, 4, dim), F32),
        pltpu.VMEM((3, 2, 4, dim), F32),
        pltpu.VMEM((2, 2, 4, dim // 2), F32),
        pltpu.VMEM((4, dim), F32),
        pltpu.VMEM((4, dim), F32),
        pltpu.VMEM((1, dim), F32),
        pltpu.VMEM((blocks, 128), F32),
        pltpu.VMEM((128, 128), F32),
        pltpu.VMEM((2, blocks, width // 2), F32),
        pltpu.VMEM((3, 2, dim), F32),
        DMA_SEM((CHUNKS,)),
        DMA_SEM((3,)),
        DMA_SEM((3,)),
        DMA_SEM((3, 2)),
    ] + ring_scratch(CHUNKS, blocks, width)
    for _ in range(6):
        scratch += quick_scratch(2, dim)
    scratch += quick_scratch(4, dim) + quick_scratch(1, dim) + sums_scratch(4, dim)
    for _ in range(4):
        scratch += sums_scratch(4, dim // 2)
    halves = jax.ShapeDtypeStruct((2, 4, dim // 2), F32)
    saved = jax.ShapeDtypeStruct((2, rows, dim), BF16)
    return pl.pallas_call(
        functools.partial(step_kernel, total_rows),
        out_shape=[jax.ShapeDtypeStruct((blocks, dim), F32)] * 3 + [
            jax.ShapeDtypeStruct((1, dim), F32), halves, halves, saved, saved],
        in_specs=[pl.BlockSpec(memory_space=pltpu.SMEM)] + [hbm] * 5 + [vm] * 4,
        out_specs=[vm] * 6 + [hbm] * 2,
        scratch_shapes=scratch,
        compiler_params=pltpu.CompilerParams(collective_id=0, has_side_effects=True, vmem_limit_bytes=vmem),
    )(lam.reshape(1), feat_a, feat_b, *[weight.reshape(*cube, dim) for weight in weights],
      *[value.reshape(1, dim) for value in vectors])


def finish_kernel(total_two, total_one, loss_cols, *refs):
    gain_one, shift_one, gain_two, shift_two, loss = refs[6:]
    for grad, out in zip(refs[:3], refs[3:6]):
        out[...] = grad[...]
    half = total_two.shape[-1]
    for total, gain, shift in ((total_two, gain_two, shift_two), (total_one, gain_one, shift_one)):
        for h in PAIR:
            cols = pl.ds(h * half, half)
            shift[:, cols] = total[h, FIRST] + total[h, SECOND]
            gain[:, cols] = total[h, THIRD] + total[h, FOURTH]
    loss[...] = jnp.sum(loss_cols[...], axis=1, keepdims=True)


def finish(total_two, total_one, loss_cols, grads):
    vm = pl.BlockSpec(memory_space=pltpu.VMEM)
    row = jax.ShapeDtypeStruct((1, loss_cols.shape[1]), F32)
    outs = pl.pallas_call(
        finish_kernel,
        out_shape=[jax.ShapeDtypeStruct(grad.shape, F32) for grad in grads] + [row] * 4 + [jax.ShapeDtypeStruct((1, 1), F32)],
        in_specs=[vm] * 6,
        out_specs=[vm] * 8,
    )(total_two, total_one, loss_cols, *grads)
    return outs[:3], [row.reshape(-1) for row in outs[3:7]], outs[7].reshape(())


def solution(mesh):
    shards = mesh.shape["data"]

    def local_step(h_a, h_b, w_one, w_two, w_three, gain_one, shift_one, gain_two, shift_two, lam_off):
        rows_dev = h_a.shape[0]
        total_rows = rows_dev * shards
        grad_w_three, grad_w_two, grad_w_one, loss_cols, total_two, total_one = step(
            total_rows, 67000000, lam_off, h_a, h_b, (w_one, w_two, w_three),
            (gain_one, shift_one, gain_two, shift_two))[:6]
        grads, vectors, loss_total = finish(total_two, total_one, loss_cols, [grad_w_one, grad_w_two, grad_w_three])
        return (loss_total, *grads, *vectors)

    row_spec = P("data", None)
    whole_mat = P(None, None)
    whole_vec = P(None)
    return jax.shard_map(
        local_step, mesh=mesh,
        in_specs=(row_spec, row_spec, whole_mat, whole_mat, whole_mat,
                  whole_vec, whole_vec, whole_vec, whole_vec, P()),
        out_specs=(P(), row_spec, row_spec, row_spec, whole_vec, whole_vec, whole_vec, whole_vec),
        check_vma=False)
```

```python
import functools

import jax
import jax.numpy as jnp
from jax import lax
from jax.experimental import pallas as pl
from jax.experimental.pallas import tpu as pltpu
from jax.sharding import PartitionSpec as P

NORM_EPS = 1e-5
MESH = pl.DeviceIdType.MESH
F32 = jnp.float32
BF16 = jnp.bfloat16


ALL = slice(None)
FIRST, SECOND, THIRD, FOURTH = [slice(k, k + 1) for k in range(4)]
PAIR = range(2)
OTHERS = range(3)
LINE = 4
CUBE = 8
DEPTH_DIMS = (((0,), (0,)), ((), ()))
LANE_DIMS = (((1,), (1,)), ((), ()))
DMA_SEM = pltpu.SemaphoreType.DMA


def loop(count):
    return pl.loop(0, count)


def col_sum(values):
    return jnp.sum(values, axis=0, keepdims=True)


class Place:
    def __init__(self):
        me = lax.axis_index("data")
        self.core = lax.rem(me, 2)
        self.x = lax.rem(lax.div(me, 2), 2)
        self.y = lax.rem(lax.div(me, 4), 2)
        self.z = lax.div(me, 8)
        self.plane = lax.rem(lax.div(me, 2), 4)
        self.partner = me + 1 - 2 * self.core
        self.x_peer = me + 2 - 4 * self.x
        self.y_peer = me + 4 - 8 * self.y
        self.low = lax.rem(me, CUBE)
        self.others = [lax.rem(self.z + d + 1, LINE) for d in OTHERS]
        self.z_peers = [z * CUBE + self.low for z in self.others]
        self.plane_peers = [self.z * CUBE + lax.rem(self.plane + d + 1, LINE) * 2 + self.core for d in OTHERS]
        self.cube_peers = [self.z * CUBE + lax.rem(self.low + d + 1, CUBE) for d in range(CUBE - 1)]
        self.near = [self.partner] + self.plane_peers + self.z_peers


def enter(peers):
    barrier = pltpu.get_barrier_semaphore()
    for peer in peers:
        pl.semaphore_signal(barrier, inc=1, device_id=(peer,), device_id_type=MESH)
    pl.semaphore_wait(barrier, len(peers))


def remote(src, dst, send_sem, recv_sem, peer):
    return pltpu.make_async_remote_copy(
        src_ref=src, dst_ref=dst, send_sem=send_sem, recv_sem=recv_sem,
        device_id=(peer,), device_id_type=MESH)


class Sums:
    def __init__(self, at, local, total, recv0, slots1, slots2, send_sem, recv_sem):
        self.at, self.refs = at, (local, total)
        self.recv0, self.slots1, self.slots2 = recv0, slots1, slots2
        self.send_sem, self.recv_sem = send_sem, recv_sem
        self.half = recv0.shape[-1]
        self.mine = pl.multiple_of(at.core * self.half, 128)
        self.theirs = pl.multiple_of((1 - at.core) * self.half, 128)

    def pick(self, k, first):
        ref, index = self.refs[k]
        return ref.at[(*index, ALL, pl.ds(first, self.half))]

    def copies(self, stage):
        at = self.at
        if stage == 0:
            pairs = [(0, self.pick(0, self.theirs), self.recv0, at.partner)]
        elif stage == 1:
            here = self.slots1.at[at.plane]
            pairs = [(1 + d, here, here, at.plane_peers[d]) for d in OTHERS]
        elif stage == 2:
            here = self.slots2.at[at.z]
            pairs = [(4 + d, here, here, at.z_peers[d]) for d in OTHERS]
        else:
            here = self.pick(1, self.mine)
            pairs = [(7, here, here, at.partner)]
        return [remote(src, dst, self.send_sem.at[k], self.recv_sem.at[k], peer) for k, src, dst, peer in pairs]

    def send(self, stage):
        for copy in self.copies(stage):
            copy.start()

    def arrive(self, stage=3):
        for copy in self.copies(stage):
            copy.wait()

    def begin(self):
        self.send(0)

    def over_plane(self):
        self.arrive(0)
        self.slots1[self.at.plane] = self.pick(0, self.mine)[...] + self.recv0[...]
        self.send(1)

    def over_line(self):
        self.arrive(1)
        self.slots2[self.at.z] = jnp.sum(self.slots1[...], axis=0)
        self.send(2)

    def over_pair(self):
        self.arrive(2)
        self.pick(1, self.mine)[...] = jnp.sum(self.slots2[...], axis=0)
        self.send(3)


class QuickSums:
    def __init__(self, at, local, total, slots1, slots2, send_sem, recv_sem):
        self.at, self.local, self.total = at, local, total
        self.slots1, self.slots2 = slots1, slots2
        self.send_sem, self.recv_sem = send_sem, recv_sem

    def copies(self, across):
        at = self.at
        if across:
            here, peers, first = self.slots2.at[at.low], at.cube_peers, len(at.z_peers)
        else:
            here, peers, first = self.slots1.at[at.z], at.z_peers, 0
        return [remote(here, here, self.send_sem.at[first + d], self.recv_sem.at[first + d], peer)
                for d, peer in enumerate(peers)]

    def begin(self):
        ref, index = self.local
        self.slots1[self.at.z] = ref[index]
        for copy in self.copies(False):
            copy.start()

    def over_plane(self):
        for copy in self.copies(False):
            copy.wait()
        self.slots2[self.at.low] = jnp.sum(self.slots1[...], axis=0)
        for copy in self.copies(True):
            copy.start()

    def arrive(self):
        for copy in self.copies(True):
            copy.wait()
        ref, index = self.total
        ref[index] = jnp.sum(self.slots2[...], axis=0)


def quick_scratch(rows, cols):
    return [
        pltpu.VMEM((LINE, rows, cols), F32),
        pltpu.VMEM((CUBE, rows, cols), F32),
        DMA_SEM((LINE + CUBE,)),
        DMA_SEM((LINE + CUBE,)),
    ]


def sums_scratch(rows, cols):
    return [
        pltpu.VMEM((rows, cols // 2), F32),
        pltpu.VMEM((4, rows, cols // 2), F32),
        pltpu.VMEM((4, rows, cols // 2), F32),
        DMA_SEM((8,)),
        DMA_SEM((8,)),
    ]


class Ring:
    def __init__(self, at, total, part, recv0, kept, snd1, recv1, snd2, recv2, snd3, recv3, send_sem, recv_sem, credit):
        self.at, self.total, self.slots = at, total, kept.shape[0]
        self.part, self.recv0, self.kept = part, recv0, kept
        self.snd1, self.recv1, self.snd2, self.recv2, self.snd3, self.recv3 = snd1, recv1, snd2, recv2, snd3, recv3
        self.send_sem, self.recv_sem, self.credit = send_sem, recv_sem, credit
        self.half = snd1.shape[-1]
        self.copies = {}
        self.peers = [at.partner, at.x_peer, at.y_peer, at.y_peer, at.x_peer] + at.z_peers
        self.givers = self.peers[:5] + at.z_peers[::-1]
        self.own = [at.y, at.x]

    def cols(self, half):
        return pl.ds(half * self.half, self.half)

    def depth(self, stage):
        return self.slots if stage else self.part.shape[0]

    def start(self, q, stage, src, dst, peer):
        copy = remote(src, dst, self.send_sem.at[q % self.slots, stage], self.recv_sem.at[q % self.slots, stage], peer)
        copy.start()
        self.copies[q, stage] = copy

    def send(self, q, stage, src, dst):
        depth = self.depth(stage)
        if q >= depth:
            pl.semaphore_wait(self.credit.at[q % depth, stage], 1)
        self.start(q, stage, src, dst, self.peers[stage])

    def give(self, q, stage):
        depth = self.depth(stage)
        if q + depth < self.total:
            pl.semaphore_signal(self.credit.at[q % depth, stage], inc=1, device_id=(self.givers[stage],),
                                device_id_type=MESH)

    def wait(self, q, stage):
        self.copies.pop((q, stage)).wait()

    def pair(self, q):
        s = q % self.depth(0)
        self.send(q, 0, self.part.at[s, :, :, :, 1 - self.at.core], self.recv0.at[s])

    def first(self, q):
        at, s, j = self.at, q % self.depth(0), q % self.slots
        self.wait(q, 0)

        @loop(LINE)
        def _(z):
            for half in PAIR:
                cols = self.cols(half)
                for k in PAIR:
                    (y, x), (oy, ox) = ((at.y, k), (1 - at.y, k)) if half else ((k, at.x), (k, 1 - at.x))
                    self.snd1[j, half, z, k] = (
                        self.part[s, z, oy, ox, at.core, :, cols] + self.recv0[s, z, oy, ox, :, cols]).astype(BF16)
                    self.kept[j, half, z, k] = self.part[s, z, y, x, at.core, :, cols] + self.recv0[s, z, y, x, :, cols]

        self.give(q, 0)
        for half in PAIR:
            self.send(q, 1 + half, self.snd1.at[j, half], self.recv1.at[j, half])

    def second(self, q):
        j = q % self.slots
        for half in PAIR:
            own = self.own[half]
            self.wait(q, 1 + half)

            @loop(LINE)
            def _(z):
                self.snd2[j, half, z] = (
                    self.kept[j, half, z, 1 - own] + self.recv1[j, half, z, 1 - own].astype(F32)).astype(BF16)
                self.kept[j, half, z, own] = self.kept[j, half, z, own] + self.recv1[j, half, z, own].astype(F32)

            self.give(q, 1 + half)
            self.send(q, 3 + half, self.snd2.at[j, half], self.recv2.at[j, half])

    def summed(self, j, half, z):
        return self.kept[j, half, z, self.own[half]] + self.recv2[j, half, z].astype(F32)

    def third(self, q):
        j = q % self.slots
        for half in PAIR:
            self.wait(q, 3 + half)

        @loop(len(OTHERS))
        def _(d):
            z = lax.rem(self.at.z + d + 1, LINE)
            for half in PAIR:
                self.snd3[j, d, :, self.cols(half)] = self.summed(j, half, z).astype(BF16)

        for d in OTHERS:
            self.send(q, 5 + d, self.snd3.at[j, d], self.recv3.at[j, d])

    def last(self, q):
        j = q % self.slots
        totals = [self.summed(j, half, self.at.z) for half in PAIR]
        for d in OTHERS:
            self.wait(q, 5 + d)
            totals = [total + self.recv3[j, d, :, self.cols(half)].astype(F32) for half, total in enumerate(totals)]
            self.give(q, 5 + d)
        for half in PAIR:
            self.give(q, 3 + half)
        return totals


def ring_scratch(slots, rows, width):
    half = width // 2
    return [
        pltpu.VMEM((2, 4, 2, 2, 2, rows, width), F32),
        pltpu.VMEM((2, 4, 2, 2, rows, width), F32),
        pltpu.VMEM((slots, 2, 4, 2, rows, half), F32),
    ] + [pltpu.VMEM((slots, 2, 4, 2, rows, half), BF16)] * 2 + [pltpu.VMEM((slots, 2, 4, rows, half), BF16)] * 2 + [
        pltpu.VMEM((slots, 3, rows, width), BF16)] * 2 + [DMA_SEM((slots, 16))] * 2 + [
        pltpu.SemaphoreType.REGULAR((slots, 8))]


CHUNKS = 8
RING = 12
SUMS = 5
QUICK = 4
SPREAD_LAGS = (1, 2, 3, 4, 6, 7, 8, 9)
RING_LAGS = (1, 3, 5, 8)
INPUT_STEPS = (((0, 1), (2,)), ((3,), (4,)), ((5,), (6,)), ((7,), ()), ((), ()))


def step_kernel(
        total_rows, lam_ref, feat_a, feat_b, w_one, w_two, w_three, gain_one, shift_one, gain_two, shift_two,
        grad_w_three, grad_w_two, grad_w_one, loss_total, total_two, total_one, saved_act, saved_norm,
        grad, pre, wide, turned, weight, normed, act, sides, side_sums, local, embed_local, embed_total, loss_local, mean_col, turned_sums, by_row, scales,
        wide_sem, w_sem, load_sem, out_sem, *scratch):
    at = Place()
    ring = Ring(at, 4 * CHUNKS, *scratch[:RING])
    rows_dev, dim = grad.shape
    width = dim // CHUNKS
    view_rows = rows_dev // 2
    block_rows = min(64, view_rows)
    quarter = dim // 4
    count = 1.0 / total_rows
    weights = [w_one, w_two, w_three]
    gains, shifts = [gain_one, gain_two], [shift_one, shift_two]
    outs = [grad_w_three, grad_w_two, grad_w_one]
    totals = [embed_total, total_two, total_one]
    views = [pl.ds(v * view_rows, view_rows) for v in PAIR]
    rest = list(scratch[RING:])

    def take(number):
        taken, rest[:] = rest[:number], rest[number:]
        return taken

    top = pl.ds(0, 2)
    side = [[QuickSums(at, (sides, (layer, v, top)), (side_sums, (layer, v, top)), *take(QUICK)) for v in PAIR] for layer in OTHERS]
    pair_sums = QuickSums(at, (sides, (0, 0)), (side_sums, (0, 0)), *take(QUICK))
    loss_sums = QuickSums(at, (loss_local, ...), (loss_total, ...), *take(QUICK))
    sums = [[Sums(at, (embed_local, ()), (embed_total, ()), *take(SUMS))]]
    for layer in PAIR:
        sums.append([Sums(at, (local, (layer, h)), (totals[layer + 1], (h,)), *take(SUMS)) for h in PAIR])

    def load(src, dst, k):
        copy = pltpu.make_async_copy(src, dst, load_sem.at[k])
        copy.start()
        return copy

    def wide_copy(layer, n):
        cols = pl.ds(pl.multiple_of(n * width, width), width)
        return pltpu.make_async_copy(weights[layer].at[:, :, :, :, :, cols], wide.at[n], wide_sem.at[n])

    feats = [load(feat_a, normed.at[0, views[0]], 0)]
    lead = 4
    for n in range(lead):
        wide_copy(0, n).start()
    feats.append(load(feat_b, normed.at[0, views[1]], 1))
    puts = {}

    def put(name, v, src, dst, k):
        copy = pltpu.make_async_copy(src, dst, out_sem.at[k, v])
        copy.start()
        puts[name, v] = copy

    def drain(*names):
        for name in names:
            for v in PAIR:
                puts.pop((name, v)).wait()

    def matmul(layer, v, hook, step):
        @loop(CHUNKS // 2)
        def _(m):
            if step:
                pl.when(m == hook)(step)
            chunks = [2 * m, 2 * m + 1]
            if v == 0:
                if layer == 0:
                    for n in chunks:
                        pl.when(n + lead < CHUNKS)(lambda n=n: wide_copy(0, n + lead).start())
                for n in chunks:
                    wide_copy(layer, n).wait()
            elif layer < 2:
                for n in chunks:
                    pl.when(m > 0)(lambda n=n: wide_copy(layer + 1, n - 2).start())
            for n in chunks:
                cols = pl.ds(pl.multiple_of(n * width, width), width)
                out = jnp.dot(normed[layer % 2, views[v]], wide[n].reshape(dim, width), preferred_element_type=F32)
                pre[views[v], cols] = out
                sides[layer, v, FIRST, cols] = col_sum(out)
                sides[layer, v, SECOND, cols] = col_sum(out * out)

        if v and layer < 2:
            for n in PAIR:
                wide_copy(layer + 1, CHUNKS - 2 + n).start()
        side[layer][v].begin()

    def normalise(layer, v):
        side[layer][v].arrive()
        mean = side_sums[layer, v, FIRST, :] / total_rows
        inv = lax.rsqrt(side_sums[layer, v, SECOND, :] / total_rows - mean * mean + NORM_EPS)
        scales[2 - layer, v:v + 1, :] = gains[layer][...] * inv if layer < 2 else inv
        sides[layer, v, FIRST, :] = mean
        sides[layer, v, SECOND, :] = inv

        @loop(CHUNKS)
        def _(n):
            cols = pl.ds(pl.multiple_of(n * width, width), width)
            mean, inv = sides[layer, v, FIRST, cols], sides[layer, v, SECOND, cols]
            if layer < 2:
                gain, shift = gains[layer][:, cols], shifts[layer][:, cols]

            @loop(view_rows // block_rows)
            def _(r):
                rows = pl.ds(pl.multiple_of(v * view_rows + r * block_rows, block_rows), block_rows)
                value = (pre[rows, cols] - mean) * inv
                if layer < 2:
                    grad[rows, cols] = value.astype(BF16)
                    value = jnp.maximum(gain * value + shift, 0.0)
                normed[(layer + 1) % 2, rows, cols] = value.astype(BF16)

        if layer < 2:
            put(("act", layer), v, normed.at[(layer + 1) % 2, views[v]], saved_act.at[layer, views[v]], layer)
            put(("norm", layer), v, grad.at[views[v]], saved_norm.at[layer, views[v]], 2)

    def turn(src, dst, first, v):
        part = view_rows // 2

        @loop(CHUNKS)
        def _(n):
            cols = pl.ds(pl.multiple_of(n * width, width), width)
            for k in PAIR:
                block = src[pl.ds(v * view_rows + k * part, part), cols].T
                dst[first + 2 * v + k, lax.div(n, 2), lax.rem(n, 2)] = block.reshape(dst.shape[3:])

    enter(at.z_peers + at.cube_peers)
    feats[0].wait()
    matmul(0, 0, 0, None)
    feats[1].wait()
    matmul(0, 1, 3, side[0][0].over_plane)
    for v in PAIR:
        turn(normed.at[0], turned, 0, v)
    normalise(0, 0)
    for layer in PAIR:
        matmul(layer + 1, 0, 0, side[layer][1].over_plane)
        normalise(layer, 1)
        matmul(layer + 1, 1, 3, side[layer + 1][0].over_plane)
        if layer == 0:
            drain(("norm", 0))
        else:
            drain(("act", 0))
        normalise(layer + 1, 0)
    side[2][1].over_plane()
    normalise(2, 1)

    drain(("act", 1), ("norm", 1))
    loads = {("act", 0): load(saved_act.at[1], act, 0)}
    slots = weight.shape[0]
    w_loads = {}

    def load_weight(layer, n):
        copy = pltpu.make_async_copy(weights[2 - layer].at[n // 2, n % 2], weight.at[n % slots], w_sem.at[n % slots])
        copy.start()
        w_loads[layer, n] = copy

    for n in range(slots):
        load_weight(0, n)

    lam = lam_ref[0]
    lane = 128
    place = (at.z, at.y, at.x, at.core)
    block_rows_dev = ring.snd1.shape[-2]
    first_row = (((at.z * 2 + at.y) * 2 + at.x) * 2 + at.core) * block_rows_dev

    def pair_rows():
        @loop(CHUNKS)
        def _(n):
            cols = pl.ds(pl.multiple_of(n * width, width), width)
            one, two = [normed[1, views[v], cols].astype(F32) for v in PAIR]
            sides[0, 0, FIRST, cols] = col_sum(one)
            sides[0, 0, SECOND, cols] = col_sum(two)
            sides[0, 0, THIRD, cols] = col_sum(one * two)
            sides[0, 0, FOURTH, cols] = jnp.zeros((1, width), F32)

        pair_sums.begin()

    block = pl.ds(pl.multiple_of(lax.div(first_row, lane) * lane, lane), lane)
    part = lax.rem(first_row, lane)

    def keep_means():
        pair_sums.arrive()
        turned_sums[...] = jnp.broadcast_to(side_sums[0, 0, FIRST, block], (lane, lane)).T
        mean_col[...] = turned_sums[pl.ds(pl.multiple_of(part, 8), block_rows_dev), :]

    def row_sums():
        for k, row in enumerate((FIRST, THIRD)):
            sums_here = col_sum(by_row[k].T)
            spread = jnp.concatenate([sums_here] * (lane // block_rows_dev), axis=1)
            position = lax.broadcasted_iota(jnp.int32, spread.shape, 1)
            mine = (position >= part) & (position < part + block_rows_dev)
            embed_local[row, :] = jnp.zeros((1, dim), F32)
            embed_local[row, block] = jnp.where(mine, spread, 0.0)


    def correlate(q):
        @loop(LINE)
        def _(z):
            rows = pl.ds(pl.multiple_of(z * quarter, quarter), quarter)
            out = lax.dot_general(normed[1, views[0], rows], normed[1, views[1], pl.ds(q * width, width)],
                                  DEPTH_DIMS, preferred_element_type=F32)
            ring.part[q % 2, z] = out.reshape(ring.part.shape[2:])

        ring.pair(q)

    def spread_line(q):
        for half, total in enumerate(ring.last(q)):
            start = q * width + half * ring.half
            row = first_row + lax.broadcasted_iota(jnp.int32, total.shape, 0)
            col = start + lax.broadcasted_iota(jnp.int32, total.shape, 1)
            diag = row == col
            cols = pl.ds(start, ring.half)
            total = jnp.where(diag, side_sums[0, 0, THIRD, cols], total)
            corr = total * count
            gap = 1.0 - corr
            loss_local[:, cols] = col_sum(jnp.where(diag, gap * gap, lam * corr * corr))
            slope = (jnp.where(diag, -2.0 * gap, 2.0 * lam * corr) * count).astype(BF16)
            wide[(q, *place, ALL, ring.cols(half))] = slope
            slope = slope.astype(F32)
            embed_local[SECOND, cols] = col_sum(slope * mean_col[:, :ring.half])
            embed_local[FOURTH, cols] = col_sum(slope * total)
            terms = [slope * side_sums[0, 0, SECOND, cols], slope * total]
            for k, term in enumerate(terms):
                by_row[k] = by_row[k] + term if q or half else term
        here = wide.at[(q, *place)]
        for d in OTHERS:
            ring.start(q, 8 + d, here, here, at.z_peers[d])

    def spread_one(q):
        for d in OTHERS:
            ring.wait(q, 8 + d)
        for half, peer in enumerate((at.y_peer, at.x_peer)):
            here = wide.at[q, :, at.y, at.x, at.core, :, ring.cols(half)]
            ring.start(q, 11 + half, here, here, peer)

    def spread_two(q):
        for half, peer in enumerate((at.x_peer, at.y_peer)):
            ring.wait(q, 11 + half)
            here = wide.at[(q, ALL, *((at.y, ALL) if half else (ALL, at.x)), at.core, ALL,
                            ring.cols(half))]
            ring.start(q, 13 + half, here, here, peer)

    def spread_pair(q):
        for half in PAIR:
            ring.wait(q, 13 + half)
        here = wide.at[q, :, :, :, at.core]
        ring.start(q, 15, here, here, at.partner)

    def embed_grad(q):
        ring.wait(q, 15)
        cols = pl.ds(q * width, width)
        pre[views[1], cols] = jnp.dot(normed[1, views[0]], wide[q].reshape(dim, width), preferred_element_type=F32)

        @loop(LINE)
        def _(z):
            into = pl.ds(pl.multiple_of(z * quarter, quarter), quarter)
            rows = lax.dot_general(normed[1, views[1], cols], wide[q, z].reshape(quarter, width), LANE_DIMS,
                                   preferred_element_type=F32)
            pre[views[0], into] = rows if q == 0 else pre[views[0], into] + rows

    first_sums = sums[0][0]
    relay = [first_sums.over_plane, first_sums.over_line, first_sums.over_pair]
    steps = (ring.first, ring.second, ring.third, spread_line, spread_one, spread_two, spread_pair, embed_grad)
    for t in range(CHUNKS + SPREAD_LAGS[-1]):
        if t < CHUNKS:
            correlate(t)
        if t == 0:
            pair_rows()
        if t == 1:
            pair_sums.over_plane()
        if t == 3:
            keep_means()
        since = t - CHUNKS - SPREAD_LAGS[3]
        if since == 0:
            row_sums()
            first_sums.begin()
        if 0 < since <= len(relay):
            relay[since - 1]()
        for step, lag in zip(steps, SPREAD_LAGS):
            if 0 <= t - lag < CHUNKS:
                step(t - lag)
                if step == embed_grad and t - lag == LINE:
                    for v in PAIR:
                        turn(normed.at[0], wide, 0, v)
                    loads["norm", 0] = load(saved_norm.at[1], normed.at[0], 2)

    loss_sums.begin()

    def finish_grad(layer, j):
        cols = pl.ds(j * width, width)
        total, first = (embed_total, j * width) if layer == 0 else (
            totals[layer].at[j // (CHUNKS // 2)], (j % (CHUNKS // 2)) * width)
        sel = pl.ds(first, width)
        for v in PAIR:
            mean0 = total[v:v + 1, sel] * count
            mean1 = total[2 + v:3 + v, sel] * count
            scale = scales[layer, v:v + 1, cols]

            @loop(view_rows // block_rows)
            def _(r):
                rows = pl.ds(pl.multiple_of(v * view_rows + r * block_rows, block_rows), block_rows)
                xhat = normed[(layer + 1) % 2, rows, cols].astype(F32)
                grad[rows, cols] = (scale * (pre[rows, cols] - (mean0 + xhat * mean1))).astype(BF16)

    def weight_grad(layer, j):
        cols = pl.ds(j * width, width)
        q = (layer + 1) * CHUNKS + j
        source, first = (turned, 0) if layer == 2 else (wide, LINE * layer)

        @loop(2)
        def _(p):
            span = pl.ds(2 * p, 2)
            feed = jnp.concatenate([source[first + k, span].reshape(2 * quarter, -1) for k in range(LINE)], axis=1)
            out = jnp.dot(feed, grad[:, cols], preferred_element_type=F32)
            ring.part[q % 2, span] = out.reshape(2, *ring.part.shape[2:])

        ring.pair(q)

    def input_grad(layer, n):
        cols = pl.ds(n * width, width)
        w_loads[layer, n].wait()
        half = local.at[layer, n // (CHUNKS // 2)]
        sel = pl.ds((n % (CHUNKS // 2)) * width, width)

        @loop(2)
        def _(v):
            rows = pl.ds(pl.multiple_of(v * view_rows, view_rows), view_rows)
            out = lax.dot_general(grad[rows, :], weight[n % slots].reshape(width, dim), LANE_DIMS,
                                  preferred_element_type=F32)
            out = jnp.where(act[rows, cols] > 0, out, 0.0)
            pre[rows, cols] = out
            half[pl.ds(v, 1), sel] = col_sum(out)
            half[pl.ds(2 + v, 1), sel] = col_sum(out * normed[layer % 2, rows, cols].astype(F32))

        if n + slots < CHUNKS:
            load_weight(layer, n + slots)

    def serve(t):
        for step, lag in zip((ring.first, ring.second, ring.third, ring.last), RING_LAGS):
            k = t - lag
            if 0 <= k < 3 * CHUNKS:
                blocks = step(CHUNKS + k)
        if 0 <= k < 3 * CHUNKS:
            for half, block in enumerate(blocks):
                outs[k // CHUNKS][:, pl.ds((k % CHUNKS) * width + half * ring.half, ring.half)] = block

    for layer in OTHERS:
        old, new = sums[layer], sums[layer + 1] if layer < 2 else None
        old[0].arrive()
        for j in range(CHUNKS):
            if j == 3 and new:
                loads["norm", layer].wait()
                if layer == 0:
                    loads["act", layer].wait()
            if j < 3:
                finish_grad(layer, j)
            elif new:
                for n in INPUT_STEPS[j - 3][0]:
                    input_grad(layer, n)
            if new and j == 4:
                new[0].begin()
            if new and j == 5:
                new[0].over_line()
            if new and j == 6:
                new[1].begin()
                new[0].over_pair()
                if layer == 0:
                    loads["act", 1] = load(saved_act.at[0], act, 0)
                    for n in range(slots):
                        load_weight(1, n)
            weight_grad(layer, j)
            if j == 0 and layer:
                old[1].over_pair()
            if j == 2:
                finish_grad(layer, 3)
                if layer:
                    old[1].arrive()
                for k in range(CHUNKS // 2, CHUNKS):
                    finish_grad(layer, k)
                if layer == 0:
                    loads["norm", 1] = load(saved_norm.at[0], normed.at[1], 1)
            if new and j > 2:
                if j == 4:
                    new[0].over_plane()
                for n in INPUT_STEPS[j - 3][1]:
                    input_grad(layer, n)
                if j == 6:
                    new[1].over_plane()
                if j == 7:
                    new[1].over_line()
            serve(layer * CHUNKS + j)
        if layer == 0:
            loads["act", 1].wait()
            for v in PAIR:
                turn(act, wide, LINE, v)
            loss_sums.over_plane()
    for k in range(RING_LAGS[-1]):
        serve(3 * CHUNKS + k)
    loss_sums.arrive()


def step(total_rows, vmem, lam, feat_a, feat_b, weights, vectors):
    view_rows, dim = feat_a.shape
    rows, width, blocks = 2 * view_rows, dim // CHUNKS, dim // 32
    hbm = pl.BlockSpec(memory_space=pl.ANY)
    vm = pl.BlockSpec(memory_space=pltpu.VMEM)
    cube = (LINE, 2, 2, 2, blocks)
    scratch = [
        pltpu.VMEM((rows, dim), BF16),
        pltpu.VMEM((rows, dim), F32),
        pltpu.VMEM((CHUNKS, *cube, width), BF16),
        pltpu.VMEM((LINE, *cube, view_rows // 2), BF16),
        pltpu.VMEM((3, 2, 2, blocks, dim), BF16),
        pltpu.VMEM((2, rows, dim), BF16),
        pltpu.VMEM((rows, dim), BF16),
        pltpu.VMEM((3, 2, 4, dim), F32),
        pltpu.VMEM((3, 2, 4, dim), F32),
        pltpu.VMEM((2, 2, 4, dim // 2), F32),
        pltpu.VMEM((4, dim), F32),
        pltpu.VMEM((4, dim), F32),
        pltpu.VMEM((1, dim), F32),
        pltpu.VMEM((blocks, 128), F32),
        pltpu.VMEM((128, 128), F32),
        pltpu.VMEM((2, blocks, width // 2), F32),
        pltpu.VMEM((3, 2, dim), F32),
        DMA_SEM((CHUNKS,)),
        DMA_SEM((3,)),
        DMA_SEM((3,)),
        DMA_SEM((3, 2)),
    ] + ring_scratch(CHUNKS, blocks, width)
    for _ in range(6):
        scratch += quick_scratch(2, dim)
    scratch += quick_scratch(4, dim) + quick_scratch(1, dim) + sums_scratch(4, dim)
    for _ in range(4):
        scratch += sums_scratch(4, dim // 2)
    halves = jax.ShapeDtypeStruct((2, 4, dim // 2), F32)
    saved = jax.ShapeDtypeStruct((2, rows, dim), BF16)
    return pl.pallas_call(
        functools.partial(step_kernel, total_rows),
        out_shape=[jax.ShapeDtypeStruct((blocks, dim), F32)] * 3 + [
            jax.ShapeDtypeStruct((1, dim), F32), halves, halves, saved, saved],
        in_specs=[pl.BlockSpec(memory_space=pltpu.SMEM)] + [hbm] * 5 + [vm] * 4,
        out_specs=[vm] * 6 + [hbm] * 2,
        scratch_shapes=scratch,
        compiler_params=pltpu.CompilerParams(collective_id=0, has_side_effects=True, vmem_limit_bytes=vmem),
    )(lam.reshape(1), feat_a, feat_b, *[weight.reshape(*cube, dim) for weight in weights],
      *[value.reshape(1, dim) for value in vectors])


def finish_kernel(total_two, total_one, loss_cols, *refs):
    gain_one, shift_one, gain_two, shift_two, loss = refs[6:]
    for grad, out in zip(refs[:3], refs[3:6]):
        out[...] = grad[...]
    half = total_two.shape[-1]
    for total, gain, shift in ((total_two, gain_two, shift_two), (total_one, gain_one, shift_one)):
        for h in PAIR:
            cols = pl.ds(h * half, half)
            shift[:, cols] = total[h, FIRST] + total[h, SECOND]
            gain[:, cols] = total[h, THIRD] + total[h, FOURTH]
    loss[...] = jnp.sum(loss_cols[...], axis=1, keepdims=True)


def finish(total_two, total_one, loss_cols, grads):
    vm = pl.BlockSpec(memory_space=pltpu.VMEM)
    row = jax.ShapeDtypeStruct((1, loss_cols.shape[1]), F32)
    outs = pl.pallas_call(
        finish_kernel,
        out_shape=[jax.ShapeDtypeStruct(grad.shape, F32) for grad in grads] + [row] * 4 + [jax.ShapeDtypeStruct((1, 1), F32)],
        in_specs=[vm] * 6,
        out_specs=[vm] * 8,
    )(total_two, total_one, loss_cols, *grads)
    return outs[:3], [row.reshape(-1) for row in outs[3:7]], outs[7].reshape(())


def solution(mesh):
    shards = mesh.shape["data"]

    def local_step(h_a, h_b, w_one, w_two, w_three, gain_one, shift_one, gain_two, shift_two, lam_off):
        rows_dev = h_a.shape[0]
        total_rows = rows_dev * shards
        grad_w_three, grad_w_two, grad_w_one, loss_cols, total_two, total_one = step(
            total_rows, 67000000, lam_off, h_a, h_b, (w_one, w_two, w_three),
            (gain_one, shift_one, gain_two, shift_two))[:6]
        grads, vectors, loss_total = finish(total_two, total_one, loss_cols, [grad_w_one, grad_w_two, grad_w_three])
        return (loss_total, *grads, *vectors)

    row_spec = P("data", None)
    whole_mat = P(None, None)
    whole_vec = P(None)
    return jax.shard_map(
        local_step, mesh=mesh,
        in_specs=(row_spec, row_spec, whole_mat, whole_mat, whole_mat,
                  whole_vec, whole_vec, whole_vec, whole_vec, P()),
        out_specs=(P(), row_spec, row_spec, row_spec, whole_vec, whole_vec, whole_vec, whole_vec),
        check_vma=False)
```

```python
import functools

import jax
import jax.numpy as jnp
from jax import lax
from jax.experimental import pallas as pl
from jax.experimental.pallas import tpu as pltpu
from jax.sharding import PartitionSpec as P

NORM_EPS = 1e-5
MESH = pl.DeviceIdType.MESH
F32 = jnp.float32
BF16 = jnp.bfloat16


ALL = slice(None)
FIRST, SECOND, THIRD, FOURTH = [slice(k, k + 1) for k in range(4)]
PAIR = range(2)
OTHERS = range(3)
LINE = 4
CUBE = 8
DEPTH_DIMS = (((0,), (0,)), ((), ()))
LANE_DIMS = (((1,), (1,)), ((), ()))
DMA_SEM = pltpu.SemaphoreType.DMA


def loop(count):
    return pl.loop(0, count)


def col_sum(values):
    return jnp.sum(values, axis=0, keepdims=True)


class Place:
    def __init__(self):
        me = lax.axis_index("data")
        self.core = lax.rem(me, 2)
        self.x = lax.rem(lax.div(me, 2), 2)
        self.y = lax.rem(lax.div(me, 4), 2)
        self.z = lax.div(me, 8)
        self.plane = lax.rem(lax.div(me, 2), 4)
        self.partner = me + 1 - 2 * self.core
        self.x_peer = me + 2 - 4 * self.x
        self.y_peer = me + 4 - 8 * self.y
        self.low = lax.rem(me, CUBE)
        self.others = [lax.rem(self.z + d + 1, LINE) for d in OTHERS]
        self.z_peers = [z * CUBE + self.low for z in self.others]
        self.plane_peers = [self.z * CUBE + lax.rem(self.plane + d + 1, LINE) * 2 + self.core for d in OTHERS]
        self.cube_peers = [self.z * CUBE + lax.rem(self.low + d + 1, CUBE) for d in range(CUBE - 1)]
        self.near = [self.partner] + self.plane_peers + self.z_peers


def enter(peers):
    barrier = pltpu.get_barrier_semaphore()
    for peer in peers:
        pl.semaphore_signal(barrier, inc=1, device_id=(peer,), device_id_type=MESH)
    pl.semaphore_wait(barrier, len(peers))


def remote(src, dst, send_sem, recv_sem, peer):
    return pltpu.make_async_remote_copy(
        src_ref=src, dst_ref=dst, send_sem=send_sem, recv_sem=recv_sem,
        device_id=(peer,), device_id_type=MESH)


class Sums:
    def __init__(self, at, local, total, recv0, slots1, slots2, send_sem, recv_sem):
        self.at, self.refs = at, (local, total)
        self.recv0, self.slots1, self.slots2 = recv0, slots1, slots2
        self.send_sem, self.recv_sem = send_sem, recv_sem
        self.half = recv0.shape[-1]
        self.mine = pl.multiple_of(at.core * self.half, 128)
        self.theirs = pl.multiple_of((1 - at.core) * self.half, 128)

    def pick(self, k, first):
        ref, index = self.refs[k]
        return ref.at[(*index, ALL, pl.ds(first, self.half))]

    def copies(self, stage):
        at = self.at
        if stage == 0:
            pairs = [(0, self.pick(0, self.theirs), self.recv0, at.partner)]
        elif stage == 1:
            here = self.slots1.at[at.plane]
            pairs = [(1 + d, here, here, at.plane_peers[d]) for d in OTHERS]
        elif stage == 2:
            here = self.slots2.at[at.z]
            pairs = [(4 + d, here, here, at.z_peers[d]) for d in OTHERS]
        else:
            here = self.pick(1, self.mine)
            pairs = [(7, here, here, at.partner)]
        return [remote(src, dst, self.send_sem.at[k], self.recv_sem.at[k], peer) for k, src, dst, peer in pairs]

    def send(self, stage):
        for copy in self.copies(stage):
            copy.start()

    def arrive(self, stage=3):
        for copy in self.copies(stage):
            copy.wait()

    def begin(self):
        self.send(0)

    def over_plane(self):
        self.arrive(0)
        self.slots1[self.at.plane] = self.pick(0, self.mine)[...] + self.recv0[...]
        self.send(1)

    def over_line(self):
        self.arrive(1)
        self.slots2[self.at.z] = jnp.sum(self.slots1[...], axis=0)
        self.send(2)

    def over_pair(self):
        self.arrive(2)
        self.pick(1, self.mine)[...] = jnp.sum(self.slots2[...], axis=0)
        self.send(3)


class QuickSums:
    def __init__(self, at, local, total, slots1, slots2, send_sem, recv_sem):
        self.at, self.local, self.total = at, local, total
        self.slots1, self.slots2 = slots1, slots2
        self.send_sem, self.recv_sem = send_sem, recv_sem

    def copies(self, across):
        at = self.at
        if across:
            here, peers, first = self.slots2.at[at.low], at.cube_peers, len(at.z_peers)
        else:
            here, peers, first = self.slots1.at[at.z], at.z_peers, 0
        return [remote(here, here, self.send_sem.at[first + d], self.recv_sem.at[first + d], peer)
                for d, peer in enumerate(peers)]

    def begin(self):
        ref, index = self.local
        self.slots1[self.at.z] = ref[index]
        for copy in self.copies(False):
            copy.start()

    def over_plane(self):
        for copy in self.copies(False):
            copy.wait()
        self.slots2[self.at.low] = jnp.sum(self.slots1[...], axis=0)
        for copy in self.copies(True):
            copy.start()

    def arrive(self):
        for copy in self.copies(True):
            copy.wait()
        ref, index = self.total
        ref[index] = jnp.sum(self.slots2[...], axis=0)


def quick_scratch(rows, cols):
    return [
        pltpu.VMEM((LINE, rows, cols), F32),
        pltpu.VMEM((CUBE, rows, cols), F32),
        DMA_SEM((LINE + CUBE,)),
        DMA_SEM((LINE + CUBE,)),
    ]


def sums_scratch(rows, cols):
    return [
        pltpu.VMEM((rows, cols // 2), F32),
        pltpu.VMEM((4, rows, cols // 2), F32),
        pltpu.VMEM((4, rows, cols // 2), F32),
        DMA_SEM((8,)),
        DMA_SEM((8,)),
    ]


class Ring:
    def __init__(self, at, total, part, recv0, kept, snd1, recv1, snd2, recv2, snd3, recv3, send_sem, recv_sem, credit):
        self.at, self.total, self.slots = at, total, kept.shape[0]
        self.part, self.recv0, self.kept = part, recv0, kept
        self.snd1, self.recv1, self.snd2, self.recv2, self.snd3, self.recv3 = snd1, recv1, snd2, recv2, snd3, recv3
        self.send_sem, self.recv_sem, self.credit = send_sem, recv_sem, credit
        self.half = snd1.shape[-1]
        self.copies = {}
        self.peers = [at.partner, at.x_peer, at.y_peer, at.y_peer, at.x_peer] + at.z_peers
        self.givers = self.peers[:5] + at.z_peers[::-1]
        self.own = [at.y, at.x]

    def cols(self, half):
        return pl.ds(half * self.half, self.half)

    def depth(self, stage):
        return self.slots if stage else self.part.shape[0]

    def start(self, q, stage, src, dst, peer):
        copy = remote(src, dst, self.send_sem.at[q % self.slots, stage], self.recv_sem.at[q % self.slots, stage], peer)
        copy.start()
        self.copies[q, stage] = copy

    def send(self, q, stage, src, dst):
        depth = self.depth(stage)
        if q >= depth:
            pl.semaphore_wait(self.credit.at[q % depth, stage], 1)
        self.start(q, stage, src, dst, self.peers[stage])

    def give(self, q, stage):
        depth = self.depth(stage)
        if q + depth < self.total:
            pl.semaphore_signal(self.credit.at[q % depth, stage], inc=1, device_id=(self.givers[stage],),
                                device_id_type=MESH)

    def wait(self, q, stage):
        self.copies.pop((q, stage)).wait()

    def pair(self, q):
        s = q % self.depth(0)
        self.send(q, 0, self.part.at[s, :, :, :, 1 - self.at.core], self.recv0.at[s])

    def first(self, q):
        at, s, j = self.at, q % self.depth(0), q % self.slots
        self.wait(q, 0)

        @loop(LINE)
        def _(z):
            for half in PAIR:
                cols = self.cols(half)
                for k in PAIR:
                    (y, x), (oy, ox) = ((at.y, k), (1 - at.y, k)) if half else ((k, at.x), (k, 1 - at.x))
                    self.snd1[j, half, z, k] = (
                        self.part[s, z, oy, ox, at.core, :, cols] + self.recv0[s, z, oy, ox, :, cols]).astype(BF16)
                    self.kept[j, half, z, k] = self.part[s, z, y, x, at.core, :, cols] + self.recv0[s, z, y, x, :, cols]

        self.give(q, 0)
        for half in PAIR:
            self.send(q, 1 + half, self.snd1.at[j, half], self.recv1.at[j, half])

    def second(self, q):
        j = q % self.slots
        for half in PAIR:
            own = self.own[half]
            self.wait(q, 1 + half)

            @loop(LINE)
            def _(z):
                self.snd2[j, half, z] = (
                    self.kept[j, half, z, 1 - own] + self.recv1[j, half, z, 1 - own].astype(F32)).astype(BF16)
                self.kept[j, half, z, own] = self.kept[j, half, z, own] + self.recv1[j, half, z, own].astype(F32)

            self.give(q, 1 + half)
            self.send(q, 3 + half, self.snd2.at[j, half], self.recv2.at[j, half])

    def summed(self, j, half, z):
        return self.kept[j, half, z, self.own[half]] + self.recv2[j, half, z].astype(F32)

    def third(self, q):
        j = q % self.slots
        for half in PAIR:
            self.wait(q, 3 + half)

        @loop(len(OTHERS))
        def _(d):
            z = lax.rem(self.at.z + d + 1, LINE)
            for half in PAIR:
                self.snd3[j, d, :, self.cols(half)] = self.summed(j, half, z).astype(BF16)

        for d in OTHERS:
            self.send(q, 5 + d, self.snd3.at[j, d], self.recv3.at[j, d])

    def last(self, q):
        j = q % self.slots
        totals = [self.summed(j, half, self.at.z) for half in PAIR]
        for d in OTHERS:
            self.wait(q, 5 + d)
            totals = [total + self.recv3[j, d, :, self.cols(half)].astype(F32) for half, total in enumerate(totals)]
            self.give(q, 5 + d)
        for half in PAIR:
            self.give(q, 3 + half)
        return totals


def ring_scratch(slots, rows, width):
    half = width // 2
    return [
        pltpu.VMEM((2, 4, 2, 2, 2, rows, width), F32),
        pltpu.VMEM((2, 4, 2, 2, rows, width), F32),
        pltpu.VMEM((slots, 2, 4, 2, rows, half), F32),
    ] + [pltpu.VMEM((slots, 2, 4, 2, rows, half), BF16)] * 2 + [pltpu.VMEM((slots, 2, 4, rows, half), BF16)] * 2 + [
        pltpu.VMEM((slots, 3, rows, width), BF16)] * 2 + [DMA_SEM((slots, 16))] * 2 + [
        pltpu.SemaphoreType.REGULAR((slots, 8))]


CHUNKS = 8
RING = 12
SUMS = 5
QUICK = 4
SPREAD_LAGS = (1, 2, 3, 4, 6, 7, 8, 9)
RING_LAGS = (1, 3, 5, 8)
INPUT_STEPS = (((0, 1), (2,)), ((3,), (4,)), ((5,), (6,)), ((7,), ()), ((), ()))


def step_kernel(
        total_rows, lam_ref, feat_a, feat_b, w_one, w_two, w_three, gain_one, shift_one, gain_two, shift_two,
        grad_w_three, grad_w_two, grad_w_one, loss_total, total_two, total_one, saved_act, saved_norm,
        grad, pre, wide, turned, weight, normed, act, sides, side_sums, local, embed_local, embed_total, loss_local, mean_col, turned_sums, by_row, scales,
        wide_sem, w_sem, load_sem, out_sem, *scratch):
    at = Place()
    ring = Ring(at, 4 * CHUNKS, *scratch[:RING])
    rows_dev, dim = grad.shape
    width = dim // CHUNKS
    view_rows = rows_dev // 2
    block_rows = min(64, view_rows)
    quarter = dim // 4
    count = 1.0 / total_rows
    weights = [w_one, w_two, w_three]
    gains, shifts = [gain_one, gain_two], [shift_one, shift_two]
    outs = [grad_w_three, grad_w_two, grad_w_one]
    totals = [embed_total, total_two, total_one]
    views = [pl.ds(v * view_rows, view_rows) for v in PAIR]
    rest = list(scratch[RING:])

    def take(number):
        taken, rest[:] = rest[:number], rest[number:]
        return taken

    top = pl.ds(0, 2)
    side = [[QuickSums(at, (sides, (layer, v, top)), (side_sums, (layer, v, top)), *take(QUICK)) for v in PAIR] for layer in OTHERS]
    pair_sums = QuickSums(at, (sides, (0, 0)), (side_sums, (0, 0)), *take(QUICK))
    loss_sums = QuickSums(at, (loss_local, ...), (loss_total, ...), *take(QUICK))
    sums = [[Sums(at, (embed_local, ()), (embed_total, ()), *take(SUMS))]]
    for layer in PAIR:
        sums.append([Sums(at, (local, (layer, h)), (totals[layer + 1], (h,)), *take(SUMS)) for h in PAIR])

    def load(src, dst, k):
        copy = pltpu.make_async_copy(src, dst, load_sem.at[k])
        copy.start()
        return copy

    def wide_copy(layer, n):
        cols = pl.ds(pl.multiple_of(n * width, width), width)
        return pltpu.make_async_copy(weights[layer].at[:, :, :, :, :, cols], wide.at[n], wide_sem.at[n])

    feats = [load(feat_a, normed.at[0, views[0]], 0)]
    lead = 4
    for n in range(lead):
        wide_copy(0, n).start()
    feats.append(load(feat_b, normed.at[0, views[1]], 1))
    puts = {}

    def put(name, v, src, dst, k):
        copy = pltpu.make_async_copy(src, dst, out_sem.at[k, v])
        copy.start()
        puts[name, v] = copy

    def drain(*names):
        for name in names:
            for v in PAIR:
                puts.pop((name, v)).wait()

    def matmul(layer, v, hook, step):
        @loop(CHUNKS // 2)
        def _(m):
            if step:
                pl.when(m == hook)(step)
            chunks = [2 * m, 2 * m + 1]
            if v == 0:
                if layer == 0:
                    for n in chunks:
                        pl.when(n + lead < CHUNKS)(lambda n=n: wide_copy(0, n + lead).start())
                for n in chunks:
                    wide_copy(layer, n).wait()
            elif layer < 2:
                for n in chunks:
                    pl.when(m > 0)(lambda n=n: wide_copy(layer + 1, n - 2).start())
            for n in chunks:
                cols = pl.ds(pl.multiple_of(n * width, width), width)
                out = jnp.dot(normed[layer % 2, views[v]], wide[n].reshape(dim, width), preferred_element_type=F32)
                pre[views[v], cols] = out
                sides[layer, v, FIRST, cols] = col_sum(out)
                sides[layer, v, SECOND, cols] = col_sum(out * out)

        if v and layer < 2:
            for n in PAIR:
                wide_copy(layer + 1, CHUNKS - 2 + n).start()
        side[layer][v].begin()

    def normalise(layer, v):
        side[layer][v].arrive()
        mean = side_sums[layer, v, FIRST, :] / total_rows
        inv = lax.rsqrt(side_sums[layer, v, SECOND, :] / total_rows - mean * mean + NORM_EPS)
        scales[2 - layer, v:v + 1, :] = gains[layer][...] * inv if layer < 2 else inv
        sides[layer, v, FIRST, :] = mean
        sides[layer, v, SECOND, :] = inv

        @loop(CHUNKS)
        def _(n):
            cols = pl.ds(pl.multiple_of(n * width, width), width)
            mean, inv = sides[layer, v, FIRST, cols], sides[layer, v, SECOND, cols]
            if layer < 2:
                gain, shift = gains[layer][:, cols], shifts[layer][:, cols]

            @loop(view_rows // block_rows)
            def _(r):
                rows = pl.ds(pl.multiple_of(v * view_rows + r * block_rows, block_rows), block_rows)
                value = (pre[rows, cols] - mean) * inv
                if layer < 2:
                    grad[rows, cols] = value.astype(BF16)
                    value = jnp.maximum(gain * value + shift, 0.0)
                normed[(layer + 1) % 2, rows, cols] = value.astype(BF16)

        if layer < 2:
            put(("act", layer), v, normed.at[(layer + 1) % 2, views[v]], saved_act.at[layer, views[v]], layer)
            put(("norm", layer), v, grad.at[views[v]], saved_norm.at[layer, views[v]], 2)

    def turn(src, dst, first, v):
        part = view_rows // 2

        @loop(CHUNKS)
        def _(n):
            cols = pl.ds(pl.multiple_of(n * width, width), width)
            for k in PAIR:
                block = src[pl.ds(v * view_rows + k * part, part), cols].T
                dst[first + 2 * v + k, lax.div(n, 2), lax.rem(n, 2)] = block.reshape(dst.shape[3:])

    enter(at.z_peers + at.cube_peers)
    feats[0].wait()
    matmul(0, 0, 0, None)
    feats[1].wait()
    matmul(0, 1, 3, side[0][0].over_plane)
    for v in PAIR:
        turn(normed.at[0], turned, 0, v)
    normalise(0, 0)
    for layer in PAIR:
        matmul(layer + 1, 0, 0, side[layer][1].over_plane)
        normalise(layer, 1)
        matmul(layer + 1, 1, 3, side[layer + 1][0].over_plane)
        if layer == 0:
            drain(("norm", 0))
        else:
            drain(("act", 0))
        normalise(layer + 1, 0)
    side[2][1].over_plane()
    normalise(2, 1)

    drain(("act", 1), ("norm", 1))
    loads = {("act", 0): load(saved_act.at[1], act, 0)}
    slots = weight.shape[0]
    w_loads = {}

    def load_weight(layer, n):
        copy = pltpu.make_async_copy(weights[2 - layer].at[n // 2, n % 2], weight.at[n % slots], w_sem.at[n % slots])
        copy.start()
        w_loads[layer, n] = copy

    for n in range(slots):
        load_weight(0, n)

    lam = lam_ref[0]
    lane = 128
    place = (at.z, at.y, at.x, at.core)
    block_rows_dev = ring.snd1.shape[-2]
    first_row = (((at.z * 2 + at.y) * 2 + at.x) * 2 + at.core) * block_rows_dev

    def pair_rows():
        @loop(CHUNKS)
        def _(n):
            cols = pl.ds(pl.multiple_of(n * width, width), width)
            one, two = [normed[1, views[v], cols].astype(F32) for v in PAIR]
            sides[0, 0, FIRST, cols] = col_sum(one)
            sides[0, 0, SECOND, cols] = col_sum(two)
            sides[0, 0, THIRD, cols] = col_sum(one * two)
            sides[0, 0, FOURTH, cols] = jnp.zeros((1, width), F32)

        pair_sums.begin()

    block = pl.ds(pl.multiple_of(lax.div(first_row, lane) * lane, lane), lane)
    part = lax.rem(first_row, lane)

    def keep_means():
        pair_sums.arrive()
        turned_sums[...] = jnp.broadcast_to(side_sums[0, 0, FIRST, block], (lane, lane)).T
        mean_col[...] = turned_sums[pl.ds(pl.multiple_of(part, 8), block_rows_dev), :]

    def row_sums():
        for k, row in enumerate((FIRST, THIRD)):
            sums_here = col_sum(by_row[k].T)
            spread = jnp.concatenate([sums_here] * (lane // block_rows_dev), axis=1)
            position = lax.broadcasted_iota(jnp.int32, spread.shape, 1)
            mine = (position >= part) & (position < part + block_rows_dev)
            embed_local[row, :] = jnp.zeros((1, dim), F32)
            embed_local[row, block] = jnp.where(mine, spread, 0.0)


    def correlate(q):
        @loop(2)
        def _(p):
            rows = pl.ds(pl.multiple_of(p * 2 * quarter, quarter), 2 * quarter)
            out = lax.dot_general(normed[1, views[0], rows], normed[1, views[1], pl.ds(q * width, width)],
                                  DEPTH_DIMS, preferred_element_type=F32)
            ring.part[q % 2, pl.ds(2 * p, 2)] = out.reshape(2, *ring.part.shape[2:])

        ring.pair(q)

    def spread_line(q):
        for half, total in enumerate(ring.last(q)):
            start = q * width + half * ring.half
            row = first_row + lax.broadcasted_iota(jnp.int32, total.shape, 0)
            col = start + lax.broadcasted_iota(jnp.int32, total.shape, 1)
            diag = row == col
            cols = pl.ds(start, ring.half)
            total = jnp.where(diag, side_sums[0, 0, THIRD, cols], total)
            corr = total * count
            gap = 1.0 - corr
            loss_local[:, cols] = col_sum(jnp.where(diag, gap * gap, lam * corr * corr))
            slope = (jnp.where(diag, -2.0 * gap, 2.0 * lam * corr) * count).astype(BF16)
            wide[(q, *place, ALL, ring.cols(half))] = slope
            slope = slope.astype(F32)
            embed_local[SECOND, cols] = col_sum(slope * mean_col[:, :ring.half])
            embed_local[FOURTH, cols] = col_sum(slope * total)
            terms = [slope * side_sums[0, 0, SECOND, cols], slope * total]
            for k, term in enumerate(terms):
                by_row[k] = by_row[k] + term if q or half else term
        here = wide.at[(q, *place)]
        for d in OTHERS:
            ring.start(q, 8 + d, here, here, at.z_peers[d])

    def spread_one(q):
        for d in OTHERS:
            ring.wait(q, 8 + d)
        for half, peer in enumerate((at.y_peer, at.x_peer)):
            here = wide.at[q, :, at.y, at.x, at.core, :, ring.cols(half)]
            ring.start(q, 11 + half, here, here, peer)

    def spread_two(q):
        for half, peer in enumerate((at.x_peer, at.y_peer)):
            ring.wait(q, 11 + half)
            here = wide.at[(q, ALL, *((at.y, ALL) if half else (ALL, at.x)), at.core, ALL,
                            ring.cols(half))]
            ring.start(q, 13 + half, here, here, peer)

    def spread_pair(q):
        for half in PAIR:
            ring.wait(q, 13 + half)
        here = wide.at[q, :, :, :, at.core]
        ring.start(q, 15, here, here, at.partner)

    def embed_grad(q):
        ring.wait(q, 15)
        cols = pl.ds(q * width, width)
        pre[views[1], cols] = jnp.dot(normed[1, views[0]], wide[q].reshape(dim, width), preferred_element_type=F32)

        @loop(2)
        def _(p):
            into = pl.ds(pl.multiple_of(p * 2 * quarter, quarter), 2 * quarter)
            rows = lax.dot_general(normed[1, views[1], cols], wide[q, pl.ds(2 * p, 2)].reshape(2 * quarter, width), LANE_DIMS,
                                   preferred_element_type=F32)
            pre[views[0], into] = rows if q == 0 else pre[views[0], into] + rows

    first_sums = sums[0][0]
    relay = [first_sums.over_plane, first_sums.over_line, first_sums.over_pair]
    steps = (ring.first, ring.second, ring.third, spread_line, spread_one, spread_two, spread_pair, embed_grad)
    for t in range(CHUNKS + SPREAD_LAGS[-1]):
        if t < CHUNKS:
            correlate(t)
        if t == 0:
            pair_rows()
        if t == 1:
            pair_sums.over_plane()
        if t == 3:
            keep_means()
        since = t - CHUNKS - SPREAD_LAGS[3]
        if since == 0:
            row_sums()
            first_sums.begin()
        if 0 < since <= len(relay):
            relay[since - 1]()
        for step, lag in zip(steps, SPREAD_LAGS):
            if 0 <= t - lag < CHUNKS:
                step(t - lag)
                if step == embed_grad and t - lag == LINE:
                    for v in PAIR:
                        turn(normed.at[0], wide, 0, v)
                    loads["norm", 0] = load(saved_norm.at[1], normed.at[0], 2)

    loss_sums.begin()

    def finish_grad(layer, j):
        cols = pl.ds(j * width, width)
        total, first = (embed_total, j * width) if layer == 0 else (
            totals[layer].at[j // (CHUNKS // 2)], (j % (CHUNKS // 2)) * width)
        sel = pl.ds(first, width)
        for v in PAIR:
            mean0 = total[v:v + 1, sel] * count
            mean1 = total[2 + v:3 + v, sel] * count
            scale = scales[layer, v:v + 1, cols]

            @loop(view_rows // block_rows)
            def _(r):
                rows = pl.ds(pl.multiple_of(v * view_rows + r * block_rows, block_rows), block_rows)
                xhat = normed[(layer + 1) % 2, rows, cols].astype(F32)
                grad[rows, cols] = (scale * (pre[rows, cols] - (mean0 + xhat * mean1))).astype(BF16)

    def weight_grad(layer, j):
        cols = pl.ds(j * width, width)
        q = (layer + 1) * CHUNKS + j
        source, first = (turned, 0) if layer == 2 else (wide, LINE * layer)

        @loop(2)
        def _(p):
            span = pl.ds(2 * p, 2)
            feed = jnp.concatenate([source[first + k, span].reshape(2 * quarter, -1) for k in range(LINE)], axis=1)
            out = jnp.dot(feed, grad[:, cols], preferred_element_type=F32)
            ring.part[q % 2, span] = out.reshape(2, *ring.part.shape[2:])

        ring.pair(q)

    def input_grad(layer, n):
        cols = pl.ds(n * width, width)
        w_loads[layer, n].wait()
        half = local.at[layer, n // (CHUNKS // 2)]
        sel = pl.ds((n % (CHUNKS // 2)) * width, width)

        out = lax.dot_general(grad[...], weight[n % slots].reshape(width, dim), LANE_DIMS, preferred_element_type=F32)
        out = jnp.where(act[:, cols] > 0, out, 0.0)
        pre[:, cols] = out
        for v, row in enumerate(views):
            half[v:v + 1, sel] = col_sum(pre[row, cols])
            half[v + 2:v + 3, sel] = col_sum(pre[row, cols] * normed[layer % 2, row, cols].astype(F32))

        if n + slots < CHUNKS:
            load_weight(layer, n + slots)

    def serve(t):
        for step, lag in zip((ring.first, ring.second, ring.third, ring.last), RING_LAGS):
            k = t - lag
            if 0 <= k < 3 * CHUNKS:
                blocks = step(CHUNKS + k)
        if 0 <= k < 3 * CHUNKS:
            for half, block in enumerate(blocks):
                outs[k // CHUNKS][:, pl.ds((k % CHUNKS) * width + half * ring.half, ring.half)] = block

    for layer in OTHERS:
        old, new = sums[layer], sums[layer + 1] if layer < 2 else None
        old[0].arrive()
        for j in range(CHUNKS):
            if j == 3 and new:
                loads["norm", layer].wait()
                if layer == 0:
                    loads["act", layer].wait()
            if j < 3:
                finish_grad(layer, j)
            elif new:
                for n in INPUT_STEPS[j - 3][0]:
                    input_grad(layer, n)
            if new and j == 4:
                new[0].begin()
            if new and j == 5:
                new[0].over_line()
            if new and j == 6:
                new[1].begin()
                new[0].over_pair()
                if layer == 0:
                    loads["act", 1] = load(saved_act.at[0], act, 0)
                    for n in range(slots):
                        load_weight(1, n)
            weight_grad(layer, j)
            if j == 0 and layer:
                old[1].over_pair()
            if j == 2:
                finish_grad(layer, 3)
                if layer:
                    old[1].arrive()
                for k in range(CHUNKS // 2, CHUNKS):
                    finish_grad(layer, k)
                if layer == 0:
                    loads["norm", 1] = load(saved_norm.at[0], normed.at[1], 1)
            if new and j > 2:
                if j == 4:
                    new[0].over_plane()
                for n in INPUT_STEPS[j - 3][1]:
                    input_grad(layer, n)
                if j == 6:
                    new[1].over_plane()
                if j == 7:
                    new[1].over_line()
            serve(layer * CHUNKS + j)
        if layer == 0:
            loads["act", 1].wait()
            for v in PAIR:
                turn(act, wide, LINE, v)
            loss_sums.over_plane()
    for k in range(RING_LAGS[-1]):
        serve(3 * CHUNKS + k)
    loss_sums.arrive()


def step(total_rows, vmem, lam, feat_a, feat_b, weights, vectors):
    view_rows, dim = feat_a.shape
    rows, width, blocks = 2 * view_rows, dim // CHUNKS, dim // 32
    hbm = pl.BlockSpec(memory_space=pl.ANY)
    vm = pl.BlockSpec(memory_space=pltpu.VMEM)
    cube = (LINE, 2, 2, 2, blocks)
    scratch = [
        pltpu.VMEM((rows, dim), BF16),
        pltpu.VMEM((rows, dim), F32),
        pltpu.VMEM((CHUNKS, *cube, width), BF16),
        pltpu.VMEM((LINE, *cube, view_rows // 2), BF16),
        pltpu.VMEM((3, 2, 2, blocks, dim), BF16),
        pltpu.VMEM((2, rows, dim), BF16),
        pltpu.VMEM((rows, dim), BF16),
        pltpu.VMEM((3, 2, 4, dim), F32),
        pltpu.VMEM((3, 2, 4, dim), F32),
        pltpu.VMEM((2, 2, 4, dim // 2), F32),
        pltpu.VMEM((4, dim), F32),
        pltpu.VMEM((4, dim), F32),
        pltpu.VMEM((1, dim), F32),
        pltpu.VMEM((blocks, 128), F32),
        pltpu.VMEM((128, 128), F32),
        pltpu.VMEM((2, blocks, width // 2), F32),
        pltpu.VMEM((3, 2, dim), F32),
        DMA_SEM((CHUNKS,)),
        DMA_SEM((3,)),
        DMA_SEM((3,)),
        DMA_SEM((3, 2)),
    ] + ring_scratch(CHUNKS, blocks, width)
    for _ in range(6):
        scratch += quick_scratch(2, dim)
    scratch += quick_scratch(4, dim) + quick_scratch(1, dim) + sums_scratch(4, dim)
    for _ in range(4):
        scratch += sums_scratch(4, dim // 2)
    halves = jax.ShapeDtypeStruct((2, 4, dim // 2), F32)
    saved = jax.ShapeDtypeStruct((2, rows, dim), BF16)
    return pl.pallas_call(
        functools.partial(step_kernel, total_rows),
        out_shape=[jax.ShapeDtypeStruct((blocks, dim), F32)] * 3 + [
            jax.ShapeDtypeStruct((1, dim), F32), halves, halves, saved, saved],
        in_specs=[pl.BlockSpec(memory_space=pltpu.SMEM)] + [hbm] * 5 + [vm] * 4,
        out_specs=[vm] * 6 + [hbm] * 2,
        scratch_shapes=scratch,
        compiler_params=pltpu.CompilerParams(collective_id=0, has_side_effects=True, vmem_limit_bytes=vmem),
    )(lam.reshape(1), feat_a, feat_b, *[weight.reshape(*cube, dim) for weight in weights],
      *[value.reshape(1, dim) for value in vectors])


def finish_kernel(total_two, total_one, loss_cols, *refs):
    gain_one, shift_one, gain_two, shift_two, loss = refs[6:]
    for grad, out in zip(refs[:3], refs[3:6]):
        out[...] = grad[...]
    half = total_two.shape[-1]
    for total, gain, shift in ((total_two, gain_two, shift_two), (total_one, gain_one, shift_one)):
        for h in PAIR:
            cols = pl.ds(h * half, half)
            shift[:, cols] = total[h, FIRST] + total[h, SECOND]
            gain[:, cols] = total[h, THIRD] + total[h, FOURTH]
    loss[...] = jnp.sum(loss_cols[...], axis=1, keepdims=True)


def finish(total_two, total_one, loss_cols, grads):
    vm = pl.BlockSpec(memory_space=pltpu.VMEM)
    row = jax.ShapeDtypeStruct((1, loss_cols.shape[1]), F32)
    outs = pl.pallas_call(
        finish_kernel,
        out_shape=[jax.ShapeDtypeStruct(grad.shape, F32) for grad in grads] + [row] * 4 + [jax.ShapeDtypeStruct((1, 1), F32)],
        in_specs=[vm] * 6,
        out_specs=[vm] * 8,
    )(total_two, total_one, loss_cols, *grads)
    return outs[:3], [row.reshape(-1) for row in outs[3:7]], outs[7].reshape(())


def solution(mesh):
    shards = mesh.shape["data"]

    def local_step(h_a, h_b, w_one, w_two, w_three, gain_one, shift_one, gain_two, shift_two, lam_off):
        rows_dev = h_a.shape[0]
        total_rows = rows_dev * shards
        grad_w_three, grad_w_two, grad_w_one, loss_cols, total_two, total_one = step(
            total_rows, 67000000, lam_off, h_a, h_b, (w_one, w_two, w_three),
            (gain_one, shift_one, gain_two, shift_two))[:6]
        grads, vectors, loss_total = finish(total_two, total_one, loss_cols, [grad_w_one, grad_w_two, grad_w_three])
        return (loss_total, *grads, *vectors)

    row_spec = P("data", None)
    whole_mat = P(None, None)
    whole_vec = P(None)
    return jax.shard_map(
        local_step, mesh=mesh,
        in_specs=(row_spec, row_spec, whole_mat, whole_mat, whole_mat,
                  whole_vec, whole_vec, whole_vec, whole_vec, P()),
        out_specs=(P(), row_spec, row_spec, row_spec, whole_vec, whole_vec, whole_vec, whole_vec),
        check_vma=False)
```

```python
import functools

import jax
import jax.numpy as jnp
from jax import lax
from jax.experimental import pallas as pl
from jax.experimental.pallas import tpu as pltpu
from jax.sharding import PartitionSpec as P

NORM_EPS = 1e-5
MESH = pl.DeviceIdType.MESH
F32 = jnp.float32
BF16 = jnp.bfloat16


ALL = slice(None)
FIRST, SECOND, THIRD, FOURTH = [slice(k, k + 1) for k in range(4)]
PAIR = range(2)
OTHERS = range(3)
LINE = 4
CUBE = 8
DEPTH_DIMS = (((0,), (0,)), ((), ()))
LANE_DIMS = (((1,), (1,)), ((), ()))
DMA_SEM = pltpu.SemaphoreType.DMA


def loop(count):
    return pl.loop(0, count)


def col_sum(values):
    return jnp.sum(values, axis=0, keepdims=True)


class Place:
    def __init__(self):
        me = lax.axis_index("data")
        self.core = lax.rem(me, 2)
        self.x = lax.rem(lax.div(me, 2), 2)
        self.y = lax.rem(lax.div(me, 4), 2)
        self.z = lax.div(me, 8)
        self.plane = lax.rem(lax.div(me, 2), 4)
        self.partner = me + 1 - 2 * self.core
        self.x_peer = me + 2 - 4 * self.x
        self.y_peer = me + 4 - 8 * self.y
        self.low = lax.rem(me, CUBE)
        self.others = [lax.rem(self.z + d + 1, LINE) for d in OTHERS]
        self.z_peers = [z * CUBE + self.low for z in self.others]
        self.plane_peers = [self.z * CUBE + lax.rem(self.plane + d + 1, LINE) * 2 + self.core for d in OTHERS]
        self.cube_peers = [self.z * CUBE + lax.rem(self.low + d + 1, CUBE) for d in range(CUBE - 1)]
        self.near = [self.partner] + self.plane_peers + self.z_peers


def enter(peers):
    barrier = pltpu.get_barrier_semaphore()
    for peer in peers:
        pl.semaphore_signal(barrier, inc=1, device_id=(peer,), device_id_type=MESH)
    pl.semaphore_wait(barrier, len(peers))


def remote(src, dst, send_sem, recv_sem, peer):
    return pltpu.make_async_remote_copy(
        src_ref=src, dst_ref=dst, send_sem=send_sem, recv_sem=recv_sem,
        device_id=(peer,), device_id_type=MESH)


class Sums:
    def __init__(self, at, local, total, recv0, slots1, slots2, send_sem, recv_sem):
        self.at, self.refs = at, (local, total)
        self.recv0, self.slots1, self.slots2 = recv0, slots1, slots2
        self.send_sem, self.recv_sem = send_sem, recv_sem
        self.half = recv0.shape[-1]
        self.mine = pl.multiple_of(at.core * self.half, 128)
        self.theirs = pl.multiple_of((1 - at.core) * self.half, 128)

    def pick(self, k, first):
        ref, index = self.refs[k]
        return ref.at[(*index, ALL, pl.ds(first, self.half))]

    def copies(self, stage):
        at = self.at
        if stage == 0:
            pairs = [(0, self.pick(0, self.theirs), self.recv0, at.partner)]
        elif stage == 1:
            here = self.slots1.at[at.plane]
            pairs = [(1 + d, here, here, at.plane_peers[d]) for d in OTHERS]
        elif stage == 2:
            here = self.slots2.at[at.z]
            pairs = [(4 + d, here, here, at.z_peers[d]) for d in OTHERS]
        else:
            here = self.pick(1, self.mine)
            pairs = [(7, here, here, at.partner)]
        return [remote(src, dst, self.send_sem.at[k], self.recv_sem.at[k], peer) for k, src, dst, peer in pairs]

    def send(self, stage):
        for copy in self.copies(stage):
            copy.start()

    def arrive(self, stage=3):
        for copy in self.copies(stage):
            copy.wait()

    def begin(self):
        self.send(0)

    def over_plane(self):
        self.arrive(0)
        self.slots1[self.at.plane] = self.pick(0, self.mine)[...] + self.recv0[...]
        self.send(1)

    def over_line(self):
        self.arrive(1)
        self.slots2[self.at.z] = jnp.sum(self.slots1[...], axis=0)
        self.send(2)

    def over_pair(self):
        self.arrive(2)
        self.pick(1, self.mine)[...] = jnp.sum(self.slots2[...], axis=0)
        self.send(3)


class QuickSums:
    def __init__(self, at, local, total, slots1, slots2, send_sem, recv_sem):
        self.at, self.local, self.total = at, local, total
        self.slots1, self.slots2 = slots1, slots2
        self.send_sem, self.recv_sem = send_sem, recv_sem

    def copies(self, across):
        at = self.at
        if across:
            here, peers, first = self.slots2.at[at.low], at.cube_peers, len(at.z_peers)
        else:
            here, peers, first = self.slots1.at[at.z], at.z_peers, 0
        return [remote(here, here, self.send_sem.at[first + d], self.recv_sem.at[first + d], peer)
                for d, peer in enumerate(peers)]

    def begin(self):
        ref, index = self.local
        self.slots1[self.at.z] = ref[index]
        for copy in self.copies(False):
            copy.start()

    def over_plane(self):
        for copy in self.copies(False):
            copy.wait()
        self.slots2[self.at.low] = jnp.sum(self.slots1[...], axis=0)
        for copy in self.copies(True):
            copy.start()

    def arrive(self):
        for copy in self.copies(True):
            copy.wait()
        ref, index = self.total
        ref[index] = jnp.sum(self.slots2[...], axis=0)


def quick_scratch(rows, cols):
    return [
        pltpu.VMEM((LINE, rows, cols), F32),
        pltpu.VMEM((CUBE, rows, cols), F32),
        DMA_SEM((LINE + CUBE,)),
        DMA_SEM((LINE + CUBE,)),
    ]


def sums_scratch(rows, cols):
    return [
        pltpu.VMEM((rows, cols // 2), F32),
        pltpu.VMEM((4, rows, cols // 2), F32),
        pltpu.VMEM((4, rows, cols // 2), F32),
        DMA_SEM((8,)),
        DMA_SEM((8,)),
    ]


class Ring:
    def __init__(self, at, total, spread, part, recv0, kept, snd1, recv1, snd2, recv2, snd3, recv3, send_sem, recv_sem, credit):
        self.at, self.total, self.slots, self.spread = at, total, kept.shape[0], spread
        self.part, self.recv0, self.kept = part, recv0, kept
        self.snd1, self.recv1, self.snd2, self.recv2, self.snd3, self.recv3 = snd1, recv1, snd2, recv2, snd3, recv3
        self.send_sem, self.recv_sem, self.credit = send_sem, recv_sem, credit
        self.half = snd1.shape[-1]
        self.peers = [at.partner, at.x_peer, at.y_peer, at.y_peer, at.x_peer] + at.z_peers
        self.givers = self.peers[:5] + at.z_peers[::-1]
        self.own = [at.y, at.x]

    def cols(self, half):
        return pl.ds(half * self.half, self.half)

    def copy(self, q, stage):
        j, s = lax.rem(q, self.slots), lax.rem(q, 2)
        if stage > 7:
            src, dst, peer = self.spread(q, stage)
        else:
            peer = self.peers[stage]
            if stage > 4:
                src, dst = self.snd3.at[j, stage - 5], self.recv3.at[j, stage - 5]
            elif stage > 2:
                src, dst = self.snd2.at[j, stage - 3], self.recv2.at[j, stage - 3]
            elif stage:
                src, dst = self.snd1.at[j, stage - 1], self.recv1.at[j, stage - 1]
            else:
                src, dst = self.part.at[s, :, :, :, 1 - self.at.core], self.recv0.at[s]
        return remote(src, dst, self.send_sem.at[j, stage], self.recv_sem.at[j, stage], peer)

    def start(self, q, *stages):
        for stage in stages:
            self.copy(q, stage).start()

    def wait(self, q, *stages):
        for stage in stages:
            self.copy(q, stage).wait()

    def depth(self, stage):
        return self.slots if stage else self.part.shape[0]

    def send(self, q, *stages):
        for stage in stages:
            depth = self.depth(stage)
            pl.when(q >= depth)(lambda: pl.semaphore_wait(self.credit.at[lax.rem(q, depth), stage], 1))
            self.start(q, stage)

    def give(self, q, *stages):
        for stage in stages:
            depth = self.depth(stage)
            pl.when(q + depth < self.total)(lambda: pl.semaphore_signal(
                self.credit.at[lax.rem(q, depth), stage], inc=1, device_id=(self.givers[stage],), device_id_type=MESH))

    def pair(self, q):
        self.send(q, 0)

    def first(self, q):
        at, s, j = self.at, lax.rem(q, 2), lax.rem(q, self.slots)
        self.wait(q, 0)

        @loop(LINE)
        def _(z):
            for half in PAIR:
                cols = self.cols(half)
                for k in PAIR:
                    (y, x), (oy, ox) = ((at.y, k), (1 - at.y, k)) if half else ((k, at.x), (k, 1 - at.x))
                    self.snd1[j, half, z, k] = (
                        self.part[s, z, oy, ox, at.core, :, cols] + self.recv0[s, z, oy, ox, :, cols]).astype(BF16)
                    self.kept[j, half, z, k] = self.part[s, z, y, x, at.core, :, cols] + self.recv0[s, z, y, x, :, cols]

        self.give(q, 0)
        self.send(q, 1, 2)

    def second(self, q):
        j = lax.rem(q, self.slots)
        for half in PAIR:
            own = self.own[half]
            self.wait(q, 1 + half)

            @loop(LINE)
            def _(z):
                self.snd2[j, half, z] = (
                    self.kept[j, half, z, 1 - own] + self.recv1[j, half, z, 1 - own].astype(F32)).astype(BF16)
                self.kept[j, half, z, own] = self.kept[j, half, z, own] + self.recv1[j, half, z, own].astype(F32)

            self.give(q, 1 + half)
            self.send(q, 3 + half)

    def summed(self, j, half, z):
        return self.kept[j, half, z, self.own[half]] + self.recv2[j, half, z].astype(F32)

    def third(self, q):
        j = lax.rem(q, self.slots)
        self.wait(q, 3, 4)

        @loop(len(OTHERS))
        def _(d):
            z = lax.rem(self.at.z + d + 1, LINE)
            for half in PAIR:
                self.snd3[j, d, :, self.cols(half)] = self.summed(j, half, z).astype(BF16)

        self.send(q, 5, 6, 7)

    def last(self, q):
        j = lax.rem(q, self.slots)
        totals = [self.summed(j, half, self.at.z) for half in PAIR]
        self.wait(q, 5, 6, 7)
        for d in OTHERS:
            totals = [total + self.recv3[j, d, :, self.cols(half)].astype(F32) for half, total in enumerate(totals)]
        self.give(q, 3, 4, 5, 6, 7)
        return totals


def ring_scratch(slots, rows, width):
    half = width // 2
    return [
        pltpu.VMEM((2, 4, 2, 2, 2, rows, width), F32),
        pltpu.VMEM((2, 4, 2, 2, rows, width), F32),
        pltpu.VMEM((slots, 2, 4, 2, rows, half), F32),
    ] + [pltpu.VMEM((slots, 2, 4, 2, rows, half), BF16)] * 2 + [pltpu.VMEM((slots, 2, 4, rows, half), BF16)] * 2 + [
        pltpu.VMEM((slots, 3, rows, width), BF16)] * 2 + [DMA_SEM((slots, 16))] * 2 + [
        pltpu.SemaphoreType.REGULAR((slots, 8))]


CHUNKS = 8
RING = 12
SUMS = 5
QUICK = 4
SPREAD_LAGS = (1, 2, 3, 4, 6, 7, 8, 9)
RING_LAGS = (1, 3, 5, 8)


def step_kernel(
        total_rows, lam_ref, feat_a, feat_b, w_one, w_two, w_three, gain_one, shift_one, gain_two, shift_two,
        grad_w_three, grad_w_two, grad_w_one, loss_total, total_two, total_one, saved_act, saved_norm,
        grad, pre, wide, turned, weight, normed, act, sides, side_sums, local, embed_local, embed_total, loss_local, mean_col, turned_sums, by_row, scales,
        wide_sem, w_sem, load_sem, out_sem, *scratch):
    at = Place()
    place = (at.z, at.y, at.x, at.core)

    def spread(q, stage):
        cols = ring.cols((stage - 1) % 2)
        if stage < 11:
            here, peer = wide.at[(q, *place)], at.z_peers[stage - 8]
        elif stage == 11:
            here, peer = wide.at[q, :, at.y, at.x, at.core, :, cols], at.y_peer
        elif stage == 12:
            here, peer = wide.at[q, :, at.y, at.x, at.core, :, cols], at.x_peer
        elif stage == 13:
            here, peer = wide.at[q, :, :, at.x, at.core, :, cols], at.x_peer
        elif stage == 14:
            here, peer = wide.at[q, :, at.y, :, at.core, :, cols], at.y_peer
        else:
            here, peer = wide.at[q, :, :, :, at.core], at.partner
        return here, here, peer

    ring = Ring(at, 4 * CHUNKS, spread, *scratch[:RING])
    rows_dev, dim = grad.shape
    width = dim // CHUNKS
    view_rows = rows_dev // 2
    block_rows = min(64, view_rows)
    quarter = dim // 4
    count = 1.0 / total_rows
    weights = [w_one, w_two, w_three]
    gains, shifts = [gain_one, gain_two], [shift_one, shift_two]
    outs = [grad_w_three, grad_w_two, grad_w_one]
    totals = [embed_total, total_two, total_one]
    views = [pl.ds(v * view_rows, view_rows) for v in PAIR]
    rest = list(scratch[RING:])

    def take(number):
        taken, rest[:] = rest[:number], rest[number:]
        return taken

    top = pl.ds(0, 2)
    side = [[QuickSums(at, (sides, (layer, v, top)), (side_sums, (layer, v, top)), *take(QUICK)) for v in PAIR] for layer in OTHERS]
    pair_sums = QuickSums(at, (sides, (0, 0)), (side_sums, (0, 0)), *take(QUICK))
    loss_sums = QuickSums(at, (loss_local, ...), (loss_total, ...), *take(QUICK))
    sums = [[Sums(at, (embed_local, ()), (embed_total, ()), *take(SUMS))]]
    for layer in PAIR:
        sums.append([Sums(at, (local, (layer, h)), (totals[layer + 1], (h,)), *take(SUMS)) for h in PAIR])

    def act_copy(layer):
        return pltpu.make_async_copy(saved_act.at[1 - layer], act, load_sem.at[0])

    def norm_copy(layer):
        return pltpu.make_async_copy(saved_norm.at[1 - layer], normed.at[layer], load_sem.at[1])

    def feat_copy(v):
        return pltpu.make_async_copy((feat_a, feat_b)[v], normed.at[0, views[v]], load_sem.at[v])

    def wide_copy(layer, n):
        cols = pl.ds(pl.multiple_of(n * width, width), width)
        return pltpu.make_async_copy(weights[layer].at[:, :, :, :, :, cols], wide.at[n], wide_sem.at[n])

    feat_copy(0).start()
    lead = 4
    for n in range(lead):
        wide_copy(0, n).start()
    feat_copy(1).start()
    puts = {}

    def put(name, v, src, dst, k):
        copy = pltpu.make_async_copy(src, dst, out_sem.at[k, v])
        copy.start()
        puts[name, v] = copy

    def drain(*names):
        for name in names:
            for v in PAIR:
                puts.pop((name, v)).wait()

    def matmul(layer, v, hook, step):
        @loop(CHUNKS // 2)
        def _(m):
            if step:
                pl.when(m == hook)(step)
            chunks = [2 * m, 2 * m + 1]
            if v == 0:
                if layer == 0:
                    for n in chunks:
                        pl.when(n + lead < CHUNKS)(lambda n=n: wide_copy(0, n + lead).start())
                for n in chunks:
                    wide_copy(layer, n).wait()
            elif layer < 2:
                for n in chunks:
                    pl.when(m > 0)(lambda n=n: wide_copy(layer + 1, n - 2).start())
            for n in chunks:
                cols = pl.ds(pl.multiple_of(n * width, width), width)
                out = jnp.dot(normed[layer % 2, views[v]], wide[n].reshape(dim, width), preferred_element_type=F32)
                pre[views[v], cols] = out
                sides[layer, v, FIRST, cols] = col_sum(out)
                sides[layer, v, SECOND, cols] = col_sum(out * out)

        if v and layer < 2:
            for n in PAIR:
                wide_copy(layer + 1, CHUNKS - 2 + n).start()
        side[layer][v].begin()

    def normalise(layer, v):
        side[layer][v].arrive()
        mean = side_sums[layer, v, FIRST, :] / total_rows
        inv = lax.rsqrt(side_sums[layer, v, SECOND, :] / total_rows - mean * mean + NORM_EPS)
        scales[2 - layer, v:v + 1, :] = gains[layer][...] * inv if layer < 2 else inv
        sides[layer, v, FIRST, :] = mean
        sides[layer, v, SECOND, :] = inv

        @loop(CHUNKS)
        def _(n):
            cols = pl.ds(pl.multiple_of(n * width, width), width)
            mean, inv = sides[layer, v, FIRST, cols], sides[layer, v, SECOND, cols]
            if layer < 2:
                gain, shift = gains[layer][:, cols], shifts[layer][:, cols]

            @loop(view_rows // block_rows)
            def _(r):
                rows = pl.ds(pl.multiple_of(v * view_rows + r * block_rows, block_rows), block_rows)
                value = (pre[rows, cols] - mean) * inv
                if layer < 2:
                    grad[rows, cols] = value.astype(BF16)
                    value = jnp.maximum(gain * value + shift, 0.0)
                normed[(layer + 1) % 2, rows, cols] = value.astype(BF16)

        if layer < 2:
            put(("act", layer), v, normed.at[(layer + 1) % 2, views[v]], saved_act.at[layer, views[v]], layer)
            put(("norm", layer), v, grad.at[views[v]], saved_norm.at[layer, views[v]], 2)

    def turn(src, dst, first, v):
        part = view_rows // 2

        @loop(CHUNKS)
        def _(n):
            cols = pl.ds(pl.multiple_of(n * width, width), width)
            for k in PAIR:
                block = src[pl.ds(v * view_rows + k * part, part), cols].T
                dst[first + 2 * v + k, lax.div(n, 2), lax.rem(n, 2)] = block.reshape(dst.shape[3:])

    enter(at.z_peers + at.cube_peers)
    feat_copy(0).wait()
    matmul(0, 0, 0, None)
    feat_copy(1).wait()
    matmul(0, 1, 3, side[0][0].over_plane)
    for v in PAIR:
        turn(normed.at[0], turned, 0, v)
    normalise(0, 0)
    for layer in PAIR:
        matmul(layer + 1, 0, 0, side[layer][1].over_plane)
        normalise(layer, 1)
        matmul(layer + 1, 1, 3, side[layer + 1][0].over_plane)
        if layer == 0:
            drain(("norm", 0))
        else:
            drain(("act", 0))
        normalise(layer + 1, 0)
    side[2][1].over_plane()
    normalise(2, 1)

    drain(("act", 1), ("norm", 1))
    act_copy(0).start()
    slots = weight.shape[0]

    def weight_copy(layer, n):
        slot = lax.rem(n, slots)
        return pltpu.make_async_copy(weights[2 - layer].at[lax.div(n, 2), lax.rem(n, 2)], weight.at[slot], w_sem.at[slot])

    for n in range(slots):
        weight_copy(0, n).start()

    lam = lam_ref[0]
    lane = 128
    block_rows_dev = ring.snd1.shape[-2]
    first_row = (((at.z * 2 + at.y) * 2 + at.x) * 2 + at.core) * block_rows_dev

    def pair_rows():
        @loop(CHUNKS)
        def _(n):
            cols = pl.ds(pl.multiple_of(n * width, width), width)
            one, two = [normed[1, views[v], cols].astype(F32) for v in PAIR]
            sides[0, 0, FIRST, cols] = col_sum(one)
            sides[0, 0, SECOND, cols] = col_sum(two)
            sides[0, 0, THIRD, cols] = col_sum(one * two)
            sides[0, 0, FOURTH, cols] = jnp.zeros((1, width), F32)
            pre[views[0], cols] = jnp.zeros((view_rows, width), F32)

        by_row[...] = jnp.zeros_like(by_row)
        pair_sums.begin()

    block = pl.ds(pl.multiple_of(lax.div(first_row, lane) * lane, lane), lane)
    part = lax.rem(first_row, lane)

    def keep_means():
        pair_sums.arrive()
        turned_sums[...] = jnp.broadcast_to(side_sums[0, 0, FIRST, block], (lane, lane)).T
        mean_col[...] = turned_sums[pl.ds(pl.multiple_of(part, 8), block_rows_dev), :]

    def row_sums():
        for k, row in enumerate((FIRST, THIRD)):
            sums_here = col_sum(by_row[k].T)
            spread = jnp.concatenate([sums_here] * (lane // block_rows_dev), axis=1)
            position = lax.broadcasted_iota(jnp.int32, spread.shape, 1)
            mine = (position >= part) & (position < part + block_rows_dev)
            embed_local[row, :] = jnp.zeros((1, dim), F32)
            embed_local[row, block] = jnp.where(mine, spread, 0.0)


    def chunk_cols(q):
        return pl.ds(pl.multiple_of(q * width, width), width)

    def correlate(q):
        @loop(LINE)
        def _(z):
            rows = pl.ds(pl.multiple_of(z * quarter, quarter), quarter)
            out = lax.dot_general(normed[1, views[0], rows], normed[1, views[1], chunk_cols(q)], DEPTH_DIMS,
                                  preferred_element_type=F32)
            ring.part[lax.rem(q, 2), z] = out.reshape(ring.part.shape[2:])

        ring.pair(q)

    def spread_line(q):
        for half, total in enumerate(ring.last(q)):
            start = q * width + half * ring.half
            row = first_row + lax.broadcasted_iota(jnp.int32, total.shape, 0)
            col = start + lax.broadcasted_iota(jnp.int32, total.shape, 1)
            diag = row == col
            cols = pl.ds(pl.multiple_of(start, ring.half), ring.half)
            total = jnp.where(diag, side_sums[0, 0, THIRD, cols], total)
            corr = total * count
            gap = 1.0 - corr
            loss_local[:, cols] = col_sum(jnp.where(diag, gap * gap, lam * corr * corr))
            slope = (jnp.where(diag, -2.0 * gap, 2.0 * lam * corr) * count).astype(BF16)
            wide[(q, *place, ALL, ring.cols(half))] = slope
            slope = slope.astype(F32)
            embed_local[SECOND, cols] = col_sum(slope * mean_col[:, :ring.half])
            embed_local[FOURTH, cols] = col_sum(slope * total)
            terms = [slope * side_sums[0, 0, SECOND, cols], slope * total]
            for k, term in enumerate(terms):
                by_row[k] = by_row[k] + term
        ring.start(q, 8, 9, 10)

    def spread_one(q):
        ring.wait(q, 8, 9, 10)
        ring.start(q, 11, 12)

    def spread_two(q):
        ring.wait(q, 11, 12)
        ring.start(q, 13, 14)

    def spread_pair(q):
        ring.wait(q, 13, 14)
        ring.start(q, 15)

    def embed_grad(q):
        ring.wait(q, 15)
        cols = chunk_cols(q)
        pre[views[1], cols] = jnp.dot(normed[1, views[0]], wide[q].reshape(dim, width), preferred_element_type=F32)

        @loop(LINE)
        def _(z):
            into = pl.ds(pl.multiple_of(z * quarter, quarter), quarter)
            rows = lax.dot_general(normed[1, views[1], cols], wide[q, z].reshape(quarter, width), LANE_DIMS,
                                   preferred_element_type=F32)
            pre[views[0], into] = pre[views[0], into] + rows

    first_sums = sums[0][0]
    steps = (ring.first, ring.second, ring.third, spread_line, spread_one, spread_two, spread_pair, embed_grad)
    done = CHUNKS + SPREAD_LAGS[3]

    def start_sums():
        row_sums()
        first_sums.begin()

    def turn_two():
        for v in PAIR:
            turn(normed.at[0], wide, 0, v)
        norm_copy(0).start()

    moves = ((0, pair_rows), (1, pair_sums.over_plane), (3, keep_means), (done, start_sums), (done + 1, first_sums.over_plane),
             (done + 2, first_sums.over_line), (done + 3, first_sums.over_pair))

    @loop(CHUNKS + SPREAD_LAGS[-1])
    def _(t):
        pl.when(t < CHUNKS)(lambda: correlate(t))
        for when, move in moves:
            pl.when(t == when)(move)
        for step, lag in zip(steps, SPREAD_LAGS):
            pl.when((t >= lag) & (t < lag + CHUNKS))(lambda step=step, lag=lag: step(t - lag))
        pl.when(t == SPREAD_LAGS[-1] + LINE)(turn_two)

    loss_sums.begin()

    def finish_grad(layer, j):
        cols = chunk_cols(j)
        per = CHUNKS // 2
        total, sel = (embed_total, cols) if layer == 0 else (totals[layer].at[lax.div(j, per)], chunk_cols(lax.rem(j, per)))
        for v in PAIR:
            mean0 = total[v:v + 1, sel] * count
            mean1 = total[2 + v:3 + v, sel] * count
            scale = scales[layer, v:v + 1, cols]

            @loop(view_rows // block_rows)
            def _(r):
                rows = pl.ds(pl.multiple_of(v * view_rows + r * block_rows, block_rows), block_rows)
                xhat = normed[(layer + 1) % 2, rows, cols].astype(F32)
                grad[rows, cols] = (scale * (pre[rows, cols] - (mean0 + xhat * mean1))).astype(BF16)

    def weight_grad(layer, j):
        q = (layer + 1) * CHUNKS + j
        source, first = (turned, 0) if layer == 2 else (wide, LINE * layer)

        @loop(2)
        def _(p):
            span = pl.ds(2 * p, 2)
            feed = jnp.concatenate([source[first + k, span].reshape(2 * quarter, -1) for k in range(LINE)], axis=1)
            out = jnp.dot(feed, grad[:, chunk_cols(j)], preferred_element_type=F32)
            ring.part[lax.rem(q, 2), span] = out.reshape(2, *ring.part.shape[2:])

        ring.pair(q)

    def input_grad(layer, n):
        cols = chunk_cols(n)
        weight_copy(layer, n).wait()
        half = local.at[layer, lax.div(n, CHUNKS // 2)]
        sel = chunk_cols(lax.rem(n, CHUNKS // 2))

        @loop(2)
        def _(v):
            rows = pl.ds(pl.multiple_of(v * view_rows, view_rows), view_rows)
            out = lax.dot_general(grad[rows, :], weight[lax.rem(n, slots)].reshape(width, dim), LANE_DIMS,
                                  preferred_element_type=F32)
            out = jnp.where(act[rows, cols] > 0, out, 0.0)
            pre[rows, cols] = out
            half[pl.ds(v, 1), sel] = col_sum(out)
            half[pl.ds(2 + v, 1), sel] = col_sum(out * normed[layer % 2, rows, cols].astype(F32))

        pl.when(n + slots < CHUNKS)(lambda: weight_copy(layer, n + slots).start())

    def serve(layer, j):
        t = layer * CHUNKS + j
        for step, lag in zip((ring.first, ring.second, ring.third), RING_LAGS):
            pl.when((t >= lag) & (t < lag + 3 * CHUNKS))(lambda step=step, lag=lag: step(CHUNKS + t - lag))
        if layer:
            for half, block in enumerate(ring.last(t)):
                outs[layer - 1][:, pl.ds(pl.multiple_of(j * width + half * ring.half, ring.half), ring.half)] = block

    for layer in OTHERS:
        old, new = sums[layer], sums[layer + 1] if layer < 2 else None
        old[0].arrive()

        def settle():
            if layer:
                old[1].arrive()

            @pl.loop(3, CHUNKS)
            def _(k):
                finish_grad(layer, k)

            if layer == 0:
                norm_copy(1).start()

        def late_loads():
            new[1].begin()
            if layer == 0:
                act_copy(1).start()
                for n in range(slots):
                    weight_copy(1, n).start()

        def relay_pair():
            new[0].over_pair()
            new[1].over_plane()

        before, middle, after = [], [(2, settle)], []
        if layer:
            middle.append((0, old[1].over_pair))
        if layer == 0:
            before.append((3, lambda: act_copy(0).wait()))
        if new:
            before += [(2, lambda: norm_copy(layer).wait()), (5, new[0].over_plane), (6, new[0].over_line), (7, relay_pair)]
            after += [(4, new[0].begin), (6, late_loads), (7, new[1].over_line)]

        @loop(CHUNKS)
        def _(j):
            for when, move in before:
                pl.when(j == when)(move)
            pl.when(j < 3)(lambda: finish_grad(layer, j))
            weight_grad(layer, j)
            for when, move in middle:
                pl.when(j == when)(move)
            if new:
                @pl.when((j > 2) & (j < 7))
                def _():
                    @loop(2)
                    def _(k):
                        input_grad(layer, 2 * (j - 3) + k)
            for when, move in after:
                pl.when(j == when)(move)
            serve(layer, j)

        if layer == 0:
            act_copy(1).wait()
            for v in PAIR:
                turn(act, wide, LINE, v)
            loss_sums.over_plane()

    @loop(CHUNKS)
    def _(j):
        serve(len(OTHERS), j)

    loss_sums.arrive()


def step(total_rows, vmem, lam, feat_a, feat_b, weights, vectors):
    view_rows, dim = feat_a.shape
    rows, width, blocks = 2 * view_rows, dim // CHUNKS, dim // 32
    hbm = pl.BlockSpec(memory_space=pl.ANY)
    vm = pl.BlockSpec(memory_space=pltpu.VMEM)
    cube = (LINE, 2, 2, 2, blocks)
    scratch = [
        pltpu.VMEM((rows, dim), BF16),
        pltpu.VMEM((rows, dim), F32),
        pltpu.VMEM((CHUNKS, *cube, width), BF16),
        pltpu.VMEM((LINE, *cube, view_rows // 2), BF16),
        pltpu.VMEM((3, 2, 2, blocks, dim), BF16),
        pltpu.VMEM((2, rows, dim), BF16),
        pltpu.VMEM((rows, dim), BF16),
        pltpu.VMEM((3, 2, 4, dim), F32),
        pltpu.VMEM((3, 2, 4, dim), F32),
        pltpu.VMEM((2, 2, 4, dim // 2), F32),
        pltpu.VMEM((4, dim), F32),
        pltpu.VMEM((4, dim), F32),
        pltpu.VMEM((1, dim), F32),
        pltpu.VMEM((blocks, 128), F32),
        pltpu.VMEM((128, 128), F32),
        pltpu.VMEM((2, blocks, width // 2), F32),
        pltpu.VMEM((3, 2, dim), F32),
        DMA_SEM((CHUNKS,)),
        DMA_SEM((3,)),
        DMA_SEM((3,)),
        DMA_SEM((3, 2)),
    ] + ring_scratch(CHUNKS, blocks, width)
    for _ in range(6):
        scratch += quick_scratch(2, dim)
    scratch += quick_scratch(4, dim) + quick_scratch(1, dim) + sums_scratch(4, dim)
    for _ in range(4):
        scratch += sums_scratch(4, dim // 2)
    halves = jax.ShapeDtypeStruct((2, 4, dim // 2), F32)
    saved = jax.ShapeDtypeStruct((2, rows, dim), BF16)
    return pl.pallas_call(
        functools.partial(step_kernel, total_rows),
        out_shape=[jax.ShapeDtypeStruct((blocks, dim), F32)] * 3 + [
            jax.ShapeDtypeStruct((1, dim), F32), halves, halves, saved, saved],
        in_specs=[pl.BlockSpec(memory_space=pltpu.SMEM)] + [hbm] * 5 + [vm] * 4,
        out_specs=[vm] * 6 + [hbm] * 2,
        scratch_shapes=scratch,
        compiler_params=pltpu.CompilerParams(collective_id=0, has_side_effects=True, vmem_limit_bytes=vmem),
    )(lam.reshape(1), feat_a, feat_b, *[weight.reshape(*cube, dim) for weight in weights],
      *[value.reshape(1, dim) for value in vectors])


def finish_kernel(total_two, total_one, loss_cols, *refs):
    gain_one, shift_one, gain_two, shift_two, loss = refs[6:]
    for grad, out in zip(refs[:3], refs[3:6]):
        out[...] = grad[...]
    half = total_two.shape[-1]
    for total, gain, shift in ((total_two, gain_two, shift_two), (total_one, gain_one, shift_one)):
        for h in PAIR:
            cols = pl.ds(h * half, half)
            shift[:, cols] = total[h, FIRST] + total[h, SECOND]
            gain[:, cols] = total[h, THIRD] + total[h, FOURTH]
    loss[...] = jnp.sum(loss_cols[...], axis=1, keepdims=True)


def finish(total_two, total_one, loss_cols, grads):
    vm = pl.BlockSpec(memory_space=pltpu.VMEM)
    row = jax.ShapeDtypeStruct((1, loss_cols.shape[1]), F32)
    outs = pl.pallas_call(
        finish_kernel,
        out_shape=[jax.ShapeDtypeStruct(grad.shape, F32) for grad in grads] + [row] * 4 + [jax.ShapeDtypeStruct((1, 1), F32)],
        in_specs=[vm] * 6,
        out_specs=[vm] * 8,
    )(total_two, total_one, loss_cols, *grads)
    return outs[:3], [row.reshape(-1) for row in outs[3:7]], outs[7].reshape(())


def solution(mesh):
    shards = mesh.shape["data"]

    def local_step(h_a, h_b, w_one, w_two, w_three, gain_one, shift_one, gain_two, shift_two, lam_off):
        rows_dev = h_a.shape[0]
        total_rows = rows_dev * shards
        grad_w_three, grad_w_two, grad_w_one, loss_cols, total_two, total_one = step(
            total_rows, 67000000, lam_off, h_a, h_b, (w_one, w_two, w_three),
            (gain_one, shift_one, gain_two, shift_two))[:6]
        grads, vectors, loss_total = finish(total_two, total_one, loss_cols, [grad_w_one, grad_w_two, grad_w_three])
        return (loss_total, *grads, *vectors)

    row_spec = P("data", None)
    whole_mat = P(None, None)
    whole_vec = P(None)
    return jax.shard_map(
        local_step, mesh=mesh,
        in_specs=(row_spec, row_spec, whole_mat, whole_mat, whole_mat,
                  whole_vec, whole_vec, whole_vec, whole_vec, P()),
        out_specs=(P(), row_spec, row_spec, row_spec, whole_vec, whole_vec, whole_vec, whole_vec),
        check_vma=False)
```

```python
import functools

import jax
import jax.numpy as jnp
from jax import lax
from jax.experimental import pallas as pl
from jax.experimental.pallas import tpu as pltpu
from jax.sharding import PartitionSpec as P

NORM_EPS = 1e-5
MESH = pl.DeviceIdType.MESH
F32 = jnp.float32
BF16 = jnp.bfloat16


ALL = slice(None)
FIRST, SECOND, THIRD, FOURTH = [slice(k, k + 1) for k in range(4)]
PAIR = range(2)
OTHERS = range(3)
LINE = 4
CUBE = 8
DEPTH_DIMS = (((0,), (0,)), ((), ()))
LANE_DIMS = (((1,), (1,)), ((), ()))
DMA_SEM = pltpu.SemaphoreType.DMA


def loop(count):
    return pl.loop(0, count)


def col_sum(values):
    return jnp.sum(values, axis=0, keepdims=True)


class Place:
    def __init__(self):
        me = lax.axis_index("data")
        self.core = lax.rem(me, 2)
        self.x = lax.rem(lax.div(me, 2), 2)
        self.y = lax.rem(lax.div(me, 4), 2)
        self.z = lax.div(me, 8)
        self.plane = lax.rem(lax.div(me, 2), 4)
        self.partner = me + 1 - 2 * self.core
        self.x_peer = me + 2 - 4 * self.x
        self.y_peer = me + 4 - 8 * self.y
        self.low = lax.rem(me, CUBE)
        self.others = [lax.rem(self.z + d + 1, LINE) for d in OTHERS]
        self.z_peers = [z * CUBE + self.low for z in self.others]
        self.plane_peers = [self.z * CUBE + lax.rem(self.plane + d + 1, LINE) * 2 + self.core for d in OTHERS]
        self.cube_peers = [self.z * CUBE + lax.rem(self.low + d + 1, CUBE) for d in range(CUBE - 1)]
        self.near = [self.partner] + self.plane_peers + self.z_peers


def enter(peers):
    barrier = pltpu.get_barrier_semaphore()
    for peer in peers:
        pl.semaphore_signal(barrier, inc=1, device_id=(peer,), device_id_type=MESH)
    pl.semaphore_wait(barrier, len(peers))


def remote(src, dst, send_sem, recv_sem, peer):
    return pltpu.make_async_remote_copy(
        src_ref=src, dst_ref=dst, send_sem=send_sem, recv_sem=recv_sem,
        device_id=(peer,), device_id_type=MESH)


class Sums:
    def __init__(self, at, local, total, recv0, slots1, slots2, send_sem, recv_sem):
        self.at, self.refs = at, (local, total)
        self.recv0, self.slots1, self.slots2 = recv0, slots1, slots2
        self.send_sem, self.recv_sem = send_sem, recv_sem
        self.half = recv0.shape[-1]
        self.mine = pl.multiple_of(at.core * self.half, 128)
        self.theirs = pl.multiple_of((1 - at.core) * self.half, 128)

    def pick(self, k, first):
        ref, index = self.refs[k]
        return ref.at[(*index, ALL, pl.ds(first, self.half))]

    def copies(self, stage):
        at = self.at
        if stage == 0:
            pairs = [(0, self.pick(0, self.theirs), self.recv0, at.partner)]
        elif stage == 1:
            here = self.slots1.at[at.plane]
            pairs = [(1 + d, here, here, at.plane_peers[d]) for d in OTHERS]
        elif stage == 2:
            here = self.slots2.at[at.z]
            pairs = [(4 + d, here, here, at.z_peers[d]) for d in OTHERS]
        else:
            here = self.pick(1, self.mine)
            pairs = [(7, here, here, at.partner)]
        return [remote(src, dst, self.send_sem.at[k], self.recv_sem.at[k], peer) for k, src, dst, peer in pairs]

    def send(self, stage):
        for copy in self.copies(stage):
            copy.start()

    def arrive(self, stage=3):
        for copy in self.copies(stage):
            copy.wait()

    def begin(self):
        self.send(0)

    def over_plane(self):
        self.arrive(0)
        self.slots1[self.at.plane] = self.pick(0, self.mine)[...] + self.recv0[...]
        self.send(1)

    def over_line(self):
        self.arrive(1)
        self.slots2[self.at.z] = jnp.sum(self.slots1[...], axis=0)
        self.send(2)

    def over_pair(self):
        self.arrive(2)
        self.pick(1, self.mine)[...] = jnp.sum(self.slots2[...], axis=0)
        self.send(3)


class QuickSums:
    def __init__(self, at, local, total, slots1, slots2, send_sem, recv_sem):
        self.at, self.local, self.total = at, local, total
        self.slots1, self.slots2 = slots1, slots2
        self.send_sem, self.recv_sem = send_sem, recv_sem

    def copies(self, across):
        at = self.at
        if across:
            here, peers, first = self.slots2.at[at.low], at.cube_peers, len(at.z_peers)
        else:
            here, peers, first = self.slots1.at[at.z], at.z_peers, 0
        return [remote(here, here, self.send_sem.at[first + d], self.recv_sem.at[first + d], peer)
                for d, peer in enumerate(peers)]

    def begin(self):
        ref, index = self.local
        self.slots1[self.at.z] = ref[index]
        for copy in self.copies(False):
            copy.start()

    def over_plane(self):
        for copy in self.copies(False):
            copy.wait()
        self.slots2[self.at.low] = jnp.sum(self.slots1[...], axis=0)
        for copy in self.copies(True):
            copy.start()

    def arrive(self):
        for copy in self.copies(True):
            copy.wait()
        ref, index = self.total
        ref[index] = jnp.sum(self.slots2[...], axis=0)


def quick_scratch(rows, cols):
    return [
        pltpu.VMEM((LINE, rows, cols), F32),
        pltpu.VMEM((CUBE, rows, cols), F32),
        DMA_SEM((LINE + CUBE,)),
        DMA_SEM((LINE + CUBE,)),
    ]


def sums_scratch(rows, cols):
    return [
        pltpu.VMEM((rows, cols // 2), F32),
        pltpu.VMEM((4, rows, cols // 2), F32),
        pltpu.VMEM((4, rows, cols // 2), F32),
        DMA_SEM((8,)),
        DMA_SEM((8,)),
    ]


class Ring:
    def __init__(self, at, total, spread, part, recv0, kept, snd1, recv1, snd2, recv2, snd3, recv3, send_sem, recv_sem, credit):
        self.at, self.total, self.slots, self.spread = at, total, kept.shape[0], spread
        self.part, self.recv0, self.kept = part, recv0, kept
        self.snd1, self.recv1, self.snd2, self.recv2, self.snd3, self.recv3 = snd1, recv1, snd2, recv2, snd3, recv3
        self.send_sem, self.recv_sem, self.credit = send_sem, recv_sem, credit
        self.half = snd1.shape[-1]
        self.peers = [at.partner, at.x_peer, at.y_peer, at.y_peer, at.x_peer] + at.z_peers
        self.givers = self.peers[:5] + at.z_peers[::-1]
        self.own = [at.y, at.x]

    def cols(self, half):
        return pl.ds(half * self.half, self.half)

    def copy(self, q, stage):
        j, s = lax.rem(q, self.slots), lax.rem(q, 2)
        if stage > 7:
            src, dst, peer = self.spread(q, stage)
        else:
            peer = self.peers[stage]
            if stage > 4:
                src, dst = self.snd3.at[j, stage - 5], self.recv3.at[j, stage - 5]
            elif stage > 2:
                src, dst = self.snd2.at[j, stage - 3], self.recv2.at[j, stage - 3]
            elif stage:
                src, dst = self.snd1.at[j, stage - 1], self.recv1.at[j, stage - 1]
            else:
                src, dst = self.part.at[s, :, :, :, 1 - self.at.core], self.recv0.at[s]
        return remote(src, dst, self.send_sem.at[j, stage], self.recv_sem.at[j, stage], peer)

    def start(self, q, *stages):
        for stage in stages:
            self.copy(q, stage).start()

    def wait(self, q, *stages):
        for stage in stages:
            self.copy(q, stage).wait()

    def depth(self, stage):
        return self.slots if stage else self.part.shape[0]

    def send(self, q, *stages):
        for stage in stages:
            depth = self.depth(stage)
            pl.when(q >= depth)(lambda: pl.semaphore_wait(self.credit.at[lax.rem(q, depth), stage], 1))
            self.start(q, stage)

    def give(self, q, *stages):
        for stage in stages:
            depth = self.depth(stage)
            pl.when(q + depth < self.total)(lambda: pl.semaphore_signal(
                self.credit.at[lax.rem(q, depth), stage], inc=1, device_id=(self.givers[stage],), device_id_type=MESH))

    def pair(self, q):
        self.send(q, 0)

    def first(self, q):
        at, s, j = self.at, lax.rem(q, 2), lax.rem(q, self.slots)
        self.wait(q, 0)

        @loop(LINE)
        def _(z):
            for half in PAIR:
                cols = self.cols(half)
                for k in PAIR:
                    (y, x), (oy, ox) = ((at.y, k), (1 - at.y, k)) if half else ((k, at.x), (k, 1 - at.x))
                    self.snd1[j, half, z, k] = (
                        self.part[s, z, oy, ox, at.core, :, cols] + self.recv0[s, z, oy, ox, :, cols]).astype(BF16)
                    self.kept[j, half, z, k] = self.part[s, z, y, x, at.core, :, cols] + self.recv0[s, z, y, x, :, cols]

        self.give(q, 0)
        self.send(q, 1, 2)

    def second(self, q):
        j = lax.rem(q, self.slots)
        for half in PAIR:
            own = self.own[half]
            self.wait(q, 1 + half)

            @loop(LINE)
            def _(z):
                self.snd2[j, half, z] = (
                    self.kept[j, half, z, 1 - own] + self.recv1[j, half, z, 1 - own].astype(F32)).astype(BF16)
                self.kept[j, half, z, own] = self.kept[j, half, z, own] + self.recv1[j, half, z, own].astype(F32)

            self.give(q, 1 + half)
            self.send(q, 3 + half)

    def summed(self, j, half, z):
        return self.kept[j, half, z, self.own[half]] + self.recv2[j, half, z].astype(F32)

    def third(self, q):
        j = lax.rem(q, self.slots)
        self.wait(q, 3, 4)

        @loop(len(OTHERS))
        def _(d):
            z = lax.rem(self.at.z + d + 1, LINE)
            for half in PAIR:
                self.snd3[j, d, :, self.cols(half)] = self.summed(j, half, z).astype(BF16)

        self.send(q, 5, 6, 7)

    def last(self, q):
        j = lax.rem(q, self.slots)
        totals = [self.summed(j, half, self.at.z) for half in PAIR]
        self.wait(q, 5, 6, 7)
        for d in OTHERS:
            totals = [total + self.recv3[j, d, :, self.cols(half)].astype(F32) for half, total in enumerate(totals)]
        self.give(q, 3, 4, 5, 6, 7)
        return totals


def ring_scratch(slots, rows, width):
    half = width // 2
    return [
        pltpu.VMEM((2, 4, 2, 2, 2, rows, width), F32),
        pltpu.VMEM((2, 4, 2, 2, rows, width), F32),
        pltpu.VMEM((slots, 2, 4, 2, rows, half), F32),
    ] + [pltpu.VMEM((slots, 2, 4, 2, rows, half), BF16)] * 2 + [pltpu.VMEM((slots, 2, 4, rows, half), BF16)] * 2 + [
        pltpu.VMEM((slots, 3, rows, width), BF16)] * 2 + [DMA_SEM((slots, 16))] * 2 + [
        pltpu.SemaphoreType.REGULAR((slots, 8))]


CHUNKS = 8
RING = 12
SUMS = 5
QUICK = 4
SPREAD_LAGS = (1, 2, 3, 4, 6, 7, 8, 9)
RING_LAGS = (1, 3, 5, 8)


def step_kernel(
        total_rows, lam_ref, feat_a, feat_b, w_one, w_two, w_three, gain_one, shift_one, gain_two, shift_two,
        grad_w_three, grad_w_two, grad_w_one, loss_total, total_two, total_one, saved_act, saved_norm,
        grad, pre, wide, turned, weight, normed, act, sides, side_sums, local, embed_local, embed_total, loss_local, mean_col, turned_sums, by_row, scales,
        wide_sem, w_sem, load_sem, out_sem, *scratch):
    at = Place()
    place = (at.z, at.y, at.x, at.core)

    def spread(q, stage):
        cols = ring.cols((stage - 1) % 2)
        if stage < 11:
            here, peer = wide.at[(q, *place)], at.z_peers[stage - 8]
        elif stage == 11:
            here, peer = wide.at[q, :, at.y, at.x, at.core, :, cols], at.y_peer
        elif stage == 12:
            here, peer = wide.at[q, :, at.y, at.x, at.core, :, cols], at.x_peer
        elif stage == 13:
            here, peer = wide.at[q, :, :, at.x, at.core, :, cols], at.x_peer
        elif stage == 14:
            here, peer = wide.at[q, :, at.y, :, at.core, :, cols], at.y_peer
        else:
            here, peer = wide.at[q, :, :, :, at.core], at.partner
        return here, here, peer

    ring = Ring(at, 4 * CHUNKS, spread, *scratch[:RING])
    rows_dev, dim = grad.shape
    width = dim // CHUNKS
    view_rows = rows_dev // 2
    block_rows = min(128, view_rows)
    quarter = dim // 4
    count = 1.0 / total_rows
    weights = [w_one, w_two, w_three]
    gains, shifts = [gain_one, gain_two], [shift_one, shift_two]
    outs = [grad_w_three, grad_w_two, grad_w_one]
    totals = [embed_total, total_two, total_one]
    views = [pl.ds(v * view_rows, view_rows) for v in PAIR]
    rest = list(scratch[RING:])

    def take(number):
        taken, rest[:] = rest[:number], rest[number:]
        return taken

    top = pl.ds(0, 2)
    side = [[QuickSums(at, (sides, (layer, v, top)), (side_sums, (layer, v, top)), *take(QUICK)) for v in PAIR] for layer in OTHERS]
    pair_sums = QuickSums(at, (sides, (0, 0)), (side_sums, (0, 0)), *take(QUICK))
    loss_sums = QuickSums(at, (loss_local, ...), (loss_total, ...), *take(QUICK))
    sums = [[Sums(at, (embed_local, ()), (embed_total, ()), *take(SUMS))]]
    for layer in PAIR:
        sums.append([Sums(at, (local, (layer, h)), (totals[layer + 1], (h,)), *take(SUMS)) for h in PAIR])

    def act_copy(layer):
        return pltpu.make_async_copy(saved_act.at[1 - layer], act, load_sem.at[0])

    def norm_copy(layer):
        return pltpu.make_async_copy(saved_norm.at[1 - layer], normed.at[layer], load_sem.at[1])

    def feat_copy(v):
        return pltpu.make_async_copy((feat_a, feat_b)[v], normed.at[0, views[v]], load_sem.at[v])

    def wide_copy(layer, n):
        cols = pl.ds(pl.multiple_of(n * width, width), width)
        return pltpu.make_async_copy(weights[layer].at[:, :, :, :, :, cols], wide.at[n], wide_sem.at[n])

    feat_copy(0).start()
    lead = 4
    for n in range(lead):
        wide_copy(0, n).start()
    feat_copy(1).start()
    puts = {}

    def put(name, v, src, dst, k):
        copy = pltpu.make_async_copy(src, dst, out_sem.at[k, v])
        copy.start()
        puts[name, v] = copy

    def drain(*names):
        for name in names:
            for v in PAIR:
                puts.pop((name, v)).wait()

    def matmul(layer, v, hook, step):
        @loop(CHUNKS // LINE)
        def _(m):
            if step:
                pl.when(m == hook)(step)
            chunks = [LINE * m + k for k in range(LINE)]
            if v == 0:
                if layer == 0:
                    for n in chunks:
                        pl.when(n + lead < CHUNKS)(lambda n=n: wide_copy(0, n + lead).start())
                for n in chunks:
                    wide_copy(layer, n).wait()
            elif layer < 2:
                for n in chunks:
                    pl.when(m > 0)(lambda n=n: wide_copy(layer + 1, n - LINE).start())
            for n in chunks:
                cols = pl.ds(pl.multiple_of(n * width, width), width)
                out = jnp.dot(normed[layer % 2, views[v]], wide[n].reshape(dim, width), preferred_element_type=F32)
                pre[views[v], cols] = out
                sides[layer, v, FIRST, cols] = col_sum(out)
                sides[layer, v, SECOND, cols] = col_sum(out * out)

        if v and layer < 2:
            for n in range(LINE):
                wide_copy(layer + 1, LINE + n).start()
        side[layer][v].begin()

    def normalise(layer, v):
        side[layer][v].arrive()
        mean = side_sums[layer, v, FIRST, :] / total_rows
        inv = lax.rsqrt(side_sums[layer, v, SECOND, :] / total_rows - mean * mean + NORM_EPS)
        scales[2 - layer, v:v + 1, :] = gains[layer][...] * inv if layer < 2 else inv
        sides[layer, v, FIRST, :] = mean
        sides[layer, v, SECOND, :] = inv

        @loop(CHUNKS)
        def _(n):
            cols = pl.ds(pl.multiple_of(n * width, width), width)
            mean, inv = sides[layer, v, FIRST, cols], sides[layer, v, SECOND, cols]
            if layer < 2:
                gain, shift = gains[layer][:, cols], shifts[layer][:, cols]

            @loop(view_rows // block_rows)
            def _(r):
                rows = pl.ds(pl.multiple_of(v * view_rows + r * block_rows, block_rows), block_rows)
                value = (pre[rows, cols] - mean) * inv
                if layer < 2:
                    grad[rows, cols] = value.astype(BF16)
                    value = jnp.maximum(gain * value + shift, 0.0)
                normed[(layer + 1) % 2, rows, cols] = value.astype(BF16)

        if layer < 2:
            put(("act", layer), v, normed.at[(layer + 1) % 2, views[v]], saved_act.at[layer, views[v]], layer)
            put(("norm", layer), v, grad.at[views[v]], saved_norm.at[layer, views[v]], 2)

    def turn(src, dst, first, v):
        part = view_rows // 2

        @loop(CHUNKS)
        def _(n):
            cols = pl.ds(pl.multiple_of(n * width, width), width)
            for k in PAIR:
                block = src[pl.ds(v * view_rows + k * part, part), cols].T
                dst[first + 2 * v + k, lax.div(n, 2), lax.rem(n, 2)] = block.reshape(dst.shape[3:])

    enter(at.z_peers + at.cube_peers)
    feat_copy(0).wait()
    matmul(0, 0, 0, None)
    feat_copy(1).wait()
    matmul(0, 1, 1, side[0][0].over_plane)
    for v in PAIR:
        turn(normed.at[0], turned, 0, v)
    normalise(0, 0)
    for layer in PAIR:
        matmul(layer + 1, 0, 0, side[layer][1].over_plane)
        normalise(layer, 1)
        matmul(layer + 1, 1, 1, side[layer + 1][0].over_plane)
        if layer == 0:
            drain(("norm", 0))
        else:
            drain(("act", 0))
        normalise(layer + 1, 0)
    side[2][1].over_plane()
    normalise(2, 1)

    drain(("act", 1), ("norm", 1))
    act_copy(0).start()
    slots = weight.shape[0]

    def weight_copy(layer, n):
        slot = lax.rem(n, slots)
        return pltpu.make_async_copy(weights[2 - layer].at[lax.div(n, 2), lax.rem(n, 2)], weight.at[slot], w_sem.at[slot])

    for n in range(slots):
        weight_copy(0, n).start()

    lam = lam_ref[0]
    lane = 128
    block_rows_dev = ring.snd1.shape[-2]
    first_row = (((at.z * 2 + at.y) * 2 + at.x) * 2 + at.core) * block_rows_dev

    def pair_rows():
        @loop(CHUNKS)
        def _(n):
            cols = pl.ds(pl.multiple_of(n * width, width), width)
            one, two = [normed[1, views[v], cols].astype(F32) for v in PAIR]
            sides[0, 0, FIRST, cols] = col_sum(one)
            sides[0, 0, SECOND, cols] = col_sum(two)
            sides[0, 0, THIRD, cols] = col_sum(one * two)
            sides[0, 0, FOURTH, cols] = jnp.zeros((1, width), F32)
            pre[views[0], cols] = jnp.zeros((view_rows, width), F32)

        by_row[...] = jnp.zeros_like(by_row)
        pair_sums.begin()

    block = pl.ds(pl.multiple_of(lax.div(first_row, lane) * lane, lane), lane)
    part = lax.rem(first_row, lane)

    def keep_means():
        pair_sums.arrive()
        turned_sums[...] = jnp.broadcast_to(side_sums[0, 0, FIRST, block], (lane, lane)).T
        mean_col[...] = turned_sums[pl.ds(pl.multiple_of(part, 8), block_rows_dev), :]

    def row_sums():
        for k, row in enumerate((FIRST, THIRD)):
            sums_here = col_sum(by_row[k].T)
            spread = jnp.concatenate([sums_here] * (lane // block_rows_dev), axis=1)
            position = lax.broadcasted_iota(jnp.int32, spread.shape, 1)
            mine = (position >= part) & (position < part + block_rows_dev)
            embed_local[row, :] = jnp.zeros((1, dim), F32)
            embed_local[row, block] = jnp.where(mine, spread, 0.0)


    def chunk_cols(q):
        return pl.ds(pl.multiple_of(q * width, width), width)

    def correlate(q):
        @loop(LINE)
        def _(z):
            rows = pl.ds(pl.multiple_of(z * quarter, quarter), quarter)
            out = lax.dot_general(normed[1, views[0], rows], normed[1, views[1], chunk_cols(q)], DEPTH_DIMS,
                                  preferred_element_type=F32)
            ring.part[lax.rem(q, 2), z] = out.reshape(ring.part.shape[2:])

        ring.pair(q)

    def spread_line(q):
        for half, total in enumerate(ring.last(q)):
            start = q * width + half * ring.half
            row = first_row + lax.broadcasted_iota(jnp.int32, total.shape, 0)
            col = start + lax.broadcasted_iota(jnp.int32, total.shape, 1)
            diag = row == col
            cols = pl.ds(pl.multiple_of(start, ring.half), ring.half)
            total = jnp.where(diag, side_sums[0, 0, THIRD, cols], total)
            corr = total * count
            gap = 1.0 - corr
            loss_local[:, cols] = col_sum(jnp.where(diag, gap * gap, lam * corr * corr))
            slope = (jnp.where(diag, -2.0 * gap, 2.0 * lam * corr) * count).astype(BF16)
            wide[(q, *place, ALL, ring.cols(half))] = slope
            slope = slope.astype(F32)
            embed_local[SECOND, cols] = col_sum(slope * mean_col[:, :ring.half])
            embed_local[FOURTH, cols] = col_sum(slope * total)
            terms = [slope * side_sums[0, 0, SECOND, cols], slope * total]
            for k, term in enumerate(terms):
                by_row[k] = by_row[k] + term
        ring.start(q, 8, 9, 10)

    def spread_one(q):
        ring.wait(q, 8, 9, 10)
        ring.start(q, 11, 12)

    def spread_two(q):
        ring.wait(q, 11, 12)
        ring.start(q, 13, 14)

    def spread_pair(q):
        ring.wait(q, 13, 14)
        ring.start(q, 15)

    def embed_grad(q):
        ring.wait(q, 15)
        cols = chunk_cols(q)
        pre[views[1], cols] = jnp.dot(normed[1, views[0]], wide[q].reshape(dim, width), preferred_element_type=F32)

        @loop(2)
        def _(p):
            into = pl.ds(pl.multiple_of(p * 2 * quarter, quarter), 2 * quarter)
            rows = lax.dot_general(normed[1, views[1], cols], wide[q, pl.ds(2 * p, 2)].reshape(2 * quarter, width), LANE_DIMS,
                                   preferred_element_type=F32)
            pre[views[0], into] = pre[views[0], into] + rows

    first_sums = sums[0][0]
    steps = (ring.first, ring.second, ring.third, spread_line, spread_one, spread_two, spread_pair, embed_grad)
    done = CHUNKS + SPREAD_LAGS[3]

    def start_sums():
        row_sums()
        first_sums.begin()

    def turn_two():
        for v in PAIR:
            turn(normed.at[0], wide, 0, v)
        norm_copy(0).start()

    moves = ((0, pair_rows), (1, pair_sums.over_plane), (3, keep_means), (done, start_sums), (done + 1, first_sums.over_plane),
             (done + 2, first_sums.over_line), (done + 3, first_sums.over_pair))

    @loop(CHUNKS + SPREAD_LAGS[-1])
    def _(t):
        pl.when(t < CHUNKS)(lambda: correlate(t))
        for when, move in moves:
            pl.when(t == when)(move)
        for step, lag in zip(steps, SPREAD_LAGS):
            pl.when((t >= lag) & (t < lag + CHUNKS))(lambda step=step, lag=lag: step(t - lag))
        pl.when(t == SPREAD_LAGS[-1] + LINE)(turn_two)

    loss_sums.begin()

    def finish_grad(layer, j):
        cols = chunk_cols(j)
        per = CHUNKS // 2
        total, sel = (embed_total, cols) if layer == 0 else (totals[layer].at[lax.div(j, per)], chunk_cols(lax.rem(j, per)))
        for v in PAIR:
            mean0 = total[v:v + 1, sel] * count
            mean1 = total[2 + v:3 + v, sel] * count
            scale = scales[layer, v:v + 1, cols]

            @loop(view_rows // block_rows)
            def _(r):
                rows = pl.ds(pl.multiple_of(v * view_rows + r * block_rows, block_rows), block_rows)
                xhat = normed[(layer + 1) % 2, rows, cols].astype(F32)
                grad[rows, cols] = (scale * (pre[rows, cols] - (mean0 + xhat * mean1))).astype(BF16)

    def weight_grad(layer, j):
        q = (layer + 1) * CHUNKS + j
        source, first = (turned, 0) if layer == 2 else (wide, LINE * layer)

        @loop(2)
        def _(p):
            span = pl.ds(2 * p, 2)
            feed = jnp.concatenate([source[first + k, span].reshape(2 * quarter, -1) for k in range(LINE)], axis=1)
            out = jnp.dot(feed, grad[:, chunk_cols(j)], preferred_element_type=F32)
            ring.part[lax.rem(q, 2), span] = out.reshape(2, *ring.part.shape[2:])

        ring.pair(q)

    def input_grad(layer, n):
        cols = chunk_cols(n)
        weight_copy(layer, n).wait()
        half = local.at[layer, lax.div(n, CHUNKS // 2)]
        sel = chunk_cols(lax.rem(n, CHUNKS // 2))

        @loop(2)
        def _(v):
            rows = pl.ds(pl.multiple_of(v * view_rows, view_rows), view_rows)
            out = lax.dot_general(grad[rows, :], weight[lax.rem(n, slots)].reshape(width, dim), LANE_DIMS,
                                  preferred_element_type=F32)
            out = jnp.where(act[rows, cols] > 0, out, 0.0)
            pre[rows, cols] = out
            half[pl.ds(v, 1), sel] = col_sum(out)
            half[pl.ds(2 + v, 1), sel] = col_sum(out * normed[layer % 2, rows, cols].astype(F32))

        pl.when(n + slots < CHUNKS)(lambda: weight_copy(layer, n + slots).start())

    def serve(layer, j):
        t = layer * CHUNKS + j
        for step, lag in zip((ring.first, ring.second, ring.third), RING_LAGS):
            pl.when((t >= lag) & (t < lag + 3 * CHUNKS))(lambda step=step, lag=lag: step(CHUNKS + t - lag))
        if layer:
            for half, block in enumerate(ring.last(t)):
                outs[layer - 1][:, pl.ds(pl.multiple_of(j * width + half * ring.half, ring.half), ring.half)] = block

    for layer in OTHERS:
        old, new = sums[layer], sums[layer + 1] if layer < 2 else None
        old[0].arrive()

        def settle():
            if layer:
                old[1].arrive()

            @pl.loop(3, CHUNKS)
            def _(k):
                finish_grad(layer, k)

            if layer == 0:
                norm_copy(1).start()

        def late_loads():
            new[1].begin()
            if layer == 0:
                act_copy(1).start()
                for n in range(slots):
                    weight_copy(1, n).start()

        def relay_pair():
            new[0].over_pair()
            new[1].over_plane()

        before, middle, after = [], [(2, settle)], []
        if layer:
            middle.append((0, old[1].over_pair))
        if layer == 0:
            before.append((3, lambda: act_copy(0).wait()))
        if new:
            before += [(2, lambda: norm_copy(layer).wait()), (5, new[0].over_plane), (6, new[0].over_line), (7, relay_pair)]
            after += [(4, new[0].begin), (6, late_loads), (7, new[1].over_line)]

        @loop(CHUNKS)
        def _(j):
            for when, move in before:
                pl.when(j == when)(move)
            pl.when(j < 3)(lambda: finish_grad(layer, j))
            weight_grad(layer, j)
            for when, move in middle:
                pl.when(j == when)(move)
            if new:
                @pl.when((j > 2) & (j < 7))
                def _():
                    @loop(2)
                    def _(k):
                        input_grad(layer, 2 * (j - 3) + k)
            for when, move in after:
                pl.when(j == when)(move)
            serve(layer, j)

        if layer == 0:
            act_copy(1).wait()
            for v in PAIR:
                turn(act, wide, LINE, v)
            loss_sums.over_plane()

    @loop(CHUNKS)
    def _(j):
        serve(len(OTHERS), j)

    loss_sums.arrive()


def step(total_rows, vmem, lam, feat_a, feat_b, weights, vectors):
    view_rows, dim = feat_a.shape
    rows, width, blocks = 2 * view_rows, dim // CHUNKS, dim // 32
    hbm = pl.BlockSpec(memory_space=pl.ANY)
    vm = pl.BlockSpec(memory_space=pltpu.VMEM)
    cube = (LINE, 2, 2, 2, blocks)
    scratch = [
        pltpu.VMEM((rows, dim), BF16),
        pltpu.VMEM((rows, dim), F32),
        pltpu.VMEM((CHUNKS, *cube, width), BF16),
        pltpu.VMEM((LINE, *cube, view_rows // 2), BF16),
        pltpu.VMEM((3, 2, 2, blocks, dim), BF16),
        pltpu.VMEM((2, rows, dim), BF16),
        pltpu.VMEM((rows, dim), BF16),
        pltpu.VMEM((3, 2, 4, dim), F32),
        pltpu.VMEM((3, 2, 4, dim), F32),
        pltpu.VMEM((2, 2, 4, dim // 2), F32),
        pltpu.VMEM((4, dim), F32),
        pltpu.VMEM((4, dim), F32),
        pltpu.VMEM((1, dim), F32),
        pltpu.VMEM((blocks, 128), F32),
        pltpu.VMEM((128, 128), F32),
        pltpu.VMEM((2, blocks, width // 2), F32),
        pltpu.VMEM((3, 2, dim), F32),
        DMA_SEM((CHUNKS,)),
        DMA_SEM((3,)),
        DMA_SEM((3,)),
        DMA_SEM((3, 2)),
    ] + ring_scratch(CHUNKS, blocks, width)
    for _ in range(6):
        scratch += quick_scratch(2, dim)
    scratch += quick_scratch(4, dim) + quick_scratch(1, dim) + sums_scratch(4, dim)
    for _ in range(4):
        scratch += sums_scratch(4, dim // 2)
    halves = jax.ShapeDtypeStruct((2, 4, dim // 2), F32)
    saved = jax.ShapeDtypeStruct((2, rows, dim), BF16)
    return pl.pallas_call(
        functools.partial(step_kernel, total_rows),
        out_shape=[jax.ShapeDtypeStruct((blocks, dim), F32)] * 3 + [
            jax.ShapeDtypeStruct((1, dim), F32), halves, halves, saved, saved],
        in_specs=[pl.BlockSpec(memory_space=pltpu.SMEM)] + [hbm] * 5 + [vm] * 4,
        out_specs=[vm] * 6 + [hbm] * 2,
        scratch_shapes=scratch,
        compiler_params=pltpu.CompilerParams(collective_id=0, has_side_effects=True, vmem_limit_bytes=vmem),
    )(lam.reshape(1), feat_a, feat_b, *[weight.reshape(*cube, dim) for weight in weights],
      *[value.reshape(1, dim) for value in vectors])


def finish_kernel(total_two, total_one, loss_cols, *refs):
    gain_one, shift_one, gain_two, shift_two, loss = refs[6:]
    for grad, out in zip(refs[:3], refs[3:6]):
        out[...] = grad[...]
    half = total_two.shape[-1]
    for total, gain, shift in ((total_two, gain_two, shift_two), (total_one, gain_one, shift_one)):
        for h in PAIR:
            cols = pl.ds(h * half, half)
            shift[:, cols] = total[h, FIRST] + total[h, SECOND]
            gain[:, cols] = total[h, THIRD] + total[h, FOURTH]
    loss[...] = jnp.sum(loss_cols[...], axis=1, keepdims=True)


def finish(total_two, total_one, loss_cols, grads):
    vm = pl.BlockSpec(memory_space=pltpu.VMEM)
    row = jax.ShapeDtypeStruct((1, loss_cols.shape[1]), F32)
    outs = pl.pallas_call(
        finish_kernel,
        out_shape=[jax.ShapeDtypeStruct(grad.shape, F32) for grad in grads] + [row] * 4 + [jax.ShapeDtypeStruct((1, 1), F32)],
        in_specs=[vm] * 6,
        out_specs=[vm] * 8,
    )(total_two, total_one, loss_cols, *grads)
    return outs[:3], [row.reshape(-1) for row in outs[3:7]], outs[7].reshape(())


def solution(mesh):
    shards = mesh.shape["data"]

    def local_step(h_a, h_b, w_one, w_two, w_three, gain_one, shift_one, gain_two, shift_two, lam_off):
        rows_dev = h_a.shape[0]
        total_rows = rows_dev * shards
        grad_w_three, grad_w_two, grad_w_one, loss_cols, total_two, total_one = step(
            total_rows, 67000000, lam_off, h_a, h_b, (w_one, w_two, w_three),
            (gain_one, shift_one, gain_two, shift_two))[:6]
        grads, vectors, loss_total = finish(total_two, total_one, loss_cols, [grad_w_one, grad_w_two, grad_w_three])
        return (loss_total, *grads, *vectors)

    row_spec = P("data", None)
    whole_mat = P(None, None)
    whole_vec = P(None)
    return jax.shard_map(
        local_step, mesh=mesh,
        in_specs=(row_spec, row_spec, whole_mat, whole_mat, whole_mat,
                  whole_vec, whole_vec, whole_vec, whole_vec, P()),
        out_specs=(P(), row_spec, row_spec, row_spec, whole_vec, whole_vec, whole_vec, whole_vec),
        check_vma=False)
```

```python
import functools

import jax
import jax.numpy as jnp
from jax import lax
from jax.experimental import pallas as pl
from jax.experimental.pallas import tpu as pltpu
from jax.sharding import PartitionSpec as P

NORM_EPS = 1e-5
MESH = pl.DeviceIdType.MESH
F32 = jnp.float32
BF16 = jnp.bfloat16


ALL = slice(None)
FIRST, SECOND, THIRD, FOURTH = [slice(k, k + 1) for k in range(4)]
PAIR = range(2)
OTHERS = range(3)
LINE = 4
CUBE = 8
DEPTH_DIMS = (((0,), (0,)), ((), ()))
LANE_DIMS = (((1,), (1,)), ((), ()))
DMA_SEM = pltpu.SemaphoreType.DMA


def loop(count):
    return pl.loop(0, count)


def col_sum(values):
    return jnp.sum(values, axis=0, keepdims=True)


class Place:
    def __init__(self):
        me = lax.axis_index("data")
        self.core = lax.rem(me, 2)
        self.x = lax.rem(lax.div(me, 2), 2)
        self.y = lax.rem(lax.div(me, 4), 2)
        self.z = lax.div(me, 8)
        self.plane = lax.rem(lax.div(me, 2), 4)
        self.partner = me + 1 - 2 * self.core
        self.x_peer = me + 2 - 4 * self.x
        self.y_peer = me + 4 - 8 * self.y
        self.low = lax.rem(me, CUBE)
        self.others = [lax.rem(self.z + d + 1, LINE) for d in OTHERS]
        self.z_peers = [z * CUBE + self.low for z in self.others]
        self.plane_peers = [self.z * CUBE + lax.rem(self.plane + d + 1, LINE) * 2 + self.core for d in OTHERS]
        self.cube_peers = [self.z * CUBE + lax.rem(self.low + d + 1, CUBE) for d in range(CUBE - 1)]
        self.near = [self.partner] + self.plane_peers + self.z_peers


def enter(peers):
    barrier = pltpu.get_barrier_semaphore()
    for peer in peers:
        pl.semaphore_signal(barrier, inc=1, device_id=(peer,), device_id_type=MESH)
    pl.semaphore_wait(barrier, len(peers))


def remote(src, dst, send_sem, recv_sem, peer):
    return pltpu.make_async_remote_copy(
        src_ref=src, dst_ref=dst, send_sem=send_sem, recv_sem=recv_sem,
        device_id=(peer,), device_id_type=MESH)


class Sums:
    def __init__(self, at, local, total, recv0, slots1, slots2, send_sem, recv_sem):
        self.at, self.refs = at, (local, total)
        self.recv0, self.slots1, self.slots2 = recv0, slots1, slots2
        self.send_sem, self.recv_sem = send_sem, recv_sem
        self.half = recv0.shape[-1]
        self.mine = pl.multiple_of(at.core * self.half, 128)
        self.theirs = pl.multiple_of((1 - at.core) * self.half, 128)

    def pick(self, k, first):
        ref, index = self.refs[k]
        return ref.at[(*index, ALL, pl.ds(first, self.half))]

    def copies(self, stage):
        at = self.at
        if stage == 0:
            pairs = [(0, self.pick(0, self.theirs), self.recv0, at.partner)]
        elif stage == 1:
            here = self.slots1.at[at.plane]
            pairs = [(1 + d, here, here, at.plane_peers[d]) for d in OTHERS]
        elif stage == 2:
            here = self.slots2.at[at.z]
            pairs = [(4 + d, here, here, at.z_peers[d]) for d in OTHERS]
        else:
            here = self.pick(1, self.mine)
            pairs = [(7, here, here, at.partner)]
        return [remote(src, dst, self.send_sem.at[k], self.recv_sem.at[k], peer) for k, src, dst, peer in pairs]

    def send(self, stage):
        for copy in self.copies(stage):
            copy.start()

    def arrive(self, stage=3):
        for copy in self.copies(stage):
            copy.wait()

    def begin(self):
        self.send(0)

    def over_plane(self):
        self.arrive(0)
        self.slots1[self.at.plane] = self.pick(0, self.mine)[...] + self.recv0[...]
        self.send(1)

    def over_line(self):
        self.arrive(1)
        self.slots2[self.at.z] = jnp.sum(self.slots1[...], axis=0)
        self.send(2)

    def over_pair(self):
        self.arrive(2)
        self.pick(1, self.mine)[...] = jnp.sum(self.slots2[...], axis=0)
        self.send(3)


class QuickSums:
    def __init__(self, at, local, total, slots1, slots2, send_sem, recv_sem):
        self.at, self.local, self.total = at, local, total
        self.slots1, self.slots2 = slots1, slots2
        self.send_sem, self.recv_sem = send_sem, recv_sem

    def copies(self, across):
        at = self.at
        if across:
            here, peers, first = self.slots2.at[at.low], at.cube_peers, len(at.z_peers)
        else:
            here, peers, first = self.slots1.at[at.z], at.z_peers, 0
        return [remote(here, here, self.send_sem.at[first + d], self.recv_sem.at[first + d], peer)
                for d, peer in enumerate(peers)]

    def begin(self):
        ref, index = self.local
        self.slots1[self.at.z] = ref[index]
        for copy in self.copies(False):
            copy.start()

    def over_plane(self):
        for copy in self.copies(False):
            copy.wait()
        self.slots2[self.at.low] = jnp.sum(self.slots1[...], axis=0)
        for copy in self.copies(True):
            copy.start()

    def arrive(self):
        for copy in self.copies(True):
            copy.wait()
        ref, index = self.total
        ref[index] = jnp.sum(self.slots2[...], axis=0)


def quick_scratch(rows, cols):
    return [
        pltpu.VMEM((LINE, rows, cols), F32),
        pltpu.VMEM((CUBE, rows, cols), F32),
        DMA_SEM((LINE + CUBE,)),
        DMA_SEM((LINE + CUBE,)),
    ]


def sums_scratch(rows, cols):
    return [
        pltpu.VMEM((rows, cols // 2), F32),
        pltpu.VMEM((4, rows, cols // 2), F32),
        pltpu.VMEM((4, rows, cols // 2), F32),
        DMA_SEM((8,)),
        DMA_SEM((8,)),
    ]


class Ring:
    def __init__(self, at, total, spread, part, recv0, kept, snd1, recv1, snd2, recv2, snd3, recv3, send_sem, recv_sem, credit):
        self.at, self.total, self.slots, self.spread = at, total, kept.shape[0], spread
        self.part, self.recv0, self.kept = part, recv0, kept
        self.snd1, self.recv1, self.snd2, self.recv2, self.snd3, self.recv3 = snd1, recv1, snd2, recv2, snd3, recv3
        self.send_sem, self.recv_sem, self.credit = send_sem, recv_sem, credit
        self.half = snd1.shape[-1]
        self.peers = [at.partner, at.x_peer, at.y_peer, at.y_peer, at.x_peer] + at.z_peers
        self.givers = self.peers[:5] + at.z_peers[::-1]
        self.own = [at.y, at.x]

    def cols(self, half):
        return pl.ds(half * self.half, self.half)

    def copy(self, q, stage):
        j, s = lax.rem(q, self.slots), lax.rem(q, 2)
        if stage > 7:
            src, dst, peer = self.spread(q, stage)
        else:
            peer = self.peers[stage]
            if stage > 4:
                src, dst = self.snd3.at[j, stage - 5], self.recv3.at[j, stage - 5]
            elif stage > 2:
                src, dst = self.snd2.at[j, stage - 3], self.recv2.at[j, stage - 3]
            elif stage:
                src, dst = self.snd1.at[j, stage - 1], self.recv1.at[j, stage - 1]
            else:
                src, dst = self.part.at[s, :, :, :, 1 - self.at.core], self.recv0.at[s]
        return remote(src, dst, self.send_sem.at[j, stage], self.recv_sem.at[j, stage], peer)

    def start(self, q, *stages):
        for stage in stages:
            self.copy(q, stage).start()

    def wait(self, q, *stages):
        for stage in stages:
            self.copy(q, stage).wait()

    def depth(self, stage):
        return self.slots if stage else self.part.shape[0]

    def send(self, q, *stages):
        for stage in stages:
            depth = self.depth(stage)
            pl.when(q >= depth)(lambda: pl.semaphore_wait(self.credit.at[lax.rem(q, depth), stage], 1))
            self.start(q, stage)

    def give(self, q, *stages):
        for stage in stages:
            depth = self.depth(stage)
            pl.when(q + depth < self.total)(lambda: pl.semaphore_signal(
                self.credit.at[lax.rem(q, depth), stage], inc=1, device_id=(self.givers[stage],), device_id_type=MESH))

    def pair(self, q):
        self.send(q, 0)

    def first(self, q):
        at, s, j = self.at, lax.rem(q, 2), lax.rem(q, self.slots)
        self.wait(q, 0)

        @loop(LINE)
        def _(z):
            for half in PAIR:
                cols = self.cols(half)
                for k in PAIR:
                    (y, x), (oy, ox) = ((at.y, k), (1 - at.y, k)) if half else ((k, at.x), (k, 1 - at.x))
                    self.snd1[j, half, z, k] = (
                        self.part[s, z, oy, ox, at.core, :, cols] + self.recv0[s, z, oy, ox, :, cols]).astype(BF16)
                    self.kept[j, half, z, k] = self.part[s, z, y, x, at.core, :, cols] + self.recv0[s, z, y, x, :, cols]

        self.give(q, 0)
        self.send(q, 1, 2)

    def second(self, q):
        j = lax.rem(q, self.slots)
        for half in PAIR:
            own = self.own[half]
            self.wait(q, 1 + half)

            @loop(LINE)
            def _(z):
                self.snd2[j, half, z] = (
                    self.kept[j, half, z, 1 - own] + self.recv1[j, half, z, 1 - own].astype(F32)).astype(BF16)
                self.kept[j, half, z, own] = self.kept[j, half, z, own] + self.recv1[j, half, z, own].astype(F32)

            self.give(q, 1 + half)
            self.send(q, 3 + half)

    def summed(self, j, half, z):
        return self.kept[j, half, z, self.own[half]] + self.recv2[j, half, z].astype(F32)

    def third(self, q):
        j = lax.rem(q, self.slots)
        self.wait(q, 3, 4)

        @loop(len(OTHERS))
        def _(d):
            z = lax.rem(self.at.z + d + 1, LINE)
            for half in PAIR:
                self.snd3[j, d, :, self.cols(half)] = self.summed(j, half, z).astype(BF16)

        self.send(q, 5, 6, 7)

    def last(self, q):
        j = lax.rem(q, self.slots)
        totals = [self.summed(j, half, self.at.z) for half in PAIR]
        self.wait(q, 5, 6, 7)
        for d in OTHERS:
            totals = [total + self.recv3[j, d, :, self.cols(half)].astype(F32) for half, total in enumerate(totals)]
        self.give(q, 3, 4, 5, 6, 7)
        return totals


def ring_scratch(slots, rows, width):
    half = width // 2
    return [
        pltpu.VMEM((2, 4, 2, 2, 2, rows, width), F32),
        pltpu.VMEM((2, 4, 2, 2, rows, width), F32),
        pltpu.VMEM((slots, 2, 4, 2, rows, half), F32),
    ] + [pltpu.VMEM((slots, 2, 4, 2, rows, half), BF16)] * 2 + [pltpu.VMEM((slots, 2, 4, rows, half), BF16)] * 2 + [
        pltpu.VMEM((slots, 3, rows, width), BF16)] * 2 + [DMA_SEM((slots, 16))] * 2 + [
        pltpu.SemaphoreType.REGULAR((slots, 8))]


CHUNKS = 8
RING = 12
SUMS = 5
QUICK = 4
SPREAD_LAGS = (1, 2, 3, 4, 6, 7, 9, 10)
RING_LAGS = (1, 3, 5, 8)


def step_kernel(
        total_rows, lam_ref, feat_a, feat_b, w_one, w_two, w_three, gain_one, shift_one, gain_two, shift_two,
        grad_w_three, grad_w_two, grad_w_one, loss_total, total_two, total_one, saved_act, saved_norm,
        grad, pre, wide, turned, weight, normed, act, sides, side_sums, local, embed_local, embed_total, loss_local, mean_col, turned_sums, by_row, scales,
        wide_sem, w_sem, load_sem, out_sem, *scratch):
    at = Place()
    place = (at.z, at.y, at.x, at.core)

    def spread(q, stage):
        cols = ring.cols((stage - 1) % 2)
        if stage < 11:
            here, peer = wide.at[(q, *place)], at.z_peers[stage - 8]
        elif stage == 11:
            here, peer = wide.at[q, :, at.y, at.x, at.core, :, cols], at.y_peer
        elif stage == 12:
            here, peer = wide.at[q, :, at.y, at.x, at.core, :, cols], at.x_peer
        elif stage == 13:
            here, peer = wide.at[q, :, :, at.x, at.core, :, cols], at.x_peer
        elif stage == 14:
            here, peer = wide.at[q, :, at.y, :, at.core, :, cols], at.y_peer
        else:
            here, peer = wide.at[q, :, :, :, at.core], at.partner
        return here, here, peer

    ring = Ring(at, 4 * CHUNKS, spread, *scratch[:RING])
    rows_dev, dim = grad.shape
    width = dim // CHUNKS
    view_rows = rows_dev // 2
    block_rows = min(128, view_rows)
    quarter = dim // 4
    count = 1.0 / total_rows
    weights = [w_one, w_two, w_three]
    gains, shifts = [gain_one, gain_two], [shift_one, shift_two]
    outs = [grad_w_three, grad_w_two, grad_w_one]
    totals = [embed_total, total_two, total_one]
    views = [pl.ds(v * view_rows, view_rows) for v in PAIR]
    rest = list(scratch[RING:])

    def take(number):
        taken, rest[:] = rest[:number], rest[number:]
        return taken

    top = pl.ds(0, 2)
    side = [[QuickSums(at, (sides, (layer, v, top)), (side_sums, (layer, v, top)), *take(QUICK)) for v in PAIR] for layer in OTHERS]
    pair_sums = QuickSums(at, (sides, (0, 0)), (side_sums, (0, 0)), *take(QUICK))
    loss_sums = QuickSums(at, (loss_local, ...), (loss_total, ...), *take(QUICK))
    sums = [[Sums(at, (embed_local, ()), (embed_total, ()), *take(SUMS))]]
    for layer in PAIR:
        sums.append([Sums(at, (local, (layer, h)), (totals[layer + 1], (h,)), *take(SUMS)) for h in PAIR])

    def act_copy(layer):
        return pltpu.make_async_copy(saved_act.at[1 - layer], act, load_sem.at[0])

    def norm_copy(layer):
        return pltpu.make_async_copy(saved_norm.at[1 - layer], normed.at[layer], load_sem.at[1])

    def feat_copy(v):
        return pltpu.make_async_copy((feat_a, feat_b)[v], normed.at[0, views[v]], load_sem.at[v])

    def wide_copy(layer, n):
        cols = pl.ds(pl.multiple_of(n * width, width), width)
        return pltpu.make_async_copy(weights[layer].at[:, :, :, :, :, cols], wide.at[n], wide_sem.at[n])

    feat_copy(0).start()
    lead = 4
    for n in range(lead):
        wide_copy(0, n).start()
    feat_copy(1).start()
    puts = {}

    def put(name, v, src, dst, k):
        copy = pltpu.make_async_copy(src, dst, out_sem.at[k, v])
        copy.start()
        puts[name, v] = copy

    def drain(*names):
        for name in names:
            for v in PAIR:
                puts.pop((name, v)).wait()

    def matmul(layer, v, hook, step):
        @loop(CHUNKS // LINE)
        def _(m):
            if step:
                pl.when(m == hook)(step)
            chunks = [LINE * m + k for k in range(LINE)]
            if v == 0:
                if layer == 0:
                    for n in chunks:
                        pl.when(n + lead < CHUNKS)(lambda n=n: wide_copy(0, n + lead).start())
                for n in chunks:
                    wide_copy(layer, n).wait()
            elif layer < 2:
                for n in chunks:
                    pl.when(m > 0)(lambda n=n: wide_copy(layer + 1, n - LINE).start())
            for n in chunks:
                cols = pl.ds(pl.multiple_of(n * width, width), width)
                out = jnp.dot(normed[layer % 2, views[v]], wide[n].reshape(dim, width), preferred_element_type=F32)
                pre[views[v], cols] = out
                sides[layer, v, FIRST, cols] = col_sum(out)
                sides[layer, v, SECOND, cols] = col_sum(out * out)

        if v and layer < 2:
            for n in range(LINE):
                wide_copy(layer + 1, LINE + n).start()
        side[layer][v].begin()

    def normalise(layer, v):
        side[layer][v].arrive()
        mean = side_sums[layer, v, FIRST, :] / total_rows
        inv = lax.rsqrt(side_sums[layer, v, SECOND, :] / total_rows - mean * mean + NORM_EPS)
        scales[2 - layer, v:v + 1, :] = gains[layer][...] * inv if layer < 2 else inv
        sides[layer, v, FIRST, :] = mean
        sides[layer, v, SECOND, :] = inv

        @loop(CHUNKS)
        def _(n):
            cols = pl.ds(pl.multiple_of(n * width, width), width)
            mean, inv = sides[layer, v, FIRST, cols], sides[layer, v, SECOND, cols]
            if layer < 2:
                gain, shift = gains[layer][:, cols], shifts[layer][:, cols]

            @loop(view_rows // block_rows)
            def _(r):
                rows = pl.ds(pl.multiple_of(v * view_rows + r * block_rows, block_rows), block_rows)
                value = (pre[rows, cols] - mean) * inv
                if layer < 2:
                    grad[rows, cols] = value.astype(BF16)
                    value = jnp.maximum(gain * value + shift, 0.0)
                normed[(layer + 1) % 2, rows, cols] = value.astype(BF16)

        if layer < 2:
            put(("act", layer), v, normed.at[(layer + 1) % 2, views[v]], saved_act.at[layer, views[v]], layer)
            put(("norm", layer), v, grad.at[views[v]], saved_norm.at[layer, views[v]], 2)

    def turn(src, dst, first, v):
        part = view_rows // 2

        @loop(CHUNKS)
        def _(n):
            cols = pl.ds(pl.multiple_of(n * width, width), width)
            for k in PAIR:
                block = src[pl.ds(v * view_rows + k * part, part), cols].T
                dst[first + 2 * v + k, lax.div(n, 2), lax.rem(n, 2)] = block.reshape(dst.shape[3:])

    enter(at.z_peers + at.cube_peers)
    feat_copy(0).wait()
    matmul(0, 0, 0, None)
    feat_copy(1).wait()
    matmul(0, 1, 1, side[0][0].over_plane)
    for v in PAIR:
        turn(normed.at[0], turned, 0, v)
    normalise(0, 0)
    for layer in PAIR:
        matmul(layer + 1, 0, 0, side[layer][1].over_plane)
        normalise(layer, 1)
        matmul(layer + 1, 1, 1, side[layer + 1][0].over_plane)
        if layer == 0:
            drain(("norm", 0))
        else:
            drain(("act", 0))
        normalise(layer + 1, 0)
    by_row[...] = jnp.zeros_like(by_row)
    sides[0, 0, FOURTH, :] = jnp.zeros((1, dim), F32)

    @loop(CHUNKS)
    def _(n):
        cols = pl.ds(pl.multiple_of(n * width, width), width)
        sides[0, 0, FIRST, cols] = col_sum(normed[1, views[0], cols].astype(F32))
        pre[views[0], cols] = jnp.zeros((view_rows, width), F32)

    side[2][1].over_plane()
    normalise(2, 1)

    drain(("act", 1), ("norm", 1))
    act_copy(0).start()
    slots = weight.shape[0]

    def weight_copy(layer, n):
        slot = lax.rem(n, slots)
        return pltpu.make_async_copy(weights[2 - layer].at[lax.div(n, 2), lax.rem(n, 2)], weight.at[slot], w_sem.at[slot])

    for n in range(slots):
        weight_copy(0, n).start()

    lam = lam_ref[0]
    lane = 128
    block_rows_dev = ring.snd1.shape[-2]
    first_row = (((at.z * 2 + at.y) * 2 + at.x) * 2 + at.core) * block_rows_dev

    def pair_rows():
        @loop(CHUNKS)
        def _(n):
            cols = pl.ds(pl.multiple_of(n * width, width), width)
            one, two = [normed[1, views[v], cols].astype(F32) for v in PAIR]
            sides[0, 0, SECOND, cols] = col_sum(two)
            sides[0, 0, THIRD, cols] = col_sum(one * two)

        pair_sums.begin()

    block = pl.ds(pl.multiple_of(lax.div(first_row, lane) * lane, lane), lane)
    part = lax.rem(first_row, lane)

    def keep_means():
        pair_sums.arrive()
        turned_sums[...] = jnp.broadcast_to(side_sums[0, 0, FIRST, block], (lane, lane)).T
        mean_col[...] = turned_sums[pl.ds(pl.multiple_of(part, 8), block_rows_dev), :]

    def row_sums():
        for k, row in enumerate((FIRST, THIRD)):
            sums_here = col_sum(by_row[k].T)
            spread = jnp.concatenate([sums_here] * (lane // block_rows_dev), axis=1)
            position = lax.broadcasted_iota(jnp.int32, spread.shape, 1)
            mine = (position >= part) & (position < part + block_rows_dev)
            embed_local[row, :] = jnp.zeros((1, dim), F32)
            embed_local[row, block] = jnp.where(mine, spread, 0.0)


    def chunk_cols(q):
        return pl.ds(pl.multiple_of(q * width, width), width)

    def correlate(q):
        @loop(LINE)
        def _(z):
            rows = pl.ds(pl.multiple_of(z * quarter, quarter), quarter)
            out = lax.dot_general(normed[1, views[0], rows], normed[1, views[1], chunk_cols(q)], DEPTH_DIMS,
                                  preferred_element_type=F32)
            ring.part[lax.rem(q, 2), z] = out.reshape(ring.part.shape[2:])

        ring.pair(q)

    def spread_line(q):
        for half, total in enumerate(ring.last(q)):
            start = q * width + half * ring.half
            row = first_row + lax.broadcasted_iota(jnp.int32, total.shape, 0)
            col = start + lax.broadcasted_iota(jnp.int32, total.shape, 1)
            diag = row == col
            cols = pl.ds(pl.multiple_of(start, ring.half), ring.half)
            total = jnp.where(diag, side_sums[0, 0, THIRD, cols], total)
            corr = total * count
            gap = 1.0 - corr
            loss_local[:, cols] = col_sum(jnp.where(diag, gap * gap, lam * corr * corr))
            slope = (jnp.where(diag, -2.0 * gap, 2.0 * lam * corr) * count).astype(BF16)
            wide[(q, *place, ALL, ring.cols(half))] = slope
            slope = slope.astype(F32)
            embed_local[SECOND, cols] = col_sum(slope * mean_col[:, :ring.half])
            embed_local[FOURTH, cols] = col_sum(slope * total)
            terms = [slope * side_sums[0, 0, SECOND, cols], slope * total]
            for k, term in enumerate(terms):
                by_row[k] = by_row[k] + term
        ring.start(q, 8, 9, 10)

    def spread_one(q):
        ring.wait(q, 8, 9, 10)
        ring.start(q, 11, 12)

    def spread_two(q):
        ring.wait(q, 11, 12)
        ring.start(q, 13, 14)

    def spread_pair(q):
        ring.wait(q, 13, 14)
        ring.start(q, 15)

    def embed_grad(q):
        ring.wait(q, 15)
        cols = chunk_cols(q)
        pre[views[1], cols] = jnp.dot(normed[1, views[0]], wide[q].reshape(dim, width), preferred_element_type=F32)

        @loop(2)
        def _(p):
            into = pl.ds(pl.multiple_of(p * 2 * quarter, quarter), 2 * quarter)
            rows = lax.dot_general(normed[1, views[1], cols], wide[q, pl.ds(2 * p, 2)].reshape(2 * quarter, width), LANE_DIMS,
                                   preferred_element_type=F32)
            pre[views[0], into] = pre[views[0], into] + rows

    first_sums = sums[0][0]
    steps = (ring.first, ring.second, ring.third, spread_line, spread_one, spread_two, spread_pair, embed_grad)
    done = CHUNKS + SPREAD_LAGS[3]

    def start_sums():
        row_sums()
        first_sums.begin()

    def turn_two():
        for v in PAIR:
            turn(normed.at[0], wide, 0, v)
        norm_copy(0).start()

    moves = ((0, pair_rows), (2, pair_sums.over_plane), (4, keep_means), (done, start_sums), (done + 1, first_sums.over_plane),
             (done + 2, first_sums.over_line), (done + 3, first_sums.over_pair))

    @loop(CHUNKS + SPREAD_LAGS[-1])
    def _(t):
        pl.when(t < CHUNKS)(lambda: correlate(t))
        for when, move in moves:
            pl.when(t == when)(move)
        for step, lag in zip(steps, SPREAD_LAGS):
            pl.when((t >= lag) & (t < lag + CHUNKS))(lambda step=step, lag=lag: step(t - lag))
        pl.when(t == SPREAD_LAGS[-1] + LINE)(turn_two)

    loss_sums.begin()

    def finish_grad(layer, j):
        cols = chunk_cols(j)
        per = CHUNKS // 2
        total, sel = (embed_total, cols) if layer == 0 else (totals[layer].at[lax.div(j, per)], chunk_cols(lax.rem(j, per)))
        for v in PAIR:
            mean0 = total[v:v + 1, sel] * count
            mean1 = total[2 + v:3 + v, sel] * count
            scale = scales[layer, v:v + 1, cols]

            @loop(view_rows // block_rows)
            def _(r):
                rows = pl.ds(pl.multiple_of(v * view_rows + r * block_rows, block_rows), block_rows)
                xhat = normed[(layer + 1) % 2, rows, cols].astype(F32)
                grad[rows, cols] = (scale * (pre[rows, cols] - (mean0 + xhat * mean1))).astype(BF16)

    def weight_grad(layer, j):
        q = (layer + 1) * CHUNKS + j
        source, first = (turned, 0) if layer == 2 else (wide, LINE * layer)

        @loop(2)
        def _(p):
            span = pl.ds(2 * p, 2)
            feed = jnp.concatenate([source[first + k, span].reshape(2 * quarter, -1) for k in range(LINE)], axis=1)
            out = jnp.dot(feed, grad[:, chunk_cols(j)], preferred_element_type=F32)
            ring.part[lax.rem(q, 2), span] = out.reshape(2, *ring.part.shape[2:])

        ring.pair(q)

    def input_grad(layer, n):
        cols = chunk_cols(n)
        weight_copy(layer, n).wait()
        half = local.at[layer, lax.div(n, CHUNKS // 2)]
        sel = chunk_cols(lax.rem(n, CHUNKS // 2))

        @loop(2)
        def _(v):
            rows = pl.ds(pl.multiple_of(v * view_rows, view_rows), view_rows)
            out = lax.dot_general(grad[rows, :], weight[lax.rem(n, slots)].reshape(width, dim), LANE_DIMS,
                                  preferred_element_type=F32)
            out = jnp.where(act[rows, cols] > 0, out, 0.0)
            pre[rows, cols] = out
            half[pl.ds(v, 1), sel] = col_sum(out)
            half[pl.ds(2 + v, 1), sel] = col_sum(out * normed[layer % 2, rows, cols].astype(F32))

        pl.when(n + slots < CHUNKS)(lambda: weight_copy(layer, n + slots).start())

    def serve(layer, j):
        t = layer * CHUNKS + j
        for step, lag in zip((ring.first, ring.second, ring.third), RING_LAGS):
            pl.when((t >= lag) & (t < lag + 3 * CHUNKS))(lambda step=step, lag=lag: step(CHUNKS + t - lag))
        if layer:
            for half, block in enumerate(ring.last(t)):
                outs[layer - 1][:, pl.ds(pl.multiple_of(j * width + half * ring.half, ring.half), ring.half)] = block

    for layer in OTHERS:
        old, new = sums[layer], sums[layer + 1] if layer < 2 else None
        old[0].arrive()

        def settle():
            if layer:
                old[1].arrive()

            @pl.loop(3, CHUNKS)
            def _(k):
                finish_grad(layer, k)

            if layer == 0:
                norm_copy(1).start()

        def late_loads():
            new[1].begin()
            if layer == 0:
                act_copy(1).start()
                for n in range(slots):
                    weight_copy(1, n).start()

        def relay_pair():
            new[0].over_pair()
            new[1].over_plane()

        before, middle, after = [], [(2, settle)], []
        if layer:
            middle.append((0, old[1].over_pair))
        if layer == 0:
            before.append((3, lambda: act_copy(0).wait()))
        if new:
            before += [(2, lambda: norm_copy(layer).wait()), (5, new[0].over_plane), (6, new[0].over_line), (7, relay_pair)]
            after += [(4, new[0].begin), (6, late_loads), (7, new[1].over_line)]

        @loop(CHUNKS)
        def _(j):
            for when, move in before:
                pl.when(j == when)(move)
            pl.when(j < 3)(lambda: finish_grad(layer, j))
            weight_grad(layer, j)
            for when, move in middle:
                pl.when(j == when)(move)
            if new:
                @pl.when((j > 2) & (j < 7))
                def _():
                    @loop(2)
                    def _(k):
                        input_grad(layer, 2 * (j - 3) + k)
            for when, move in after:
                pl.when(j == when)(move)
            serve(layer, j)

        if layer == 0:
            act_copy(1).wait()
            for v in PAIR:
                turn(act, wide, LINE, v)
            loss_sums.over_plane()

    @loop(CHUNKS)
    def _(j):
        serve(len(OTHERS), j)

    loss_sums.arrive()


def step(total_rows, vmem, lam, feat_a, feat_b, weights, vectors):
    view_rows, dim = feat_a.shape
    rows, width, blocks = 2 * view_rows, dim // CHUNKS, dim // 32
    hbm = pl.BlockSpec(memory_space=pl.ANY)
    vm = pl.BlockSpec(memory_space=pltpu.VMEM)
    cube = (LINE, 2, 2, 2, blocks)
    scratch = [
        pltpu.VMEM((rows, dim), BF16),
        pltpu.VMEM((rows, dim), F32),
        pltpu.VMEM((CHUNKS, *cube, width), BF16),
        pltpu.VMEM((LINE, *cube, view_rows // 2), BF16),
        pltpu.VMEM((3, 2, 2, blocks, dim), BF16),
        pltpu.VMEM((2, rows, dim), BF16),
        pltpu.VMEM((rows, dim), BF16),
        pltpu.VMEM((3, 2, 4, dim), F32),
        pltpu.VMEM((3, 2, 4, dim), F32),
        pltpu.VMEM((2, 2, 4, dim // 2), F32),
        pltpu.VMEM((4, dim), F32),
        pltpu.VMEM((4, dim), F32),
        pltpu.VMEM((1, dim), F32),
        pltpu.VMEM((blocks, 128), F32),
        pltpu.VMEM((128, 128), F32),
        pltpu.VMEM((2, blocks, width // 2), F32),
        pltpu.VMEM((3, 2, dim), F32),
        DMA_SEM((CHUNKS,)),
        DMA_SEM((3,)),
        DMA_SEM((3,)),
        DMA_SEM((3, 2)),
    ] + ring_scratch(CHUNKS, blocks, width)
    for _ in range(6):
        scratch += quick_scratch(2, dim)
    scratch += quick_scratch(4, dim) + quick_scratch(1, dim) + sums_scratch(4, dim)
    for _ in range(4):
        scratch += sums_scratch(4, dim // 2)
    halves = jax.ShapeDtypeStruct((2, 4, dim // 2), F32)
    saved = jax.ShapeDtypeStruct((2, rows, dim), BF16)
    return pl.pallas_call(
        functools.partial(step_kernel, total_rows),
        out_shape=[jax.ShapeDtypeStruct((blocks, dim), F32)] * 3 + [
            jax.ShapeDtypeStruct((1, dim), F32), halves, halves, saved, saved],
        in_specs=[pl.BlockSpec(memory_space=pltpu.SMEM)] + [hbm] * 5 + [vm] * 4,
        out_specs=[vm] * 6 + [hbm] * 2,
        scratch_shapes=scratch,
        compiler_params=pltpu.CompilerParams(collective_id=0, has_side_effects=True, vmem_limit_bytes=vmem),
    )(lam.reshape(1), feat_a, feat_b, *[weight.reshape(*cube, dim) for weight in weights],
      *[value.reshape(1, dim) for value in vectors])


def finish_kernel(total_two, total_one, loss_cols, *refs):
    gain_one, shift_one, gain_two, shift_two, loss = refs[6:]
    for grad, out in zip(refs[:3], refs[3:6]):
        out[...] = grad[...]
    half = total_two.shape[-1]
    for total, gain, shift in ((total_two, gain_two, shift_two), (total_one, gain_one, shift_one)):
        for h in PAIR:
            cols = pl.ds(h * half, half)
            shift[:, cols] = total[h, FIRST] + total[h, SECOND]
            gain[:, cols] = total[h, THIRD] + total[h, FOURTH]
    loss[...] = jnp.sum(loss_cols[...], axis=1, keepdims=True)


def finish(total_two, total_one, loss_cols, grads):
    vm = pl.BlockSpec(memory_space=pltpu.VMEM)
    row = jax.ShapeDtypeStruct((1, loss_cols.shape[1]), F32)
    outs = pl.pallas_call(
        finish_kernel,
        out_shape=[jax.ShapeDtypeStruct(grad.shape, F32) for grad in grads] + [row] * 4 + [jax.ShapeDtypeStruct((1, 1), F32)],
        in_specs=[vm] * 6,
        out_specs=[vm] * 8,
    )(total_two, total_one, loss_cols, *grads)
    return outs[:3], [row.reshape(-1) for row in outs[3:7]], outs[7].reshape(())


def solution(mesh):
    shards = mesh.shape["data"]

    def local_step(h_a, h_b, w_one, w_two, w_three, gain_one, shift_one, gain_two, shift_two, lam_off):
        rows_dev = h_a.shape[0]
        total_rows = rows_dev * shards
        grad_w_three, grad_w_two, grad_w_one, loss_cols, total_two, total_one = step(
            total_rows, 67000000, lam_off, h_a, h_b, (w_one, w_two, w_three),
            (gain_one, shift_one, gain_two, shift_two))[:6]
        grads, vectors, loss_total = finish(total_two, total_one, loss_cols, [grad_w_one, grad_w_two, grad_w_three])
        return (loss_total, *grads, *vectors)

    row_spec = P("data", None)
    whole_mat = P(None, None)
    whole_vec = P(None)
    return jax.shard_map(
        local_step, mesh=mesh,
        in_specs=(row_spec, row_spec, whole_mat, whole_mat, whole_mat,
                  whole_vec, whole_vec, whole_vec, whole_vec, P()),
        out_specs=(P(), row_spec, row_spec, row_spec, whole_vec, whole_vec, whole_vec, whole_vec),
        check_vma=False)
```

```python
import functools

import jax
import jax.numpy as jnp
from jax import lax
from jax.experimental import pallas as pl
from jax.experimental.pallas import tpu as pltpu
from jax.sharding import PartitionSpec as P

NORM_EPS = 1e-5
MESH = pl.DeviceIdType.MESH
F32 = jnp.float32
BF16 = jnp.bfloat16


ALL = slice(None)
FIRST, SECOND, THIRD, FOURTH = [slice(k, k + 1) for k in range(4)]
PAIR = range(2)
OTHERS = range(3)
LINE = 4
CUBE = 8
DEPTH_DIMS = (((0,), (0,)), ((), ()))
LANE_DIMS = (((1,), (1,)), ((), ()))
DMA_SEM = pltpu.SemaphoreType.DMA


def loop(count):
    return pl.loop(0, count)


def col_sum(values):
    return jnp.sum(values, axis=0, keepdims=True)


class Place:
    def __init__(self):
        me = lax.axis_index("data")
        self.core = lax.rem(me, 2)
        self.x = lax.rem(lax.div(me, 2), 2)
        self.y = lax.rem(lax.div(me, 4), 2)
        self.z = lax.div(me, 8)
        self.plane = lax.rem(lax.div(me, 2), 4)
        self.partner = me + 1 - 2 * self.core
        self.x_peer = me + 2 - 4 * self.x
        self.y_peer = me + 4 - 8 * self.y
        self.low = lax.rem(me, CUBE)
        self.others = [lax.rem(self.z + d + 1, LINE) for d in OTHERS]
        self.z_peers = [z * CUBE + self.low for z in self.others]
        self.plane_peers = [self.z * CUBE + lax.rem(self.plane + d + 1, LINE) * 2 + self.core for d in OTHERS]
        self.cube_peers = [self.z * CUBE + lax.rem(self.low + d + 1, CUBE) for d in range(CUBE - 1)]
        self.near = [self.partner] + self.plane_peers + self.z_peers


def enter(peers):
    barrier = pltpu.get_barrier_semaphore()
    for peer in peers:
        pl.semaphore_signal(barrier, inc=1, device_id=(peer,), device_id_type=MESH)
    pl.semaphore_wait(barrier, len(peers))


def remote(src, dst, send_sem, recv_sem, peer):
    return pltpu.make_async_remote_copy(
        src_ref=src, dst_ref=dst, send_sem=send_sem, recv_sem=recv_sem,
        device_id=(peer,), device_id_type=MESH)


class Sums:
    def __init__(self, at, local, total, recv0, slots1, slots2, send_sem, recv_sem):
        self.at, self.refs = at, (local, total)
        self.recv0, self.slots1, self.slots2 = recv0, slots1, slots2
        self.send_sem, self.recv_sem = send_sem, recv_sem
        self.half = recv0.shape[-1]
        self.mine = pl.multiple_of(at.core * self.half, 128)
        self.theirs = pl.multiple_of((1 - at.core) * self.half, 128)

    def pick(self, k, first):
        ref, index = self.refs[k]
        return ref.at[(*index, ALL, pl.ds(first, self.half))]

    def copies(self, stage):
        at = self.at
        if stage == 0:
            pairs = [(0, self.pick(0, self.theirs), self.recv0, at.partner)]
        elif stage == 1:
            here = self.slots1.at[at.plane]
            pairs = [(1 + d, here, here, at.plane_peers[d]) for d in OTHERS]
        elif stage == 2:
            here = self.slots2.at[at.z]
            pairs = [(4 + d, here, here, at.z_peers[d]) for d in OTHERS]
        else:
            here = self.pick(1, self.mine)
            pairs = [(7, here, here, at.partner)]
        return [remote(src, dst, self.send_sem.at[k], self.recv_sem.at[k], peer) for k, src, dst, peer in pairs]

    def send(self, stage):
        for copy in self.copies(stage):
            copy.start()

    def arrive(self, stage=3):
        for copy in self.copies(stage):
            copy.wait()

    def begin(self):
        self.send(0)

    def over_plane(self):
        self.arrive(0)
        self.slots1[self.at.plane] = self.pick(0, self.mine)[...] + self.recv0[...]
        self.send(1)

    def over_line(self):
        self.arrive(1)
        self.slots2[self.at.z] = jnp.sum(self.slots1[...], axis=0)
        self.send(2)

    def over_pair(self):
        self.arrive(2)
        self.pick(1, self.mine)[...] = jnp.sum(self.slots2[...], axis=0)
        self.send(3)


class QuickSums:
    def __init__(self, at, local, total, slots1, slots2, send_sem, recv_sem):
        self.at, self.local, self.total = at, local, total
        self.slots1, self.slots2 = slots1, slots2
        self.send_sem, self.recv_sem = send_sem, recv_sem

    def copies(self, across):
        at = self.at
        if across:
            here, peers, first = self.slots2.at[at.low], at.cube_peers, len(at.z_peers)
        else:
            here, peers, first = self.slots1.at[at.z], at.z_peers, 0
        return [remote(here, here, self.send_sem.at[first + d], self.recv_sem.at[first + d], peer)
                for d, peer in enumerate(peers)]

    def begin(self):
        ref, index = self.local
        self.slots1[self.at.z] = ref[index]
        for copy in self.copies(False):
            copy.start()

    def over_plane(self):
        for copy in self.copies(False):
            copy.wait()
        self.slots2[self.at.low] = jnp.sum(self.slots1[...], axis=0)
        for copy in self.copies(True):
            copy.start()

    def arrive(self):
        for copy in self.copies(True):
            copy.wait()
        ref, index = self.total
        ref[index] = jnp.sum(self.slots2[...], axis=0)


def quick_scratch(rows, cols):
    return [
        pltpu.VMEM((LINE, rows, cols), F32),
        pltpu.VMEM((CUBE, rows, cols), F32),
        DMA_SEM((LINE + CUBE,)),
        DMA_SEM((LINE + CUBE,)),
    ]


def sums_scratch(rows, cols):
    return [
        pltpu.VMEM((rows, cols // 2), F32),
        pltpu.VMEM((4, rows, cols // 2), F32),
        pltpu.VMEM((4, rows, cols // 2), F32),
    ] + [DMA_SEM((CUBE,))] * 2


class Ring:
    def __init__(self, at, total, spread, part, recv0, kept, snd1, recv1, snd2, recv2, snd3, recv3, send_sem, recv_sem, credit):
        self.at, self.total, self.slots, self.spread = at, total, kept.shape[0], spread
        self.part, self.recv0, self.kept = part, recv0, kept
        self.snd1, self.recv1, self.snd2, self.recv2, self.snd3, self.recv3 = snd1, recv1, snd2, recv2, snd3, recv3
        self.send_sem, self.recv_sem, self.credit = send_sem, recv_sem, credit
        self.half = snd1.shape[-1]
        self.peers = [at.partner, at.x_peer, at.y_peer, at.y_peer, at.x_peer] + at.z_peers
        self.givers = self.peers[:5] + at.z_peers[::-1]
        self.own = [at.y, at.x]

    def cols(self, half):
        return pl.ds(half * self.half, self.half)

    def copy(self, q, stage):
        j, s = lax.rem(q, self.slots), lax.rem(q, 2)
        if stage > 7:
            src, dst, peer = self.spread(q, stage)
        else:
            peer = self.peers[stage]
            if stage > 4:
                src, dst = self.snd3.at[j, stage - 5], self.recv3.at[j, stage - 5]
            elif stage > 2:
                src, dst = self.snd2.at[j, stage - 3], self.recv2.at[j, stage - 3]
            elif stage:
                src, dst = self.snd1.at[j, stage - 1], self.recv1.at[j, stage - 1]
            else:
                src, dst = self.part.at[s, :, :, :, 1 - self.at.core], self.recv0.at[s]
        return remote(src, dst, self.send_sem.at[j, stage], self.recv_sem.at[j, stage], peer)

    def start(self, q, *stages):
        for stage in stages:
            self.copy(q, stage).start()

    def wait(self, q, *stages):
        for stage in stages:
            self.copy(q, stage).wait()

    def depth(self, stage):
        return self.slots if stage else self.part.shape[0]

    def send(self, q, *stages):
        for stage in stages:
            depth = self.depth(stage)
            pl.when(q >= depth)(lambda: pl.semaphore_wait(self.credit.at[lax.rem(q, depth), stage], 1))
            self.start(q, stage)

    def give(self, q, *stages):
        for stage in stages:
            depth = self.depth(stage)
            pl.when(q + depth < self.total)(lambda: pl.semaphore_signal(
                self.credit.at[lax.rem(q, depth), stage], inc=1, device_id=(self.givers[stage],), device_id_type=MESH))

    def pair(self, q):
        self.send(q, 0)

    def first(self, q):
        at, s, j = self.at, lax.rem(q, 2), lax.rem(q, self.slots)
        self.wait(q, 0)

        @loop(LINE)
        def _(z):
            for half in PAIR:
                cols = self.cols(half)
                for k in PAIR:
                    (y, x), (oy, ox) = ((at.y, k), (1 - at.y, k)) if half else ((k, at.x), (k, 1 - at.x))
                    self.snd1[j, half, z, k] = (
                        self.part[s, z, oy, ox, at.core, :, cols] + self.recv0[s, z, oy, ox, :, cols]).astype(BF16)
                    self.kept[j, half, z, k] = self.part[s, z, y, x, at.core, :, cols] + self.recv0[s, z, y, x, :, cols]

        self.give(q, 0)
        self.send(q, 1, 2)

    def second(self, q):
        j = lax.rem(q, self.slots)
        for half in PAIR:
            own = self.own[half]
            self.wait(q, 1 + half)

            @loop(LINE)
            def _(z):
                self.snd2[j, half, z] = (
                    self.kept[j, half, z, 1 - own] + self.recv1[j, half, z, 1 - own].astype(F32)).astype(BF16)
                self.kept[j, half, z, own] = self.kept[j, half, z, own] + self.recv1[j, half, z, own].astype(F32)

            self.give(q, 1 + half)
            self.send(q, 3 + half)

    def summed(self, j, half, z):
        return self.kept[j, half, z, self.own[half]] + self.recv2[j, half, z].astype(F32)

    def third(self, q):
        j = lax.rem(q, self.slots)
        self.wait(q, 3, 4)

        @loop(len(OTHERS))
        def _(d):
            z = lax.rem(self.at.z + d + 1, LINE)
            for half in PAIR:
                self.snd3[j, d, :, self.cols(half)] = self.summed(j, half, z).astype(BF16)

        self.send(q, 5, 6, 7)

    def last(self, q):
        j = lax.rem(q, self.slots)
        totals = [self.summed(j, half, self.at.z) for half in PAIR]
        self.wait(q, 5, 6, 7)
        for d in OTHERS:
            totals = [total + self.recv3[j, d, :, self.cols(half)].astype(F32) for half, total in enumerate(totals)]
        self.give(q, 3, 4, 5, 6, 7)
        return totals


def ring_scratch(slots, rows, width):
    half = width // 2
    return [
        pltpu.VMEM((2, 4, 2, 2, 2, rows, width), F32),
        pltpu.VMEM((2, 4, 2, 2, rows, width), F32),
        pltpu.VMEM((slots, 2, 4, 2, rows, half), F32),
    ] + [pltpu.VMEM((slots, 2, 4, 2, rows, half), BF16)] * 2 + [pltpu.VMEM((slots, 2, 4, rows, half), BF16)] * 2 + [
        pltpu.VMEM((slots, 3, rows, width), BF16)] * 2 + [DMA_SEM((slots, 16))] * 2 + [
        pltpu.SemaphoreType.REGULAR((slots, 8))]


CHUNKS = 8
RING = 12
SUMS = 5
QUICK = 4
SPREAD_LAGS = (1, 2, 3, 4, 6, 7, 9, 10)
RING_LAGS = (1, 3, 5, 8)


def step_kernel(
        total_rows, lam_ref, feat_a, feat_b, w_one, w_two, w_three, gain_one, shift_one, gain_two, shift_two,
        grad_w_three, grad_w_two, grad_w_one, loss_total, total_two, total_one, saved_act, saved_norm,
        grad, pre, wide, turned, weight, normed, act, sides, side_sums, local, embed_local, embed_total, loss_local, mean_col, turned_sums, by_row, scales,
        wide_sem, w_sem, load_sem, out_sem, *scratch):
    at = Place()
    place = (at.z, at.y, at.x, at.core)

    def spread(q, stage):
        cols = ring.cols((stage - 1) % 2)
        if stage < 11:
            here, peer = wide.at[(q, *place)], at.z_peers[stage - 8]
        elif stage == 11:
            here, peer = wide.at[q, :, at.y, at.x, at.core, :, cols], at.y_peer
        elif stage == 12:
            here, peer = wide.at[q, :, at.y, at.x, at.core, :, cols], at.x_peer
        elif stage == 13:
            here, peer = wide.at[q, :, :, at.x, at.core, :, cols], at.x_peer
        elif stage == 14:
            here, peer = wide.at[q, :, at.y, :, at.core, :, cols], at.y_peer
        else:
            here, peer = wide.at[q, :, :, :, at.core], at.partner
        return here, here, peer

    ring = Ring(at, 4 * CHUNKS, spread, *scratch[:RING])
    rows_dev, dim = grad.shape
    width = dim // CHUNKS
    view_rows = rows_dev // 2
    block_rows = min(128, view_rows)
    quarter = dim // 4
    count = 1.0 / total_rows
    weights = [w_one, w_two, w_three]
    gains, shifts = [gain_one, gain_two], [shift_one, shift_two]
    outs = [grad_w_three, grad_w_two, grad_w_one]
    totals = [embed_total, total_two, total_one]
    views = [pl.ds(v * view_rows, view_rows) for v in PAIR]
    rest = list(scratch[RING:])

    def take(number):
        taken, rest[:] = rest[:number], rest[number:]
        return taken

    top = pl.ds(0, 2)
    side = [[QuickSums(at, (sides, (layer, v, top)), (side_sums, (layer, v, top)), *take(QUICK)) for v in PAIR] for layer in OTHERS]
    pair_sums = QuickSums(at, (sides, (0, 0)), (side_sums, (0, 0)), *take(QUICK))
    loss_sums = QuickSums(at, (loss_local, ...), (loss_total, ...), *take(QUICK))
    sums = [[Sums(at, (embed_local, ()), (embed_total, ()), *take(SUMS))]]
    for layer in PAIR:
        sums.append([Sums(at, (local, (layer, h)), (totals[layer + 1], (h,)), *take(SUMS)) for h in PAIR])

    def act_copy(layer):
        return pltpu.make_async_copy(saved_act.at[1 - layer], act, load_sem.at[0])

    def norm_copy(layer):
        return pltpu.make_async_copy(saved_norm.at[1 - layer], normed.at[layer], load_sem.at[1])

    def feat_copy(v):
        return pltpu.make_async_copy((feat_a, feat_b)[v], normed.at[0, views[v]], load_sem.at[v])

    def wide_copy(layer, n):
        cols = pl.ds(pl.multiple_of(n * width, width), width)
        return pltpu.make_async_copy(weights[layer].at[:, :, :, :, :, cols], wide.at[n], wide_sem.at[n])

    feat_copy(0).start()
    lead = 4
    for n in range(lead):
        wide_copy(0, n).start()
    feat_copy(1).start()
    puts = {}

    def put(name, v, src, dst, k):
        copy = pltpu.make_async_copy(src, dst, out_sem.at[k, v])
        copy.start()
        puts[name, v] = copy

    def drain(*names):
        for name in names:
            for v in PAIR:
                puts.pop((name, v)).wait()

    def matmul(layer, v, hook, step):
        @loop(CHUNKS // LINE)
        def _(m):
            if step:
                pl.when(m == hook)(step)
            chunks = [LINE * m + k for k in range(LINE)]
            if v == 0:
                if layer == 0:
                    for n in chunks:
                        pl.when(n + lead < CHUNKS)(lambda n=n: wide_copy(0, n + lead).start())
                for n in chunks:
                    wide_copy(layer, n).wait()
            elif layer < 2:
                for n in chunks:
                    pl.when(m > 0)(lambda n=n: wide_copy(layer + 1, n - LINE).start())
            for n in chunks:
                cols = pl.ds(pl.multiple_of(n * width, width), width)
                out = jnp.dot(normed[layer % 2, views[v]], wide[n].reshape(dim, width), preferred_element_type=F32)
                pre[views[v], cols] = out
                sides[layer, v, FIRST, cols] = col_sum(out)
                sides[layer, v, SECOND, cols] = col_sum(out * out)

        if v and layer < 2:
            for n in range(LINE):
                wide_copy(layer + 1, LINE + n).start()
        side[layer][v].begin()

    def normalise(layer, v):
        side[layer][v].arrive()
        mean = side_sums[layer, v, FIRST, :] / total_rows
        inv = lax.rsqrt(side_sums[layer, v, SECOND, :] / total_rows - mean * mean + NORM_EPS)
        scales[2 - layer, v:v + 1, :] = gains[layer][...] * inv if layer < 2 else inv
        sides[layer, v, FIRST, :] = mean
        sides[layer, v, SECOND, :] = inv

        @loop(CHUNKS)
        def _(n):
            cols = pl.ds(pl.multiple_of(n * width, width), width)
            mean, inv = sides[layer, v, FIRST, cols], sides[layer, v, SECOND, cols]
            if layer < 2:
                gain, shift = gains[layer][:, cols], shifts[layer][:, cols]

            @loop(view_rows // block_rows)
            def _(r):
                rows = pl.ds(pl.multiple_of(v * view_rows + r * block_rows, block_rows), block_rows)
                value = (pre[rows, cols] - mean) * inv
                if layer < 2:
                    grad[rows, cols] = value.astype(BF16)
                    value = jnp.maximum(gain * value + shift, 0.0)
                normed[(layer + 1) % 2, rows, cols] = value.astype(BF16)

        if layer < 2:
            put(("act", layer), v, normed.at[(layer + 1) % 2, views[v]], saved_act.at[layer, views[v]], layer)
            put(("norm", layer), v, grad.at[views[v]], saved_norm.at[layer, views[v]], 2)

    def turn(src, dst, first, v):
        part = view_rows // 2

        @loop(CHUNKS)
        def _(n):
            cols = pl.ds(pl.multiple_of(n * width, width), width)
            for k in PAIR:
                block = src[pl.ds(v * view_rows + k * part, part), cols].T
                dst[first + 2 * v + k, lax.div(n, 2), lax.rem(n, 2)] = block.reshape(dst.shape[3:])

    enter(at.z_peers + at.cube_peers)
    feat_copy(0).wait()
    matmul(0, 0, 0, None)
    feat_copy(1).wait()
    matmul(0, 1, 1, side[0][0].over_plane)
    for v in PAIR:
        turn(normed.at[0], turned, 0, v)
    normalise(0, 0)
    for layer in PAIR:
        matmul(layer + 1, 0, 1, side[layer][1].over_plane)
        normalise(layer, 1)
        matmul(layer + 1, 1, 1, side[layer + 1][0].over_plane)
        if layer == 0:
            drain(("norm", 0))
        else:
            drain(("act", 0))
        normalise(layer + 1, 0)
    by_row[...] = jnp.zeros_like(by_row)
    sides[0, 0, FOURTH, :] = jnp.zeros((1, dim), F32)

    @loop(CHUNKS)
    def _(n):
        cols = pl.ds(pl.multiple_of(n * width, width), width)
        sides[0, 0, FIRST, cols] = col_sum(normed[1, views[0], cols].astype(F32))
        pre[views[0], cols] = jnp.zeros((view_rows, width), F32)

    side[2][1].over_plane()
    normalise(2, 1)

    drain(("act", 1), ("norm", 1))
    act_copy(0).start()
    slots = weight.shape[0]

    def weight_copy(layer, n):
        slot = lax.rem(n, slots)
        return pltpu.make_async_copy(weights[2 - layer].at[lax.div(n, 2), lax.rem(n, 2)], weight.at[slot], w_sem.at[slot])

    for n in range(slots):
        weight_copy(0, n).start()

    lam = lam_ref[0]
    lane = 128
    block_rows_dev = ring.snd1.shape[-2]
    first_row = (((at.z * 2 + at.y) * 2 + at.x) * 2 + at.core) * block_rows_dev

    def pair_rows():
        @loop(CHUNKS)
        def _(n):
            cols = pl.ds(pl.multiple_of(n * width, width), width)
            one, two = [normed[1, views[v], cols].astype(F32) for v in PAIR]
            sides[0, 0, SECOND, cols] = col_sum(two)
            sides[0, 0, THIRD, cols] = col_sum(one * two)

        pair_sums.begin()

    block = pl.ds(pl.multiple_of(lax.div(first_row, lane) * lane, lane), lane)
    part = lax.rem(first_row, lane)

    def keep_means():
        pair_sums.arrive()
        turned_sums[...] = jnp.broadcast_to(side_sums[0, 0, FIRST, block], (lane, lane)).T
        mean_col[...] = turned_sums[pl.ds(pl.multiple_of(part, 8), block_rows_dev), :]

    def row_sums():
        for k, row in enumerate((FIRST, THIRD)):
            sums_here = col_sum(by_row[k].T)
            spread = jnp.concatenate([sums_here] * (lane // block_rows_dev), axis=1)
            position = lax.broadcasted_iota(jnp.int32, spread.shape, 1)
            mine = (position >= part) & (position < part + block_rows_dev)
            embed_local[row, :] = jnp.zeros((1, dim), F32)
            embed_local[row, block] = jnp.where(mine, spread, 0.0)


    def chunk_cols(q):
        return pl.ds(pl.multiple_of(q * width, width), width)

    def correlate(q):
        @loop(LINE)
        def _(z):
            rows = pl.ds(pl.multiple_of(z * quarter, quarter), quarter)
            out = lax.dot_general(normed[1, views[0], rows], normed[1, views[1], chunk_cols(q)], DEPTH_DIMS,
                                  preferred_element_type=F32)
            ring.part[lax.rem(q, 2), z] = out.reshape(ring.part.shape[2:])

        ring.pair(q)

    def spread_line(q):
        for half, total in enumerate(ring.last(q)):
            start = q * width + half * ring.half
            row = first_row + lax.broadcasted_iota(jnp.int32, total.shape, 0)
            col = start + lax.broadcasted_iota(jnp.int32, total.shape, 1)
            diag = row == col
            cols = pl.ds(pl.multiple_of(start, ring.half), ring.half)
            total = jnp.where(diag, side_sums[0, 0, THIRD, cols], total)
            corr = total * count
            gap = 1.0 - corr
            loss_local[:, cols] = col_sum(jnp.where(diag, gap * gap, lam * corr * corr))
            slope = (jnp.where(diag, -2.0 * gap, 2.0 * lam * corr) * count).astype(BF16)
            wide[(q, *place, ALL, ring.cols(half))] = slope
            slope = slope.astype(F32)
            embed_local[SECOND, cols] = col_sum(slope * mean_col[:, :ring.half])
            embed_local[FOURTH, cols] = col_sum(slope * total)
            terms = [slope * side_sums[0, 0, SECOND, cols], slope * total]
            for k, term in enumerate(terms):
                by_row[k] = by_row[k] + term
        ring.start(q, 8, 9, 10)

    def spread_one(q):
        ring.wait(q, 8, 9, 10)
        ring.start(q, 11, 12)

    def spread_two(q):
        ring.wait(q, 11, 12)
        ring.start(q, 13, 14)

    def spread_pair(q):
        ring.wait(q, 13, 14)
        ring.start(q, 15)

    def embed_grad(q):
        ring.wait(q, 15)
        cols = chunk_cols(q)
        pre[views[1], cols] = jnp.dot(normed[1, views[0]], wide[q].reshape(dim, width), preferred_element_type=F32)

        @loop(len(PAIR))
        def _(p):
            into = pl.ds(pl.multiple_of(p * 2 * quarter, quarter), 2 * quarter)
            rows = lax.dot_general(normed[1, views[1], cols], wide[q, pl.ds(2 * p, 2)].reshape(2 * quarter, width), LANE_DIMS,
                                   preferred_element_type=F32)
            pre[views[0], into] = pre[views[0], into] + rows

    first_sums = sums[0][0]
    steps = (ring.first, ring.second, ring.third, spread_line, spread_one, spread_two, spread_pair, embed_grad)
    done = CHUNKS + SPREAD_LAGS[3]

    def start_sums():
        row_sums()
        first_sums.begin()

    def turn_two():
        for v in PAIR:
            turn(normed.at[0], wide, 0, v)
        norm_copy(0).start()

    moves = ((0, pair_rows), (2, pair_sums.over_plane), (4, keep_means), (done, start_sums), (done + 1, first_sums.over_plane),
             (done + 2, first_sums.over_line), (done + 3, first_sums.over_pair))

    @loop(CHUNKS + SPREAD_LAGS[-1])
    def _(t):
        pl.when(t < CHUNKS)(lambda: correlate(t))
        for when, move in moves:
            pl.when(t == when)(move)
        for step, lag in zip(steps, SPREAD_LAGS):
            pl.when((t >= lag) & (t < lag + CHUNKS))(lambda step=step, lag=lag: step(t - lag))
        pl.when(t == SPREAD_LAGS[-1] + LINE)(turn_two)

    loss_sums.begin()

    def finish_grad(layer, j):
        cols = chunk_cols(j)
        per = CHUNKS // 2
        total, sel = (embed_total, cols) if layer == 0 else (totals[layer].at[lax.div(j, per)], chunk_cols(lax.rem(j, per)))
        for v in PAIR:
            mean0 = total[v:v + 1, sel] * count
            mean1 = total[2 + v:3 + v, sel] * count
            scale = scales[layer, v:v + 1, cols]

            @loop(view_rows // block_rows)
            def _(r):
                rows = pl.ds(pl.multiple_of(v * view_rows + r * block_rows, block_rows), block_rows)
                xhat = normed[(layer + 1) % 2, rows, cols].astype(F32)
                grad[rows, cols] = (scale * (pre[rows, cols] - (mean0 + xhat * mean1))).astype(BF16)

    def weight_grad(layer, j):
        q = (layer + 1) * CHUNKS + j
        source, first = (turned, 0) if layer == 2 else (wide, LINE * layer)

        @loop(len(PAIR))
        def _(p):
            span = pl.ds(2 * p, 2)
            feed = jnp.concatenate([source[first + k, span].reshape(2 * quarter, -1) for k in range(LINE)], axis=1)
            out = jnp.dot(feed, grad[:, chunk_cols(j)], preferred_element_type=F32)
            ring.part[lax.rem(q, 2), span] = out.reshape(2, *ring.part.shape[2:])

        ring.pair(q)

    def input_grad(layer, p):
        two = 2 * width
        cols = pl.ds(pl.multiple_of(p * two, two), two)
        for n in PAIR:
            weight_copy(layer, 2 * p + n).wait()
        half = local.at[layer, lax.div(p, 2)]
        sel = pl.ds(pl.multiple_of(lax.rem(p, 2) * two, two), two)

        @loop(len(PAIR))
        def _(v):
            rows = pl.ds(pl.multiple_of(v * view_rows, view_rows), view_rows)
            block = weight[pl.ds(2 * lax.rem(p, 2), 2)].reshape(two, dim)
            out = lax.dot_general(grad[rows, :], block, LANE_DIMS, preferred_element_type=F32)
            out = jnp.where(act[rows, cols] > 0, out, 0.0)
            pre[rows, cols] = out
            half[pl.ds(v, 1), sel] = col_sum(out)
            half[pl.ds(2 + v, 1), sel] = col_sum(out * normed[layer % 2, rows, cols].astype(F32))

        @pl.when(p < 2)
        def _():
            for n in PAIR:
                weight_copy(layer, 2 * p + n + slots).start()

    def serve(layer, j):
        t = layer * CHUNKS + j
        for step, lag in zip((ring.first, ring.second, ring.third), RING_LAGS):
            pl.when((t >= lag) & (t < lag + 3 * CHUNKS))(lambda step=step, lag=lag: step(CHUNKS + t - lag))
        if layer:
            for half, block in enumerate(ring.last(t)):
                outs[layer - 1][:, pl.ds(pl.multiple_of(j * width + half * ring.half, ring.half), ring.half)] = block

    for layer in OTHERS:
        old, new = sums[layer], sums[layer + 1] if layer < 2 else None
        old[0].arrive()

        def settle():
            if layer:
                old[1].arrive()

            @pl.loop(3, CHUNKS)
            def _(k):
                finish_grad(layer, k)

            if layer == 0:
                norm_copy(1).start()

        def late_loads():
            new[1].begin()
            if layer == 0:
                act_copy(1).start()
                for n in range(slots):
                    weight_copy(1, n).start()

        def relay_pair():
            new[0].over_pair()
            new[1].over_plane()

        before, middle, after = [], [(2, settle)], []
        if layer:
            middle.append((0, old[1].over_pair))
        if layer == 0:
            before.append((3, lambda: act_copy(0).wait()))
        if new:
            before += [(2, lambda: norm_copy(layer).wait()), (5, new[0].over_plane), (6, new[0].over_line), (7, relay_pair)]
            after += [(4, new[0].begin), (6, late_loads), (7, new[1].over_line)]

        @loop(CHUNKS)
        def _(j):
            for when, move in before:
                pl.when(j == when)(move)
            pl.when(j < 3)(lambda: finish_grad(layer, j))
            weight_grad(layer, j)
            for when, move in middle:
                pl.when(j == when)(move)
            if new:
                pl.when((j > 2) & (j < 7))(lambda: input_grad(layer, j - 3))
            for when, move in after:
                pl.when(j == when)(move)
            serve(layer, j)

        if layer == 0:
            act_copy(1).wait()
            for v in PAIR:
                turn(act, wide, LINE, v)
            loss_sums.over_plane()

    @loop(CHUNKS)
    def _(j):
        serve(len(OTHERS), j)

    loss_sums.arrive()


def step(total_rows, vmem, lam, feat_a, feat_b, weights, vectors):
    view_rows, dim = feat_a.shape
    rows, width, blocks = 2 * view_rows, dim // CHUNKS, dim // 32
    hbm = pl.BlockSpec(memory_space=pl.ANY)
    vm = pl.BlockSpec(memory_space=pltpu.VMEM)
    cube = (LINE, 2, 2, 2, blocks)
    scratch = [
        pltpu.VMEM((rows, dim), BF16),
        pltpu.VMEM((rows, dim), F32),
        pltpu.VMEM((CHUNKS, *cube, width), BF16),
        pltpu.VMEM((LINE, *cube, view_rows // 2), BF16),
        pltpu.VMEM((LINE, 2, 2, blocks, dim), BF16),
        pltpu.VMEM((2, rows, dim), BF16),
        pltpu.VMEM((rows, dim), BF16),
        pltpu.VMEM((3, 2, 4, dim), F32),
        pltpu.VMEM((3, 2, 4, dim), F32),
        pltpu.VMEM((2, 2, 4, dim // 2), F32),
        pltpu.VMEM((4, dim), F32),
        pltpu.VMEM((4, dim), F32),
        pltpu.VMEM((1, dim), F32),
        pltpu.VMEM((blocks, 128), F32),
        pltpu.VMEM((128, 128), F32),
        pltpu.VMEM((2, blocks, width // 2), F32),
        pltpu.VMEM((3, 2, dim), F32),
        DMA_SEM((CHUNKS,)),
        DMA_SEM((LINE,)),
        DMA_SEM((3,)),
        DMA_SEM((3, 2)),
    ] + ring_scratch(CHUNKS, blocks, width)
    for _ in range(6):
        scratch += quick_scratch(2, dim)
    scratch += quick_scratch(4, dim) + quick_scratch(1, dim) + sums_scratch(4, dim)
    for _ in range(4):
        scratch += sums_scratch(4, dim // 2)
    halves = jax.ShapeDtypeStruct((2, 4, dim // 2), F32)
    saved = jax.ShapeDtypeStruct((2, rows, dim), BF16)
    return pl.pallas_call(
        functools.partial(step_kernel, total_rows),
        out_shape=[jax.ShapeDtypeStruct((blocks, dim), F32)] * 3 + [
            jax.ShapeDtypeStruct((1, dim), F32), halves, halves, saved, saved],
        in_specs=[pl.BlockSpec(memory_space=pltpu.SMEM)] + [hbm] * 5 + [vm] * 4,
        out_specs=[vm] * 6 + [hbm] * 2,
        scratch_shapes=scratch,
        compiler_params=pltpu.CompilerParams(collective_id=0, has_side_effects=True, vmem_limit_bytes=vmem),
    )(lam.reshape(1), feat_a, feat_b, *[weight.reshape(*cube, dim) for weight in weights],
      *[value.reshape(1, dim) for value in vectors])


def finish_kernel(total_two, total_one, loss_cols, *refs):
    gain_one, shift_one, gain_two, shift_two, loss = refs[6:]
    for grad, out in zip(refs[:3], refs[3:6]):
        out[...] = grad[...]
    half = total_two.shape[-1]
    for total, gain, shift in ((total_two, gain_two, shift_two), (total_one, gain_one, shift_one)):
        for h in PAIR:
            cols = pl.ds(h * half, half)
            shift[:, cols] = total[h, FIRST] + total[h, SECOND]
            gain[:, cols] = total[h, THIRD] + total[h, FOURTH]
    loss[...] = jnp.sum(loss_cols[...], axis=1, keepdims=True)


def finish(total_two, total_one, loss_cols, grads):
    vm = pl.BlockSpec(memory_space=pltpu.VMEM)
    row = jax.ShapeDtypeStruct((1, loss_cols.shape[1]), F32)
    outs = pl.pallas_call(
        finish_kernel,
        out_shape=[jax.ShapeDtypeStruct(grad.shape, F32) for grad in grads] + [row] * 4 + [jax.ShapeDtypeStruct((1, 1), F32)],
        in_specs=[vm] * 6,
        out_specs=[vm] * 8,
    )(total_two, total_one, loss_cols, *grads)
    return outs[:3], [row.reshape(-1) for row in outs[3:7]], outs[7].reshape(())


def solution(mesh):
    shards = mesh.shape["data"]

    def local_step(h_a, h_b, w_one, w_two, w_three, gain_one, shift_one, gain_two, shift_two, lam_off):
        rows_dev = h_a.shape[0]
        total_rows = rows_dev * shards
        grad_w_three, grad_w_two, grad_w_one, loss_cols, total_two, total_one = step(
            total_rows, 67000000, lam_off, h_a, h_b, (w_one, w_two, w_three),
            (gain_one, shift_one, gain_two, shift_two))[:6]
        grads, vectors, loss_total = finish(total_two, total_one, loss_cols, [grad_w_one, grad_w_two, grad_w_three])
        return (loss_total, *grads, *vectors)

    row_spec = P("data", None)
    whole_mat = P(None, None)
    whole_vec = P(None)
    return jax.shard_map(
        local_step, mesh=mesh,
        in_specs=(row_spec, row_spec, whole_mat, whole_mat, whole_mat,
                  whole_vec, whole_vec, whole_vec, whole_vec, P()),
        out_specs=(P(), row_spec, row_spec, row_spec, whole_vec, whole_vec, whole_vec, whole_vec),
        check_vma=False)
```

```python
import functools

import jax
import jax.numpy as jnp
from jax import lax
from jax.experimental import pallas as pl
from jax.experimental.pallas import tpu as pltpu
from jax.sharding import PartitionSpec as P

NORM_EPS = 1e-5
MESH = pl.DeviceIdType.MESH
F32 = jnp.float32
BF16 = jnp.bfloat16


ALL = slice(None)
FIRST, SECOND, THIRD, FOURTH = [slice(k, k + 1) for k in range(4)]
PAIR = range(2)
OTHERS = range(3)
LINE = 4
CUBE = 8
DEPTH_DIMS = (((0,), (0,)), ((), ()))
LANE_DIMS = (((1,), (1,)), ((), ()))
DMA_SEM = pltpu.SemaphoreType.DMA


def loop(count):
    return pl.loop(0, count)


def col_sum(values):
    return jnp.sum(values, axis=0, keepdims=True)


class Place:
    def __init__(self):
        me = lax.axis_index("data")
        self.core = lax.rem(me, 2)
        self.x = lax.rem(lax.div(me, 2), 2)
        self.y = lax.rem(lax.div(me, 4), 2)
        self.z = lax.div(me, 8)
        self.plane = lax.rem(lax.div(me, 2), 4)
        self.partner = me + 1 - 2 * self.core
        self.x_peer = me + 2 - 4 * self.x
        self.y_peer = me + 4 - 8 * self.y
        self.low = lax.rem(me, CUBE)
        self.others = [lax.rem(self.z + d + 1, LINE) for d in OTHERS]
        self.z_peers = [z * CUBE + self.low for z in self.others]
        self.plane_peers = [self.z * CUBE + lax.rem(self.plane + d + 1, LINE) * 2 + self.core for d in OTHERS]
        self.cube_peers = [self.z * CUBE + lax.rem(self.low + d + 1, CUBE) for d in range(CUBE - 1)]
        self.near = [self.partner] + self.plane_peers + self.z_peers


def enter(peers):
    barrier = pltpu.get_barrier_semaphore()
    for peer in peers:
        pl.semaphore_signal(barrier, inc=1, device_id=(peer,), device_id_type=MESH)
    pl.semaphore_wait(barrier, len(peers))


def remote(src, dst, send_sem, recv_sem, peer):
    return pltpu.make_async_remote_copy(
        src_ref=src, dst_ref=dst, send_sem=send_sem, recv_sem=recv_sem,
        device_id=(peer,), device_id_type=MESH)


class Sums:
    def __init__(self, at, local, total, recv0, slots1, slots2, send_sem, recv_sem):
        self.at, self.refs = at, (local, total)
        self.recv0, self.slots1, self.slots2 = recv0, slots1, slots2
        self.send_sem, self.recv_sem = send_sem, recv_sem
        self.half = recv0.shape[-1]
        self.mine = pl.multiple_of(at.core * self.half, 128)
        self.theirs = pl.multiple_of((1 - at.core) * self.half, 128)

    def pick(self, k, first):
        ref, index = self.refs[k]
        return ref.at[(*index, ALL, pl.ds(first, self.half))]

    def copies(self, stage):
        at = self.at
        if stage == 0:
            pairs = [(0, self.pick(0, self.theirs), self.recv0, at.partner)]
        elif stage == 1:
            here = self.slots1.at[at.plane]
            pairs = [(1 + d, here, here, at.plane_peers[d]) for d in OTHERS]
        elif stage == 2:
            here = self.slots2.at[at.z]
            pairs = [(4 + d, here, here, at.z_peers[d]) for d in OTHERS]
        else:
            here = self.pick(1, self.mine)
            pairs = [(7, here, here, at.partner)]
        return [remote(src, dst, self.send_sem.at[k], self.recv_sem.at[k], peer) for k, src, dst, peer in pairs]

    def send(self, stage):
        for copy in self.copies(stage):
            copy.start()

    def arrive(self, stage=3):
        for copy in self.copies(stage):
            copy.wait()

    def begin(self):
        self.send(0)

    def over_plane(self):
        self.arrive(0)
        self.slots1[self.at.plane] = self.pick(0, self.mine)[...] + self.recv0[...]
        self.send(1)

    def over_line(self):
        self.arrive(1)
        self.slots2[self.at.z] = jnp.sum(self.slots1[...], axis=0)
        self.send(2)

    def over_pair(self):
        self.arrive(2)
        self.pick(1, self.mine)[...] = jnp.sum(self.slots2[...], axis=0)
        self.send(3)


class QuickSums:
    def __init__(self, at, local, total, slots1, slots2, send_sem, recv_sem):
        self.at, self.local, self.total = at, local, total
        self.slots1, self.slots2 = slots1, slots2
        self.send_sem, self.recv_sem = send_sem, recv_sem

    def copies(self, across):
        at = self.at
        if across:
            here, peers, first = self.slots2.at[at.low], at.cube_peers, len(at.z_peers)
        else:
            here, peers, first = self.slots1.at[at.z], at.z_peers, 0
        return [remote(here, here, self.send_sem.at[first + d], self.recv_sem.at[first + d], peer)
                for d, peer in enumerate(peers)]

    def begin(self):
        ref, index = self.local
        self.slots1[self.at.z] = ref[index]
        for copy in self.copies(False):
            copy.start()

    def over_plane(self):
        for copy in self.copies(False):
            copy.wait()
        self.slots2[self.at.low] = jnp.sum(self.slots1[...], axis=0)
        for copy in self.copies(True):
            copy.start()

    def arrive(self):
        for copy in self.copies(True):
            copy.wait()
        ref, index = self.total
        ref[index] = jnp.sum(self.slots2[...], axis=0)


def quick_scratch(rows, cols):
    return [
        pltpu.VMEM((LINE, rows, cols), F32),
        pltpu.VMEM((CUBE, rows, cols), F32),
        DMA_SEM((LINE + CUBE,)),
        DMA_SEM((LINE + CUBE,)),
    ]


def sums_scratch(rows, cols):
    return [
        pltpu.VMEM((rows, cols // 2), F32),
        pltpu.VMEM((4, rows, cols // 2), F32),
        pltpu.VMEM((4, rows, cols // 2), F32),
    ] + [DMA_SEM((CUBE,))] * 2


class Ring:
    def __init__(self, at, total, spread, part, recv0, kept, snd1, recv1, snd2, recv2, snd3, recv3, send_sem, recv_sem, credit):
        self.at, self.total, self.slots, self.spread = at, total, kept.shape[0], spread
        self.part, self.recv0, self.kept = part, recv0, kept
        self.snd1, self.recv1, self.snd2, self.recv2, self.snd3, self.recv3 = snd1, recv1, snd2, recv2, snd3, recv3
        self.send_sem, self.recv_sem, self.credit = send_sem, recv_sem, credit
        self.half = snd1.shape[-1]
        self.peers = [at.partner, at.x_peer, at.y_peer, at.y_peer, at.x_peer] + at.z_peers
        self.givers = self.peers[:5] + at.z_peers[::-1]
        self.own = [at.y, at.x]

    def cols(self, half):
        return pl.ds(half * self.half, self.half)

    def copy(self, q, stage):
        j, s = lax.rem(q, self.slots), lax.rem(q, 2)
        if stage % REST == 0:
            z, peer = pl.ds(2 * (stage // REST), 2), self.at.partner
            src, dst = self.part.at[s, z, :, :, 1 - self.at.core], self.recv0.at[s, z]
        elif stage > 7:
            src, dst, peer = self.spread(q, stage)
        else:
            peer = self.peers[stage]
            if stage > 4:
                src, dst = self.snd3.at[j, stage - 5], self.recv3.at[j, stage - 5]
            elif stage > 2:
                src, dst = self.snd2.at[j, stage - 3], self.recv2.at[j, stage - 3]
            else:
                src, dst = self.snd1.at[j, stage - 1], self.recv1.at[j, stage - 1]
        return remote(src, dst, self.send_sem.at[j, stage], self.recv_sem.at[j, stage], peer)

    def start(self, q, *stages):
        for stage in stages:
            self.copy(q, stage).start()

    def wait(self, q, *stages):
        for stage in stages:
            self.copy(q, stage).wait()

    def depth(self, stage):
        return self.slots if stage else self.part.shape[0]

    def send(self, q, *stages):
        for stage in stages:
            depth = self.depth(stage)
            pl.when(q >= depth)(lambda: pl.semaphore_wait(self.credit.at[lax.rem(q, depth), stage], 1))
            self.start(q, stage)

    def give(self, q, *stages):
        for stage in stages:
            depth = self.depth(stage)
            pl.when(q + depth < self.total)(lambda: pl.semaphore_signal(
                self.credit.at[lax.rem(q, depth), stage], inc=1, device_id=(self.givers[stage],), device_id_type=MESH))

    def first(self, q):
        at, s, j = self.at, lax.rem(q, 2), lax.rem(q, self.slots)
        self.wait(q, 0, REST)

        @loop(LINE)
        def _(z):
            for half in PAIR:
                cols = self.cols(half)
                for k in PAIR:
                    (y, x), (oy, ox) = ((at.y, k), (1 - at.y, k)) if half else ((k, at.x), (k, 1 - at.x))
                    self.snd1[j, half, z, k] = (
                        self.part[s, z, oy, ox, at.core, :, cols] + self.recv0[s, z, oy, ox, :, cols]).astype(BF16)
                    self.kept[j, half, z, k] = self.part[s, z, y, x, at.core, :, cols] + self.recv0[s, z, y, x, :, cols]

        self.give(q, 0)
        self.send(q, 1, 2)

    def second(self, q):
        j = lax.rem(q, self.slots)
        for half in PAIR:
            own = self.own[half]
            self.wait(q, 1 + half)

            @loop(LINE)
            def _(z):
                self.snd2[j, half, z] = (
                    self.kept[j, half, z, 1 - own] + self.recv1[j, half, z, 1 - own].astype(F32)).astype(BF16)
                self.kept[j, half, z, own] = self.kept[j, half, z, own] + self.recv1[j, half, z, own].astype(F32)

            self.give(q, 1 + half)
            self.send(q, 3 + half)

    def summed(self, j, half, z):
        return self.kept[j, half, z, self.own[half]] + self.recv2[j, half, z].astype(F32)

    def third(self, q):
        j = lax.rem(q, self.slots)
        self.wait(q, 3, 4)

        @loop(len(OTHERS))
        def _(d):
            z = lax.rem(self.at.z + d + 1, LINE)
            for half in PAIR:
                self.snd3[j, d, :, self.cols(half)] = self.summed(j, half, z).astype(BF16)

        self.send(q, 5, 6, 7)

    def last(self, q):
        j = lax.rem(q, self.slots)
        totals = [self.summed(j, half, self.at.z) for half in PAIR]
        self.wait(q, 5, 6, 7)
        for d in OTHERS:
            totals = [total + self.recv3[j, d, :, self.cols(half)].astype(F32) for half, total in enumerate(totals)]
        self.give(q, 3, 4, 5, 6, 7)
        return totals


def ring_scratch(slots, rows, width):
    half = width // 2
    box, pairs = (LINE, 2, 2), (slots, 2, LINE)
    return [
        pltpu.VMEM((2, *box, 2, rows, width), F32),
        pltpu.VMEM((2, *box, rows, width), F32),
        pltpu.VMEM((*pairs, 2, rows, half), F32),
    ] + [pltpu.VMEM((*pairs, 2, rows, half), BF16)] * 2 + [pltpu.VMEM((*pairs, rows, half), BF16)] * 2 + [
        pltpu.VMEM((slots, 3, rows, width), BF16)] * 2 + [DMA_SEM((slots, REST + 1))] * 2 + [
        pltpu.SemaphoreType.REGULAR((slots, 8))]


CHUNKS = 8
RING = 12
SUMS = 5
REST = 16
QUICK = 4
SPREAD_LAGS = (1, 2, 3, 4, 6, 7, 9, 10)
RING_LAGS = (1, 3, 5, 8)


def step_kernel(
        total_rows, lam_ref, feat_a, feat_b, w_one, w_two, w_three, gain_one, shift_one, gain_two, shift_two,
        grad_w_three, grad_w_two, grad_w_one, loss_total, total_two, total_one, saved_act, saved_norm,
        grad, pre, wide, turned, weight, normed, act, sides, side_sums, local, embed_local, embed_total, loss_local, mean_col, turned_sums, by_row, scales,
        wide_sem, w_sem, load_sem, out_sem, *scratch):
    at = Place()
    place = (at.z, at.y, at.x, at.core)

    def spread(q, stage):
        cols = ring.cols((stage - 1) % 2)
        if stage < 11:
            here, peer = wide.at[(q, *place)], at.z_peers[stage - 8]
        elif stage == 11:
            here, peer = wide.at[q, :, at.y, at.x, at.core, :, cols], at.y_peer
        elif stage == 12:
            here, peer = wide.at[q, :, at.y, at.x, at.core, :, cols], at.x_peer
        elif stage == 13:
            here, peer = wide.at[q, :, :, at.x, at.core, :, cols], at.x_peer
        elif stage == 14:
            here, peer = wide.at[q, :, at.y, :, at.core, :, cols], at.y_peer
        else:
            here, peer = wide.at[q, :, :, :, at.core], at.partner
        return here, here, peer

    ring = Ring(at, 4 * CHUNKS, spread, *scratch[:RING])
    rows_dev, dim = grad.shape
    width = dim // CHUNKS
    view_rows = rows_dev // 2
    block_rows = min(128, view_rows)
    quarter = dim // 4
    count = 1.0 / total_rows
    weights = [w_one, w_two, w_three]
    gains, shifts = [gain_one, gain_two], [shift_one, shift_two]
    outs = [grad_w_three, grad_w_two, grad_w_one]
    totals = [embed_total, total_two, total_one]
    views = [pl.ds(v * view_rows, view_rows) for v in PAIR]
    rest = list(scratch[RING:])

    def take(number):
        taken, rest[:] = rest[:number], rest[number:]
        return taken

    top = pl.ds(0, 2)
    side = [[QuickSums(at, (sides, (layer, v, top)), (side_sums, (layer, v, top)), *take(QUICK)) for v in PAIR] for layer in OTHERS]
    pair_sums = QuickSums(at, (sides, (0, 0)), (side_sums, (0, 0)), *take(QUICK))
    loss_sums = QuickSums(at, (loss_local, ...), (loss_total, ...), *take(QUICK))
    sums = [[Sums(at, (embed_local, ()), (embed_total, ()), *take(SUMS))]]
    for layer in PAIR:
        sums.append([Sums(at, (local, (layer, h)), (totals[layer + 1], (h,)), *take(SUMS)) for h in PAIR])

    def act_copy(layer):
        return pltpu.make_async_copy(saved_act.at[1 - layer], act, load_sem.at[0])

    def norm_copy(layer):
        return pltpu.make_async_copy(saved_norm.at[1 - layer], normed.at[layer], load_sem.at[1])

    def feat_copy(v):
        return pltpu.make_async_copy((feat_a, feat_b)[v], normed.at[0, views[v]], load_sem.at[v])

    def wide_copy(layer, n):
        cols = pl.ds(pl.multiple_of(n * width, width), width)
        return pltpu.make_async_copy(weights[layer].at[:, :, :, :, :, cols], wide.at[n], wide_sem.at[n])

    feat_copy(0).start()
    lead = 4
    for n in range(lead):
        wide_copy(0, n).start()
    feat_copy(1).start()
    puts = {}

    def put(name, v, src, dst, k):
        copy = pltpu.make_async_copy(src, dst, out_sem.at[k, v])
        copy.start()
        puts[name, v] = copy

    def drain(*names):
        for name in names:
            for v in PAIR:
                puts.pop((name, v)).wait()

    def matmul(layer, v, hook, step):
        @loop(CHUNKS // LINE)
        def _(m):
            if step:
                pl.when(m == hook)(step)
            chunks = [LINE * m + k for k in range(LINE)]
            if v == 0:
                if layer == 0:
                    for n in chunks:
                        pl.when(n + lead < CHUNKS)(lambda n=n: wide_copy(0, n + lead).start())
                for n in chunks:
                    wide_copy(layer, n).wait()
            elif layer < 2:
                for n in chunks:
                    pl.when(m > 0)(lambda n=n: wide_copy(layer + 1, n - LINE).start())
            for n in chunks:
                cols = pl.ds(pl.multiple_of(n * width, width), width)
                out = jnp.dot(normed[layer % 2, views[v]], wide[n].reshape(dim, width), preferred_element_type=F32)
                pre[views[v], cols] = out
                sides[layer, v, FIRST, cols] = col_sum(out)
                sides[layer, v, SECOND, cols] = col_sum(out * out)

        if v and layer < 2:
            for n in range(LINE):
                wide_copy(layer + 1, LINE + n).start()
        side[layer][v].begin()

    def normalise(layer, v):
        side[layer][v].arrive()
        mean = side_sums[layer, v, FIRST, :] / total_rows
        inv = lax.rsqrt(side_sums[layer, v, SECOND, :] / total_rows - mean * mean + NORM_EPS)
        scales[2 - layer, v:v + 1, :] = gains[layer][...] * inv if layer < 2 else inv
        sides[layer, v, FIRST, :] = mean
        sides[layer, v, SECOND, :] = inv

        @loop(CHUNKS)
        def _(n):
            cols = pl.ds(pl.multiple_of(n * width, width), width)
            mean, inv = sides[layer, v, FIRST, cols], sides[layer, v, SECOND, cols]
            if layer < 2:
                gain, shift = gains[layer][:, cols], shifts[layer][:, cols]

            @loop(view_rows // block_rows)
            def _(r):
                rows = pl.ds(pl.multiple_of(v * view_rows + r * block_rows, block_rows), block_rows)
                value = (pre[rows, cols] - mean) * inv
                if layer < 2:
                    grad[rows, cols] = value.astype(BF16)
                    value = jnp.maximum(gain * value + shift, 0.0)
                normed[(layer + 1) % 2, rows, cols] = value.astype(BF16)

        if layer < 2:
            put(("act", layer), v, normed.at[(layer + 1) % 2, views[v]], saved_act.at[layer, views[v]], layer)
            put(("norm", layer), v, grad.at[views[v]], saved_norm.at[layer, views[v]], 2)

    def turn(src, dst, first, v):
        part = view_rows // 2

        @loop(CHUNKS)
        def _(n):
            cols = pl.ds(pl.multiple_of(n * width, width), width)
            for k in PAIR:
                block = src[pl.ds(v * view_rows + k * part, part), cols].T
                dst[first + 2 * v + k, lax.div(n, 2), lax.rem(n, 2)] = block.reshape(dst.shape[3:])

    enter(at.z_peers + at.cube_peers)
    feat_copy(0).wait()
    matmul(0, 0, 0, None)
    feat_copy(1).wait()
    matmul(0, 1, 1, side[0][0].over_plane)
    for v in PAIR:
        turn(normed.at[0], turned, 0, v)
    normalise(0, 0)
    for layer in PAIR:
        matmul(layer + 1, 0, 1, side[layer][1].over_plane)
        normalise(layer, 1)
        matmul(layer + 1, 1, 1, side[layer + 1][0].over_plane)
        if layer == 0:
            drain(("norm", 0))
        else:
            drain(("act", 0))
        normalise(layer + 1, 0)
    by_row[...] = jnp.zeros_like(by_row)
    sides[0, 0, FOURTH, :] = jnp.zeros((1, dim), F32)

    @loop(CHUNKS)
    def _(n):
        cols = pl.ds(pl.multiple_of(n * width, width), width)
        sides[0, 0, FIRST, cols] = col_sum(normed[1, views[0], cols].astype(F32))
        pre[views[0], cols] = jnp.zeros((view_rows, width), F32)

    side[2][1].over_plane()
    normalise(2, 1)

    drain(("act", 1), ("norm", 1))
    act_copy(0).start()
    slots = weight.shape[0]

    def weight_copy(layer, n):
        slot = lax.rem(n, slots)
        return pltpu.make_async_copy(weights[2 - layer].at[lax.div(n, 2), lax.rem(n, 2)], weight.at[slot], w_sem.at[slot])

    for n in range(slots):
        weight_copy(0, n).start()

    lam = lam_ref[0]
    lane = 128
    block_rows_dev = ring.snd1.shape[-2]
    first_row = (((at.z * 2 + at.y) * 2 + at.x) * 2 + at.core) * block_rows_dev

    def pair_rows():
        @loop(CHUNKS)
        def _(n):
            cols = pl.ds(pl.multiple_of(n * width, width), width)
            one, two = [normed[1, views[v], cols].astype(F32) for v in PAIR]
            sides[0, 0, SECOND, cols] = col_sum(two)
            sides[0, 0, THIRD, cols] = col_sum(one * two)

        pair_sums.begin()

    block = pl.ds(pl.multiple_of(lax.div(first_row, lane) * lane, lane), lane)
    part = lax.rem(first_row, lane)

    def keep_means():
        pair_sums.arrive()
        turned_sums[...] = jnp.broadcast_to(side_sums[0, 0, FIRST, block], (lane, lane)).T
        mean_col[...] = turned_sums[pl.ds(pl.multiple_of(part, 8), block_rows_dev), :]

    def row_sums():
        for k, row in enumerate((FIRST, THIRD)):
            sums_here = col_sum(by_row[k].T)
            spread = jnp.concatenate([sums_here] * (lane // block_rows_dev), axis=1)
            position = lax.broadcasted_iota(jnp.int32, spread.shape, 1)
            mine = (position >= part) & (position < part + block_rows_dev)
            embed_local[row, :] = jnp.zeros((1, dim), F32)
            embed_local[row, block] = jnp.where(mine, spread, 0.0)


    def chunk_cols(q):
        return pl.ds(pl.multiple_of(q * width, width), width)

    def correlate(q):
        @loop(LINE)
        def _(z):
            rows = pl.ds(pl.multiple_of(z * quarter, quarter), quarter)
            out = lax.dot_general(normed[1, views[0], rows], normed[1, views[1], chunk_cols(q)], DEPTH_DIMS,
                                  preferred_element_type=F32)
            ring.part[lax.rem(q, 2), z] = out.reshape(ring.part.shape[2:])
            pl.when(z == 1)(lambda: ring.send(q, 0))

        ring.start(q, REST)

    def spread_line(q):
        for half, total in enumerate(ring.last(q)):
            start = q * width + half * ring.half
            row = first_row + lax.broadcasted_iota(jnp.int32, total.shape, 0)
            col = start + lax.broadcasted_iota(jnp.int32, total.shape, 1)
            diag = row == col
            cols = pl.ds(pl.multiple_of(start, ring.half), ring.half)
            total = jnp.where(diag, side_sums[0, 0, THIRD, cols], total)
            corr = total * count
            gap = 1.0 - corr
            loss_local[:, cols] = col_sum(jnp.where(diag, gap * gap, lam * corr * corr))
            slope = (jnp.where(diag, -2.0 * gap, 2.0 * lam * corr) * count).astype(BF16)
            wide[(q, *place, ALL, ring.cols(half))] = slope
            slope = slope.astype(F32)
            embed_local[SECOND, cols] = col_sum(slope * mean_col[:, :ring.half])
            embed_local[FOURTH, cols] = col_sum(slope * total)
            terms = [slope * side_sums[0, 0, SECOND, cols], slope * total]
            for k, term in enumerate(terms):
                by_row[k] = by_row[k] + term
        ring.start(q, 8, 9, 10)

    def spread_one(q):
        ring.wait(q, 8, 9, 10)
        ring.start(q, 11, 12)

    def spread_two(q):
        ring.wait(q, 11, 12)
        ring.start(q, 13, 14)

    def spread_pair(q):
        ring.wait(q, 13, 14)
        ring.start(q, 15)

    def embed_grad(q):
        ring.wait(q, 15)
        cols = chunk_cols(q)
        pre[views[1], cols] = jnp.dot(normed[1, views[0]], wide[q].reshape(dim, width), preferred_element_type=F32)

        @loop(len(PAIR))
        def _(p):
            into = pl.ds(pl.multiple_of(p * 2 * quarter, quarter), 2 * quarter)
            rows = lax.dot_general(normed[1, views[1], cols], wide[q, pl.ds(2 * p, 2)].reshape(2 * quarter, width), LANE_DIMS,
                                   preferred_element_type=F32)
            pre[views[0], into] = pre[views[0], into] + rows

    first_sums = sums[0][0]
    steps = (ring.first, ring.second, ring.third, spread_line, spread_one, spread_two, spread_pair, embed_grad)
    done = CHUNKS + SPREAD_LAGS[3]

    def start_sums():
        row_sums()
        first_sums.begin()

    def turn_two():
        for v in PAIR:
            turn(normed.at[0], wide, 0, v)
        norm_copy(0).start()

    moves = ((0, pair_rows), (2, pair_sums.over_plane), (4, keep_means), (done, start_sums), (done + 1, first_sums.over_plane),
             (done + 2, first_sums.over_line), (done + 3, first_sums.over_pair))

    @loop(CHUNKS + SPREAD_LAGS[-1])
    def _(t):
        pl.when(t < CHUNKS)(lambda: correlate(t))
        for when, move in moves:
            pl.when(t == when)(move)
        for step, lag in zip(steps, SPREAD_LAGS):
            pl.when((t >= lag) & (t < lag + CHUNKS))(lambda step=step, lag=lag: step(t - lag))
        pl.when(t == SPREAD_LAGS[-1] + LINE - 1)(turn_two)

    loss_sums.begin()

    def finish_grad(layer, j):
        cols = chunk_cols(j)
        per = CHUNKS // 2
        total, sel = (embed_total, cols) if layer == 0 else (totals[layer].at[lax.div(j, per)], chunk_cols(lax.rem(j, per)))
        for v in PAIR:
            mean0 = total[v:v + 1, sel] * count
            mean1 = total[2 + v:3 + v, sel] * count
            scale = scales[layer, v:v + 1, cols]

            @loop(view_rows // block_rows)
            def _(r):
                rows = pl.ds(pl.multiple_of(v * view_rows + r * block_rows, block_rows), block_rows)
                xhat = normed[(layer + 1) % 2, rows, cols].astype(F32)
                grad[rows, cols] = (scale * (pre[rows, cols] - (mean0 + xhat * mean1))).astype(BF16)

    def weight_grad(layer, j):
        q = (layer + 1) * CHUNKS + j
        source, first = (turned, 0) if layer == 2 else (wide, LINE * layer)

        @loop(len(PAIR))
        def _(p):
            span = pl.ds(2 * p, 2)
            feed = jnp.concatenate([source[first + k, span].reshape(2 * quarter, -1) for k in range(LINE)], axis=1)
            out = jnp.dot(feed, grad[:, chunk_cols(j)], preferred_element_type=F32)
            ring.part[lax.rem(q, 2), span] = out.reshape(2, *ring.part.shape[2:])
            pl.when(p == 0)(lambda: ring.send(q, 0))

        ring.start(q, REST)

    def input_grad(layer, p):
        two = 2 * width
        cols = pl.ds(pl.multiple_of(p * two, two), two)
        for n in PAIR:
            weight_copy(layer, 2 * p + n).wait()
        half = local.at[layer, lax.div(p, 2)]
        sel = pl.ds(pl.multiple_of(lax.rem(p, 2) * two, two), two)

        @loop(len(PAIR))
        def _(v):
            rows = pl.ds(pl.multiple_of(v * view_rows, view_rows), view_rows)
            block = weight[pl.ds(2 * lax.rem(p, 2), 2)].reshape(two, dim)
            out = lax.dot_general(grad[rows, :], block, LANE_DIMS, preferred_element_type=F32)
            out = jnp.where(act[rows, cols] > 0, out, 0.0)
            pre[rows, cols] = out
            half[pl.ds(v, 1), sel] = col_sum(out)
            half[pl.ds(2 + v, 1), sel] = col_sum(out * normed[layer % 2, rows, cols].astype(F32))

        @pl.when(p < 2)
        def _():
            for n in PAIR:
                weight_copy(layer, 2 * p + n + slots).start()

    def serve(layer, j):
        t = layer * CHUNKS + j
        for step, lag in zip((ring.first, ring.second, ring.third), RING_LAGS):
            pl.when((t >= lag) & (t < lag + 3 * CHUNKS))(lambda step=step, lag=lag: step(CHUNKS + t - lag))
        if layer:
            for half, block in enumerate(ring.last(t)):
                outs[layer - 1][:, pl.ds(pl.multiple_of(j * width + half * ring.half, ring.half), ring.half)] = block

    for layer in OTHERS:
        old, new = sums[layer], sums[layer + 1] if layer < 2 else None
        old[0].arrive()

        def settle():
            if layer:
                old[1].arrive()

            @pl.loop(3, CHUNKS)
            def _(k):
                finish_grad(layer, k)

            if layer == 0:
                norm_copy(1).start()

        def late_loads():
            new[1].begin()
            if layer == 0:
                act_copy(1).start()
                for n in range(slots):
                    weight_copy(1, n).start()

        def relay_pair():
            new[0].over_pair()
            new[1].over_plane()

        before, middle, after = [], [(2, settle)], []
        if layer:
            middle.append((0, old[1].over_pair))
        if layer == 0:
            before.append((3, lambda: act_copy(0).wait()))
        if new:
            before += [(2, lambda: norm_copy(layer).wait()), (5, new[0].over_plane), (6, new[0].over_line), (7, relay_pair)]
            after += [(4, new[0].begin), (6, late_loads), (7, new[1].over_line)]

        @loop(CHUNKS)
        def _(j):
            for when, move in before:
                pl.when(j == when)(move)
            pl.when(j < 3)(lambda: finish_grad(layer, j))
            weight_grad(layer, j)
            for when, move in middle:
                pl.when(j == when)(move)
            if new:
                pl.when((j > 2) & (j < 7))(lambda: input_grad(layer, j - 3))
            for when, move in after:
                pl.when(j == when)(move)
            serve(layer, j)

        if layer == 0:
            act_copy(1).wait()
            for v in PAIR:
                turn(act, wide, LINE, v)
            loss_sums.over_plane()

    @loop(CHUNKS)
    def _(j):
        serve(len(OTHERS), j)

    loss_sums.arrive()


def step(total_rows, vmem, lam, feat_a, feat_b, weights, vectors):
    view_rows, dim = feat_a.shape
    rows, width, blocks = 2 * view_rows, dim // CHUNKS, dim // 32
    hbm = pl.BlockSpec(memory_space=pl.ANY)
    vm = pl.BlockSpec(memory_space=pltpu.VMEM)
    cube = (LINE, 2, 2, 2, blocks)
    scratch = [
        pltpu.VMEM((rows, dim), BF16),
        pltpu.VMEM((rows, dim), F32),
        pltpu.VMEM((CHUNKS, *cube, width), BF16),
        pltpu.VMEM((LINE, *cube, view_rows // 2), BF16),
        pltpu.VMEM((LINE, 2, 2, blocks, dim), BF16),
        pltpu.VMEM((2, rows, dim), BF16),
        pltpu.VMEM((rows, dim), BF16),
        pltpu.VMEM((3, 2, 4, dim), F32),
        pltpu.VMEM((3, 2, 4, dim), F32),
        pltpu.VMEM((2, 2, 4, dim // 2), F32),
        pltpu.VMEM((4, dim), F32),
        pltpu.VMEM((4, dim), F32),
        pltpu.VMEM((1, dim), F32),
        pltpu.VMEM((blocks, 128), F32),
        pltpu.VMEM((128, 128), F32),
        pltpu.VMEM((2, blocks, width // 2), F32),
        pltpu.VMEM((3, 2, dim), F32),
        DMA_SEM((CHUNKS,)),
        DMA_SEM((LINE,)),
        DMA_SEM((3,)),
        DMA_SEM((3, 2)),
    ] + ring_scratch(CHUNKS, blocks, width)
    for _ in range(6):
        scratch += quick_scratch(2, dim)
    scratch += quick_scratch(4, dim) + quick_scratch(1, dim) + sums_scratch(4, dim)
    for _ in range(4):
        scratch += sums_scratch(4, dim // 2)
    halves = jax.ShapeDtypeStruct((2, 4, dim // 2), F32)
    saved = jax.ShapeDtypeStruct((2, rows, dim), BF16)
    return pl.pallas_call(
        functools.partial(step_kernel, total_rows),
        out_shape=[jax.ShapeDtypeStruct((blocks, dim), F32)] * 3 + [
            jax.ShapeDtypeStruct((1, dim), F32), halves, halves, saved, saved],
        in_specs=[pl.BlockSpec(memory_space=pltpu.SMEM)] + [hbm] * 5 + [vm] * 4,
        out_specs=[vm] * 6 + [hbm] * 2,
        scratch_shapes=scratch,
        compiler_params=pltpu.CompilerParams(collective_id=0, has_side_effects=True, vmem_limit_bytes=vmem),
    )(lam.reshape(1), feat_a, feat_b, *[weight.reshape(*cube, dim) for weight in weights],
      *[value.reshape(1, dim) for value in vectors])


def finish_kernel(total_two, total_one, loss_cols, *refs):
    gain_one, shift_one, gain_two, shift_two, loss = refs[6:]
    for grad, out in zip(refs[:3], refs[3:6]):
        out[...] = grad[...]
    half = total_two.shape[-1]
    for total, gain, shift in ((total_two, gain_two, shift_two), (total_one, gain_one, shift_one)):
        for h in PAIR:
            cols = pl.ds(h * half, half)
            shift[:, cols] = total[h, FIRST] + total[h, SECOND]
            gain[:, cols] = total[h, THIRD] + total[h, FOURTH]
    loss[...] = jnp.sum(loss_cols[...], axis=1, keepdims=True)


def finish(total_two, total_one, loss_cols, grads):
    vm = pl.BlockSpec(memory_space=pltpu.VMEM)
    row = jax.ShapeDtypeStruct((1, loss_cols.shape[1]), F32)
    outs = pl.pallas_call(
        finish_kernel,
        out_shape=[jax.ShapeDtypeStruct(grad.shape, F32) for grad in grads] + [row] * 4 + [jax.ShapeDtypeStruct((1, 1), F32)],
        in_specs=[vm] * 6,
        out_specs=[vm] * 8,
    )(total_two, total_one, loss_cols, *grads)
    return outs[:3], [row.reshape(-1) for row in outs[3:7]], outs[7].reshape(())


def solution(mesh):
    shards = mesh.shape["data"]

    def local_step(h_a, h_b, w_one, w_two, w_three, gain_one, shift_one, gain_two, shift_two, lam_off):
        rows_dev = h_a.shape[0]
        total_rows = rows_dev * shards
        grad_w_three, grad_w_two, grad_w_one, loss_cols, total_two, total_one = step(
            total_rows, 67000000, lam_off, h_a, h_b, (w_one, w_two, w_three),
            (gain_one, shift_one, gain_two, shift_two))[:6]
        grads, vectors, loss_total = finish(total_two, total_one, loss_cols, [grad_w_one, grad_w_two, grad_w_three])
        return (loss_total, *grads, *vectors)

    row_spec = P("data", None)
    whole_mat = P(None, None)
    whole_vec = P(None)
    return jax.shard_map(
        local_step, mesh=mesh,
        in_specs=(row_spec, row_spec, whole_mat, whole_mat, whole_mat,
                  whole_vec, whole_vec, whole_vec, whole_vec, P()),
        out_specs=(P(), row_spec, row_spec, row_spec, whole_vec, whole_vec, whole_vec, whole_vec),
        check_vma=False)
```

```python
import functools

import jax
import jax.numpy as jnp
from jax import lax
from jax.experimental import pallas as pl
from jax.experimental.pallas import tpu as pltpu
from jax.sharding import PartitionSpec as P

NORM_EPS = 1e-5
MESH = pl.DeviceIdType.MESH
F32 = jnp.float32
BF16 = jnp.bfloat16


ALL = slice(None)
FIRST, SECOND, THIRD, FOURTH = [slice(k, k + 1) for k in range(4)]
PAIR = range(2)
OTHERS = range(3)
LINE = 4
CUBE = 8
DEPTH_DIMS = (((0,), (0,)), ((), ()))
LANE_DIMS = (((1,), (1,)), ((), ()))
DMA_SEM = pltpu.SemaphoreType.DMA


def loop(count):
    return pl.loop(0, count)


def col_sum(values):
    return jnp.sum(values, axis=0, keepdims=True)


class Place:
    def __init__(self):
        me = lax.axis_index("data")
        self.core = lax.rem(me, 2)
        self.x = lax.rem(lax.div(me, 2), 2)
        self.y = lax.rem(lax.div(me, 4), 2)
        self.z = lax.div(me, 8)
        self.plane = lax.rem(lax.div(me, 2), 4)
        self.partner = me + 1 - 2 * self.core
        self.x_peer = me + 2 - 4 * self.x
        self.y_peer = me + 4 - 8 * self.y
        self.low = lax.rem(me, CUBE)
        self.others = [lax.rem(self.z + d + 1, LINE) for d in OTHERS]
        self.z_peers = [z * CUBE + self.low for z in self.others]
        self.plane_peers = [self.z * CUBE + lax.rem(self.plane + d + 1, LINE) * 2 + self.core for d in OTHERS]
        self.cube_peers = [self.z * CUBE + lax.rem(self.low + d + 1, CUBE) for d in range(CUBE - 1)]
        self.near = [self.partner] + self.plane_peers + self.z_peers


def enter(peers):
    barrier = pltpu.get_barrier_semaphore()
    for peer in peers:
        pl.semaphore_signal(barrier, inc=1, device_id=(peer,), device_id_type=MESH)
    pl.semaphore_wait(barrier, len(peers))


def remote(src, dst, send_sem, recv_sem, peer):
    return pltpu.make_async_remote_copy(
        src_ref=src, dst_ref=dst, send_sem=send_sem, recv_sem=recv_sem,
        device_id=(peer,), device_id_type=MESH)


class Sums:
    def __init__(self, at, local, total, recv0, slots1, slots2, send_sem, recv_sem):
        self.at, self.refs = at, (local, total)
        self.recv0, self.slots1, self.slots2 = recv0, slots1, slots2
        self.send_sem, self.recv_sem = send_sem, recv_sem
        self.half = recv0.shape[-1]
        self.mine = pl.multiple_of(at.core * self.half, 128)
        self.theirs = pl.multiple_of((1 - at.core) * self.half, 128)

    def pick(self, k, first):
        ref, index = self.refs[k]
        return ref.at[(*index, ALL, pl.ds(first, self.half))]

    def copies(self, stage):
        at = self.at
        if stage == 0:
            pairs = [(0, self.pick(0, self.theirs), self.recv0, at.partner)]
        elif stage == 1:
            here = self.slots1.at[at.plane]
            pairs = [(1 + d, here, here, at.plane_peers[d]) for d in OTHERS]
        elif stage == 2:
            here = self.slots2.at[at.z]
            pairs = [(4 + d, here, here, at.z_peers[d]) for d in OTHERS]
        else:
            here = self.pick(1, self.mine)
            pairs = [(7, here, here, at.partner)]
        return [remote(src, dst, self.send_sem.at[k], self.recv_sem.at[k], peer) for k, src, dst, peer in pairs]

    def send(self, stage):
        for copy in self.copies(stage):
            copy.start()

    def arrive(self, stage=3):
        for copy in self.copies(stage):
            copy.wait()

    def begin(self):
        self.send(0)

    def over_plane(self):
        self.arrive(0)
        self.slots1[self.at.plane] = self.pick(0, self.mine)[...] + self.recv0[...]
        self.send(1)

    def over_line(self):
        self.arrive(1)
        self.slots2[self.at.z] = jnp.sum(self.slots1[...], axis=0)
        self.send(2)

    def over_pair(self):
        self.arrive(2)
        self.pick(1, self.mine)[...] = jnp.sum(self.slots2[...], axis=0)
        self.send(3)


class QuickSums:
    def __init__(self, at, local, total, slots1, slots2, send_sem, recv_sem):
        self.at, self.local, self.total = at, local, total
        self.slots1, self.slots2 = slots1, slots2
        self.send_sem, self.recv_sem = send_sem, recv_sem

    def copies(self, across):
        at = self.at
        if across:
            here, peers, first = self.slots2.at[at.low], at.cube_peers, len(at.z_peers)
        else:
            here, peers, first = self.slots1.at[at.z], at.z_peers, 0
        return [remote(here, here, self.send_sem.at[first + d], self.recv_sem.at[first + d], peer)
                for d, peer in enumerate(peers)]

    def begin(self):
        ref, index = self.local
        self.slots1[self.at.z] = ref[index]
        for copy in self.copies(False):
            copy.start()

    def over_plane(self):
        for copy in self.copies(False):
            copy.wait()
        self.slots2[self.at.low] = jnp.sum(self.slots1[...], axis=0)
        for copy in self.copies(True):
            copy.start()

    def arrive(self):
        for copy in self.copies(True):
            copy.wait()
        ref, index = self.total
        ref[index] = jnp.sum(self.slots2[...], axis=0)


def quick_scratch(rows, cols):
    return [
        pltpu.VMEM((LINE, rows, cols), F32),
        pltpu.VMEM((CUBE, rows, cols), F32),
        DMA_SEM((LINE + CUBE,)),
        DMA_SEM((LINE + CUBE,)),
    ]


def sums_scratch(rows, cols):
    return [
        pltpu.VMEM((rows, cols // 2), F32),
        pltpu.VMEM((4, rows, cols // 2), F32),
        pltpu.VMEM((4, rows, cols // 2), F32),
    ] + [DMA_SEM((CUBE,))] * 2


class Ring:
    def __init__(self, at, total, spread, part, recv0, kept, snd1, recv1, snd2, recv2, snd3, recv3, send_sem, recv_sem, credit):
        self.at, self.total, self.slots, self.spread = at, total, kept.shape[0], spread
        self.part, self.recv0, self.kept = part, recv0, kept
        self.snd1, self.recv1, self.snd2, self.recv2, self.snd3, self.recv3 = snd1, recv1, snd2, recv2, snd3, recv3
        self.send_sem, self.recv_sem, self.credit = send_sem, recv_sem, credit
        self.half = snd1.shape[-1]
        self.peers = [at.partner, at.x_peer, at.y_peer, at.y_peer, at.x_peer] + at.z_peers
        self.givers = self.peers[:5] + at.z_peers[::-1]
        self.own = [at.y, at.x]

    def cols(self, half):
        return pl.ds(half * self.half, self.half)

    def copy(self, q, stage):
        j, s = lax.rem(q, self.slots), lax.rem(q, 2)
        if stage % REST == 0:
            z, peer = pl.ds(2 * (stage // REST), 2), self.at.partner
            src, dst = self.part.at[s, z, :, :, 1 - self.at.core], self.recv0.at[s, z]
        elif stage > 7:
            src, dst, peer = self.spread(q, stage)
        else:
            peer = self.peers[stage]
            if stage > 4:
                src, dst = self.snd3.at[j, stage - 5], self.recv3.at[j, stage - 5]
            elif stage > 2:
                src, dst = self.snd2.at[j, stage - 3], self.recv2.at[j, stage - 3]
            else:
                src, dst = self.snd1.at[j, stage - 1], self.recv1.at[j, stage - 1]
        return remote(src, dst, self.send_sem.at[j, stage], self.recv_sem.at[j, stage], peer)

    def start(self, q, *stages):
        for stage in stages:
            self.copy(q, stage).start()

    def wait(self, q, *stages):
        for stage in stages:
            self.copy(q, stage).wait()

    def depth(self, stage):
        return self.slots if stage else self.part.shape[0]

    def send(self, q, *stages):
        for stage in stages:
            depth = self.depth(stage)
            pl.when(q >= depth)(lambda: pl.semaphore_wait(self.credit.at[lax.rem(q, depth), stage], 1))
            self.start(q, stage)

    def give(self, q, *stages):
        for stage in stages:
            depth = self.depth(stage)
            pl.when(q + depth < self.total)(lambda: pl.semaphore_signal(
                self.credit.at[lax.rem(q, depth), stage], inc=1, device_id=(self.givers[stage],), device_id_type=MESH))

    def first(self, q):
        at, s, j = self.at, lax.rem(q, 2), lax.rem(q, self.slots)
        self.wait(q, 0, REST)

        @loop(LINE)
        def _(z):
            for half in PAIR:
                cols = self.cols(half)
                for k in PAIR:
                    (y, x), (oy, ox) = ((at.y, k), (1 - at.y, k)) if half else ((k, at.x), (k, 1 - at.x))
                    self.snd1[j, half, z, k] = (
                        self.part[s, z, oy, ox, at.core, :, cols] + self.recv0[s, z, oy, ox, :, cols]).astype(BF16)
                    self.kept[j, half, z, k] = self.part[s, z, y, x, at.core, :, cols] + self.recv0[s, z, y, x, :, cols]

        self.give(q, 0)
        self.send(q, 1, 2)

    def second(self, q):
        j = lax.rem(q, self.slots)
        for half in PAIR:
            own = self.own[half]
            self.wait(q, 1 + half)

            @loop(LINE)
            def _(z):
                self.snd2[j, half, z] = (
                    self.kept[j, half, z, 1 - own] + self.recv1[j, half, z, 1 - own].astype(F32)).astype(BF16)
                self.kept[j, half, z, own] = self.kept[j, half, z, own] + self.recv1[j, half, z, own].astype(F32)

            self.give(q, 1 + half)
            self.send(q, 3 + half)

    def summed(self, j, half, z):
        return self.kept[j, half, z, self.own[half]] + self.recv2[j, half, z].astype(F32)

    def third(self, q):
        j = lax.rem(q, self.slots)
        self.wait(q, 3, 4)

        @loop(len(OTHERS))
        def _(d):
            z = lax.rem(self.at.z + d + 1, LINE)
            for half in PAIR:
                self.snd3[j, d, :, self.cols(half)] = self.summed(j, half, z).astype(BF16)

        self.send(q, 5, 6, 7)

    def last(self, q):
        j = lax.rem(q, self.slots)
        totals = [self.summed(j, half, self.at.z) for half in PAIR]
        self.wait(q, 5, 6, 7)
        for d in OTHERS:
            totals = [total + self.recv3[j, d, :, self.cols(half)].astype(F32) for half, total in enumerate(totals)]
        self.give(q, 3, 4, 5, 6, 7)
        return totals


def ring_scratch(slots, rows, width):
    half = width // 2
    box, pairs = (LINE, 2, 2), (slots, 2, LINE)
    return [
        pltpu.VMEM((2, *box, 2, rows, width), F32),
        pltpu.VMEM((2, *box, rows, width), F32),
        pltpu.VMEM((*pairs, 2, rows, half), F32),
    ] + [pltpu.VMEM((*pairs, 2, rows, half), BF16)] * 2 + [pltpu.VMEM((*pairs, rows, half), BF16)] * 2 + [
        pltpu.VMEM((slots, 3, rows, width), BF16)] * 2 + [DMA_SEM((slots, REST + 1))] * 2 + [
        pltpu.SemaphoreType.REGULAR((slots, 8))]


CHUNKS = 8
RING = 12
SUMS = 5
REST = 16
QUICK = 4
SPREAD_LAGS = (1, 2, 3, 4, 6, 7, 9, 10)
RING_LAGS = (1, 3, 5, 8)


def step_kernel(
        total_rows, lam_ref, feat_a, feat_b, w_one, w_two, w_three, gain_one, shift_one, gain_two, shift_two,
        grad_w_three, grad_w_two, grad_w_one, loss_total, total_two, total_one, saved_act, saved_norm,
        grad, pre, wide, turned, weight, normed, act, sides, side_sums, local, embed_local, embed_total, loss_local, mean_col, turned_sums, by_row, scales,
        wide_sem, w_sem, load_sem, out_sem, *scratch):
    at = Place()
    place = (at.z, at.y, at.x, at.core)

    def spread(q, stage):
        cols = ring.cols((stage - 1) % 2)
        if stage < 11:
            here, peer = wide.at[(q, *place)], at.z_peers[stage - 8]
        elif stage == 11:
            here, peer = wide.at[q, :, at.y, at.x, at.core, :, cols], at.y_peer
        elif stage == 12:
            here, peer = wide.at[q, :, at.y, at.x, at.core, :, cols], at.x_peer
        elif stage == 13:
            here, peer = wide.at[q, :, :, at.x, at.core, :, cols], at.x_peer
        elif stage == 14:
            here, peer = wide.at[q, :, at.y, :, at.core, :, cols], at.y_peer
        else:
            here, peer = wide.at[q, :, :, :, at.core], at.partner
        return here, here, peer

    ring = Ring(at, 4 * CHUNKS, spread, *scratch[:RING])
    rows_dev, dim = grad.shape
    width = dim // CHUNKS
    view_rows = rows_dev // 2
    block_rows = min(128, view_rows)
    quarter = dim // 4
    count = 1.0 / total_rows
    weights = [w_one, w_two, w_three]
    gains, shifts = [gain_one, gain_two], [shift_one, shift_two]
    outs = [grad_w_three, grad_w_two, grad_w_one]
    totals = [embed_total, total_two, total_one]
    views = [pl.ds(v * view_rows, view_rows) for v in PAIR]
    rest = list(scratch[RING:])

    def take(number):
        taken, rest[:] = rest[:number], rest[number:]
        return taken

    top = pl.ds(0, 2)
    side = [[QuickSums(at, (sides, (layer, v, top)), (side_sums, (layer, v, top)), *take(QUICK)) for v in PAIR] for layer in OTHERS]
    pair_sums = QuickSums(at, (sides, (0, 0)), (side_sums, (0, 0)), *take(QUICK))
    loss_sums = QuickSums(at, (loss_local, ...), (loss_total, ...), *take(QUICK))
    sums = [[Sums(at, (embed_local, ()), (embed_total, ()), *take(SUMS))]]
    for layer in PAIR:
        sums.append([Sums(at, (local, (layer, h)), (totals[layer + 1], (h,)), *take(SUMS)) for h in PAIR])

    def act_copy(layer):
        return pltpu.make_async_copy(saved_act.at[1 - layer], act, load_sem.at[0])

    def norm_copy(layer):
        return pltpu.make_async_copy(saved_norm.at[1 - layer], normed.at[layer], load_sem.at[1])

    def feat_copy(v):
        return pltpu.make_async_copy((feat_a, feat_b)[v], normed.at[0, views[v]], load_sem.at[v])

    def wide_copy(layer, n):
        cols = pl.ds(pl.multiple_of(n * width, width), width)
        return pltpu.make_async_copy(weights[layer].at[:, :, :, :, :, cols], wide.at[n], wide_sem.at[n])

    feat_copy(0).start()
    lead = 4
    for n in range(lead):
        wide_copy(0, n).start()
    feat_copy(1).start()
    puts = {}

    def put(name, v, src, dst, k):
        copy = pltpu.make_async_copy(src, dst, out_sem.at[k, v])
        copy.start()
        puts[name, v] = copy

    def drain(*names):
        for name in names:
            for v in PAIR:
                puts.pop((name, v)).wait()

    def matmul(layer, v, hook, step):
        @loop(CHUNKS // LINE)
        def _(m):
            if step:
                pl.when(m == hook)(step)
            chunks = [LINE * m + k for k in range(LINE)]
            if v == 0:
                if layer == 0:
                    for n in chunks:
                        pl.when(n + lead < CHUNKS)(lambda n=n: wide_copy(0, n + lead).start())
                for n in chunks:
                    wide_copy(layer, n).wait()
            elif layer < 2:
                for n in chunks:
                    pl.when(m > 0)(lambda n=n: wide_copy(layer + 1, n - LINE).start())
            for n in chunks:
                cols = pl.ds(pl.multiple_of(n * width, width), width)
                out = jnp.dot(normed[layer % 2, views[v]], wide[n].reshape(dim, width), preferred_element_type=F32)
                pre[views[v], cols] = out
                sides[layer, v, FIRST, cols] = col_sum(out)
                sides[layer, v, SECOND, cols] = col_sum(out * out)

        if v and layer < 2:
            for n in range(LINE):
                wide_copy(layer + 1, LINE + n).start()
        side[layer][v].begin()

    def normalise(layer, v):
        side[layer][v].arrive()
        mean = side_sums[layer, v, FIRST, :] / total_rows
        inv = lax.rsqrt(side_sums[layer, v, SECOND, :] / total_rows - mean * mean + NORM_EPS)
        scales[2 - layer, v:v + 1, :] = gains[layer][...] * inv if layer < 2 else inv
        sides[layer, v, FIRST, :] = mean
        sides[layer, v, SECOND, :] = inv

        @loop(CHUNKS)
        def _(n):
            cols = pl.ds(pl.multiple_of(n * width, width), width)
            mean, inv = sides[layer, v, FIRST, cols], sides[layer, v, SECOND, cols]
            if layer < 2:
                gain, shift = gains[layer][:, cols], shifts[layer][:, cols]

            @loop(view_rows // block_rows)
            def _(r):
                rows = pl.ds(pl.multiple_of(v * view_rows + r * block_rows, block_rows), block_rows)
                value = (pre[rows, cols] - mean) * inv
                if layer < 2:
                    grad[rows, cols] = value.astype(BF16)
                    value = jnp.maximum(gain * value + shift, 0.0)
                normed[(layer + 1) % 2, rows, cols] = value.astype(BF16)

        if layer < 2:
            put(("act", layer), v, normed.at[(layer + 1) % 2, views[v]], saved_act.at[layer, views[v]], layer)
            put(("norm", layer), v, grad.at[views[v]], saved_norm.at[layer, views[v]], 2)

    def turn(src, dst, first, v):
        part = view_rows // 2

        @loop(CHUNKS)
        def _(n):
            cols = pl.ds(pl.multiple_of(n * width, width), width)
            for k in PAIR:
                block = src[pl.ds(v * view_rows + k * part, part), cols].T
                dst[first + 2 * v + k, lax.div(n, 2), lax.rem(n, 2)] = block.reshape(dst.shape[3:])

    enter(at.z_peers + at.cube_peers)
    feat_copy(0).wait()
    matmul(0, 0, 0, None)
    feat_copy(1).wait()
    matmul(0, 1, 1, side[0][0].over_plane)
    for v in PAIR:
        turn(normed.at[0], turned, 0, v)
    normalise(0, 0)
    for layer in PAIR:
        matmul(layer + 1, 0, 1, side[layer][1].over_plane)
        normalise(layer, 1)
        matmul(layer + 1, 1, 1, side[layer + 1][0].over_plane)
        if layer == 0:
            drain(("norm", 0))
        else:
            drain(("act", 0))
        normalise(layer + 1, 0)
    by_row[...] = jnp.zeros_like(by_row)
    sides[0, 0, FOURTH, :] = jnp.zeros((1, dim), F32)

    @loop(CHUNKS)
    def _(n):
        cols = pl.ds(pl.multiple_of(n * width, width), width)
        sides[0, 0, FIRST, cols] = col_sum(normed[1, views[0], cols].astype(F32))
        pre[views[0], cols] = jnp.zeros((view_rows, width), F32)

    side[2][1].over_plane()
    normalise(2, 1)

    drain(("act", 1), ("norm", 1))
    act_copy(0).start()
    slots = weight.shape[0]

    def weight_copy(layer, n):
        slot = lax.rem(n, slots)
        return pltpu.make_async_copy(weights[2 - layer].at[lax.div(n, 2), lax.rem(n, 2)], weight.at[slot], w_sem.at[slot])

    for n in range(slots):
        weight_copy(0, n).start()

    lam = lam_ref[0]
    lane = 128
    block_rows_dev = ring.snd1.shape[-2]
    first_row = (((at.z * 2 + at.y) * 2 + at.x) * 2 + at.core) * block_rows_dev

    def pair_rows():
        @loop(CHUNKS)
        def _(n):
            cols = pl.ds(pl.multiple_of(n * width, width), width)
            one, two = [normed[1, views[v], cols].astype(F32) for v in PAIR]
            sides[0, 0, SECOND, cols] = col_sum(two)
            sides[0, 0, THIRD, cols] = col_sum(one * two)

        pair_sums.begin()

    block = pl.ds(pl.multiple_of(lax.div(first_row, lane) * lane, lane), lane)
    part = lax.rem(first_row, lane)

    def keep_means():
        pair_sums.arrive()
        turned_sums[...] = jnp.broadcast_to(side_sums[0, 0, FIRST, block], (lane, lane)).T
        mean_col[...] = turned_sums[pl.ds(pl.multiple_of(part, 8), block_rows_dev), :]

    def row_sums():
        for k, row in enumerate((FIRST, THIRD)):
            sums_here = col_sum(by_row[k].T)
            spread = jnp.concatenate([sums_here] * (lane // block_rows_dev), axis=1)
            position = lax.broadcasted_iota(jnp.int32, spread.shape, 1)
            mine = (position >= part) & (position < part + block_rows_dev)
            embed_local[row, :] = jnp.zeros((1, dim), F32)
            embed_local[row, block] = jnp.where(mine, spread, 0.0)


    def chunk_cols(q):
        return pl.ds(pl.multiple_of(q * width, width), width)

    def correlate(q):
        @loop(LINE)
        def _(z):
            rows = pl.ds(pl.multiple_of(z * quarter, quarter), quarter)
            out = lax.dot_general(normed[1, views[0], rows], normed[1, views[1], chunk_cols(q)], DEPTH_DIMS,
                                  preferred_element_type=F32)
            ring.part[lax.rem(q, 2), z] = out.reshape(ring.part.shape[2:])
            pl.when(z == 1)(lambda: ring.send(q, 0))

        ring.start(q, REST)

    def spread_line(q):
        for half, total in enumerate(ring.last(q)):
            start = q * width + half * ring.half
            row = first_row + lax.broadcasted_iota(jnp.int32, total.shape, 0)
            col = start + lax.broadcasted_iota(jnp.int32, total.shape, 1)
            diag = row == col
            cols = pl.ds(pl.multiple_of(start, ring.half), ring.half)
            total = jnp.where(diag, side_sums[0, 0, THIRD, cols], total)
            corr = total * count
            gap = 1.0 - corr
            loss_local[:, cols] = col_sum(jnp.where(diag, gap * gap, lam * corr * corr))
            slope = (jnp.where(diag, -2.0 * gap, 2.0 * lam * corr) * count).astype(BF16)
            wide[(q, *place, ALL, ring.cols(half))] = slope
            slope = slope.astype(F32)
            embed_local[SECOND, cols] = col_sum(slope * mean_col[:, :ring.half])
            embed_local[FOURTH, cols] = col_sum(slope * total)
            terms = [slope * side_sums[0, 0, SECOND, cols], slope * total]
            for k, term in enumerate(terms):
                by_row[k] = by_row[k] + term
        ring.start(q, 8, 9, 10)

    def spread_one(q):
        ring.wait(q, 8, 9, 10)
        ring.start(q, 11, 12)

    def spread_two(q):
        ring.wait(q, 11, 12)
        ring.start(q, 13, 14)

    def spread_pair(q):
        ring.wait(q, 13, 14)
        ring.start(q, 15)

    def embed_grad(q):
        ring.wait(q, 15)
        cols = chunk_cols(q)
        pre[views[1], cols] = jnp.dot(normed[1, views[0]], wide[q].reshape(dim, width), preferred_element_type=F32)

        @loop(len(PAIR))
        def _(p):
            into = pl.ds(pl.multiple_of(p * 2 * quarter, quarter), 2 * quarter)
            rows = lax.dot_general(normed[1, views[1], cols], wide[q, pl.ds(2 * p, 2)].reshape(2 * quarter, width), LANE_DIMS,
                                   preferred_element_type=F32)
            pre[views[0], into] = pre[views[0], into] + rows

    first_sums = sums[0][0]
    steps = (ring.first, ring.second, ring.third, spread_line, spread_one, spread_two, spread_pair, embed_grad)
    done = CHUNKS + SPREAD_LAGS[3]

    def start_sums():
        row_sums()
        first_sums.begin()

    def turn_two():
        for v in PAIR:
            turn(normed.at[0], wide, 0, v)
        norm_copy(0).start()

    moves = ((3, pair_sums.over_plane), (4, keep_means), (done, start_sums), (done + 1, first_sums.over_plane),
             (done + 2, first_sums.over_line), (done + 3, first_sums.over_pair))

    @loop(CHUNKS + SPREAD_LAGS[-1])
    def _(t):
        pl.when(t < CHUNKS)(lambda: correlate(t))
        for when, move in moves:
            pl.when(t == when)(move)
        for step, lag in zip(steps, SPREAD_LAGS):
            pl.when((t >= lag) & (t < lag + CHUNKS))(lambda step=step, lag=lag: step(t - lag))
        pl.when(t == 1)(pair_rows)
        pl.when(t == SPREAD_LAGS[-1] + LINE - 1)(turn_two)

    loss_sums.begin()

    def finish_grad(layer, j):
        cols = chunk_cols(j)
        per = CHUNKS // 2
        total, sel = (embed_total, cols) if layer == 0 else (totals[layer].at[lax.div(j, per)], chunk_cols(lax.rem(j, per)))
        for v in PAIR:
            mean0 = total[v:v + 1, sel] * count
            mean1 = total[2 + v:3 + v, sel] * count
            scale = scales[layer, v:v + 1, cols]

            @loop(view_rows // block_rows)
            def _(r):
                rows = pl.ds(pl.multiple_of(v * view_rows + r * block_rows, block_rows), block_rows)
                xhat = normed[(layer + 1) % 2, rows, cols].astype(F32)
                grad[rows, cols] = (scale * (pre[rows, cols] - (mean0 + xhat * mean1))).astype(BF16)

    def weight_grad(layer, j):
        q = (layer + 1) * CHUNKS + j
        source, first = (turned, 0) if layer == 2 else (wide, LINE * layer)

        @loop(len(PAIR))
        def _(p):
            span = pl.ds(2 * p, 2)
            feed = jnp.concatenate([source[first + k, span].reshape(2 * quarter, -1) for k in range(LINE)], axis=1)
            out = jnp.dot(feed, grad[:, chunk_cols(j)], preferred_element_type=F32)
            ring.part[lax.rem(q, 2), span] = out.reshape(2, *ring.part.shape[2:])
            pl.when(p == 0)(lambda: ring.send(q, 0))

        ring.start(q, REST)

    def input_grad(layer, p):
        two = 2 * width
        cols = pl.ds(pl.multiple_of(p * two, two), two)
        for n in PAIR:
            weight_copy(layer, 2 * p + n).wait()
        half = local.at[layer, lax.div(p, 2)]
        sel = pl.ds(pl.multiple_of(lax.rem(p, 2) * two, two), two)

        @loop(len(PAIR))
        def _(v):
            rows = pl.ds(pl.multiple_of(v * view_rows, view_rows), view_rows)
            block = weight[pl.ds(2 * lax.rem(p, 2), 2)].reshape(two, dim)
            out = lax.dot_general(grad[rows, :], block, LANE_DIMS, preferred_element_type=F32)
            out = jnp.where(act[rows, cols] > 0, out, 0.0)
            pre[rows, cols] = out
            half[pl.ds(v, 1), sel] = col_sum(out)
            half[pl.ds(2 + v, 1), sel] = col_sum(out * normed[layer % 2, rows, cols].astype(F32))

        @pl.when(p < 2)
        def _():
            for n in PAIR:
                weight_copy(layer, 2 * p + n + slots).start()

    def serve(layer, j):
        t = layer * CHUNKS + j
        for step, lag in zip((ring.first, ring.second, ring.third), RING_LAGS):
            pl.when((t >= lag) & (t < lag + 3 * CHUNKS))(lambda step=step, lag=lag: step(CHUNKS + t - lag))
        if layer:
            for half, block in enumerate(ring.last(t)):
                outs[layer - 1][:, pl.ds(pl.multiple_of(j * width + half * ring.half, ring.half), ring.half)] = block

    for layer in OTHERS:
        old, new = sums[layer], sums[layer + 1] if layer < 2 else None
        old[0].arrive()

        def settle():
            if layer:
                old[1].arrive()

            @pl.loop(3, CHUNKS)
            def _(k):
                finish_grad(layer, k)

            if layer == 0:
                norm_copy(1).start()

        def late_loads():
            new[1].begin()
            if layer == 0:
                act_copy(1).start()
                for n in range(slots):
                    weight_copy(1, n).start()

        def relay_pair():
            new[0].over_pair()
            new[1].over_plane()

        before, middle, after = [], [(2, settle)], []
        if layer:
            middle.append((0, old[1].over_pair))
        if layer == 0:
            before.append((3, lambda: act_copy(0).wait()))
        if new:
            before += [(2, lambda: norm_copy(layer).wait()), (5, new[0].over_plane), (6, new[0].over_line), (7, relay_pair)]
            after += [(4, new[0].begin), (6, late_loads), (7, new[1].over_line)]

        @loop(CHUNKS)
        def _(j):
            for when, move in before:
                pl.when(j == when)(move)
            pl.when(j < 3)(lambda: finish_grad(layer, j))
            weight_grad(layer, j)
            for when, move in middle:
                pl.when(j == when)(move)
            if new:
                pl.when((j > 2) & (j < 7))(lambda: input_grad(layer, j - 3))
            for when, move in after:
                pl.when(j == when)(move)
            serve(layer, j)

        if layer == 0:
            act_copy(1).wait()
            for v in PAIR:
                turn(act, wide, LINE, v)
            loss_sums.over_plane()

    @loop(CHUNKS)
    def _(j):
        serve(len(OTHERS), j)

    loss_sums.arrive()


def step(total_rows, vmem, lam, feat_a, feat_b, weights, vectors):
    view_rows, dim = feat_a.shape
    rows, width, blocks = 2 * view_rows, dim // CHUNKS, dim // 32
    hbm = pl.BlockSpec(memory_space=pl.ANY)
    vm = pl.BlockSpec(memory_space=pltpu.VMEM)
    cube = (LINE, 2, 2, 2, blocks)
    scratch = [
        pltpu.VMEM((rows, dim), BF16),
        pltpu.VMEM((rows, dim), F32),
        pltpu.VMEM((CHUNKS, *cube, width), BF16),
        pltpu.VMEM((LINE, *cube, view_rows // 2), BF16),
        pltpu.VMEM((LINE, 2, 2, blocks, dim), BF16),
        pltpu.VMEM((2, rows, dim), BF16),
        pltpu.VMEM((rows, dim), BF16),
        pltpu.VMEM((3, 2, 4, dim), F32),
        pltpu.VMEM((3, 2, 4, dim), F32),
        pltpu.VMEM((2, 2, 4, dim // 2), F32),
        pltpu.VMEM((4, dim), F32),
        pltpu.VMEM((4, dim), F32),
        pltpu.VMEM((1, dim), F32),
        pltpu.VMEM((blocks, 128), F32),
        pltpu.VMEM((128, 128), F32),
        pltpu.VMEM((2, blocks, width // 2), F32),
        pltpu.VMEM((3, 2, dim), F32),
        DMA_SEM((CHUNKS,)),
        DMA_SEM((LINE,)),
        DMA_SEM((3,)),
        DMA_SEM((3, 2)),
    ] + ring_scratch(CHUNKS, blocks, width)
    for _ in range(6):
        scratch += quick_scratch(2, dim)
    scratch += quick_scratch(4, dim) + quick_scratch(1, dim) + sums_scratch(4, dim)
    for _ in range(4):
        scratch += sums_scratch(4, dim // 2)
    halves = jax.ShapeDtypeStruct((2, 4, dim // 2), F32)
    saved = jax.ShapeDtypeStruct((2, rows, dim), BF16)
    return pl.pallas_call(
        functools.partial(step_kernel, total_rows),
        out_shape=[jax.ShapeDtypeStruct((blocks, dim), F32)] * 3 + [
            jax.ShapeDtypeStruct((1, dim), F32), halves, halves, saved, saved],
        in_specs=[pl.BlockSpec(memory_space=pltpu.SMEM)] + [hbm] * 5 + [vm] * 4,
        out_specs=[vm] * 6 + [hbm] * 2,
        scratch_shapes=scratch,
        compiler_params=pltpu.CompilerParams(collective_id=0, has_side_effects=True, vmem_limit_bytes=vmem),
    )(lam.reshape(1), feat_a, feat_b, *[weight.reshape(*cube, dim) for weight in weights],
      *[value.reshape(1, dim) for value in vectors])


def finish_kernel(total_two, total_one, loss_cols, *refs):
    gain_one, shift_one, gain_two, shift_two, loss = refs[6:]
    for grad, out in zip(refs[:3], refs[3:6]):
        out[...] = grad[...]
    half = total_two.shape[-1]
    for total, gain, shift in ((total_two, gain_two, shift_two), (total_one, gain_one, shift_one)):
        for h in PAIR:
            cols = pl.ds(h * half, half)
            shift[:, cols] = total[h, FIRST] + total[h, SECOND]
            gain[:, cols] = total[h, THIRD] + total[h, FOURTH]
    loss[...] = jnp.sum(loss_cols[...], axis=1, keepdims=True)


def finish(total_two, total_one, loss_cols, grads):
    vm = pl.BlockSpec(memory_space=pltpu.VMEM)
    row = jax.ShapeDtypeStruct((1, loss_cols.shape[1]), F32)
    outs = pl.pallas_call(
        finish_kernel,
        out_shape=[jax.ShapeDtypeStruct(grad.shape, F32) for grad in grads] + [row] * 4 + [jax.ShapeDtypeStruct((1, 1), F32)],
        in_specs=[vm] * 6,
        out_specs=[vm] * 8,
    )(total_two, total_one, loss_cols, *grads)
    return outs[:3], [row.reshape(-1) for row in outs[3:7]], outs[7].reshape(())


def solution(mesh):
    shards = mesh.shape["data"]

    def local_step(h_a, h_b, w_one, w_two, w_three, gain_one, shift_one, gain_two, shift_two, lam_off):
        rows_dev = h_a.shape[0]
        total_rows = rows_dev * shards
        grad_w_three, grad_w_two, grad_w_one, loss_cols, total_two, total_one = step(
            total_rows, 67000000, lam_off, h_a, h_b, (w_one, w_two, w_three),
            (gain_one, shift_one, gain_two, shift_two))[:6]
        grads, vectors, loss_total = finish(total_two, total_one, loss_cols, [grad_w_one, grad_w_two, grad_w_three])
        return (loss_total, *grads, *vectors)

    row_spec = P("data", None)
    whole_mat = P(None, None)
    whole_vec = P(None)
    return jax.shard_map(
        local_step, mesh=mesh,
        in_specs=(row_spec, row_spec, whole_mat, whole_mat, whole_mat,
                  whole_vec, whole_vec, whole_vec, whole_vec, P()),
        out_specs=(P(), row_spec, row_spec, row_spec, whole_vec, whole_vec, whole_vec, whole_vec),
        check_vma=False)
```
